32 devices in a mesh: dp: 8 (over y, x, core), tensor: 4 (over z).
Axes of the slice: x: 2, y: 2, z: 4, core: 2. Of those that a mesh axis runs over, the one named last changes fastest.
Arguments:
- tokens: bfloat16 [2048, 8, 1024], P('tensor', 'dp'), may hold values from -6 to 6
- weights: bfloat16 [1024, 12288], P(None, 'tensor'), may hold values from -0.71 to 0.71
- norms: float32 [4, 1024], replicated, may hold values from -0.75 to 1.5
- cotangent: bfloat16 [2048, 8, 1024], P('tensor', 'dp'), may hold values from -6 to 6
- lengths: int32 [8], P('dp'), may hold values from 512 to 2048, as said below
- owners: int32 [7], replicated, may hold values from 0 to 7, as said below
- master: float32 [8, 1024, 4096], P('dp', None, 'tensor'), may hold values from -0.05 to 0.05
- moment_one: float32 [8, 1024, 4096], P('dp', None, 'tensor'), may hold values from -24 to 24
- moment_two: float32 [8, 1024, 4096], P('dp', None, 'tensor'), may hold values from 0.5 to 8
- norm_master: float32 [8, 4, 1024], P('dp'), may hold values from 0.5 to 1.5
- norm_one: float32 [8, 4, 1024], P('dp'), may hold values from -24 to 24
- norm_two: float32 [8, 4, 1024], P('dp'), may hold values from 0.5 to 8
Outputs:
- outputs: bfloat16 [2048, 8, 1024], P('tensor', 'dp')
- input_grad: bfloat16 [2048, 8, 1024], P('tensor', 'dp')
- weight_grads: float32 [8, 1024, 4096], P('dp', None, 'tensor')
- new_master: float32 [8, 1024, 4096], P('dp', None, 'tensor')
- new_one: float32 [8, 1024, 4096], P('dp', None, 'tensor')
- new_two: float32 [8, 1024, 4096], P('dp', None, 'tensor')
- new_weights: bfloat16 [1024, 12288], P(None, 'tensor')
- norm_grads: float32 [4, 1024], replicated
- new_norm_master: float32 [8, 4, 1024], P('dp')
- new_norm_one: float32 [8, 4, 1024], P('dp')
- new_norm_two: float32 [8, 4, 1024], P('dp')
The draws below stay inside these ranges and needn't reach their ends.
Inputs may be any that keep to these rules, and one draw needn't show every extreme that they name: `lengths`: some sequence fills all 2048 positions. The up and down matrices have different owners that own no other matrix; the four attention matrices have at most two owners between them, neither of them an owner of up or down, so no index owns more than 4 tiles of a block and the owner of up owns exactly 4.
All inputs are finite; a program needn't handle non-finite values.
Results may differ from the reference program's by a relative error of at most 0.02.
Values may be sent and summed in bfloat16 or wider, within the bound.
A program may use at most 192 MiB of HBM per device.

```python
import math
import jax
import jax.numpy as jnp
from jax import lax

D = 1024
HEADS = 16
FF = 4096
SEQ = 2048
ADAM_STEP = 10
HEAD_DIM = 64
CAP = 4
NSEQ = 8
N_DP = 8
N_TENSOR = 4


def draw_weights(key, part):
    tile_width = D // N_TENSOR
    hidden_width = FF // N_TENSOR
    per_rank = 4 * tile_width + 2 * hidden_width
    column = jnp.arange(N_TENSOR * per_rank) % per_rank
    spread = jnp.where(column < 2 * tile_width, math.sqrt(2.0 / D), jnp.where(column < 3 * tile_width, math.sqrt(1.0 / D), jnp.where(column < 4 * tile_width, math.sqrt(1.0 / 32.0), jnp.where(column < 4 * tile_width + hidden_width, math.sqrt(1.0 / D), math.sqrt(1.0 / FF)))))
    sample = jnp.clip(jax.random.normal(key, (D, N_TENSOR * per_rank), jnp.float32), -4.0, 4.0)
    return (sample * spread[None, :]).astype(jnp.bfloat16)


def draw_norms(key, part):
    sample = jnp.clip(jax.random.normal(key, (4, D), jnp.float32), -2.5, 2.5)
    row_ids = jnp.arange(4)[:, None]
    return jnp.where(row_ids % 2 == 0, 1.0 + 0.2 * sample, 0.3 * sample).astype(jnp.float32)


def draw_lengths(key, part):
    sampled = jax.random.randint(jax.random.fold_in(key, 11), (NSEQ,), SEQ // 4, SEQ + 1, dtype=jnp.int32)
    chosen = jax.random.randint(jax.random.fold_in(key, 12), (), 0, NSEQ, dtype=jnp.int32)
    return jnp.where(jnp.arange(NSEQ, dtype=jnp.int32) == chosen, SEQ, sampled).astype(jnp.int32)


def draw_owners(key, part):
    shuffled = jax.random.permutation(jax.random.fold_in(key, 21), NSEQ).astype(jnp.int32)
    chosen_ranks = jax.random.randint(jax.random.fold_in(key, 22), (4,), 2, 4, dtype=jnp.int32)
    attention_owners = jnp.take(shuffled, chosen_ranks)
    norm_owner = jax.random.randint(jax.random.fold_in(key, 23), (1,), 0, NSEQ, dtype=jnp.int32)
    return jnp.concatenate([attention_owners, shuffled[0:2], norm_owner]).astype(jnp.int32)


def level_of(rng, shape, shards, low, largest):
    def one(dim, blocks):
        draws = jax.random.uniform(jax.random.fold_in(jax.random.fold_in(rng, 6), dim), (blocks,), jnp.float32, low / len(shards), largest / len(shards))
        return jnp.repeat(jnp.exp(draws), shape[dim] // blocks).reshape((-1,) + (1,) * (len(shape) - dim - 1))

    loudness = one(*shards[0])
    for cut in shards[1:]:
        loudness = loudness * one(*cut)
    return loudness


def gaussian(own_key, dims, width, most, cuts=(), held_as=jnp.bfloat16):
    result = width * jax.random.normal(own_key, dims, jnp.float32)
    if cuts:
        result = result * level_of(own_key, dims, cuts, -0.22, 0.18)
    return jnp.clip(result, -most, most).astype(held_as)


def setup_inputs(seed: int = 0) -> dict:
    splits = jax.random.split(jax.random.key(seed), 13)
    tokens = gaussian(splits[0], (SEQ, NSEQ, D), 1.0, 6.0, ((0, 4), (1, 8)))
    weights = draw_weights(jax.random.fold_in(splits[12], 71), 0)
    norms = draw_norms(jax.random.fold_in(splits[12], 71), 0)
    cotangent = gaussian(splits[3], (SEQ, NSEQ, D), 1.0, 6.0, ((0, 4), (1, 8)))
    lengths = draw_lengths(jax.random.fold_in(splits[12], 71), 0)
    owners = draw_owners(jax.random.fold_in(splits[12], 71), 0)
    master = jnp.clip(jax.random.uniform(splits[6], (N_DP, D, CAP * D), jnp.float32, -0.05, 0.05) * level_of(splits[6], (N_DP, D, CAP * D), ((0, 8), (2, 4)), -0.4, 0.0), -0.05, 0.05)
    moment_one = gaussian(splits[7], (N_DP, D, CAP * D), 4.0, 24.0, ((0, 8), (2, 4)), jnp.float32)
    moment_two = jnp.clip(jnp.exp(math.log(8.0) - 2.7725887 * jax.random.uniform(splits[8], (N_DP, D, CAP * D), jnp.float32) ** level_of(splits[8], (N_DP, D, CAP * D), ((0, 8), (2, 4)), -0.2, 0.2)), 0.5, 8.0)
    norm_master = jnp.clip(0.5 + 1.0 * jax.random.uniform(splits[9], (N_DP, 4, D), jnp.float32) ** level_of(splits[9], (N_DP, 4, D), ((0, 8),), -0.2, 0.2), 0.5, 1.5)
    norm_one = gaussian(splits[10], (N_DP, 4, D), 4.0, 24.0, ((0, 8),), jnp.float32)
    norm_two = jnp.clip(jnp.exp(math.log(8.0) - 2.7725887 * jax.random.uniform(splits[11], (N_DP, 4, D), jnp.float32) ** level_of(splits[11], (N_DP, 4, D), ((0, 8),), -0.2, 0.2)), 0.5, 8.0)
    return {"tokens": tokens, "weights": weights, "norms": norms, "cotangent": cotangent, "lengths": lengths, "owners": owners, "master": master, "moment_one": moment_one, "moment_two": moment_two, "norm_master": norm_master, "norm_one": norm_one, "norm_two": norm_two}


@jax.custom_vjp
def low(v):
    return lax.optimization_barrier(v.astype(jnp.bfloat16)).astype(jnp.float32)

@jax.custom_vjp
def low_back(v):
    return v

def low_keep(v):
    return (low(v), None)

def low_pass(kept, grad):
    return (grad,)

def back_keep(v):
    return (v, None)

def back_low(kept, grad):
    return (low(grad),)
low.defvjp(low_keep, low_pass)
low_back.defvjp(back_keep, back_low)
precise = lax.Precision.HIGHEST
beta_one = 0.9
beta_two = 0.999
learn_rate = 0.02
weight_decay = 0.1
adam_eps = 1e-08
norm_eps = 1e-05
masked_score = -1e+30

def layer_norm(value, gain, shift):
    average = lax.optimization_barrier(jnp.mean(value, axis=-1, keepdims=True))
    centred = value - average
    variance = lax.optimization_barrier(jnp.mean(centred * centred, axis=-1, keepdims=True))
    return centred * lax.rsqrt(variance + norm_eps) * gain + shift

def unpack(packed):
    tile_width = D // N_TENSOR
    hidden_width = FF // N_TENSOR
    columns = packed.reshape(D, N_TENSOR, 4 * tile_width + 2 * hidden_width)

    def columns_of(begin_col, size_cols):
        return columns[:, :, begin_col:begin_col + size_cols].reshape(D, N_TENSOR * size_cols)
    return (columns_of(0, tile_width), columns_of(tile_width, tile_width), columns_of(2 * tile_width, tile_width), columns_of(3 * tile_width, tile_width), columns_of(4 * tile_width, hidden_width), columns_of(4 * tile_width + hidden_width, hidden_width))

def sequence_forward(sequence, length, w_query, w_key, w_value, w_out, w_up, w_down, norms):
    present = jnp.arange(SEQ) < length
    score_scale = HEAD_DIM ** (-0.5)

    def heads_of(weight):
        return low(low_back(jnp.dot(sequence, weight, precision=precise))).reshape(SEQ, HEADS, HEAD_DIM)
    queries = heads_of(w_query)
    key_rows = heads_of(w_key)
    value_rows = heads_of(w_value)
    block_rows = min(512, SEQ)

    def attend_block(query_block):
        scores = low_back(jnp.einsum('qhe,khe->hqk', query_block, key_rows, precision=precise) * score_scale)
        scores = jnp.where(present[None, None, :], scores, masked_score)
        attention = jax.nn.softmax(scores, axis=-1)
        return jnp.einsum('hqk,khe->qhe', low(attention), value_rows, precision=precise)
    context = lax.map(jax.checkpoint(attend_block), queries.reshape(SEQ // block_rows, block_rows, HEADS, HEAD_DIM))
    context = low(low_back(context.reshape(SEQ, D)))
    branch = low_back(jnp.dot(context, w_out.T, precision=precise))
    first_norm = layer_norm(sequence + branch, norms[0], norms[1])
    hidden_pre = low_back(jnp.dot(low(first_norm), w_up, precision=precise))
    hidden = low(jax.nn.gelu(hidden_pre, approximate=False))
    feed = low_back(jnp.dot(hidden, w_down.T, precision=precise))
    return layer_norm(first_norm + feed, norms[2], norms[3])

def forward(inputs, packed, norms, lengths):
    w_query, w_key, w_value, w_out, w_up, w_down = unpack(packed)

    def one_sequence(running, sequence_items):
        sequence, length = sequence_items
        return (running, sequence_forward(sequence, length, w_query, w_key, w_value, w_out, w_up, w_down, norms))
    running, results = lax.scan(one_sequence, jnp.zeros((), jnp.float32), (jnp.transpose(inputs, (1, 0, 2)), lengths))
    return jnp.transpose(results, (1, 0, 2))

def slot_table(owners):
    repeat = FF // D
    tile_matrix = jnp.array([0, 1, 2, 3] + [4] * repeat + [5] * repeat, dtype=jnp.int32)
    choose = (tile_matrix[:, None] == jnp.arange(7, dtype=jnp.int32)[None, :]).astype(jnp.int32)
    tile_owner = lax.optimization_barrier(jnp.sum(choose * owners[None, :].astype(jnp.int32), axis=1)).astype(jnp.int32)
    position = jnp.arange(tile_matrix.shape[0], dtype=jnp.int32)
    before = (tile_owner[None, :] == tile_owner[:, None]) & (position[None, :] < position[:, None])
    slot_index = lax.optimization_barrier(jnp.sum(before.astype(jnp.int32), axis=1)).astype(jnp.int32)
    return (tile_owner, slot_index)

def adam_update(grad, param, first, second, occupied, decay_rate):
    first_new = occupied * (beta_one * first + (1.0 - beta_one) * grad)
    second_new = occupied * (beta_two * second + (1.0 - beta_two) * grad * grad)
    correct_one = 1.0 - beta_one ** ADAM_STEP
    correct_two = 1.0 - beta_two ** ADAM_STEP
    direction = first_new / correct_one / (jnp.sqrt(second_new / correct_two) + adam_eps)
    param_new = occupied * (param - learn_rate * (direction + decay_rate * param))
    return (param_new, first_new, second_new)

def reference(tokens, weights, norms, cotangent, lengths, owners, master, moment_one, moment_two, norm_master, norm_one, norm_two):
    inputs = tokens.astype(jnp.float32)
    packed = weights.astype(jnp.float32)
    outputs, pullback = jax.vjp(lambda source, matrices, gains: forward(source, matrices, gains, lengths), inputs, packed, norms)
    present = (jnp.arange(SEQ)[:, None] < lengths[None, :]).astype(jnp.float32)
    seed_grad = cotangent.astype(jnp.float32) * present[:, :, None]
    input_grad, packed_grad, norm_grads = pullback(seed_grad)
    tile_width = D // N_TENSOR
    tile_owner, slot_index = slot_table(owners)
    devices = jnp.arange(N_DP, dtype=jnp.int32)
    slot_ids = jnp.arange(CAP, dtype=jnp.int32)
    owned = ((tile_owner[None, None, :] == devices[:, None, None]) & (slot_index[None, None, :] == slot_ids[None, :, None])).astype(jnp.float32)
    tile_count = tile_owner.shape[0]
    grad_tiles = packed_grad.reshape(D, N_TENSOR, tile_count, tile_width)
    store_shape = (N_DP, D, N_TENSOR * CAP * tile_width)
    weight_grads = jnp.einsum('xtiw,dsi->dxtsw', grad_tiles, owned, precision=precise).reshape(store_shape)
    occupied = jnp.broadcast_to(lax.optimization_barrier(jnp.sum(owned, axis=2))[:, None, None, :, None], (N_DP, D, N_TENSOR, CAP, tile_width)).reshape(store_shape)
    new_master, new_one, new_two = adam_update(weight_grads, master, moment_one, moment_two, occupied, weight_decay)
    rounded = lax.optimization_barrier(new_master.astype(jnp.bfloat16)).astype(jnp.float32)
    placed = jnp.einsum('dxtsw,dsi->xtiw', rounded.reshape(N_DP, D, N_TENSOR, CAP, tile_width), owned, precision=precise)
    new_weights = placed.reshape(D, N_TENSOR * tile_count * tile_width).astype(jnp.bfloat16)
    norm_owner = (devices == owners[6]).astype(jnp.float32)[:, None, None]
    new_norm_master, new_norm_one, new_norm_two = adam_update(norm_grads[None], norm_master, norm_one, norm_two, norm_owner, 0.0)
    return (outputs.astype(jnp.bfloat16), input_grad.astype(jnp.bfloat16), weight_grads, new_master, new_one, new_two, new_weights, norm_grads, new_norm_master, new_norm_one, new_norm_two)
```

```python
from functools import partial

import jax
import jax.numpy as jnp
from jax import lax
from jax.experimental import pallas as pl
from jax.experimental.pallas import tpu as pltpu
from jax.sharding import PartitionSpec as P

D = 1024
FF = 4096
ADAM_STEP = 10
HEAD_DIM = 64
SHARE = 8


f32, bf16 = jnp.float32, jnp.bfloat16
beta_one = 0.9
beta_two = 0.999
learn_rate = 0.02
weight_decay = 0.1
adam_eps = 1e-08
norm_eps = 1e-05
masked_score = -1e30
AXES = ("dp", "tensor")


def contract(a, b, ca, cb):
    return lax.dot_general(a, b, (((ca,), (cb,)), ((), ())), preferred_element_type=f32)


def norm_parts(value, gain, shift):
    average = jnp.mean(value, axis=-1, keepdims=True)
    centred = value - average
    variance = jnp.mean(centred * centred, axis=-1, keepdims=True)
    inverse = lax.rsqrt(variance + norm_eps)
    normed = centred * inverse
    return normed * gain + shift, normed, inverse


def norm_back(upstream, normed, inverse, gain):
    scaled = upstream * gain
    inner = (
        scaled
        - jnp.mean(scaled, axis=-1, keepdims=True)
        - normed * jnp.mean(scaled * normed, axis=-1, keepdims=True)
    )
    return inner * inverse


def slot_table(owners):
    repeat = FF // D
    tile_matrix = jnp.array([0, 1, 2, 3] + [4] * repeat + [5] * repeat, dtype=jnp.int32)
    choose = (tile_matrix[:, None] == jnp.arange(7, dtype=jnp.int32)[None, :]).astype(jnp.int32)
    tile_owner = jnp.sum(choose * owners[None, :], axis=1)
    position = jnp.arange(tile_matrix.shape[0], dtype=jnp.int32)
    before = (tile_owner[None, :] == tile_owner[:, None]) & (position[None, :] < position[:, None])
    slot_index = jnp.sum(before.astype(jnp.int32), axis=1)
    return (tile_owner, slot_index)


def adam_update(grad, param, first, second, occupied, decay_rate):
    first_new = occupied * (beta_one * first + (1.0 - beta_one) * grad)
    second_new = occupied * (beta_two * second + (1.0 - beta_two) * grad * grad)
    correct_one = 1.0 - beta_one**ADAM_STEP
    correct_two = 1.0 - beta_two**ADAM_STEP
    direction = first_new / correct_one / (jnp.sqrt(second_new / correct_two) + adam_eps)
    param_new = occupied * (param - learn_rate * (direction + decay_rate * param))
    return (param_new, first_new, second_new)


def head_keys(keys, half, start, length):
    lane = lax.broadcasted_iota(jnp.int32, keys.shape, 1)
    row = lax.broadcasted_iota(jnp.int32, keys.shape, 0)
    bias = jnp.where(start + row < length, 0.0, masked_score).astype(f32)
    extra = jnp.where(lane == (1 - half) * HEAD_DIM, bias, 0.0)
    return jnp.where(lane // HEAD_DIM == half, keys.astype(f32), extra).astype(bf16)


def head_half(rows, half):
    lane = lax.broadcasted_iota(jnp.int32, rows.shape, 1)
    return jnp.where(lane // HEAD_DIM == half, rows, jnp.zeros_like(rows))


def head_queries(rows, half):
    lane = lax.broadcasted_iota(jnp.int32, rows.shape, 1)
    scaled = rows.astype(f32) * HEAD_DIM ** (-0.5)
    extra = jnp.where(lane == (1 - half) * HEAD_DIM, 1.0, 0.0)
    return jnp.where(lane // HEAD_DIM == half, scaled, extra).astype(bf16)


def attention_forward_body(info, mixed_ref, context_ref, lse_ref, keys, values):
    step = pl.program_id(0)
    chunks, rows, _ = mixed_ref.shape
    width = context_ref.shape[-1]

    @pl.when(step == 0)
    def _():
        for j in range(chunks):
            for h in range(width // HEAD_DIM):
                at = width + (h // 2) * 128
                keys[h, j * rows : (j + 1) * rows, :] = head_keys(
                    mixed_ref[j, :, at : at + 128], h % 2, info[1 + j], info[0]
                )
            values[j * rows : (j + 1) * rows, :] = mixed_ref[j, :, 2 * width :]

    lane = lax.broadcasted_iota(jnp.int32, (rows, 128), 1)
    logs = jnp.zeros((rows, 128), f32)
    for pair in range(width // 128):
        queries = mixed_ref[step, :, pair * 128 : pair * 128 + 128]
        both = []
        for half in range(2):
            h = pair * 2 + half
            scores = contract(head_queries(queries, half), keys[h], 1, 1)
            top = jnp.max(scores, axis=1, keepdims=True)
            weight = jnp.exp(scores - top)
            total = jnp.sum(weight, axis=1, keepdims=True)
            out = contract(weight.astype(bf16), values[:, pair * 128 : pair * 128 + 128], 1, 0)
            both.append(out / total)
            logs = jnp.where(lane == h, top + jnp.log(total), logs)
        context_ref[0, :, pair * 128 : pair * 128 + 128] = jnp.where(
            lane < HEAD_DIM, both[0], both[1]
        ).astype(bf16)
    lse_ref[0] = jnp.transpose(logs)[:8, :]


def attention_forward(info, mixed):
    chunks, rows, width3 = mixed.shape
    width = width3 // 3
    seq = chunks * rows
    heads = width // HEAD_DIM
    return pl.pallas_call(
        attention_forward_body,
        grid=(chunks,),
        name="attention_forward",
        in_specs=[
            pl.BlockSpec(memory_space=pltpu.SMEM),
            pl.BlockSpec((chunks, rows, width3), lambda i: (0, 0, 0)),
        ],
        out_specs=[
            pl.BlockSpec((1, rows, width), lambda i: (i, 0, 0)),
            pl.BlockSpec((1, 8, rows), lambda i: (i, 0, 0)),
        ],
        out_shape=[
            jax.ShapeDtypeStruct((chunks, rows, width), bf16),
            jax.ShapeDtypeStruct((chunks, 8, rows), f32),
        ],
        scratch_shapes=[pltpu.VMEM((heads, seq, 128), bf16), pltpu.VMEM((seq, width), bf16)],
        compiler_params=pltpu.CompilerParams(vmem_limit_bytes=48 << 20),
        cost_estimate=pl.CostEstimate(
            flops=16 * heads * seq * seq * HEAD_DIM, bytes_accessed=8 << 20, transcendentals=0
        ),
    )(info, mixed)


def attention_backward_body(
    info, mixed_ref, context_ref, upstream_ref, lse_ref, out_ref, keys, turned, key_sum, value_sum, query_t
):
    step = pl.program_id(0)
    chunks, rows, _ = mixed_ref.shape
    width = context_ref.shape[-1]
    scale = HEAD_DIM ** (-0.5)

    @pl.when(step == 0)
    def _():
        key_sum[...] = jnp.zeros_like(key_sum)
        value_sum[...] = jnp.zeros_like(value_sum)
        for j in range(chunks):
            for h in range(width // HEAD_DIM):
                at = width + (h // 2) * 128
                keys[h, j * rows : (j + 1) * rows, :] = head_keys(
                    mixed_ref[j, :, at : at + 128], h % 2, info[1 + j], info[0]
                )
            turned[:, j * rows : (j + 1) * rows] = jnp.transpose(
                mixed_ref[j, :, width : 2 * width].astype(f32)
            ).astype(bf16)

    upstream = upstream_ref[0]
    product = upstream.astype(f32) * context_ref[0].astype(f32)
    feature = lax.broadcasted_iota(jnp.int32, (8, width), 1) // HEAD_DIM
    picks = (feature == lax.broadcasted_iota(jnp.int32, (8, width), 0)).astype(f32)
    delta = lax.dot_general(
        picks, product, (((1,), (1,)), ((), ())), precision=lax.Precision.HIGHEST,
        preferred_element_type=f32,
    )
    lse = lse_ref[0]
    for pair in range(width // 128):
        lanes = slice(pair * 128, pair * 128 + 128)
        queries = mixed_ref[step, :, lanes]
        value_rows = mixed_ref[:, :, 2 * width + pair * 128 : 2 * width + pair * 128 + 128]
        value_rows = value_rows.reshape(chunks * rows, 128)
        for half in range(2):
            h = pair * 2 + half
            scores = contract(keys[h], head_queries(queries, half), 1, 1)
            weight = jnp.exp(scores - lse[h : h + 1, :])
            up_half = head_half(upstream[:, lanes], half)
            back = contract(value_rows, up_half, 1, 1)
            score_grad = (weight * (back - delta[h : h + 1, :])).astype(bf16)
            value_sum[pair] += contract(weight.astype(bf16), up_half, 1, 0)
            key_sum[pair] += contract(score_grad, head_half(queries, half), 1, 0)
            query_t[h * HEAD_DIM : (h + 1) * HEAD_DIM, :] = (
                contract(turned[h * HEAD_DIM : (h + 1) * HEAD_DIM, :], score_grad, 1, 0) * scale
            )
    out_ref[step, :, :width] = jnp.transpose(query_t[...]).astype(bf16)

    @pl.when(step == chunks - 1)
    def _():
        for j in range(chunks):
            at = slice(j * rows, (j + 1) * rows)
            for pair in range(width // 128):
                left = width + pair * 128
                out_ref[j, :, left : left + 128] = (key_sum[pair, at, :] * scale).astype(bf16)
                out_ref[j, :, left + width : left + width + 128] = value_sum[pair, at, :].astype(bf16)


def attention_backward(info, mixed, context, upstream, lse):
    chunks, rows, width3 = mixed.shape
    width = width3 // 3
    seq = chunks * rows
    heads = width // HEAD_DIM
    return pl.pallas_call(
        attention_backward_body,
        grid=(chunks,),
        name="attention_backward",
        in_specs=[
            pl.BlockSpec(memory_space=pltpu.SMEM),
            pl.BlockSpec((chunks, rows, width3), lambda i: (0, 0, 0)),
            pl.BlockSpec((1, rows, width), lambda i: (i, 0, 0)),
            pl.BlockSpec((1, rows, width), lambda i: (i, 0, 0)),
            pl.BlockSpec((1, 8, rows), lambda i: (i, 0, 0)),
        ],
        out_specs=pl.BlockSpec((chunks, rows, width3), lambda i: (0, 0, 0)),
        out_shape=jax.ShapeDtypeStruct((chunks, rows, width3), bf16),
        scratch_shapes=[
            pltpu.VMEM((heads, seq, 128), bf16),
            pltpu.VMEM((width, seq), bf16),
            pltpu.VMEM((width // 128, seq, 128), f32),
            pltpu.VMEM((width // 128, seq, 128), f32),
            pltpu.VMEM((width, rows), f32),
        ],
        compiler_params=pltpu.CompilerParams(vmem_limit_bytes=56 << 20),
        cost_estimate=pl.CostEstimate(
            flops=40 * heads * seq * seq * HEAD_DIM, bytes_accessed=8 << 20, transcendentals=0
        ),
    )(info, mixed, context, upstream, lse)


def joined(piece_ref, kind):
    return jnp.concatenate([piece_ref[0, kind], piece_ref[1, kind]], axis=-1)


def feed_body(count, info, first_ref, cotangent_ref, norms_ref, *refs):
    pieces = refs[:count]
    out_ref, low_ref, hidden_ref, pre_ref, grad_ref, sums_ref = refs[count : count + 6]
    held, slope, feed, sems = refs[count + 6 :]
    rows = first_ref.shape[0]
    for i in range(count):
        pltpu.make_async_copy(pieces[i], held.at[i], sems.at[i]).start()
    first_low = first_ref[...].astype(bf16)
    feed[...] = jnp.zeros_like(feed)

    def forward(i, carry):
        pltpu.make_async_copy(pieces[0], held.at[i], sems.at[i]).wait()
        value = jnp.dot(first_low, joined(held.at[i], 0), preferred_element_type=f32)
        area = 0.5 + 0.5 * lax.erf(value * (0.5**0.5))
        density = jnp.exp(-0.5 * value * value) * (0.5 / jnp.pi) ** 0.5
        hidden = (value * area).astype(bf16)
        slope[i] = (area + value * density).astype(bf16)
        hidden_ref[i] = hidden
        feed[...] += contract(hidden, joined(held.at[i], 1), 1, 1)
        return carry

    lax.fori_loop(0, count, forward, 0)
    sums_ref[...] = jnp.zeros_like(sums_ref)
    part = 128

    def middle(r, carry):
        at = pl.ds(pl.multiple_of(r * part, part), part)
        second, normed, inverse = norm_parts(
            first_ref[at, :] + feed[at, :], norms_ref[2:3, :], norms_ref[3:4, :]
        )
        out_ref[at, :] = second.astype(bf16)
        row = lax.broadcasted_iota(jnp.int32, (part, 1), 0) + r * part + info[1]
        seed = cotangent_ref[at, :].astype(f32) * (row < info[0]).astype(f32)
        back = norm_back(seed, normed, inverse, norms_ref[2:3, :])
        sums_ref[0:1, :] += jnp.sum(seed * normed, axis=0, keepdims=True)
        sums_ref[1:2, :] += jnp.sum(seed, axis=0, keepdims=True)
        grad_ref[at, :] = back
        low_ref[at, :] = back.astype(bf16)
        return carry

    lax.fori_loop(0, rows // part, middle, 0)
    feed_low = low_ref[...]

    def backward(i, carry):
        back = jnp.dot(feed_low, joined(held.at[i], 1), preferred_element_type=f32)
        pre = (back * slope[i].astype(f32)).astype(bf16)
        pre_ref[i] = pre
        grad_ref[...] += contract(pre, joined(held.at[i], 0), 1, 1)
        return carry

    lax.fori_loop(0, count, backward, 0)


def feed_block(info, first, cotangent, norms, pieces):
    rows = first.shape[0]
    count = len(pieces)
    _, _, _, lanes = pieces[0].shape
    width = 2 * lanes
    vmem = pl.BlockSpec(memory_space=pltpu.VMEM)
    return pl.pallas_call(
        partial(feed_body, count),
        name="feed_block",
        in_specs=[pl.BlockSpec(memory_space=pltpu.SMEM), vmem, vmem, vmem]
        + [pl.BlockSpec(memory_space=pl.ANY)] * count,
        out_specs=[vmem] * 6,
        out_shape=[
            jax.ShapeDtypeStruct((rows, D), bf16),
            jax.ShapeDtypeStruct((rows, D), bf16),
            jax.ShapeDtypeStruct((count, rows, width), bf16),
            jax.ShapeDtypeStruct((count, rows, width), bf16),
            jax.ShapeDtypeStruct((rows, D), f32),
            jax.ShapeDtypeStruct((2, D), f32),
        ],
        scratch_shapes=[
            pltpu.VMEM((count,) + pieces[0].shape, bf16),
            pltpu.VMEM((count, rows, width), bf16),
            pltpu.VMEM((rows, D), f32),
            pltpu.SemaphoreType.DMA((count,)),
        ],
        compiler_params=pltpu.CompilerParams(vmem_limit_bytes=60 << 20),
        cost_estimate=pl.CostEstimate(
            flops=8 * rows * D * width * count, bytes_accessed=30 << 20, transcendentals=0
        ),
    )(info, first, cotangent, norms, *pieces)


def feed_grads_body(first_ref, low_ref, hidden_ref, pre_ref, out_ref, first_t, low_t):
    @pl.when(pl.program_id(0) == 0)
    def _():
        first_t[...] = jnp.transpose(first_ref[...])
        low_t[...] = jnp.transpose(low_ref[...].astype(f32)).astype(bf16)

    lanes = out_ref.shape[-1]
    up = jnp.dot(first_t[...].astype(bf16), pre_ref[0], preferred_element_type=f32).astype(bf16)
    down = jnp.dot(low_t[...], hidden_ref[0], preferred_element_type=f32).astype(bf16)
    for k in range(2):
        out_ref[0, k, 0] = up[:, k * lanes : (k + 1) * lanes]
        out_ref[0, k, 1] = down[:, k * lanes : (k + 1) * lanes]


def feed_grads(first, low, hidden, pre, start, count):
    rows = first.shape[0]
    width = hidden.shape[-1]
    full = pl.BlockSpec((rows, D), lambda i: (0, 0))
    piece = pl.BlockSpec((1, rows, width), lambda i: (i + start, 0, 0))
    return pl.pallas_call(
        feed_grads_body,
        grid=(count,),
        name="feed_grads",
        in_specs=[full, full, piece, piece],
        out_specs=pl.BlockSpec((1, 2, 2, D, width // 2), lambda i: (i, 0, 0, 0, 0)),
        out_shape=jax.ShapeDtypeStruct((count, 2, 2, D, width // 2), bf16),
        scratch_shapes=[pltpu.VMEM((D, rows), f32), pltpu.VMEM((D, rows), bf16)],
        compiler_params=pltpu.CompilerParams(vmem_limit_bytes=40 << 20),
        cost_estimate=pl.CostEstimate(
            flops=4 * rows * D * width * count, bytes_accessed=(2 << 20) * count, transcendentals=0
        ),
    )(first, low, hidden, pre)


def layer(n_dp, n_tensor, tokens, weights, norms, cotangent, lengths, owners, master, moment_one,
          moment_two, norm_master, norm_one, norm_two):
    tile = D // n_tensor
    hidden_width = FF // n_tensor
    rows = tokens.shape[0]
    lanes = hidden_width // SHARE
    device = lax.axis_index("dp")
    z = lax.axis_index("tensor")
    core = device % 2
    matched = core == z // 2
    quarter = jnp.where(matched, z, z ^ 2)

    def flip(x, dd, dz):
        pairs = [
            (d * n_tensor + t, (d ^ dd) * n_tensor + (t ^ dz))
            for d in range(n_dp)
            for t in range(n_tensor)
        ]
        return lax.ppermute(x, AXES, pairs)

    def some(x, dd, dz, want):
        pairs = [
            (d * n_tensor + t, (d ^ dd) * n_tensor + (t ^ dz))
            for d in range(n_dp)
            for t in range(n_tensor)
            if (t // 2 == d % 2) == want
        ]
        return lax.ppermute(x, AXES, pairs)

    def swap(x):
        return jnp.where(matched, x, some(x, 1, 2, False))

    w_mixed = weights[:, : 3 * tile]
    w_out = weights[:, 3 * tile : 4 * tile]
    share_rows = D // n_dp
    length = jnp.where(matched, lengths, flip(lengths, 1, 0))[0]
    base = jnp.stack([quarter ^ k for k in (0, 2, 1, 3)]) * rows
    info = jnp.concatenate([length[None], base]).astype(jnp.int32)

    inputs = tokens[:, 0, :]
    own = swap(inputs)
    far = some(inputs, 0, 1, True) + some(own, 0, 1, False)
    near = flip(own, 1, 0)
    gathered = jnp.stack([own, near, far, flip(far, 1, 0)])

    def my_rows(x):
        return lax.dynamic_slice_in_dim(x, device * share_rows, share_rows, 0)

    other = lax.all_gather(flip(my_rows(w_mixed), 0, 2), "dp", axis=0, tiled=True)
    w_heads = jnp.where(matched, w_mixed, other)
    out_own = my_rows(w_out)
    out_two = jnp.concatenate([out_own, flip(out_own, 0, 1)], axis=1)
    out_four = jnp.concatenate([out_two, flip(out_two, 0, 2)], axis=1)
    w_out_all = lax.all_gather(out_four, "dp", axis=0, tiled=True)

    at = (device % SHARE) * lanes + 4 * tile
    own_piece = jnp.stack(
        [
            lax.dynamic_slice(weights, (0, at), (D, lanes)),
            lax.dynamic_slice(weights, (0, at + hidden_width), (D, lanes)),
        ]
    )
    near_pieces = jnp.stack([own_piece, flip(own_piece, 0, 1)])
    far_pieces = flip(near_pieces, 0, 2)

    def spread(first_pieces, one, two):
        a = first_pieces
        b = flip(a, one, 0)
        c, e = flip(a, two, 0), flip(b, two, 0)
        return [a, b, c, e], [flip(v, 1, 0) for v in (a, b, c, e)]

    near_here, near_there = spread(near_pieces, 2, 4)
    far_here, far_there = spread(far_pieces, 4, 2)
    far_order = (0, 2, 1, 3)
    pieces = (
        near_there
        + [far_there[k] for k in far_order]
        + near_here
        + [far_here[k] for k in far_order]
    )

    mixed = jnp.einsum(
        "csd,de->cse", gathered, w_heads, preferred_element_type=f32
    ).astype(bf16)
    context, lse = attention_forward(info, mixed)

    parts = [context[0], flip(context[1], 1, 0), flip(context[2], 0, 1), flip(context[3], 1, 1)]
    context_all = jnp.where(
        matched,
        jnp.concatenate([parts[k] for k in (0, 2, 1, 3)], axis=1),
        jnp.concatenate([parts[k] for k in (1, 3, 0, 2)], axis=1),
    )
    branch = contract(context_all, w_out_all, 1, 1)
    first, first_normed, first_inverse = norm_parts(
        own.astype(f32) + branch, norms[0], norms[1]
    )
    seed = swap(cotangent[:, 0, :])
    outputs, feed_low, hidden, pre_grad, first_grad, sums_two = feed_block(
        info, first, seed, norms, pieces
    )
    branch_grad = norm_back(first_grad, first_normed, first_inverse, norms[0])
    gain_one = jnp.sum(first_grad * first_normed, axis=0)
    shift_one = jnp.sum(first_grad, axis=0)
    branch_low = branch_grad.astype(bf16)
    context_grad = jnp.dot(branch_low, w_out_all, preferred_element_type=f32).astype(bf16)
    blocks = [context_grad[:, k * tile : (k + 1) * tile] for k in range(4)]
    blocks = [
        jnp.where(matched, blocks[a], blocks[b]) for a, b in ((0, 2), (2, 0), (1, 3), (3, 1))
    ]
    upstream = jnp.stack(
        [blocks[0], flip(blocks[1], 1, 0), flip(blocks[2], 0, 1), flip(blocks[3], 1, 1)]
    )

    half = len(pieces) // 2
    grads_there = feed_grads(first, feed_low, hidden, pre_grad, 0, half)
    grads_here = feed_grads(first, feed_low, hidden, pre_grad, half, half)

    def add(a, b):
        return (a.astype(f32) + b.astype(f32)).astype(bf16)

    near_sum = add(grads_here[:4], flip(grads_there[:4], 1, 0))
    far_sum = add(grads_here[4:], flip(grads_there[4:], 1, 0))
    near_sum = near_sum.reshape((2, 2) + near_sum.shape[1:])
    far_sum = far_sum.reshape((2, 2) + far_sum.shape[1:])
    near_sum = add(near_sum[:, 0], flip(near_sum[:, 1], 2, 0))
    far_sum = add(far_sum[0], flip(far_sum[1], 4, 0))
    near_sum = add(near_sum[0], flip(near_sum[1], 4, 0))
    far_sum = add(far_sum[0], flip(far_sum[1], 2, 0))
    near_sum = add(near_sum, flip(far_sum, 0, 2))
    feed_share = add(near_sum[0], flip(near_sum[1], 0, 1))
    bit = SHARE
    while bit < n_dp:
        feed_share = add(feed_share, flip(feed_share, bit, 0))
        bit *= 2

    out_grad = contract(branch_low, context_all, 0, 0).astype(bf16)
    out_share = lax.psum_scatter(out_grad, "dp", scatter_dimension=0, tiled=True)
    out_share = add(out_share[:, : 2 * tile], flip(out_share[:, 2 * tile :], 0, 2))
    out_share = add(out_share[:, :tile], flip(out_share[:, tile:], 0, 1))

    norm_grads = jnp.concatenate([jnp.stack([gain_one, shift_one]), sums_two])
    for dd, dz in [(1 << k, 0) for k in range(n_dp.bit_length() - 1)] + [(0, 1), (0, 2)]:
        norm_grads = norm_grads + flip(norm_grads, dd, dz)

    mixed_grad = attention_backward(info, mixed, context, upstream, lse)
    back_rows = jnp.einsum("cse,de->csd", mixed_grad, w_heads, preferred_element_type=f32)
    back_low = back_rows.astype(bf16)
    back_pair = [
        back_rows[0] + flip(back_low[1], 1, 0).astype(f32),
        back_rows[2] + flip(back_low[3], 1, 0).astype(f32),
    ]
    input_total = branch_grad + back_pair[0] + flip(back_pair[1].astype(bf16), 0, 1).astype(f32)
    input_grad = swap(input_total.astype(bf16))[:, None, :]

    heads_grad = jnp.einsum("csd,cse->de", gathered, mixed_grad, preferred_element_type=f32)
    heads_grad = heads_grad.astype(bf16)
    zero = jnp.zeros_like(heads_grad)
    both = jnp.concatenate(
        [jnp.where(matched, heads_grad, zero), jnp.where(matched, zero, heads_grad)], axis=1
    )
    heads_share = lax.psum_scatter(both, "dp", scatter_dimension=0, tiled=True)
    heads_share = add(heads_share[:, : 3 * tile], flip(heads_share[:, 3 * tile :], 0, 2))

    feed_grad = lax.all_gather(feed_share, "dp", axis=0, tiled=False)[:SHARE]
    attention_grad = lax.all_gather(
        jnp.concatenate([heads_share, out_share], axis=1), "dp", axis=0, tiled=True
    )
    tile_owner, slot_index = slot_table(owners)
    capacity = FF // D
    slot_ids = jnp.arange(capacity, dtype=jnp.int32)
    owned = (tile_owner[None, :] == device) & (slot_index[None, :] == slot_ids[:, None])
    occupied = jnp.sum(owned.astype(f32), axis=1)
    tile_ids = jnp.sum(owned.astype(jnp.int32) * jnp.arange(owned.shape[1], dtype=jnp.int32), axis=1)
    attention_slots = jnp.concatenate(
        [
            lax.dynamic_slice(
                attention_grad, (0, jnp.minimum(tile_ids[s], 3) * tile), (D, tile)
            )
            for s in range(capacity)
        ],
        axis=1,
    )
    feed_flat = [jnp.concatenate([feed_grad[k, m] for k in range(SHARE)], axis=1) for m in range(2)]
    occupied_columns = jnp.repeat(occupied, tile)[None, :]
    slot_grad = (
        jnp.where(
            owners[4] == device,
            feed_flat[0],
            jnp.where(owners[5] == device, feed_flat[1], attention_slots),
        ).astype(f32)
        * occupied_columns
    )
    new_master, new_one, new_two = adam_update(
        slot_grad, master[0], moment_one[0], moment_two[0], occupied_columns, weight_decay
    )
    returned = lax.all_to_all(
        new_master.astype(bf16).reshape(n_dp, share_rows, capacity * tile),
        "dp", split_axis=0, concat_axis=0, tiled=True,
    )
    row_shard = jnp.concatenate(
        [
            lax.dynamic_slice(
                returned, (tile_owner[i], 0, slot_index[i] * tile), (1, share_rows, tile)
            )[0]
            for i in range(tile_owner.shape[0])
        ],
        axis=1,
    )
    new_weights = lax.all_gather(row_shard, "dp", axis=0, tiled=True)
    norm_owner = (device == owners[6]).astype(f32)
    new_norm_master, new_norm_one, new_norm_two = adam_update(
        norm_grads, norm_master[0], norm_one[0], norm_two[0], norm_owner, 0.0
    )
    return (
        swap(outputs)[:, None, :],
        input_grad,
        slot_grad[None],
        new_master[None],
        new_one[None],
        new_two[None],
        new_weights,
        norm_grads,
        new_norm_master[None],
        new_norm_one[None],
        new_norm_two[None],
    )


def solution(mesh):
    in_specs = (
        P("tensor", "dp", None),
        P(None, "tensor"),
        P(),
        P("tensor", "dp", None),
        P("dp"),
        P(),
        P("dp", None, "tensor"),
        P("dp", None, "tensor"),
        P("dp", None, "tensor"),
        P("dp", None, None),
        P("dp", None, None),
        P("dp", None, None),
    )
    out_specs = (
        P("tensor", "dp", None),
        P("tensor", "dp", None),
        P("dp", None, "tensor"),
        P("dp", None, "tensor"),
        P("dp", None, "tensor"),
        P("dp", None, "tensor"),
        P(None, "tensor"),
        P(),
        P("dp", None, None),
        P("dp", None, None),
        P("dp", None, None),
    )
    return jax.shard_map(
        partial(layer, mesh.shape["dp"], mesh.shape["tensor"]),
        mesh=mesh,
        in_specs=in_specs,
        out_specs=out_specs,
        check_vma=False,
    )
```

```python
from functools import partial

import jax
import jax.numpy as jnp
from jax import lax
from jax.experimental import pallas as pl
from jax.experimental.pallas import tpu as pltpu
from jax.sharding import PartitionSpec as P

D = 1024
FF = 4096
ADAM_STEP = 10
HEAD_DIM = 64
SHARE = 8


f32, bf16 = jnp.float32, jnp.bfloat16
beta_one = 0.9
beta_two = 0.999
learn_rate = 0.02
weight_decay = 0.1
adam_eps = 1e-08
norm_eps = 1e-05
masked_score = -1e30
AXES = ("dp", "tensor")


def contract(a, b, ca, cb):
    return lax.dot_general(a, b, (((ca,), (cb,)), ((), ())), preferred_element_type=f32)


def norm_parts(value, gain, shift):
    average = jnp.mean(value, axis=-1, keepdims=True)
    centred = value - average
    variance = jnp.mean(centred * centred, axis=-1, keepdims=True)
    inverse = lax.rsqrt(variance + norm_eps)
    normed = centred * inverse
    return normed * gain + shift, normed, inverse


def norm_back(upstream, normed, inverse, gain):
    scaled = upstream * gain
    inner = (
        scaled
        - jnp.mean(scaled, axis=-1, keepdims=True)
        - normed * jnp.mean(scaled * normed, axis=-1, keepdims=True)
    )
    return inner * inverse


def slot_table(owners):
    repeat = FF // D
    tile_matrix = jnp.array([0, 1, 2, 3] + [4] * repeat + [5] * repeat, dtype=jnp.int32)
    choose = (tile_matrix[:, None] == jnp.arange(7, dtype=jnp.int32)[None, :]).astype(jnp.int32)
    tile_owner = jnp.sum(choose * owners[None, :], axis=1)
    position = jnp.arange(tile_matrix.shape[0], dtype=jnp.int32)
    before = (tile_owner[None, :] == tile_owner[:, None]) & (position[None, :] < position[:, None])
    slot_index = jnp.sum(before.astype(jnp.int32), axis=1)
    return (tile_owner, slot_index)


def adam_update(grad, param, first, second, occupied, decay_rate):
    first_new = occupied * (beta_one * first + (1.0 - beta_one) * grad)
    second_new = occupied * (beta_two * second + (1.0 - beta_two) * grad * grad)
    correct_one = 1.0 - beta_one**ADAM_STEP
    correct_two = 1.0 - beta_two**ADAM_STEP
    direction = first_new / correct_one / (jnp.sqrt(second_new / correct_two) + adam_eps)
    param_new = occupied * (param - learn_rate * (direction + decay_rate * param))
    return (param_new, first_new, second_new)


def head_keys(keys, half, start, length):
    lane = lax.broadcasted_iota(jnp.int32, keys.shape, 1)
    row = lax.broadcasted_iota(jnp.int32, keys.shape, 0)
    bias = jnp.where(start + row < length, 0.0, masked_score).astype(f32)
    extra = jnp.where(lane == (1 - half) * HEAD_DIM, bias, 0.0)
    return jnp.where(lane // HEAD_DIM == half, keys.astype(f32), extra).astype(bf16)


def head_half(rows, half):
    lane = lax.broadcasted_iota(jnp.int32, rows.shape, 1)
    return jnp.where(lane // HEAD_DIM == half, rows, jnp.zeros_like(rows))


def head_queries(rows, half):
    lane = lax.broadcasted_iota(jnp.int32, rows.shape, 1)
    scaled = rows.astype(f32) * HEAD_DIM ** (-0.5)
    extra = jnp.where(lane == (1 - half) * HEAD_DIM, 1.0, 0.0)
    return jnp.where(lane // HEAD_DIM == half, scaled, extra).astype(bf16)


def attention_forward_body(info, mixed_ref, context_ref, lse_ref, keys, values):
    step = pl.program_id(0)
    chunks, rows, _ = mixed_ref.shape
    width = context_ref.shape[-1]

    @pl.when(step == 0)
    def _():
        for j in range(chunks):
            for h in range(width // HEAD_DIM):
                at = width + (h // 2) * 128
                keys[h, j * rows : (j + 1) * rows, :] = head_keys(
                    mixed_ref[j, :, at : at + 128], h % 2, info[1 + j], info[0]
                )
            values[j * rows : (j + 1) * rows, :] = mixed_ref[j, :, 2 * width :]

    lane = lax.broadcasted_iota(jnp.int32, (rows, 128), 1)
    logs = jnp.zeros((rows, 128), f32)
    for pair in range(width // 128):
        queries = mixed_ref[step, :, pair * 128 : pair * 128 + 128]
        both = []
        for half in range(2):
            h = pair * 2 + half
            scores = contract(head_queries(queries, half), keys[h], 1, 1)
            top = jnp.max(scores, axis=1, keepdims=True)
            weight = jnp.exp(scores - top)
            total = jnp.sum(weight, axis=1, keepdims=True)
            out = contract(weight.astype(bf16), values[:, pair * 128 : pair * 128 + 128], 1, 0)
            both.append(out / total)
            logs = jnp.where(lane == h, top + jnp.log(total), logs)
        context_ref[0, :, pair * 128 : pair * 128 + 128] = jnp.where(
            lane < HEAD_DIM, both[0], both[1]
        ).astype(bf16)
    lse_ref[0] = jnp.transpose(logs)[:8, :]


def attention_forward(info, mixed):
    chunks, rows, width3 = mixed.shape
    width = width3 // 3
    seq = chunks * rows
    heads = width // HEAD_DIM
    return pl.pallas_call(
        attention_forward_body,
        grid=(chunks,),
        name="attention_forward",
        in_specs=[
            pl.BlockSpec(memory_space=pltpu.SMEM),
            pl.BlockSpec((chunks, rows, width3), lambda i: (0, 0, 0)),
        ],
        out_specs=[
            pl.BlockSpec((1, rows, width), lambda i: (i, 0, 0)),
            pl.BlockSpec((1, 8, rows), lambda i: (i, 0, 0)),
        ],
        out_shape=[
            jax.ShapeDtypeStruct((chunks, rows, width), bf16),
            jax.ShapeDtypeStruct((chunks, 8, rows), f32),
        ],
        scratch_shapes=[pltpu.VMEM((heads, seq, 128), bf16), pltpu.VMEM((seq, width), bf16)],
        compiler_params=pltpu.CompilerParams(vmem_limit_bytes=48 << 20),
        cost_estimate=pl.CostEstimate(
            flops=16 * heads * seq * seq * HEAD_DIM, bytes_accessed=8 << 20, transcendentals=0
        ),
    )(info, mixed)


def attention_backward_body(
    info, mixed_ref, context_ref, upstream_ref, lse_ref, out_ref, keys, turned, key_sum, value_sum, query_t
):
    step = pl.program_id(0)
    chunks, rows, _ = mixed_ref.shape
    width = context_ref.shape[-1]
    scale = HEAD_DIM ** (-0.5)

    @pl.when(step == 0)
    def _():
        key_sum[...] = jnp.zeros_like(key_sum)
        value_sum[...] = jnp.zeros_like(value_sum)
        for j in range(chunks):
            for h in range(width // HEAD_DIM):
                at = width + (h // 2) * 128
                keys[h, j * rows : (j + 1) * rows, :] = head_keys(
                    mixed_ref[j, :, at : at + 128], h % 2, info[1 + j], info[0]
                )
            turned[:, j * rows : (j + 1) * rows] = jnp.transpose(
                mixed_ref[j, :, width : 2 * width].astype(f32)
            ).astype(bf16)

    upstream = upstream_ref[0]
    product = upstream.astype(f32) * context_ref[0].astype(f32)
    feature = lax.broadcasted_iota(jnp.int32, (8, width), 1) // HEAD_DIM
    picks = (feature == lax.broadcasted_iota(jnp.int32, (8, width), 0)).astype(f32)
    delta = lax.dot_general(
        picks, product, (((1,), (1,)), ((), ())), precision=lax.Precision.HIGHEST,
        preferred_element_type=f32,
    )
    lse = lse_ref[0]
    for pair in range(width // 128):
        lanes = slice(pair * 128, pair * 128 + 128)
        queries = mixed_ref[step, :, lanes]
        value_rows = mixed_ref[:, :, 2 * width + pair * 128 : 2 * width + pair * 128 + 128]
        value_rows = value_rows.reshape(chunks * rows, 128)
        for half in range(2):
            h = pair * 2 + half
            scores = contract(keys[h], head_queries(queries, half), 1, 1)
            weight = jnp.exp(scores - lse[h : h + 1, :])
            up_half = head_half(upstream[:, lanes], half)
            back = contract(value_rows, up_half, 1, 1)
            score_grad = (weight * (back - delta[h : h + 1, :])).astype(bf16)
            value_sum[pair] += contract(weight.astype(bf16), up_half, 1, 0)
            key_sum[pair] += contract(score_grad, head_half(queries, half), 1, 0)
            query_t[h * HEAD_DIM : (h + 1) * HEAD_DIM, :] = (
                contract(turned[h * HEAD_DIM : (h + 1) * HEAD_DIM, :], score_grad, 1, 0) * scale
            )
    out_ref[step, :, :width] = jnp.transpose(query_t[...]).astype(bf16)

    @pl.when(step == chunks - 1)
    def _():
        for j in range(chunks):
            at = slice(j * rows, (j + 1) * rows)
            for pair in range(width // 128):
                left = width + pair * 128
                out_ref[j, :, left : left + 128] = (key_sum[pair, at, :] * scale).astype(bf16)
                out_ref[j, :, left + width : left + width + 128] = value_sum[pair, at, :].astype(bf16)


def attention_backward(info, mixed, context, upstream, lse):
    chunks, rows, width3 = mixed.shape
    width = width3 // 3
    seq = chunks * rows
    heads = width // HEAD_DIM
    return pl.pallas_call(
        attention_backward_body,
        grid=(chunks,),
        name="attention_backward",
        in_specs=[
            pl.BlockSpec(memory_space=pltpu.SMEM),
            pl.BlockSpec((chunks, rows, width3), lambda i: (0, 0, 0)),
            pl.BlockSpec((1, rows, width), lambda i: (i, 0, 0)),
            pl.BlockSpec((1, rows, width), lambda i: (i, 0, 0)),
            pl.BlockSpec((1, 8, rows), lambda i: (i, 0, 0)),
        ],
        out_specs=pl.BlockSpec((chunks, rows, width3), lambda i: (0, 0, 0)),
        out_shape=jax.ShapeDtypeStruct((chunks, rows, width3), bf16),
        scratch_shapes=[
            pltpu.VMEM((heads, seq, 128), bf16),
            pltpu.VMEM((width, seq), bf16),
            pltpu.VMEM((width // 128, seq, 128), f32),
            pltpu.VMEM((width // 128, seq, 128), f32),
            pltpu.VMEM((width, rows), f32),
        ],
        compiler_params=pltpu.CompilerParams(vmem_limit_bytes=56 << 20),
        cost_estimate=pl.CostEstimate(
            flops=40 * heads * seq * seq * HEAD_DIM, bytes_accessed=8 << 20, transcendentals=0
        ),
    )(info, mixed, context, upstream, lse)


def other_core():
    device = lax.axis_index("dp")
    return device + 1 - 2 * (device % 2)


def greet(peers):
    barrier = pltpu.get_barrier_semaphore()
    for peer in peers:
        pl.semaphore_signal(barrier, inc=1, device_id=peer, device_id_type=pl.DeviceIdType.MESH)
    pl.semaphore_wait(barrier, len(peers))


def joined(held, i, kind):
    return jnp.concatenate([held[2 * i + k, m, kind] for k in range(2) for m in range(2)], axis=-1)


def gelu_parts(value):
    bell = jnp.exp(-0.5 * value * value)
    t = 1.0 / (1.0 + (0.3275911 * 0.5**0.5) * jnp.abs(value))
    tail = 0.5 * 1.061405429
    for c in (-1.453152027, 1.421413741, -0.284496736, 0.254829592):
        tail = tail * t + 0.5 * c
    tail = tail * t * bell
    area = jnp.where(value > 0, 1.0 - tail, tail)
    return value * area, area + value * bell * (0.5 / jnp.pi) ** 0.5


def feed_body(count, info, first_ref, cotangent_ref, norms_ref, *refs):
    pieces = refs[:count]
    out_ref, low_ref, both_ref, hidden_ref, pre_ref, grad_ref, sums_ref = refs[count : count + 7]
    held, slope, total, leaving, landed, local_sems, send_sems, recv_sems = refs[count + 7 :]
    rows = first_ref.shape[0]
    width = hidden_ref.shape[-1]
    peer = (other_core(), lax.axis_index("tensor"))
    for i in range(count):
        pltpu.make_async_copy(pieces[i], held.at[i], local_sems.at[i]).start()
    greet([peer])

    def across(source, target, k):
        return pltpu.make_async_remote_copy(
            source, target, send_sems.at[k], recv_sems.at[k], device_id=peer,
            device_id_type=pl.DeviceIdType.MESH,
        )

    half = rows // 2
    both_ref[0] = first_ref[...].astype(bf16)
    first_copy = across(both_ref.at[0], both_ref.at[1], 0)
    first_copy.start()

    def up(i, slot):
        weight = joined(held, i, 0)
        for r in range(0, rows, half):
            value = jnp.dot(both_ref[slot, r : r + half, :], weight, preferred_element_type=f32)
            hidden, steep = gelu_parts(value)
            hidden_ref[i, slot, r : r + half, :] = hidden.astype(bf16)
            slope[i, slot, r : r + half, :] = steep.astype(bf16)

    def down(i, slot):
        total[slot] += contract(hidden_ref[i, slot], joined(held, i, 1), 1, 1)

    def back(i, slot):
        weight = joined(held, i, 1)
        for r in range(0, rows, half):
            value = jnp.dot(low_ref[slot, r : r + half, :], weight, preferred_element_type=f32)
            steep = slope[i, slot, r : r + half, :].astype(f32)
            pre_ref[i, slot, r : r + half, :] = (value * steep).astype(bf16)

    def back_up(i, slot):
        total[slot] += contract(pre_ref[i, slot], joined(held, i, 0), 1, 1)

    def loop(*works):
        def body(i, carry):
            for work in works:
                work(i)
            return carry

        lax.fori_loop(0, count // 2, body, 0)

    def arrive(i):
        for k in range(2):
            pltpu.make_async_copy(
                pieces[0], held.at[2 * i + k], local_sems.at[2 * i + k]
            ).wait()

    total[...] = jnp.zeros_like(total)
    loop(arrive, lambda i: up(i, 0))
    first_copy.wait()
    loop(lambda i: up(i, 1), lambda i: down(i, 1))
    leaving[...] = total[1].astype(bf16)
    feed_copy = across(leaving, landed.at[0], 1)
    feed_copy.start()
    loop(lambda i: down(i, 0))
    feed_copy.wait()

    sums_ref[...] = jnp.zeros_like(sums_ref)
    part = 128

    def middle(r, carry):
        at = pl.ds(pl.multiple_of(r * part, part), part)
        second, normed, inverse = norm_parts(
            first_ref[at, :] + (total[0, at, :] + landed[0, at, :].astype(f32)),
            norms_ref[2:3, :], norms_ref[3:4, :],
        )
        out_ref[at, :] = second.astype(bf16)
        row = lax.broadcasted_iota(jnp.int32, (part, 1), 0) + r * part + info[1]
        seed = cotangent_ref[at, :].astype(f32) * (row < info[0]).astype(f32)
        grad = norm_back(seed, normed, inverse, norms_ref[2:3, :])
        sums_ref[0:1, :] += jnp.sum(seed * normed, axis=0, keepdims=True)
        sums_ref[1:2, :] += jnp.sum(seed, axis=0, keepdims=True)
        total[0, at, :] = grad
        low_ref[0, at, :] = grad.astype(bf16)
        return carry

    lax.fori_loop(0, rows // part, middle, 0)
    low_copy = across(low_ref.at[0], low_ref.at[1], 2)
    low_copy.start()
    total[1] = jnp.zeros_like(total[1])
    loop(lambda i: back(i, 0))
    low_copy.wait()
    loop(lambda i: back(i, 1), lambda i: back_up(i, 1))
    leaving[...] = total[1].astype(bf16)
    grad_copy = across(leaving, landed.at[1], 3)
    grad_copy.start()
    loop(lambda i: back_up(i, 0))
    grad_copy.wait()
    grad_ref[...] = total[0] + landed[1].astype(f32)


def feed_block(info, first, cotangent, norms, pieces):
    rows = first.shape[0]
    count = len(pieces)
    lanes = pieces[0].shape[-1]
    width = 4 * lanes
    vmem = pl.BlockSpec(memory_space=pltpu.VMEM)
    return pl.pallas_call(
        partial(feed_body, count),
        name="feed_block",
        in_specs=[pl.BlockSpec(memory_space=pltpu.SMEM), vmem, vmem, vmem]
        + [pl.BlockSpec(memory_space=pl.ANY)] * count,
        out_specs=[vmem] * 7,
        out_shape=[
            jax.ShapeDtypeStruct((rows, D), bf16),
            jax.ShapeDtypeStruct((2, rows, D), bf16),
            jax.ShapeDtypeStruct((2, rows, D), bf16),
            jax.ShapeDtypeStruct((count // 2, 2, rows, width), bf16),
            jax.ShapeDtypeStruct((count // 2, 2, rows, width), bf16),
            jax.ShapeDtypeStruct((rows, D), f32),
            jax.ShapeDtypeStruct((2, D), f32),
        ],
        scratch_shapes=[
            pltpu.VMEM((count,) + pieces[0].shape, bf16),
            pltpu.VMEM((count // 2, 2, rows, width), bf16),
            pltpu.VMEM((2, rows, D), f32),
            pltpu.VMEM((rows, D), bf16),
            pltpu.VMEM((2, rows, D), bf16),
            pltpu.SemaphoreType.DMA((count,)),
            pltpu.SemaphoreType.DMA((4,)),
            pltpu.SemaphoreType.DMA((4,)),
        ],
        compiler_params=pltpu.CompilerParams(
            vmem_limit_bytes=60 << 20, collective_id=1, has_side_effects=True
        ),
        cost_estimate=pl.CostEstimate(
            flops=8 * rows * D * width * count, bytes_accessed=30 << 20, transcendentals=0
        ),
    )(info, first, cotangent, norms, *pieces)


def feed_grads_body(first_ref, low_ref, hidden_ref, pre_ref, up_ref, down_ref, first_t, low_t):
    rows = first_ref.shape[1]

    @pl.when(pl.program_id(0) == 0)
    def _():
        for slot in range(2):
            at = slice(slot * rows, (slot + 1) * rows)
            first_t[:, at] = jnp.transpose(first_ref[slot].astype(f32)).astype(bf16)
            low_t[:, at] = jnp.transpose(low_ref[slot].astype(f32)).astype(bf16)

    lanes = up_ref.shape[-1]
    width = pre_ref.shape[-1]
    for target, source, turned in ((up_ref, pre_ref, first_t), (down_ref, hidden_ref, low_t)):
        grad = jnp.dot(
            turned[...], source[0].reshape(2 * rows, width), preferred_element_type=f32
        ).astype(bf16)
        for k in range(2):
            for m in range(2):
                at = (2 * k + m) * lanes
                if target is up_ref:
                    target[m, k, 0] = grad[:, at : at + lanes]
                else:
                    target[m, 0, k] = grad[:, at : at + lanes]


def feed_grads(first, low, hidden, pre):
    count, _, rows, width = hidden.shape
    full = pl.BlockSpec((2, rows, D), lambda i: (0, 0, 0))
    piece = pl.BlockSpec((1, 2, rows, width), lambda i: (i, 0, 0, 0))
    lanes = width // 4
    return pl.pallas_call(
        feed_grads_body,
        grid=(count,),
        name="feed_grads",
        in_specs=[full, full, piece, piece],
        out_specs=[
            pl.BlockSpec((2, 2, 1, D, lanes), lambda i: (i // 2, 0, i % 2, 0, 0)),
            pl.BlockSpec((2, 1, 2, D, lanes), lambda i: (i // 2, i % 2, 0, 0, 0)),
        ],
        out_shape=[jax.ShapeDtypeStruct((count, 2, 2, D, lanes), bf16)] * 2,
        scratch_shapes=[pltpu.VMEM((D, 2 * rows), bf16), pltpu.VMEM((D, 2 * rows), bf16)],
        compiler_params=pltpu.CompilerParams(vmem_limit_bytes=48 << 20),
        cost_estimate=pl.CostEstimate(
            flops=8 * rows * D * width * count, bytes_accessed=20 << 20, transcendentals=0
        ),
    )(first, low, hidden, pre)


def layer(n_dp, n_tensor, tokens, weights, norms, cotangent, lengths, owners, master, moment_one,
          moment_two, norm_master, norm_one, norm_two):
    tile = D // n_tensor
    hidden_width = FF // n_tensor
    rows = tokens.shape[0]
    lanes = hidden_width // SHARE
    device = lax.axis_index("dp")
    z = lax.axis_index("tensor")
    core = device % 2
    matched = core == z // 2
    quarter = jnp.where(matched, z, z ^ 2)

    def flip(x, dd, dz):
        pairs = [
            (d * n_tensor + t, (d ^ dd) * n_tensor + (t ^ dz))
            for d in range(n_dp)
            for t in range(n_tensor)
        ]
        return lax.ppermute(x, AXES, pairs)

    def some(x, dd, dz, want):
        pairs = [
            (d * n_tensor + t, (d ^ dd) * n_tensor + (t ^ dz))
            for d in range(n_dp)
            for t in range(n_tensor)
            if (t // 2 == d % 2) == want
        ]
        return lax.ppermute(x, AXES, pairs)

    def swap(x):
        return jnp.where(matched, x, some(x, 1, 2, False))

    w_mixed = weights[:, : 3 * tile]
    w_out = weights[:, 3 * tile : 4 * tile]
    share_rows = D // n_dp
    length = jnp.where(matched, lengths, flip(lengths, 1, 0))[0]
    base = jnp.stack([quarter ^ k for k in (0, 2, 1, 3)]) * rows
    info = jnp.concatenate([length[None], base]).astype(jnp.int32)

    inputs = tokens[:, 0, :]
    own = swap(inputs)
    far = some(inputs, 0, 1, True) + some(own, 0, 1, False)
    near = flip(own, 1, 0)
    gathered = jnp.stack([own, near, far, flip(far, 1, 0)])

    def my_rows(x):
        return lax.dynamic_slice_in_dim(x, device * share_rows, share_rows, 0)

    other = lax.all_gather(flip(my_rows(w_mixed), 0, 2), "dp", axis=0, tiled=True)
    w_heads = jnp.where(matched, w_mixed, other)
    out_own = my_rows(w_out)
    out_two = jnp.concatenate([out_own, flip(out_own, 0, 1)], axis=1)
    out_four = jnp.concatenate([out_two, flip(out_two, 0, 2)], axis=1)
    w_out_all = lax.all_gather(out_four, "dp", axis=0, tiled=True)

    at = (device % SHARE) * lanes + 4 * tile
    own_piece = jnp.stack(
        [
            lax.dynamic_slice(weights, (0, at), (D, lanes)),
            lax.dynamic_slice(weights, (0, at + hidden_width), (D, lanes)),
        ]
    )
    near_pieces = jnp.stack([own_piece, flip(own_piece, 0, 1)])
    far_pieces = flip(near_pieces, 0, 2)

    def spread(first_pieces, one, two):
        a = first_pieces
        b = flip(a, one, 0)
        return [a, b, flip(a, two, 0), flip(b, two, 0)]

    near_four = spread(near_pieces, 2, 4)
    far_four = spread(far_pieces, 4, 2)
    pieces = near_four + [far_four[k] for k in (0, 2, 1, 3)]

    mixed = jnp.einsum(
        "csd,de->cse", gathered, w_heads, preferred_element_type=f32
    ).astype(bf16)
    context, lse = attention_forward(info, mixed)

    parts = [context[0], flip(context[1], 1, 0), flip(context[2], 0, 1), flip(context[3], 1, 1)]
    context_all = jnp.where(
        matched,
        jnp.concatenate([parts[k] for k in (0, 2, 1, 3)], axis=1),
        jnp.concatenate([parts[k] for k in (1, 3, 0, 2)], axis=1),
    )
    branch = contract(context_all, w_out_all, 1, 1)
    first, first_normed, first_inverse = norm_parts(
        own.astype(f32) + branch, norms[0], norms[1]
    )
    seed = swap(cotangent[:, 0, :])
    outputs, both_low, both_first, hidden, pre_grad, first_grad, sums_two = feed_block(
        info, first, seed, norms, pieces
    )
    branch_grad = norm_back(first_grad, first_normed, first_inverse, norms[0])
    gain_one = jnp.sum(first_grad * first_normed, axis=0)
    shift_one = jnp.sum(first_grad, axis=0)
    branch_low = branch_grad.astype(bf16)
    context_grad = jnp.dot(branch_low, w_out_all, preferred_element_type=f32).astype(bf16)
    blocks = [context_grad[:, k * tile : (k + 1) * tile] for k in range(4)]
    blocks = [
        jnp.where(matched, blocks[a], blocks[b]) for a, b in ((0, 2), (2, 0), (1, 3), (3, 1))
    ]
    upstream = jnp.stack(
        [blocks[0], flip(blocks[1], 1, 0), flip(blocks[2], 0, 1), flip(blocks[3], 1, 1)]
    )

    def add(a, b):
        return (a.astype(f32) + b.astype(f32)).astype(bf16)

    up_sum, down_sum = feed_grads(both_first, both_low, hidden, pre_grad)
    up_sum = add(up_sum[:, 0], flip(up_sum[:, 1], 2, 0))
    down_sum = add(down_sum[:, 0], flip(down_sum[:, 1], 4, 0))
    up_sum = add(up_sum[:, 0], flip(up_sum[:, 1], 4, 0))
    down_sum = add(down_sum[:, 0], flip(down_sum[:, 1], 2, 0))
    feed_share = jnp.stack([up_sum, down_sum], axis=1)
    feed_share = add(feed_share[:2], flip(feed_share[2:], 0, 2))
    feed_share = add(feed_share[0], flip(feed_share[1], 0, 1))
    bit = SHARE
    while bit < n_dp:
        feed_share = add(feed_share, flip(feed_share, bit, 0))
        bit *= 2

    out_grad = contract(branch_low, context_all, 0, 0).astype(bf16)
    out_share = lax.psum_scatter(out_grad, "dp", scatter_dimension=0, tiled=True)
    out_share = add(out_share[:, : 2 * tile], flip(out_share[:, 2 * tile :], 0, 2))
    out_share = add(out_share[:, :tile], flip(out_share[:, tile:], 0, 1))

    norm_grads = jnp.concatenate([jnp.stack([gain_one, shift_one]), sums_two])
    for dd, dz in [(1 << k, 0) for k in range(n_dp.bit_length() - 1)] + [(0, 1), (0, 2)]:
        norm_grads = norm_grads + flip(norm_grads, dd, dz)

    mixed_grad = attention_backward(info, mixed, context, upstream, lse)
    back_rows = jnp.einsum("cse,de->csd", mixed_grad, w_heads, preferred_element_type=f32)
    back_low = back_rows.astype(bf16)
    back_pair = [
        back_rows[0] + flip(back_low[1], 1, 0).astype(f32),
        back_rows[2] + flip(back_low[3], 1, 0).astype(f32),
    ]
    input_total = branch_grad + back_pair[0] + flip(back_pair[1].astype(bf16), 0, 1).astype(f32)
    input_grad = swap(input_total.astype(bf16))[:, None, :]

    heads_grad = jnp.einsum("csd,cse->de", gathered, mixed_grad, preferred_element_type=f32)
    heads_grad = heads_grad.astype(bf16)
    zero = jnp.zeros_like(heads_grad)
    both = jnp.concatenate(
        [jnp.where(matched, heads_grad, zero), jnp.where(matched, zero, heads_grad)], axis=1
    )
    heads_share = lax.psum_scatter(both, "dp", scatter_dimension=0, tiled=True)
    heads_share = add(heads_share[:, : 3 * tile], flip(heads_share[:, 3 * tile :], 0, 2))

    feed_grad = lax.all_gather(feed_share, "dp", axis=0, tiled=False)[:SHARE]
    attention_grad = lax.all_gather(
        jnp.concatenate([heads_share, out_share], axis=1), "dp", axis=0, tiled=True
    )
    tile_owner, slot_index = slot_table(owners)
    capacity = FF // D
    slot_ids = jnp.arange(capacity, dtype=jnp.int32)
    owned = (tile_owner[None, :] == device) & (slot_index[None, :] == slot_ids[:, None])
    occupied = jnp.sum(owned.astype(f32), axis=1)
    tile_ids = jnp.sum(owned.astype(jnp.int32) * jnp.arange(owned.shape[1], dtype=jnp.int32), axis=1)
    attention_slots = jnp.concatenate(
        [
            lax.dynamic_slice(
                attention_grad, (0, jnp.minimum(tile_ids[s], 3) * tile), (D, tile)
            )
            for s in range(capacity)
        ],
        axis=1,
    )
    feed_flat = [jnp.concatenate([feed_grad[k, m] for k in range(SHARE)], axis=1) for m in range(2)]
    occupied_columns = jnp.repeat(occupied, tile)[None, :]
    slot_grad = (
        jnp.where(
            owners[4] == device,
            feed_flat[0],
            jnp.where(owners[5] == device, feed_flat[1], attention_slots),
        ).astype(f32)
        * occupied_columns
    )
    new_master, new_one, new_two = adam_update(
        slot_grad, master[0], moment_one[0], moment_two[0], occupied_columns, weight_decay
    )
    returned = lax.all_to_all(
        new_master.astype(bf16).reshape(n_dp, share_rows, capacity * tile),
        "dp", split_axis=0, concat_axis=0, tiled=True,
    )
    row_shard = jnp.concatenate(
        [
            lax.dynamic_slice(
                returned, (tile_owner[i], 0, slot_index[i] * tile), (1, share_rows, tile)
            )[0]
            for i in range(tile_owner.shape[0])
        ],
        axis=1,
    )
    new_weights = lax.all_gather(row_shard, "dp", axis=0, tiled=True)
    norm_owner = (device == owners[6]).astype(f32)
    new_norm_master, new_norm_one, new_norm_two = adam_update(
        norm_grads, norm_master[0], norm_one[0], norm_two[0], norm_owner, 0.0
    )
    return (
        swap(outputs)[:, None, :],
        input_grad,
        slot_grad[None],
        new_master[None],
        new_one[None],
        new_two[None],
        new_weights,
        norm_grads,
        new_norm_master[None],
        new_norm_one[None],
        new_norm_two[None],
    )


def solution(mesh):
    in_specs = (
        P("tensor", "dp", None),
        P(None, "tensor"),
        P(),
        P("tensor", "dp", None),
        P("dp"),
        P(),
        P("dp", None, "tensor"),
        P("dp", None, "tensor"),
        P("dp", None, "tensor"),
        P("dp", None, None),
        P("dp", None, None),
        P("dp", None, None),
    )
    out_specs = (
        P("tensor", "dp", None),
        P("tensor", "dp", None),
        P("dp", None, "tensor"),
        P("dp", None, "tensor"),
        P("dp", None, "tensor"),
        P("dp", None, "tensor"),
        P(None, "tensor"),
        P(),
        P("dp", None, None),
        P("dp", None, None),
        P("dp", None, None),
    )
    return jax.shard_map(
        partial(layer, mesh.shape["dp"], mesh.shape["tensor"]),
        mesh=mesh,
        in_specs=in_specs,
        out_specs=out_specs,
        check_vma=False,
    )
```

```python
from functools import partial

import jax
import jax.numpy as jnp
from jax import lax
from jax.experimental import pallas as pl
from jax.experimental.pallas import tpu as pltpu
from jax.sharding import PartitionSpec as P

D = 1024
FF = 4096
ADAM_STEP = 10
HEAD_DIM = 64
SHARE = 8


f32, bf16 = jnp.float32, jnp.bfloat16
beta_one = 0.9
beta_two = 0.999
learn_rate = 0.02
weight_decay = 0.1
adam_eps = 1e-08
norm_eps = 1e-05
masked_score = -1e30
AXES = ("dp", "tensor")


def contract(a, b, ca, cb):
    return lax.dot_general(a, b, (((ca,), (cb,)), ((), ())), preferred_element_type=f32)


def norm_parts(value, gain, shift):
    average = jnp.mean(value, axis=-1, keepdims=True)
    centred = value - average
    variance = jnp.mean(centred * centred, axis=-1, keepdims=True)
    inverse = lax.rsqrt(variance + norm_eps)
    normed = centred * inverse
    return normed * gain + shift, normed, inverse


def norm_back(upstream, normed, inverse, gain):
    scaled = upstream * gain
    inner = (
        scaled
        - jnp.mean(scaled, axis=-1, keepdims=True)
        - normed * jnp.mean(scaled * normed, axis=-1, keepdims=True)
    )
    return inner * inverse


def slot_table(owners):
    repeat = FF // D
    tile_matrix = jnp.array([0, 1, 2, 3] + [4] * repeat + [5] * repeat, dtype=jnp.int32)
    choose = (tile_matrix[:, None] == jnp.arange(7, dtype=jnp.int32)[None, :]).astype(jnp.int32)
    tile_owner = jnp.sum(choose * owners[None, :], axis=1)
    position = jnp.arange(tile_matrix.shape[0], dtype=jnp.int32)
    before = (tile_owner[None, :] == tile_owner[:, None]) & (position[None, :] < position[:, None])
    slot_index = jnp.sum(before.astype(jnp.int32), axis=1)
    return (tile_owner, slot_index)


def adam_update(grad, param, first, second, occupied, decay_rate):
    first_new = occupied * (beta_one * first + (1.0 - beta_one) * grad)
    second_new = occupied * (beta_two * second + (1.0 - beta_two) * grad * grad)
    correct_one = 1.0 - beta_one**ADAM_STEP
    correct_two = 1.0 - beta_two**ADAM_STEP
    direction = first_new / correct_one / (jnp.sqrt(second_new / correct_two) + adam_eps)
    param_new = occupied * (param - learn_rate * (direction + decay_rate * param))
    return (param_new, first_new, second_new)


def head_keys(keys, half, start, length):
    lane = lax.broadcasted_iota(jnp.int32, keys.shape, 1)
    row = lax.broadcasted_iota(jnp.int32, keys.shape, 0)
    bias = jnp.where(start + row < length, 0.0, masked_score).astype(f32)
    extra = jnp.where(lane == (1 - half) * HEAD_DIM, bias, 0.0)
    return jnp.where(lane // HEAD_DIM == half, keys.astype(f32), extra).astype(bf16)


def head_half(rows, half):
    lane = lax.broadcasted_iota(jnp.int32, rows.shape, 1)
    return jnp.where(lane // HEAD_DIM == half, rows, jnp.zeros_like(rows))


def head_queries(rows, half):
    lane = lax.broadcasted_iota(jnp.int32, rows.shape, 1)
    scaled = rows.astype(f32) * HEAD_DIM ** (-0.5)
    extra = jnp.where(lane == (1 - half) * HEAD_DIM, 1.0, 0.0)
    return jnp.where(lane // HEAD_DIM == half, scaled, extra).astype(bf16)


def attention_forward_body(info, mixed_ref, context_ref, lse_ref, keys, values):
    step = pl.program_id(0)
    chunks, rows, _ = mixed_ref.shape
    width = context_ref.shape[-1]

    @pl.when(step == 0)
    def _():
        for j in range(chunks):
            for h in range(width // HEAD_DIM):
                at = width + (h // 2) * 128
                keys[h, j * rows : (j + 1) * rows, :] = head_keys(
                    mixed_ref[j, :, at : at + 128], h % 2, info[1 + j], info[0]
                )
            values[j * rows : (j + 1) * rows, :] = mixed_ref[j, :, 2 * width :]

    lane = lax.broadcasted_iota(jnp.int32, (rows, 128), 1)
    logs = jnp.zeros((rows, 128), f32)
    for pair in range(width // 128):
        queries = mixed_ref[step, :, pair * 128 : pair * 128 + 128]
        both = []
        for half in range(2):
            h = pair * 2 + half
            scores = contract(head_queries(queries, half), keys[h], 1, 1)
            top = jnp.max(scores, axis=1, keepdims=True)
            weight = jnp.exp(scores - top)
            total = jnp.sum(weight, axis=1, keepdims=True)
            out = contract(weight.astype(bf16), values[:, pair * 128 : pair * 128 + 128], 1, 0)
            both.append(out / total)
            logs = jnp.where(lane == h, top + jnp.log(total), logs)
        context_ref[0, :, pair * 128 : pair * 128 + 128] = jnp.where(
            lane < HEAD_DIM, both[0], both[1]
        ).astype(bf16)
    lse_ref[0] = jnp.transpose(logs)[:8, :]


def attention_forward(info, mixed):
    chunks, rows, width3 = mixed.shape
    width = width3 // 3
    seq = chunks * rows
    heads = width // HEAD_DIM
    return pl.pallas_call(
        attention_forward_body,
        grid=(chunks,),
        name="attention_forward",
        in_specs=[
            pl.BlockSpec(memory_space=pltpu.SMEM),
            pl.BlockSpec((chunks, rows, width3), lambda i: (0, 0, 0)),
        ],
        out_specs=[
            pl.BlockSpec((1, rows, width), lambda i: (i, 0, 0)),
            pl.BlockSpec((1, 8, rows), lambda i: (i, 0, 0)),
        ],
        out_shape=[
            jax.ShapeDtypeStruct((chunks, rows, width), bf16),
            jax.ShapeDtypeStruct((chunks, 8, rows), f32),
        ],
        scratch_shapes=[pltpu.VMEM((heads, seq, 128), bf16), pltpu.VMEM((seq, width), bf16)],
        compiler_params=pltpu.CompilerParams(vmem_limit_bytes=48 << 20),
        cost_estimate=pl.CostEstimate(
            flops=16 * heads * seq * seq * HEAD_DIM, bytes_accessed=8 << 20, transcendentals=0
        ),
    )(info, mixed)


def other_core():
    device = lax.axis_index("dp")
    return device + 1 - 2 * (device % 2)


def peer_of(bit, turn):
    device, z = lax.axis_index("dp"), lax.axis_index("tensor")
    if bit:
        device = device + bit - 2 * bit * ((device // bit) % 2)
    if turn == 1:
        z = z + 1 - 2 * (z % 2)
    elif turn == 2:
        z = z + 2 - 4 * (z // 2)
    elif turn == 3:
        z = 3 - z
    return (device, z)


def greet(peers):
    barrier = pltpu.get_barrier_semaphore()
    for peer in peers:
        pl.semaphore_signal(barrier, inc=1, device_id=peer, device_id_type=pl.DeviceIdType.MESH)
    pl.semaphore_wait(barrier, len(peers))


def sender(send_sems, recv_sems):
    def send(source, target, k, peer):
        return pltpu.make_async_remote_copy(
            source, target, send_sems.at[k], recv_sems.at[k], device_id=peer,
            device_id_type=pl.DeviceIdType.MESH,
        )

    return send


def back_body(
    info, mixed_ref, context_ref, upstream_ref, lse_ref, weight_ref, branch_ref, gathered, up_grads, down_grads,
    input_ref, heads_ref, share_ref,
    keys, turned, key_sum, value_sum, query_t, grad, rows_held, heads_sum, kept, got_one, got_two, got_three,
    leaving, landed, local_sems, send_sems, recv_sems,
):
    chunks, rows, _ = mixed_ref.shape
    width = context_ref.shape[-1]
    scale = HEAD_DIM ** (-0.5)
    part = 256
    core, near_z = peer_of(1, 0), peer_of(0, 1)
    across = (peer_of(2, 0), peer_of(4, 0))
    send = sender(send_sems, recv_sems)
    sources = (up_grads, down_grads)

    def stage_one(b, kind):
        return send(sources[kind].at[b, 1], got_one.at[b, kind], 2 * b + kind, across[kind])

    def stage_two(b, kind):
        return send(kept.at[b, kind, 1], got_two.at[b, kind], 8 + 2 * b + kind, across[1 - kind])

    def stage_three(b):
        return send(kept.at[b, :, 0], got_three.at[b - 1], 15 + b, peer_of(0, b))

    def load(b, kind):
        return pltpu.make_async_copy(
            sources[kind].at[b, 0], kept.at[b, kind], local_sems.at[2 * b + kind]
        )

    def start_one(b):
        for kind in range(2):
            stage_one(b, kind).start()

    def start_two(b):
        for kind in range(2):
            load(b, kind).wait()
            stage_one(b, kind).wait()
            for k in (1, 0):
                kept[b, kind, k] = (
                    kept[b, kind, k].astype(f32) + got_one[b, kind, k].astype(f32)
                ).astype(bf16)
        for kind in range(2):
            stage_two(b, kind).start()

    def start_three(b):
        for kind in range(2):
            stage_two(b, kind).wait()
            kept[b, kind, 0] = (
                kept[b, kind, 0].astype(f32) + got_two[b, kind].astype(f32)
            ).astype(bf16)
        if b:
            stage_three(b).start()

    def load_rows(j):
        return pltpu.make_async_copy(gathered.at[j], rows_held.at[j], local_sems.at[8 + j])

    for b in (3, 2, 1, 0):
        for kind in range(2):
            load(b, kind).start()
    for j in range(chunks):
        load_rows(j).start()
    greet([core, near_z, across[0], across[1], peer_of(0, 2), peer_of(0, 3)])
    start_one(3)

    key_sum[...] = jnp.zeros_like(key_sum)
    value_sum[...] = jnp.zeros_like(value_sum)
    for j in range(chunks):
        for h in range(width // HEAD_DIM):
            at = width + (h // 2) * 128
            keys[h, j * rows : (j + 1) * rows, :] = head_keys(
                mixed_ref[j, :, at : at + 128], h % 2, info[1 + j], info[0]
            )
        turned[:, j * rows : (j + 1) * rows] = jnp.transpose(
            mixed_ref[j, :, width : 2 * width].astype(f32)
        ).astype(bf16)
    feature = lax.broadcasted_iota(jnp.int32, (8, width), 1) // HEAD_DIM
    picks = (feature == lax.broadcasted_iota(jnp.int32, (8, width), 0)).astype(f32)
    per_chunk = rows // part

    def attend(step, carry):
        chunk = step // per_chunk
        at = pl.ds(pl.multiple_of((step % per_chunk) * part, part), part)
        upstream = upstream_ref[chunk, at, :]
        product = upstream.astype(f32) * context_ref[chunk, at, :].astype(f32)
        delta = lax.dot_general(
            picks, product, (((1,), (1,)), ((), ())), precision=lax.Precision.HIGHEST,
            preferred_element_type=f32,
        )
        lse = lse_ref[chunk, :, at]
        for pair in range(width // 128):
            lanes = slice(pair * 128, pair * 128 + 128)
            queries = mixed_ref[chunk, at, lanes]
            value_rows = mixed_ref[:, :, 2 * width + pair * 128 : 2 * width + pair * 128 + 128]
            value_rows = value_rows.reshape(chunks * rows, 128)
            for half in range(2):
                h = pair * 2 + half
                scores = contract(keys[h], head_queries(queries, half), 1, 1)
                weight = jnp.exp(scores - lse[h : h + 1, :])
                up_half = head_half(upstream[:, lanes], half)
                back = contract(value_rows, up_half, 1, 1)
                score_grad = (weight * (back - delta[h : h + 1, :])).astype(bf16)
                value_sum[pair] += contract(weight.astype(bf16), up_half, 1, 0)
                key_sum[pair] += contract(score_grad, head_half(queries, half), 1, 0)
                query_t[h * HEAD_DIM : (h + 1) * HEAD_DIM, :] = (
                    contract(turned[h * HEAD_DIM : (h + 1) * HEAD_DIM, :], score_grad, 1, 0) * scale
                )
        grad[chunk, at, :width] = jnp.transpose(query_t[...]).astype(bf16)

        @pl.when(step == 1)
        def _():
            start_two(3)
            start_one(2)

        @pl.when(step == 4)
        def _():
            start_two(2)
            start_one(1)
            start_three(3)

        return carry

    lax.fori_loop(0, chunks * per_chunk, attend, 0)
    for j in range(chunks):
        at = slice(j * rows, (j + 1) * rows)
        for pair in range(width // 128):
            left = width + pair * 128
            grad[j, :, left : left + 128] = (key_sum[pair, at, :] * scale).astype(bf16)
            grad[j, :, left + width : left + width + 128] = value_sum[pair, at, :].astype(bf16)
    start_two(1)
    start_one(0)
    start_three(2)

    def rows_back(j):
        return contract(grad[j], weight_ref[...], 1, 1)

    core_copies = {}
    for k, j in enumerate((3, 1)):
        leaving[k] = rows_back(j).astype(bf16)
        core_copies[j] = send(leaving.at[k], landed.at[k], 19 + k, core)
        core_copies[j].start()
    far = rows_back(2)
    core_copies[3].wait()
    leaving[2] = (far + landed[0].astype(f32)).astype(bf16)
    far_copy = send(leaving.at[2], landed.at[2], 21, near_z)
    branch_ref_value = branch_ref[...] + rows_back(0)
    far_copy.start()
    core_copies[1].wait()
    own = branch_ref_value + landed[1].astype(f32)

    heads_sum[...] = jnp.zeros_like(heads_sum)
    for j in range(chunks):
        load_rows(j).wait()

    def weigh(j, carry):
        heads_sum[...] += contract(rows_held[j], grad[j], 0, 0)
        return carry

    lax.fori_loop(0, chunks, weigh, 0)
    heads_ref[...] = heads_sum[...].astype(bf16)
    start_two(0)
    start_three(1)
    far_copy.wait()
    input_ref[...] = (own + landed[2].astype(f32)).astype(bf16)
    start_three(0)
    total = kept[0, :, 0].astype(f32)
    for b in (3, 2, 1):
        stage_three(b).wait()
        total = total + got_three[b - 1].astype(f32)
    share_ref[...] = total.astype(bf16)


def back_block(info, mixed, context, upstream, lse, weight, branch, gathered, up_grads, down_grads):
    chunks, rows, width3 = mixed.shape
    width = width3 // 3
    seq = chunks * rows
    heads = width // HEAD_DIM
    lanes = up_grads.shape[-1]
    vmem, anywhere = pl.BlockSpec(memory_space=pltpu.VMEM), pl.BlockSpec(memory_space=pl.ANY)
    return pl.pallas_call(
        back_body,
        name="back_block",
        in_specs=[pl.BlockSpec(memory_space=pltpu.SMEM)] + [vmem] * 6 + [anywhere] * 3,
        out_specs=[vmem] * 3,
        out_shape=[
            jax.ShapeDtypeStruct((rows, D), bf16),
            jax.ShapeDtypeStruct((D, width3), bf16),
            jax.ShapeDtypeStruct((2, D, lanes), bf16),
        ],
        scratch_shapes=[
            pltpu.VMEM((heads, seq, 128), bf16),
            pltpu.VMEM((width, seq), bf16),
            pltpu.VMEM((width // 128, seq, 128), f32),
            pltpu.VMEM((width // 128, seq, 128), f32),
            pltpu.VMEM((width, 256), f32),
            pltpu.VMEM((chunks, rows, width3), bf16),
            pltpu.VMEM((chunks, rows, D), bf16),
            pltpu.VMEM((D, width3), f32),
            pltpu.VMEM((4, 2, 2, D, lanes), bf16),
            pltpu.VMEM((4, 2, 2, D, lanes), bf16),
            pltpu.VMEM((4, 2, D, lanes), bf16),
            pltpu.VMEM((3, 2, D, lanes), bf16),
            pltpu.VMEM((3, rows, D), bf16),
            pltpu.VMEM((3, rows, D), bf16),
            pltpu.SemaphoreType.DMA((12,)),
            pltpu.SemaphoreType.DMA((22,)),
            pltpu.SemaphoreType.DMA((22,)),
        ],
        compiler_params=pltpu.CompilerParams(
            vmem_limit_bytes=67043328, collective_id=2, has_side_effects=True
        ),
        cost_estimate=pl.CostEstimate(
            flops=40 * heads * seq * seq * HEAD_DIM, bytes_accessed=40 << 20, transcendentals=0
        ),
    )(info, mixed, context, upstream, lse, weight, branch, gathered, up_grads, down_grads)


def joined(held, i, kind):
    return jnp.concatenate([held[2 * i + k, m, kind] for k in range(2) for m in range(2)], axis=-1)


def gelu_parts(value):
    bell = jnp.exp(-0.5 * value * value)
    t = 1.0 / (1.0 + (0.3275911 * 0.5**0.5) * jnp.abs(value))
    tail = 0.5 * 1.061405429
    for c in (-1.453152027, 1.421413741, -0.284496736, 0.254829592):
        tail = tail * t + 0.5 * c
    tail = tail * t * bell
    area = jnp.where(value > 0, 1.0 - tail, tail)
    return value * area, area + value * bell * (0.5 / jnp.pi) ** 0.5


def feed_body(count, info, first_ref, cotangent_ref, norms_ref, *refs):
    pieces = refs[:count]
    out_ref, low_ref, both_ref, hidden_ref, pre_ref, grad_ref, sums_ref = refs[count : count + 7]
    held, slope, total, leaving, landed, local_sems, send_sems, recv_sems = refs[count + 7 :]
    rows = first_ref.shape[0]
    width = hidden_ref.shape[-1]
    peer = (other_core(), lax.axis_index("tensor"))
    for i in range(count):
        pltpu.make_async_copy(pieces[i], held.at[i], local_sems.at[i]).start()
    greet([peer])

    def across(source, target, k):
        return pltpu.make_async_remote_copy(
            source, target, send_sems.at[k], recv_sems.at[k], device_id=peer,
            device_id_type=pl.DeviceIdType.MESH,
        )

    half = rows // 2
    both_ref[0] = first_ref[...].astype(bf16)
    first_copy = across(both_ref.at[0], both_ref.at[1], 0)
    first_copy.start()

    def up(i, slot):
        weight = joined(held, i, 0)
        for r in range(0, rows, half):
            value = jnp.dot(both_ref[slot, r : r + half, :], weight, preferred_element_type=f32)
            hidden, steep = gelu_parts(value)
            hidden_ref[i, slot, r : r + half, :] = hidden.astype(bf16)
            slope[i, slot, r : r + half, :] = steep.astype(bf16)

    def down(i, slot):
        total[slot] += contract(hidden_ref[i, slot], joined(held, i, 1), 1, 1)

    def back(i, slot):
        weight = joined(held, i, 1)
        for r in range(0, rows, half):
            value = jnp.dot(low_ref[slot, r : r + half, :], weight, preferred_element_type=f32)
            steep = slope[i, slot, r : r + half, :].astype(f32)
            pre_ref[i, slot, r : r + half, :] = (value * steep).astype(bf16)

    def back_up(i, slot):
        total[slot] += contract(pre_ref[i, slot], joined(held, i, 0), 1, 1)

    def loop(*works):
        def body(i, carry):
            for work in works:
                work(i)
            return carry

        lax.fori_loop(0, count // 2, body, 0)

    def arrive(i):
        for k in range(2):
            pltpu.make_async_copy(
                pieces[0], held.at[2 * i + k], local_sems.at[2 * i + k]
            ).wait()

    total[...] = jnp.zeros_like(total)
    loop(arrive, lambda i: up(i, 0))
    first_copy.wait()
    loop(lambda i: up(i, 1), lambda i: down(i, 1))
    leaving[...] = total[1].astype(bf16)
    feed_copy = across(leaving, landed.at[0], 1)
    feed_copy.start()
    loop(lambda i: down(i, 0))
    feed_copy.wait()

    sums_ref[...] = jnp.zeros_like(sums_ref)
    part = 128

    def middle(r, carry):
        at = pl.ds(pl.multiple_of(r * part, part), part)
        second, normed, inverse = norm_parts(
            first_ref[at, :] + (total[0, at, :] + landed[0, at, :].astype(f32)),
            norms_ref[2:3, :], norms_ref[3:4, :],
        )
        out_ref[at, :] = second.astype(bf16)
        row = lax.broadcasted_iota(jnp.int32, (part, 1), 0) + r * part + info[1]
        seed = cotangent_ref[at, :].astype(f32) * (row < info[0]).astype(f32)
        grad = norm_back(seed, normed, inverse, norms_ref[2:3, :])
        sums_ref[0:1, :] += jnp.sum(seed * normed, axis=0, keepdims=True)
        sums_ref[1:2, :] += jnp.sum(seed, axis=0, keepdims=True)
        total[0, at, :] = grad
        low_ref[0, at, :] = grad.astype(bf16)
        return carry

    lax.fori_loop(0, rows // part, middle, 0)
    low_copy = across(low_ref.at[0], low_ref.at[1], 2)
    low_copy.start()
    total[1] = jnp.zeros_like(total[1])
    loop(lambda i: back(i, 0))
    low_copy.wait()
    loop(lambda i: back(i, 1), lambda i: back_up(i, 1))
    leaving[...] = total[1].astype(bf16)
    grad_copy = across(leaving, landed.at[1], 3)
    grad_copy.start()
    loop(lambda i: back_up(i, 0))
    grad_copy.wait()
    grad_ref[...] = total[0] + landed[1].astype(f32)


def feed_block(info, first, cotangent, norms, pieces):
    rows = first.shape[0]
    count = len(pieces)
    lanes = pieces[0].shape[-1]
    width = 4 * lanes
    vmem = pl.BlockSpec(memory_space=pltpu.VMEM)
    return pl.pallas_call(
        partial(feed_body, count),
        name="feed_block",
        in_specs=[pl.BlockSpec(memory_space=pltpu.SMEM), vmem, vmem, vmem]
        + [pl.BlockSpec(memory_space=pl.ANY)] * count,
        out_specs=[vmem] * 7,
        out_shape=[
            jax.ShapeDtypeStruct((rows, D), bf16),
            jax.ShapeDtypeStruct((2, rows, D), bf16),
            jax.ShapeDtypeStruct((2, rows, D), bf16),
            jax.ShapeDtypeStruct((count // 2, 2, rows, width), bf16),
            jax.ShapeDtypeStruct((count // 2, 2, rows, width), bf16),
            jax.ShapeDtypeStruct((rows, D), f32),
            jax.ShapeDtypeStruct((2, D), f32),
        ],
        scratch_shapes=[
            pltpu.VMEM((count,) + pieces[0].shape, bf16),
            pltpu.VMEM((count // 2, 2, rows, width), bf16),
            pltpu.VMEM((2, rows, D), f32),
            pltpu.VMEM((rows, D), bf16),
            pltpu.VMEM((2, rows, D), bf16),
            pltpu.SemaphoreType.DMA((count,)),
            pltpu.SemaphoreType.DMA((4,)),
            pltpu.SemaphoreType.DMA((4,)),
        ],
        compiler_params=pltpu.CompilerParams(
            vmem_limit_bytes=60 << 20, collective_id=1, has_side_effects=True
        ),
        cost_estimate=pl.CostEstimate(
            flops=8 * rows * D * width * count, bytes_accessed=30 << 20, transcendentals=0
        ),
    )(info, first, cotangent, norms, *pieces)


def feed_grads_body(first_ref, low_ref, hidden_ref, pre_ref, up_ref, down_ref, first_t, low_t):
    rows = first_ref.shape[1]

    @pl.when(pl.program_id(0) == 0)
    def _():
        for slot in range(2):
            at = slice(slot * rows, (slot + 1) * rows)
            first_t[:, at] = jnp.transpose(first_ref[slot].astype(f32)).astype(bf16)
            low_t[:, at] = jnp.transpose(low_ref[slot].astype(f32)).astype(bf16)

    lanes = up_ref.shape[-1]
    width = pre_ref.shape[-1]
    for target, source, turned in ((up_ref, pre_ref, first_t), (down_ref, hidden_ref, low_t)):
        grad = jnp.dot(
            turned[...], source[0].reshape(2 * rows, width), preferred_element_type=f32
        ).astype(bf16)
        for k in range(2):
            for m in range(2):
                at = (2 * k + m) * lanes
                if target is up_ref:
                    target[m, k, 0] = grad[:, at : at + lanes]
                else:
                    target[m, 0, k] = grad[:, at : at + lanes]


def feed_grads(first, low, hidden, pre):
    count, _, rows, width = hidden.shape
    full = pl.BlockSpec((2, rows, D), lambda i: (0, 0, 0))
    piece = pl.BlockSpec((1, 2, rows, width), lambda i: (i, 0, 0, 0))
    lanes = width // 4
    return pl.pallas_call(
        feed_grads_body,
        grid=(count,),
        name="feed_grads",
        in_specs=[full, full, piece, piece],
        out_specs=[
            pl.BlockSpec((2, 2, 1, D, lanes), lambda i: (i // 2, 0, i % 2, 0, 0)),
            pl.BlockSpec((2, 1, 2, D, lanes), lambda i: (i // 2, i % 2, 0, 0, 0)),
        ],
        out_shape=[jax.ShapeDtypeStruct((count, 2, 2, D, lanes), bf16)] * 2,
        scratch_shapes=[pltpu.VMEM((D, 2 * rows), bf16), pltpu.VMEM((D, 2 * rows), bf16)],
        compiler_params=pltpu.CompilerParams(vmem_limit_bytes=48 << 20),
        cost_estimate=pl.CostEstimate(
            flops=8 * rows * D * width * count, bytes_accessed=20 << 20, transcendentals=0
        ),
    )(first, low, hidden, pre)


def layer(n_dp, n_tensor, tokens, weights, norms, cotangent, lengths, owners, master, moment_one,
          moment_two, norm_master, norm_one, norm_two):
    tile = D // n_tensor
    hidden_width = FF // n_tensor
    rows = tokens.shape[0]
    lanes = hidden_width // SHARE
    device = lax.axis_index("dp")
    z = lax.axis_index("tensor")
    core = device % 2
    matched = core == z // 2
    quarter = jnp.where(matched, z, z ^ 2)

    def flip(x, dd, dz):
        pairs = [
            (d * n_tensor + t, (d ^ dd) * n_tensor + (t ^ dz))
            for d in range(n_dp)
            for t in range(n_tensor)
        ]
        return lax.ppermute(x, AXES, pairs)

    def some(x, dd, dz, want):
        pairs = [
            (d * n_tensor + t, (d ^ dd) * n_tensor + (t ^ dz))
            for d in range(n_dp)
            for t in range(n_tensor)
            if (t // 2 == d % 2) == want
        ]
        return lax.ppermute(x, AXES, pairs)

    def swap(x):
        return jnp.where(matched, x, some(x, 1, 2, False))

    w_mixed = weights[:, : 3 * tile]
    w_out = weights[:, 3 * tile : 4 * tile]
    share_rows = D // n_dp
    length = jnp.where(matched, lengths, flip(lengths, 1, 0))[0]
    base = jnp.stack([quarter ^ k for k in (0, 2, 1, 3)]) * rows
    info = jnp.concatenate([length[None], base]).astype(jnp.int32)

    inputs = tokens[:, 0, :]
    own = swap(inputs)
    far = some(inputs, 0, 1, True) + some(own, 0, 1, False)
    near = flip(own, 1, 0)
    gathered = jnp.stack([own, near, far, flip(far, 1, 0)])

    def my_rows(x):
        return lax.dynamic_slice_in_dim(x, device * share_rows, share_rows, 0)

    other = lax.all_gather(flip(my_rows(w_mixed), 0, 2), "dp", axis=0, tiled=True)
    w_heads = jnp.where(matched, w_mixed, other)
    out_own = my_rows(w_out)
    out_two = jnp.concatenate([out_own, flip(out_own, 0, 1)], axis=1)
    out_four = jnp.concatenate([out_two, flip(out_two, 0, 2)], axis=1)
    w_out_all = lax.all_gather(out_four, "dp", axis=0, tiled=True)

    at = (device % SHARE) * lanes + 4 * tile
    own_piece = jnp.stack(
        [
            lax.dynamic_slice(weights, (0, at), (D, lanes)),
            lax.dynamic_slice(weights, (0, at + hidden_width), (D, lanes)),
        ]
    )
    near_pieces = jnp.stack([own_piece, flip(own_piece, 0, 1)])
    far_pieces = flip(near_pieces, 0, 2)

    def spread(first_pieces, one, two):
        a = first_pieces
        b = flip(a, one, 0)
        return [a, b, flip(a, two, 0), flip(b, two, 0)]

    near_four = spread(near_pieces, 2, 4)
    far_four = spread(far_pieces, 4, 2)
    pieces = near_four + [far_four[k] for k in (0, 2, 1, 3)]

    mixed = jnp.einsum(
        "csd,de->cse", gathered, w_heads, preferred_element_type=f32
    ).astype(bf16)
    context, lse = attention_forward(info, mixed)

    parts = [context[0], flip(context[1], 1, 0), flip(context[2], 0, 1), flip(context[3], 1, 1)]
    context_all = jnp.where(
        matched,
        jnp.concatenate([parts[k] for k in (0, 2, 1, 3)], axis=1),
        jnp.concatenate([parts[k] for k in (1, 3, 0, 2)], axis=1),
    )
    branch = contract(context_all, w_out_all, 1, 1)
    first, first_normed, first_inverse = norm_parts(
        own.astype(f32) + branch, norms[0], norms[1]
    )
    seed = swap(cotangent[:, 0, :])
    outputs, both_low, both_first, hidden, pre_grad, first_grad, sums_two = feed_block(
        info, first, seed, norms, pieces
    )
    branch_grad = norm_back(first_grad, first_normed, first_inverse, norms[0])
    gain_one = jnp.sum(first_grad * first_normed, axis=0)
    shift_one = jnp.sum(first_grad, axis=0)
    branch_low = branch_grad.astype(bf16)
    context_grad = jnp.dot(branch_low, w_out_all, preferred_element_type=f32).astype(bf16)
    blocks = [context_grad[:, k * tile : (k + 1) * tile] for k in range(4)]
    blocks = [
        jnp.where(matched, blocks[a], blocks[b]) for a, b in ((0, 2), (2, 0), (1, 3), (3, 1))
    ]
    upstream = jnp.stack(
        [blocks[0], flip(blocks[1], 1, 0), flip(blocks[2], 0, 1), flip(blocks[3], 1, 1)]
    )

    def add(a, b):
        return (a.astype(f32) + b.astype(f32)).astype(bf16)

    up_grads, down_grads = feed_grads(both_first, both_low, hidden, pre_grad)
    out_grad = contract(branch_low, context_all, 0, 0).astype(bf16)
    out_share = lax.psum_scatter(out_grad, "dp", scatter_dimension=0, tiled=True)
    out_share = add(out_share[:, : 2 * tile], flip(out_share[:, 2 * tile :], 0, 2))
    out_share = add(out_share[:, :tile], flip(out_share[:, tile:], 0, 1))

    norm_grads = jnp.concatenate([jnp.stack([gain_one, shift_one]), sums_two])
    for dd, dz in [(1 << k, 0) for k in range(n_dp.bit_length() - 1)] + [(0, 1), (0, 2)]:
        norm_grads = norm_grads + flip(norm_grads, dd, dz)

    input_total, heads_grad, feed_share = back_block(
        info, mixed, context, upstream, lse, w_heads, branch_grad, gathered, up_grads, down_grads
    )
    input_grad = swap(input_total)[:, None, :]
    bit = SHARE
    while bit < n_dp:
        feed_share = add(feed_share, flip(feed_share, bit, 0))
        bit *= 2

    zero = jnp.zeros_like(heads_grad)
    both = jnp.concatenate(
        [jnp.where(matched, heads_grad, zero), jnp.where(matched, zero, heads_grad)], axis=1
    )
    heads_share = lax.psum_scatter(both, "dp", scatter_dimension=0, tiled=True)
    heads_share = add(heads_share[:, : 3 * tile], flip(heads_share[:, 3 * tile :], 0, 2))

    feed_grad = lax.all_gather(feed_share, "dp", axis=0, tiled=False)[:SHARE]
    attention_grad = lax.all_gather(
        jnp.concatenate([heads_share, out_share], axis=1), "dp", axis=0, tiled=True
    )
    tile_owner, slot_index = slot_table(owners)
    capacity = FF // D
    slot_ids = jnp.arange(capacity, dtype=jnp.int32)
    owned = (tile_owner[None, :] == device) & (slot_index[None, :] == slot_ids[:, None])
    occupied = jnp.sum(owned.astype(f32), axis=1)
    tile_ids = jnp.sum(owned.astype(jnp.int32) * jnp.arange(owned.shape[1], dtype=jnp.int32), axis=1)
    attention_slots = jnp.concatenate(
        [
            lax.dynamic_slice(
                attention_grad, (0, jnp.minimum(tile_ids[s], 3) * tile), (D, tile)
            )
            for s in range(capacity)
        ],
        axis=1,
    )
    feed_flat = [jnp.concatenate([feed_grad[k, m] for k in range(SHARE)], axis=1) for m in range(2)]
    occupied_columns = jnp.repeat(occupied, tile)[None, :]
    slot_grad = (
        jnp.where(
            owners[4] == device,
            feed_flat[0],
            jnp.where(owners[5] == device, feed_flat[1], attention_slots),
        ).astype(f32)
        * occupied_columns
    )
    new_master, new_one, new_two = adam_update(
        slot_grad, master[0], moment_one[0], moment_two[0], occupied_columns, weight_decay
    )
    returned = lax.all_to_all(
        new_master.astype(bf16).reshape(n_dp, share_rows, capacity * tile),
        "dp", split_axis=0, concat_axis=0, tiled=True,
    )
    row_shard = jnp.concatenate(
        [
            lax.dynamic_slice(
                returned, (tile_owner[i], 0, slot_index[i] * tile), (1, share_rows, tile)
            )[0]
            for i in range(tile_owner.shape[0])
        ],
        axis=1,
    )
    new_weights = lax.all_gather(row_shard, "dp", axis=0, tiled=True)
    norm_owner = (device == owners[6]).astype(f32)
    new_norm_master, new_norm_one, new_norm_two = adam_update(
        norm_grads, norm_master[0], norm_one[0], norm_two[0], norm_owner, 0.0
    )
    return (
        swap(outputs)[:, None, :],
        input_grad,
        slot_grad[None],
        new_master[None],
        new_one[None],
        new_two[None],
        new_weights,
        norm_grads,
        new_norm_master[None],
        new_norm_one[None],
        new_norm_two[None],
    )


def solution(mesh):
    in_specs = (
        P("tensor", "dp", None),
        P(None, "tensor"),
        P(),
        P("tensor", "dp", None),
        P("dp"),
        P(),
        P("dp", None, "tensor"),
        P("dp", None, "tensor"),
        P("dp", None, "tensor"),
        P("dp", None, None),
        P("dp", None, None),
        P("dp", None, None),
    )
    out_specs = (
        P("tensor", "dp", None),
        P("tensor", "dp", None),
        P("dp", None, "tensor"),
        P("dp", None, "tensor"),
        P("dp", None, "tensor"),
        P("dp", None, "tensor"),
        P(None, "tensor"),
        P(),
        P("dp", None, None),
        P("dp", None, None),
        P("dp", None, None),
    )
    return jax.shard_map(
        partial(layer, mesh.shape["dp"], mesh.shape["tensor"]),
        mesh=mesh,
        in_specs=in_specs,
        out_specs=out_specs,
        check_vma=False,
    )
```

```python
from functools import partial

import jax
import jax.numpy as jnp
from jax import lax
from jax.experimental import pallas as pl
from jax.experimental.pallas import tpu as pltpu
from jax.sharding import PartitionSpec as P

D = 1024
FF = 4096
ADAM_STEP = 10
HEAD_DIM = 64
SHARE = 8


f32, bf16 = jnp.float32, jnp.bfloat16
beta_one = 0.9
beta_two = 0.999
learn_rate = 0.02
weight_decay = 0.1
adam_eps = 1e-08
norm_eps = 1e-05
masked_score = -1e30
AXES = ("dp", "tensor")


def contract(a, b, ca, cb):
    return lax.dot_general(a, b, (((ca,), (cb,)), ((), ())), preferred_element_type=f32)


def norm_parts(value, gain, shift):
    average = jnp.mean(value, axis=-1, keepdims=True)
    centred = value - average
    variance = jnp.mean(centred * centred, axis=-1, keepdims=True)
    inverse = lax.rsqrt(variance + norm_eps)
    normed = centred * inverse
    return normed * gain + shift, normed, inverse


def norm_back(upstream, normed, inverse, gain):
    scaled = upstream * gain
    inner = (
        scaled
        - jnp.mean(scaled, axis=-1, keepdims=True)
        - normed * jnp.mean(scaled * normed, axis=-1, keepdims=True)
    )
    return inner * inverse


def slot_table(owners):
    repeat = FF // D
    tile_matrix = jnp.array([0, 1, 2, 3] + [4] * repeat + [5] * repeat, dtype=jnp.int32)
    choose = (tile_matrix[:, None] == jnp.arange(7, dtype=jnp.int32)[None, :]).astype(jnp.int32)
    tile_owner = jnp.sum(choose * owners[None, :], axis=1)
    position = jnp.arange(tile_matrix.shape[0], dtype=jnp.int32)
    before = (tile_owner[None, :] == tile_owner[:, None]) & (position[None, :] < position[:, None])
    slot_index = jnp.sum(before.astype(jnp.int32), axis=1)
    return (tile_owner, slot_index)


def adam_update(grad, param, first, second, occupied, decay_rate):
    first_new = occupied * (beta_one * first + (1.0 - beta_one) * grad)
    second_new = occupied * (beta_two * second + (1.0 - beta_two) * grad * grad)
    correct_one = 1.0 - beta_one**ADAM_STEP
    correct_two = 1.0 - beta_two**ADAM_STEP
    direction = first_new / correct_one / (jnp.sqrt(second_new / correct_two) + adam_eps)
    param_new = occupied * (param - learn_rate * (direction + decay_rate * param))
    return (param_new, first_new, second_new)


def head_keys(keys, half, start, length):
    lane = lax.broadcasted_iota(jnp.int32, keys.shape, 1)
    row = lax.broadcasted_iota(jnp.int32, keys.shape, 0)
    bias = jnp.where(start + row < length, 0.0, masked_score).astype(f32)
    extra = jnp.where(lane == (1 - half) * HEAD_DIM, bias, 0.0)
    return jnp.where(lane // HEAD_DIM == half, keys.astype(f32), extra).astype(bf16)


def head_half(rows, half):
    lane = lax.broadcasted_iota(jnp.int32, rows.shape, 1)
    return jnp.where(lane // HEAD_DIM == half, rows, jnp.zeros_like(rows))


def head_queries(rows, half):
    lane = lax.broadcasted_iota(jnp.int32, rows.shape, 1)
    scaled = rows.astype(f32) * HEAD_DIM ** (-0.5)
    extra = jnp.where(lane == (1 - half) * HEAD_DIM, 1.0, 0.0)
    return jnp.where(lane // HEAD_DIM == half, scaled, extra).astype(bf16)


def attention_forward_body(info, mixed_ref, context_ref, lse_ref, keys, values):
    step = pl.program_id(0)
    chunks, rows, _ = mixed_ref.shape
    width = context_ref.shape[-1]

    @pl.when(step == 0)
    def _():
        for j in range(chunks):
            for h in range(width // HEAD_DIM):
                at = width + (h // 2) * 128
                keys[h, j * rows : (j + 1) * rows, :] = head_keys(
                    mixed_ref[j, :, at : at + 128], h % 2, info[1 + j], info[0]
                )
            values[j * rows : (j + 1) * rows, :] = mixed_ref[j, :, 2 * width :]

    lane = lax.broadcasted_iota(jnp.int32, (rows, 128), 1)
    logs = jnp.zeros((rows, 128), f32)
    for pair in range(width // 128):
        queries = mixed_ref[step, :, pair * 128 : pair * 128 + 128]
        both = []
        for half in range(2):
            h = pair * 2 + half
            scores = contract(head_queries(queries, half), keys[h], 1, 1)
            top = jnp.max(scores, axis=1, keepdims=True)
            weight = jnp.exp(scores - top)
            total = jnp.sum(weight, axis=1, keepdims=True)
            out = contract(weight.astype(bf16), values[:, pair * 128 : pair * 128 + 128], 1, 0)
            both.append(out / total)
            logs = jnp.where(lane == h, top + jnp.log(total), logs)
        context_ref[0, :, pair * 128 : pair * 128 + 128] = jnp.where(
            lane < HEAD_DIM, both[0], both[1]
        ).astype(bf16)
    lse_ref[0] = jnp.transpose(logs)[:8, :]


def attention_forward(info, mixed):
    chunks, rows, width3 = mixed.shape
    width = width3 // 3
    seq = chunks * rows
    heads = width // HEAD_DIM
    return pl.pallas_call(
        attention_forward_body,
        grid=(chunks,),
        name="attention_forward",
        in_specs=[
            pl.BlockSpec(memory_space=pltpu.SMEM),
            pl.BlockSpec((chunks, rows, width3), lambda i: (0, 0, 0)),
        ],
        out_specs=[
            pl.BlockSpec((1, rows, width), lambda i: (i, 0, 0)),
            pl.BlockSpec((1, 8, rows), lambda i: (i, 0, 0)),
        ],
        out_shape=[
            jax.ShapeDtypeStruct((chunks, rows, width), bf16),
            jax.ShapeDtypeStruct((chunks, 8, rows), f32),
        ],
        scratch_shapes=[pltpu.VMEM((heads, seq, 128), bf16), pltpu.VMEM((seq, width), bf16)],
        compiler_params=pltpu.CompilerParams(vmem_limit_bytes=48 << 20),
        cost_estimate=pl.CostEstimate(
            flops=16 * heads * seq * seq * HEAD_DIM, bytes_accessed=8 << 20, transcendentals=0
        ),
    )(info, mixed)


def other_core():
    device = lax.axis_index("dp")
    return device + 1 - 2 * (device % 2)


def peer_of(bit, turn):
    device, z = lax.axis_index("dp"), lax.axis_index("tensor")
    if bit:
        device = device + bit - 2 * bit * ((device // bit) % 2)
    if turn == 1:
        z = z + 1 - 2 * (z % 2)
    elif turn == 2:
        z = z + 2 - 4 * (z // 2)
    elif turn == 3:
        z = 3 - z
    return (device, z)


def greet(peers):
    barrier = pltpu.get_barrier_semaphore()
    for peer in peers:
        pl.semaphore_signal(barrier, inc=1, device_id=peer, device_id_type=pl.DeviceIdType.MESH)
    pl.semaphore_wait(barrier, len(peers))


def sender(send_sems, recv_sems):
    def send(source, target, k, peer):
        return pltpu.make_async_remote_copy(
            source, target, send_sems.at[k], recv_sems.at[k], device_id=peer,
            device_id_type=pl.DeviceIdType.MESH,
        )

    return send


def bits():
    device = lax.axis_index("dp")
    return (device // 4) % 2, (device // 2) % 2, device % 2


def block_of(y, x, c):
    return 4 * y + 2 * x + c


def row_block(index, count=1):
    rows = D // SHARE
    return pl.ds(pl.multiple_of(index * rows, rows), count * rows)


class Gather:
    def __init__(self, send, view, first_sem, x_first):
        self.send, self.view, self.sem = send, view, first_sem
        self.y, self.x, self.c = bits()
        self.one, self.two = (2, 4) if x_first else (4, 2)

    def block(self, turn):
        y, x, c = self.y, self.x, self.c
        y = 1 - y if turn & 4 else y
        x = 1 - x if turn & 2 else x
        c = 1 - c if turn & 1 else c
        return block_of(y, x, c)

    def copy(self, turn, over, k):
        place = self.view(self.block(turn))
        return self.send(place, place, self.sem + k, peer_of(over, 0))

    def start(self):
        self.copy(0, self.one, 0).start()
        self.copy(0, self.two, 1).start()
        self.copy(0, 1, 3).start()

    def relay(self):
        self.copy(0, self.one, 0).wait()
        self.copy(self.one, self.two, 2).start()
        self.copy(self.one, 1, 4).start()
        self.copy(0, self.two, 1).wait()
        self.copy(self.two, 1, 5).start()

    def last(self):
        self.copy(self.one, self.two, 2).wait()
        self.copy(6, 1, 6).start()

    def finish(self):
        for turn, k in ((0, 3), (self.one, 4), (self.two, 5), (6, 6)):
            self.copy(turn, 1, k).wait()


GATHER_SEMS = 7


class RowSums:
    def __init__(self, send, ref, place, height, got_one, got_two, first_sem):
        self.send, self.ref, self.place, self.height = send, ref, place, height
        self.got_one, self.got_two, self.sem = got_one, got_two, first_sem
        self.y, self.x, _ = bits()
        self.half = ref.shape[-1] // 2

    def at(self, y, x, side):
        rows = pl.ds(pl.multiple_of(self.place(y, x), 128), self.height)
        return (rows, slice(side * self.half, (side + 1) * self.half))

    def pairs(self, k, mine):
        y, x = self.y, self.x
        return [
            (y if mine else 1 - y, k, 0),
            (k, x if mine else 1 - x, 1),
        ]

    def first(self, k, side):
        y, x, _ = self.pairs(k, False)[side]
        return self.send(
            self.ref.at[self.at(y, x, side)], self.got_one.at[side, k], self.sem + 2 * side + k,
            peer_of((4, 2)[side], 0),
        )

    def second(self, side):
        y, x = ((self.y, 1 - self.x), (1 - self.y, self.x))[side]
        return self.send(
            self.ref.at[self.at(y, x, side)], self.got_two.at[side], self.sem + 4 + side,
            peer_of((2, 4)[side], 0),
        )

    def start(self):
        for side in range(2):
            for k in range(2):
                self.first(k, side).start()

    def relay(self):
        for side in range(2):
            for k in range(2):
                self.first(k, side).wait()
        for side in range(2):
            for k in range(2):
                y, x, _ = self.pairs(k, True)[side]
                at = self.at(y, x, side)
                self.ref[at] = (
                    self.ref[at].astype(f32) + self.got_one[side, k].astype(f32)
                ).astype(bf16)
        for side in range(2):
            self.second(side).start()

    def finish(self):
        for side in range(2):
            self.second(side).wait()
            at = self.at(self.y, self.x, side)
            self.ref[at] = (
                self.ref[at].astype(f32) + self.got_two[side].astype(f32)
            ).astype(bf16)


ROW_SEMS = 6


def back_body(
    info, mixed_ref, context_ref, upstream_ref, lse_ref, weight_ref, branch_ref, norm_ref, gathered, up_grads, down_grads,
    out_grads,
    input_ref, norm_out, attention_out, feed_out,
    keys, turned, key_sum, value_sum, query_t, grad, rows_held, heads_sum, kept, got_one, got_two, got_three,
    leaving, landed, share, heads, heads_one, heads_two, heads_mine, heads_far, out_held, out_core, out_one, out_two, out_z,
    attention_all, norm_here, norm_there, local_sems, send_sems, recv_sems,
):
    chunks, rows, _ = mixed_ref.shape
    width = context_ref.shape[-1]
    scale = HEAD_DIM ** (-0.5)
    part = 256
    core, near_z = peer_of(1, 0), peer_of(0, 1)
    across = (peer_of(2, 0), peer_of(4, 0))
    send = sender(send_sems, recv_sems)
    sources = (up_grads, down_grads)
    y, x, c = bits()
    z = lax.axis_index("tensor")
    matched = c == z // 2
    own_block = block_of(y, x, c)

    def stage_one(b, kind):
        return send(sources[kind].at[b, 1], got_one.at[b, kind], 2 * b + kind, across[kind])

    def stage_two(b, kind):
        return send(kept.at[b, kind, 1], got_two.at[b, kind], 8 + 2 * b + kind, across[1 - kind])

    def stage_three(b):
        return send(kept.at[b, :, 0], got_three.at[b - 1], 15 + b, peer_of(0, b))

    def load(b, kind):
        return pltpu.make_async_copy(
            sources[kind].at[b, 0], kept.at[b, kind], local_sems.at[2 * b + kind]
        )

    def start_one(b):
        for kind in range(2):
            stage_one(b, kind).start()

    def start_two(b):
        for kind in range(2):
            load(b, kind).wait()
            stage_one(b, kind).wait()
            for k in (1, 0):
                kept[b, kind, k] = (
                    kept[b, kind, k].astype(f32) + got_one[b, kind, k].astype(f32)
                ).astype(bf16)
        for kind in range(2):
            stage_two(b, kind).start()

    def start_three(b):
        for kind in range(2):
            stage_two(b, kind).wait()
            kept[b, kind, 0] = (
                kept[b, kind, 0].astype(f32) + got_two[b, kind].astype(f32)
            ).astype(bf16)
        if b:
            stage_three(b).start()

    def load_rows(j):
        return pltpu.make_async_copy(gathered.at[j], rows_held.at[j], local_sems.at[8 + j])

    def out_load():
        return pltpu.make_async_copy(out_grads, out_held, local_sems.at[12])

    def out_core_copy(k):
        at = row_block(block_of(k // 2, k % 2, 1 - c))
        return send(out_grads.at[at, :], out_core.at[k], 22 + k, core)

    out_sums = RowSums(
        send, out_held, lambda yy, xx: block_of(yy, xx, c) * 128, 128, out_one, out_two, 26
    )

    def out_z_copy(e):
        at = (row_block(own_block), slice(e * width, (e + 1) * width))
        return send(out_held.at[at], out_z.at[e - 1], 31 + e, peer_of(0, e))

    def out_start():
        out_load().wait()
        for k in range(4):
            out_core_copy(k).wait()
        for k in range(4):
            at = row_block(block_of(k // 2, k % 2, c))
            out_held[at, :] = (out_held[at, :].astype(f32) + out_core[k].astype(f32)).astype(bf16)
        out_sums.start()

    def out_last():
        out_sums.finish()
        for e in (1, 2, 3):
            out_z_copy(e).start()

    norm_turns = ((1, 0), (2, 0), (4, 0), (0, 1), (0, 2))

    def norm_copy(k):
        return send(norm_here.at[k], norm_there.at[k], 35 + k, peer_of(*norm_turns[k]))

    def norm_step(k):
        norm_copy(k).wait()
        total = norm_here[k] + norm_there[k]
        if k + 1 < len(norm_turns):
            norm_here[k + 1] = total
            norm_copy(k + 1).start()
        else:
            norm_out[...] = total

    for b in (3, 2, 1, 0):
        for kind in range(2):
            load(b, kind).start()
    for j in range(chunks):
        load_rows(j).start()
    out_load().start()
    norm_here[0] = norm_ref[...]
    greet([core, near_z, across[0], across[1], peer_of(0, 2), peer_of(0, 3), peer_of(1, 2)])
    for k in range(4):
        out_core_copy(k).start()
    norm_copy(0).start()
    start_one(3)

    key_sum[...] = jnp.zeros_like(key_sum)
    value_sum[...] = jnp.zeros_like(value_sum)
    for j in range(chunks):
        for h in range(width // HEAD_DIM):
            at = width + (h // 2) * 128
            keys[h, j * rows : (j + 1) * rows, :] = head_keys(
                mixed_ref[j, :, at : at + 128], h % 2, info[1 + j], info[0]
            )
        turned[:, j * rows : (j + 1) * rows] = jnp.transpose(
            mixed_ref[j, :, width : 2 * width].astype(f32)
        ).astype(bf16)
    feature = lax.broadcasted_iota(jnp.int32, (8, width), 1) // HEAD_DIM
    picks = (feature == lax.broadcasted_iota(jnp.int32, (8, width), 0)).astype(f32)
    per_chunk = rows // part

    def attend(step, carry):
        chunk = step // per_chunk
        at = pl.ds(pl.multiple_of((step % per_chunk) * part, part), part)
        upstream = upstream_ref[chunk, at, :]
        product = upstream.astype(f32) * context_ref[chunk, at, :].astype(f32)
        delta = lax.dot_general(
            picks, product, (((1,), (1,)), ((), ())), precision=lax.Precision.HIGHEST,
            preferred_element_type=f32,
        )
        lse = lse_ref[chunk, :, at]
        for pair in range(width // 128):
            lanes = slice(pair * 128, pair * 128 + 128)
            queries = mixed_ref[chunk, at, lanes]
            value_rows = mixed_ref[:, :, 2 * width + pair * 128 : 2 * width + pair * 128 + 128]
            value_rows = value_rows.reshape(chunks * rows, 128)
            for half in range(2):
                h = pair * 2 + half
                scores = contract(keys[h], head_queries(queries, half), 1, 1)
                weight = jnp.exp(scores - lse[h : h + 1, :])
                up_half = head_half(upstream[:, lanes], half)
                back = contract(value_rows, up_half, 1, 1)
                score_grad = (weight * (back - delta[h : h + 1, :])).astype(bf16)
                value_sum[pair] += contract(weight.astype(bf16), up_half, 1, 0)
                key_sum[pair] += contract(score_grad, head_half(queries, half), 1, 0)
                query_t[h * HEAD_DIM : (h + 1) * HEAD_DIM, :] = (
                    contract(turned[h * HEAD_DIM : (h + 1) * HEAD_DIM, :], score_grad, 1, 0) * scale
                )
        grad[chunk, at, :width] = jnp.transpose(query_t[...]).astype(bf16)

        @pl.when(step == 0)
        def _():
            norm_step(0)
            out_start()

        @pl.when(step == 1)
        def _():
            norm_step(1)
            start_two(3)
            start_one(2)

        @pl.when(step == 2)
        def _():
            norm_step(2)
            out_sums.relay()

        @pl.when(step == 3)
        def _():
            norm_step(3)
            out_last()

        @pl.when(step == 4)
        def _():
            norm_step(4)
            start_two(2)
            start_one(1)
            start_three(3)

        return carry

    lax.fori_loop(0, chunks * per_chunk, attend, 0)
    for j in range(chunks):
        at = slice(j * rows, (j + 1) * rows)
        for pair in range(width // 128):
            left = width + pair * 128
            grad[j, :, left : left + 128] = (key_sum[pair, at, :] * scale).astype(bf16)
            grad[j, :, left + width : left + width + 128] = value_sum[pair, at, :].astype(bf16)
    start_two(1)
    start_one(0)
    start_three(2)

    def rows_back(j):
        return contract(grad[j], weight_ref[...], 1, 1)

    core_copies = {}
    for k, j in enumerate((3, 1)):
        leaving[k] = rows_back(j).astype(bf16)
        core_copies[j] = send(leaving.at[k], landed.at[k], 19 + k, core)
        core_copies[j].start()
    far = rows_back(2)
    core_copies[3].wait()
    leaving[2] = (far + landed[0].astype(f32)).astype(bf16)
    far_copy = send(leaving.at[2], landed.at[2], 21, near_z)
    branch_ref_value = branch_ref[...] + rows_back(0)
    far_copy.start()
    core_copies[1].wait()
    own_rows = branch_ref_value + landed[1].astype(f32)

    heads_sum[...] = jnp.zeros_like(heads_sum)
    for j in range(chunks):
        load_rows(j).wait()

    def weigh(j, carry):
        heads_sum[...] += contract(rows_held[j], grad[j], 0, 0)
        return carry

    lax.fori_loop(0, chunks, weigh, 0)
    heads[...] = heads_sum[...].astype(bf16)
    start_two(0)
    head_sums = RowSums(
        send, heads, lambda yy, xx: block_of(yy, xx, 0) * 128, 256, heads_one, heads_two, 40
    )
    head_sums.start()
    start_three(1)
    far_copy.wait()
    input_ref[...] = (own_rows + landed[2].astype(f32)).astype(bf16)
    start_three(0)
    head_sums.relay()
    total = kept[0, :, 0].astype(f32)
    for b in (3, 2, 1):
        stage_three(b).wait()
        total = total + got_three[b - 1].astype(f32)
    share[...] = total.astype(bf16)
    own_feed = [
        pltpu.make_async_copy(share.at[kind], feed_out.at[own_block, kind], local_sems.at[13 + kind])
        for kind in range(2)
    ]
    for copy in own_feed:
        copy.start()
    head_sums.finish()

    def half_rows(k):
        return row_block(block_of(y, x, k))

    @pl.when(matched)
    def _():
        send(heads.at[half_rows(1 - c), :], heads_mine, 46, core).start()

    @pl.when(jnp.logical_not(matched))
    def _():
        send(heads.at[half_rows(c), :], heads_far, 47, peer_of(0, 2)).start()
        send(heads.at[half_rows(1 - c), :], heads_far, 48, peer_of(1, 2)).start()

    feeds = [
        Gather(send, lambda k, kind=kind: feed_out.at[k, kind], 49 + kind * GATHER_SEMS, kind == 0)
        for kind in range(2)
    ]
    for copy in own_feed:
        copy.wait()
    for feed in feeds:
        feed.start()
    sum_out = out_held[row_block(own_block), :width].astype(f32)
    for e in (1, 2, 3):
        out_z_copy(e).wait()
        sum_out = sum_out + out_z[e - 1].astype(f32)
    attention_all[row_block(own_block), 3 * width :] = sum_out.astype(bf16)

    @pl.when(matched)
    def _():
        send(heads.at[half_rows(1 - c), :], heads_mine, 46, core).wait_send()
        heads_mine[...] = heads[half_rows(c), :]

    @pl.when(jnp.logical_not(matched))
    def _():
        send(heads.at[half_rows(c), :], heads_far, 47, peer_of(0, 2)).wait_send()
        send(heads.at[half_rows(1 - c), :], heads_far, 48, peer_of(1, 2)).wait_send()
        send(heads.at[half_rows(c), :], heads_mine, 46, core).wait_recv()

    @pl.when(matched)
    def _():
        send(heads.at[half_rows(c), :], heads_far, 47, peer_of(0, 2)).wait_recv()

    @pl.when(jnp.logical_not(matched))
    def _():
        send(heads.at[half_rows(c), :], heads_far, 48, peer_of(1, 2)).wait_recv()

    attention_all[row_block(own_block), : 3 * width] = (
        heads_mine[...].astype(f32) + heads_far[...].astype(f32)
    ).astype(bf16)
    sides = [
        Gather(
            send,
            lambda k, side=side: attention_all.at[row_block(k), side * 2 * width : (side + 1) * 2 * width],
            49 + (2 + side) * GATHER_SEMS, side == 0,
        )
        for side in range(2)
    ]
    for side in sides:
        side.start()
    for gather in feeds + sides:
        gather.relay()
    for gather in feeds + sides:
        gather.last()
    for gather in feeds + sides:
        gather.finish()
    attention_out[...] = attention_all[...]


def back_block(info, mixed, context, upstream, lse, weight, branch, norm_sums, gathered, up_grads, down_grads, out_grads):
    chunks, rows, width3 = mixed.shape
    width = width3 // 3
    seq = chunks * rows
    heads = width // HEAD_DIM
    lanes = up_grads.shape[-1]
    share_rows = D // SHARE
    sems = 49 + 4 * GATHER_SEMS
    vmem, anywhere = pl.BlockSpec(memory_space=pltpu.VMEM), pl.BlockSpec(memory_space=pl.ANY)
    return pl.pallas_call(
        back_body,
        name="back_block",
        in_specs=[pl.BlockSpec(memory_space=pltpu.SMEM)] + [vmem] * 7 + [anywhere] * 4,
        out_specs=[vmem, vmem, vmem, anywhere],
        out_shape=[
            jax.ShapeDtypeStruct((rows, D), bf16),
            jax.ShapeDtypeStruct((4, D), f32),
            jax.ShapeDtypeStruct((D, 4 * width), bf16),
            jax.ShapeDtypeStruct((SHARE, 2, D, lanes), bf16),
        ],
        scratch_shapes=[
            pltpu.VMEM((heads, seq, 128), bf16),
            pltpu.VMEM((width, seq), bf16),
            pltpu.VMEM((width // 128, seq, 128), f32),
            pltpu.VMEM((width // 128, seq, 128), f32),
            pltpu.VMEM((width, 256), f32),
            pltpu.VMEM((chunks, rows, width3), bf16),
            pltpu.VMEM((chunks, rows, D), bf16),
            pltpu.VMEM((D, width3), f32),
            pltpu.VMEM((4, 2, 2, D, lanes), bf16),
            pltpu.VMEM((4, 2, 2, D, lanes), bf16),
            pltpu.VMEM((4, 2, D, lanes), bf16),
            pltpu.VMEM((3, 2, D, lanes), bf16),
            pltpu.VMEM((3, rows, D), bf16),
            pltpu.VMEM((3, rows, D), bf16),
            pltpu.VMEM((2, D, lanes), bf16),
            pltpu.VMEM((D, width3), bf16),
            pltpu.VMEM((2, 2, 2 * share_rows, width3 // 2), bf16),
            pltpu.VMEM((2, 2 * share_rows, width3 // 2), bf16),
            pltpu.VMEM((share_rows, width3), bf16),
            pltpu.VMEM((share_rows, width3), bf16),
            pltpu.VMEM((D, 4 * width), bf16),
            pltpu.VMEM((4, share_rows, 4 * width), bf16),
            pltpu.VMEM((2, 2, share_rows, 2 * width), bf16),
            pltpu.VMEM((2, share_rows, 2 * width), bf16),
            pltpu.VMEM((3, share_rows, width), bf16),
            pltpu.VMEM((D, 4 * width), bf16),
            pltpu.VMEM((5, 4, D), f32),
            pltpu.VMEM((5, 4, D), f32),
            pltpu.SemaphoreType.DMA((15,)),
            pltpu.SemaphoreType.DMA((sems,)),
            pltpu.SemaphoreType.DMA((sems,)),
        ],
        compiler_params=pltpu.CompilerParams(
            vmem_limit_bytes=67043328, collective_id=2, has_side_effects=True
        ),
        cost_estimate=pl.CostEstimate(
            flops=40 * heads * seq * seq * HEAD_DIM, bytes_accessed=40 << 20, transcendentals=0
        ),
    )(info, mixed, context, upstream, lse, weight, branch, norm_sums, gathered, up_grads, down_grads, out_grads)


def adam_body(owned, attention_ref, feed_ref, master_ref, one_ref, two_ref,
              grad_out, master_out, one_out, two_out, tiles_out, up_out, down_out):
    tile = grad_out.shape[-1] // 4
    for s in range(4):
        at = slice(s * tile, (s + 1) * tile)
        grad = jnp.zeros((grad_out.shape[0], tile), f32)
        for i in range(4):
            value = attention_ref[:, i * tile : (i + 1) * tile].astype(f32)
            grad = jnp.where(owned[s, i] > 0, value, grad)
        for kind in range(2):
            value = jnp.concatenate([feed_ref[2 * s + k, kind] for k in range(2)], axis=-1)
            grad = jnp.where(owned[s, 4 + 4 * kind + s] > 0, value.astype(f32), grad)
        occupied = (owned[s, 12] > 0).astype(f32)
        param, first, second = adam_update(
            grad, master_ref[:, at], one_ref[:, at], two_ref[:, at], occupied, weight_decay
        )
        grad_out[:, at] = grad
        master_out[:, at] = param
        one_out[:, at] = first
        two_out[:, at] = second
        low = param.astype(bf16)
        none = jnp.zeros_like(low)
        for i in range(4):
            mine = jnp.where(owned[s, i] > 0, low, none)
            there = slice(i * tile, (i + 1) * tile)
            tiles_out[:, there] = mine if s == 0 else tiles_out[:, there] + mine
        for kind, target in ((0, up_out), (1, down_out)):
            mine = jnp.where(owned[s, 4 + 4 * kind + s] > 0, low, none)
            for k in range(2):
                target[2 * s + k] = mine[:, k * tile // 2 : (k + 1) * tile // 2]


def adam_block(owned, attention_grad, feed_grad, master, one, two):
    part = 128
    wide = pl.BlockSpec((part, D), lambda i: (i, 0))
    lanes = feed_grad.shape[-1]
    split = pl.BlockSpec((SHARE, part, lanes), lambda i: (0, i, 0))
    return pl.pallas_call(
        adam_body,
        grid=(D // part,),
        name="adam_block",
        in_specs=[
            pl.BlockSpec(memory_space=pltpu.SMEM), wide,
            pl.BlockSpec((SHARE, 2, part, lanes), lambda i: (0, 0, i, 0)), wide, wide, wide,
        ],
        out_specs=[wide] * 5 + [split] * 2,
        out_shape=[jax.ShapeDtypeStruct((D, D), f32)] * 4
        + [jax.ShapeDtypeStruct((D, D), bf16)]
        + [jax.ShapeDtypeStruct((SHARE, D, lanes), bf16)] * 2,
        compiler_params=pltpu.CompilerParams(vmem_limit_bytes=32 << 20),
        cost_estimate=pl.CostEstimate(flops=40 * D * D, bytes_accessed=40 << 20, transcendentals=0),
    )(owned, attention_grad, feed_grad, master, one, two)


def tiles_body(tiles_ref, up_ref, down_ref, tiles_out, up_out, down_out, *scratch):
    core_got = scratch[:3]
    one_got, two_got = scratch[3:5], scratch[5:7]
    work = scratch[7:10]
    row_one, row_two, send_sems, recv_sems = scratch[10:]
    send = sender(send_sems, recv_sems)
    y, x, c = bits()
    core = peer_of(1, 0)
    own_block = block_of(y, x, c)
    greet([core, peer_of(2, 0), peer_of(4, 0)])
    arrays = ((up_ref, up_out), (down_ref, down_out), (tiles_ref, tiles_out))

    def place(n, ref, block):
        return ref.at[row_block(block), :] if n == 2 else ref.at[block]

    def core_copy(n, k):
        return send(
            place(n, arrays[n][0], block_of(k // 2, k % 2, 1 - c)), core_got[n].at[k], 4 * n + k, core
        )

    def core_add(n):
        source, target = arrays[n][0], work[n]
        for k in range(4):
            core_copy(n, k).wait()
        for k in range(4):
            block = block_of(k // 2, k % 2, c)
            if n == 2:
                at = row_block(block)
                target[at, :] = source[at, :] + core_got[n][k]
            else:
                target[k] = source[block] + core_got[n][k]

    def first(n, k):
        y_, x_ = ((k, 1 - x), (1 - y, k))[n]
        return send(
            work[n].at[2 * y_ + x_], one_got[n].at[k], 12 + 2 * n + k,
            peer_of((2, 4)[n], 0),
        )

    def second(n):
        y_, x_ = ((1 - y, x), (y, 1 - x))[n]
        return send(
            work[n].at[2 * y_ + x_], two_got[n], 16 + n, peer_of((4, 2)[n], 0)
        )

    def relay(n):
        target = work[n]
        for k in range(2):
            first(n, k).wait()
        for k in range(2):
            y_, x_ = ((k, x), (y, k))[n]
            block = 2 * y_ + x_
            target[block] = target[block] + one_got[n][k]
        second(n).start()

    def settle(n):
        second(n).wait()
        arrays[n][1][own_block] = work[n][2 * y + x] + two_got[n][...]

    for n in range(3):
        for k in range(4):
            core_copy(n, k).start()
    for n in range(2):
        core_add(n)
        for k in range(2):
            first(n, k).start()
    core_add(2)
    rows = RowSums(
        send, work[2], lambda yy, xx: block_of(yy, xx, c) * 128, 128, row_one, row_two, 18
    )
    rows.start()
    for n in range(2):
        relay(n)
    rows.relay()
    gathers = []
    for n in range(2):
        settle(n)
        gathers.append(
            Gather(send, lambda k, n=n: arrays[n][1].at[k], 24 + n * GATHER_SEMS, n == 0)
        )
        gathers[-1].start()
    rows.finish()
    tiles_out[row_block(own_block), :] = work[2][row_block(own_block), :]
    half = tiles_out.shape[-1] // 2
    for side in range(2):
        gathers.append(
            Gather(
                send,
                lambda k, side=side: tiles_out.at[row_block(k), side * half : (side + 1) * half],
                24 + (2 + side) * GATHER_SEMS, side == 0,
            )
        )
        gathers[-1].start()
    for gather in gathers:
        gather.relay()
    for gather in gathers:
        gather.last()
    for gather in gathers:
        gather.finish()


def spread_tiles(tiles, up, down):
    share_rows = D // SHARE
    lanes = up.shape[-1]
    sems = 24 + 4 * GATHER_SEMS
    piece = (D, lanes)
    vmem = pl.BlockSpec(memory_space=pltpu.VMEM)
    return pl.pallas_call(
        tiles_body,
        name="spread_tiles",
        in_specs=[vmem] * 3,
        out_specs=[vmem] * 3,
        out_shape=[jax.ShapeDtypeStruct(v.shape, bf16) for v in (tiles, up, down)],
        scratch_shapes=[
            pltpu.VMEM((4,) + piece, bf16),
            pltpu.VMEM((4,) + piece, bf16),
            pltpu.VMEM((4, share_rows, D), bf16),
            pltpu.VMEM((2,) + piece, bf16),
            pltpu.VMEM((2,) + piece, bf16),
            pltpu.VMEM(piece, bf16),
            pltpu.VMEM(piece, bf16),
            pltpu.VMEM((4,) + piece, bf16),
            pltpu.VMEM((4,) + piece, bf16),
            pltpu.VMEM((D, D), bf16),
            pltpu.VMEM((2, 2, share_rows, D // 2), bf16),
            pltpu.VMEM((2, share_rows, D // 2), bf16),
            pltpu.SemaphoreType.DMA((sems,)),
            pltpu.SemaphoreType.DMA((sems,)),
        ],
        compiler_params=pltpu.CompilerParams(
            vmem_limit_bytes=48 << 20, collective_id=3, has_side_effects=True
        ),
        cost_estimate=pl.CostEstimate(flops=D * D, bytes_accessed=12 << 20, transcendentals=0),
    )(tiles, up, down)


def joined(held, i, kind):
    return jnp.concatenate([held[2 * i + k, m, kind] for k in range(2) for m in range(2)], axis=-1)


def gelu_parts(value):
    bell = jnp.exp(-0.5 * value * value)
    t = 1.0 / (1.0 + (0.3275911 * 0.5**0.5) * jnp.abs(value))
    tail = 0.5 * 1.061405429
    for c in (-1.453152027, 1.421413741, -0.284496736, 0.254829592):
        tail = tail * t + 0.5 * c
    tail = tail * t * bell
    area = jnp.where(value > 0, 1.0 - tail, tail)
    return value * area, area + value * bell * (0.5 / jnp.pi) ** 0.5


def feed_body(count, info, first_ref, cotangent_ref, norms_ref, *refs):
    pieces = refs[:count]
    out_ref, low_ref, both_ref, hidden_ref, pre_ref, grad_ref, sums_ref = refs[count : count + 7]
    held, slope, total, leaving, landed, local_sems, send_sems, recv_sems = refs[count + 7 :]
    rows = first_ref.shape[0]
    width = hidden_ref.shape[-1]
    peer = (other_core(), lax.axis_index("tensor"))
    for i in range(count):
        pltpu.make_async_copy(pieces[i], held.at[i], local_sems.at[i]).start()
    greet([peer])

    def across(source, target, k):
        return pltpu.make_async_remote_copy(
            source, target, send_sems.at[k], recv_sems.at[k], device_id=peer,
            device_id_type=pl.DeviceIdType.MESH,
        )

    half = rows // 2
    both_ref[0] = first_ref[...].astype(bf16)
    first_copy = across(both_ref.at[0], both_ref.at[1], 0)
    first_copy.start()

    def up(i, slot):
        weight = joined(held, i, 0)
        for r in range(0, rows, half):
            value = jnp.dot(both_ref[slot, r : r + half, :], weight, preferred_element_type=f32)
            hidden, steep = gelu_parts(value)
            hidden_ref[i, slot, r : r + half, :] = hidden.astype(bf16)
            slope[i, slot, r : r + half, :] = steep.astype(bf16)

    def down(i, slot):
        total[slot] += contract(hidden_ref[i, slot], joined(held, i, 1), 1, 1)

    def back(i, slot):
        weight = joined(held, i, 1)
        for r in range(0, rows, half):
            value = jnp.dot(low_ref[slot, r : r + half, :], weight, preferred_element_type=f32)
            steep = slope[i, slot, r : r + half, :].astype(f32)
            pre_ref[i, slot, r : r + half, :] = (value * steep).astype(bf16)

    def back_up(i, slot):
        total[slot] += contract(pre_ref[i, slot], joined(held, i, 0), 1, 1)

    def loop(*works):
        def body(i, carry):
            for work in works:
                work(i)
            return carry

        lax.fori_loop(0, count // 2, body, 0)

    def arrive(i):
        for k in range(2):
            pltpu.make_async_copy(
                pieces[0], held.at[2 * i + k], local_sems.at[2 * i + k]
            ).wait()

    total[...] = jnp.zeros_like(total)
    loop(arrive, lambda i: up(i, 0))
    first_copy.wait()
    loop(lambda i: up(i, 1), lambda i: down(i, 1))
    leaving[...] = total[1].astype(bf16)
    feed_copy = across(leaving, landed.at[0], 1)
    feed_copy.start()
    loop(lambda i: down(i, 0))
    feed_copy.wait()

    sums_ref[...] = jnp.zeros_like(sums_ref)
    part = 128

    def middle(r, carry):
        at = pl.ds(pl.multiple_of(r * part, part), part)
        second, normed, inverse = norm_parts(
            first_ref[at, :] + (total[0, at, :] + landed[0, at, :].astype(f32)),
            norms_ref[2:3, :], norms_ref[3:4, :],
        )
        out_ref[at, :] = second.astype(bf16)
        row = lax.broadcasted_iota(jnp.int32, (part, 1), 0) + r * part + info[1]
        seed = cotangent_ref[at, :].astype(f32) * (row < info[0]).astype(f32)
        grad = norm_back(seed, normed, inverse, norms_ref[2:3, :])
        sums_ref[0:1, :] += jnp.sum(seed * normed, axis=0, keepdims=True)
        sums_ref[1:2, :] += jnp.sum(seed, axis=0, keepdims=True)
        total[0, at, :] = grad
        low_ref[0, at, :] = grad.astype(bf16)
        return carry

    lax.fori_loop(0, rows // part, middle, 0)
    low_copy = across(low_ref.at[0], low_ref.at[1], 2)
    low_copy.start()
    total[1] = jnp.zeros_like(total[1])
    loop(lambda i: back(i, 0))
    low_copy.wait()
    loop(lambda i: back(i, 1), lambda i: back_up(i, 1))
    leaving[...] = total[1].astype(bf16)
    grad_copy = across(leaving, landed.at[1], 3)
    grad_copy.start()
    loop(lambda i: back_up(i, 0))
    grad_copy.wait()
    grad_ref[...] = total[0] + landed[1].astype(f32)


def feed_block(info, first, cotangent, norms, pieces):
    rows = first.shape[0]
    count = len(pieces)
    lanes = pieces[0].shape[-1]
    width = 4 * lanes
    vmem = pl.BlockSpec(memory_space=pltpu.VMEM)
    return pl.pallas_call(
        partial(feed_body, count),
        name="feed_block",
        in_specs=[pl.BlockSpec(memory_space=pltpu.SMEM), vmem, vmem, vmem]
        + [pl.BlockSpec(memory_space=pl.ANY)] * count,
        out_specs=[vmem] * 7,
        out_shape=[
            jax.ShapeDtypeStruct((rows, D), bf16),
            jax.ShapeDtypeStruct((2, rows, D), bf16),
            jax.ShapeDtypeStruct((2, rows, D), bf16),
            jax.ShapeDtypeStruct((count // 2, 2, rows, width), bf16),
            jax.ShapeDtypeStruct((count // 2, 2, rows, width), bf16),
            jax.ShapeDtypeStruct((rows, D), f32),
            jax.ShapeDtypeStruct((2, D), f32),
        ],
        scratch_shapes=[
            pltpu.VMEM((count,) + pieces[0].shape, bf16),
            pltpu.VMEM((count // 2, 2, rows, width), bf16),
            pltpu.VMEM((2, rows, D), f32),
            pltpu.VMEM((rows, D), bf16),
            pltpu.VMEM((2, rows, D), bf16),
            pltpu.SemaphoreType.DMA((count,)),
            pltpu.SemaphoreType.DMA((4,)),
            pltpu.SemaphoreType.DMA((4,)),
        ],
        compiler_params=pltpu.CompilerParams(
            vmem_limit_bytes=60 << 20, collective_id=1, has_side_effects=True
        ),
        cost_estimate=pl.CostEstimate(
            flops=8 * rows * D * width * count, bytes_accessed=30 << 20, transcendentals=0
        ),
    )(info, first, cotangent, norms, *pieces)


def feed_grads_body(first_ref, low_ref, hidden_ref, pre_ref, up_ref, down_ref, first_t, low_t):
    rows = first_ref.shape[1]

    @pl.when(pl.program_id(0) == 0)
    def _():
        for slot in range(2):
            at = slice(slot * rows, (slot + 1) * rows)
            first_t[:, at] = jnp.transpose(first_ref[slot].astype(f32)).astype(bf16)
            low_t[:, at] = jnp.transpose(low_ref[slot].astype(f32)).astype(bf16)

    lanes = up_ref.shape[-1]
    width = pre_ref.shape[-1]
    for target, source, turned in ((up_ref, pre_ref, first_t), (down_ref, hidden_ref, low_t)):
        grad = jnp.dot(
            turned[...], source[0].reshape(2 * rows, width), preferred_element_type=f32
        ).astype(bf16)
        for k in range(2):
            for m in range(2):
                at = (2 * k + m) * lanes
                if target is up_ref:
                    target[m, k, 0] = grad[:, at : at + lanes]
                else:
                    target[m, 0, k] = grad[:, at : at + lanes]


def feed_grads(first, low, hidden, pre):
    count, _, rows, width = hidden.shape
    full = pl.BlockSpec((2, rows, D), lambda i: (0, 0, 0))
    piece = pl.BlockSpec((1, 2, rows, width), lambda i: (i, 0, 0, 0))
    lanes = width // 4
    return pl.pallas_call(
        feed_grads_body,
        grid=(count,),
        name="feed_grads",
        in_specs=[full, full, piece, piece],
        out_specs=[
            pl.BlockSpec((2, 2, 1, D, lanes), lambda i: (i // 2, 0, i % 2, 0, 0)),
            pl.BlockSpec((2, 1, 2, D, lanes), lambda i: (i // 2, i % 2, 0, 0, 0)),
        ],
        out_shape=[jax.ShapeDtypeStruct((count, 2, 2, D, lanes), bf16)] * 2,
        scratch_shapes=[pltpu.VMEM((D, 2 * rows), bf16), pltpu.VMEM((D, 2 * rows), bf16)],
        compiler_params=pltpu.CompilerParams(vmem_limit_bytes=48 << 20),
        cost_estimate=pl.CostEstimate(
            flops=8 * rows * D * width * count, bytes_accessed=20 << 20, transcendentals=0
        ),
    )(first, low, hidden, pre)


def layer(n_dp, n_tensor, tokens, weights, norms, cotangent, lengths, owners, master, moment_one,
          moment_two, norm_master, norm_one, norm_two):
    tile = D // n_tensor
    hidden_width = FF // n_tensor
    rows = tokens.shape[0]
    lanes = hidden_width // SHARE
    device = lax.axis_index("dp")
    z = lax.axis_index("tensor")
    core = device % 2
    matched = core == z // 2
    quarter = jnp.where(matched, z, z ^ 2)

    def flip(x, dd, dz):
        pairs = [
            (d * n_tensor + t, (d ^ dd) * n_tensor + (t ^ dz))
            for d in range(n_dp)
            for t in range(n_tensor)
        ]
        return lax.ppermute(x, AXES, pairs)

    def some(x, dd, dz, want):
        pairs = [
            (d * n_tensor + t, (d ^ dd) * n_tensor + (t ^ dz))
            for d in range(n_dp)
            for t in range(n_tensor)
            if (t // 2 == d % 2) == want
        ]
        return lax.ppermute(x, AXES, pairs)

    def swap(x):
        return jnp.where(matched, x, some(x, 1, 2, False))

    w_mixed = weights[:, : 3 * tile]
    w_out = weights[:, 3 * tile : 4 * tile]
    share_rows = D // n_dp
    length = jnp.where(matched, lengths, flip(lengths, 1, 0))[0]
    base = jnp.stack([quarter ^ k for k in (0, 2, 1, 3)]) * rows
    info = jnp.concatenate([length[None], base]).astype(jnp.int32)

    inputs = tokens[:, 0, :]
    own = swap(inputs)
    far = some(inputs, 0, 1, True) + some(own, 0, 1, False)
    near = flip(own, 1, 0)
    gathered = jnp.stack([own, near, far, flip(far, 1, 0)])

    def my_rows(x):
        return lax.dynamic_slice_in_dim(x, device * share_rows, share_rows, 0)

    other = lax.all_gather(flip(my_rows(w_mixed), 0, 2), "dp", axis=0, tiled=True)
    w_heads = jnp.where(matched, w_mixed, other)
    out_own = my_rows(w_out)
    out_two = jnp.concatenate([out_own, flip(out_own, 0, 1)], axis=1)
    out_four = jnp.concatenate([out_two, flip(out_two, 0, 2)], axis=1)
    w_out_all = lax.all_gather(out_four, "dp", axis=0, tiled=True)

    at = (device % SHARE) * lanes + 4 * tile
    own_piece = jnp.stack(
        [
            lax.dynamic_slice(weights, (0, at), (D, lanes)),
            lax.dynamic_slice(weights, (0, at + hidden_width), (D, lanes)),
        ]
    )
    near_pieces = jnp.stack([own_piece, flip(own_piece, 0, 1)])
    far_pieces = flip(near_pieces, 0, 2)

    def spread(first_pieces, one, two):
        a = first_pieces
        b = flip(a, one, 0)
        return [a, b, flip(a, two, 0), flip(b, two, 0)]

    near_four = spread(near_pieces, 2, 4)
    far_four = spread(far_pieces, 4, 2)
    pieces = near_four + [far_four[k] for k in (0, 2, 1, 3)]

    mixed = jnp.einsum(
        "csd,de->cse", gathered, w_heads, preferred_element_type=f32
    ).astype(bf16)
    context, lse = attention_forward(info, mixed)

    parts = [context[0], flip(context[1], 1, 0), flip(context[2], 0, 1), flip(context[3], 1, 1)]
    context_all = jnp.where(
        matched,
        jnp.concatenate([parts[k] for k in (0, 2, 1, 3)], axis=1),
        jnp.concatenate([parts[k] for k in (1, 3, 0, 2)], axis=1),
    )
    branch = contract(context_all, w_out_all, 1, 1)
    first, first_normed, first_inverse = norm_parts(
        own.astype(f32) + branch, norms[0], norms[1]
    )
    seed = swap(cotangent[:, 0, :])
    outputs, both_low, both_first, hidden, pre_grad, first_grad, sums_two = feed_block(
        info, first, seed, norms, pieces
    )
    branch_grad = norm_back(first_grad, first_normed, first_inverse, norms[0])
    gain_one = jnp.sum(first_grad * first_normed, axis=0)
    shift_one = jnp.sum(first_grad, axis=0)
    branch_low = branch_grad.astype(bf16)
    context_grad = jnp.dot(branch_low, w_out_all, preferred_element_type=f32).astype(bf16)
    blocks = [context_grad[:, k * tile : (k + 1) * tile] for k in range(4)]
    blocks = [
        jnp.where(matched, blocks[a], blocks[b]) for a, b in ((0, 2), (2, 0), (1, 3), (3, 1))
    ]
    upstream = jnp.stack(
        [blocks[0], flip(blocks[1], 1, 0), flip(blocks[2], 0, 1), flip(blocks[3], 1, 1)]
    )

    def add(a, b):
        return (a.astype(f32) + b.astype(f32)).astype(bf16)

    up_grads, down_grads = feed_grads(both_first, both_low, hidden, pre_grad)
    out_grad = contract(branch_low, context_all, 0, 0).astype(bf16)
    norm_sums = jnp.concatenate([jnp.stack([gain_one, shift_one]), sums_two])
    input_total, norm_grads, attention_grad, feed_grad = back_block(
        info, mixed, context, upstream, lse, w_heads, branch_grad, norm_sums, gathered, up_grads, down_grads, out_grad
    )
    input_grad = swap(input_total)[:, None, :]

    def over_groups(value, combine):
        bit = SHARE
        while bit < n_dp:
            value = combine(value, flip(value, bit, 0))
            bit *= 2
        return value

    def plus(a, b):
        return a + b

    norm_grads = over_groups(norm_grads, plus)
    attention_grad = over_groups(attention_grad, add)
    feed_grad = over_groups(feed_grad, add)

    tile_owner, slot_index = slot_table(owners)
    slot_ids = jnp.arange(FF // D, dtype=jnp.int32)
    owned = (
        (tile_owner[None, :] == device) & (slot_index[None, :] == slot_ids[:, None])
    ).astype(jnp.int32)
    owned = jnp.concatenate([owned, jnp.sum(owned, axis=1, keepdims=True)], axis=1)
    slot_grad, new_master, new_one, new_two, tiles, up_tiles, down_tiles = adam_block(
        owned, attention_grad, feed_grad, master[0], moment_one[0], moment_two[0]
    )
    tiles, up_tiles, down_tiles = (
        over_groups(v, plus) for v in spread_tiles(tiles, up_tiles, down_tiles)
    )
    new_weights = jnp.concatenate(
        [tiles] + [up_tiles[k] for k in range(SHARE)] + [down_tiles[k] for k in range(SHARE)], axis=1
    )
    norm_owner = (device == owners[6]).astype(f32)
    new_norm_master, new_norm_one, new_norm_two = adam_update(
        norm_grads, norm_master[0], norm_one[0], norm_two[0], norm_owner, 0.0
    )
    return (
        swap(outputs)[:, None, :],
        input_grad,
        slot_grad[None],
        new_master[None],
        new_one[None],
        new_two[None],
        new_weights,
        norm_grads,
        new_norm_master[None],
        new_norm_one[None],
        new_norm_two[None],
    )


def solution(mesh):
    in_specs = (
        P("tensor", "dp", None),
        P(None, "tensor"),
        P(),
        P("tensor", "dp", None),
        P("dp"),
        P(),
        P("dp", None, "tensor"),
        P("dp", None, "tensor"),
        P("dp", None, "tensor"),
        P("dp", None, None),
        P("dp", None, None),
        P("dp", None, None),
    )
    out_specs = (
        P("tensor", "dp", None),
        P("tensor", "dp", None),
        P("dp", None, "tensor"),
        P("dp", None, "tensor"),
        P("dp", None, "tensor"),
        P("dp", None, "tensor"),
        P(None, "tensor"),
        P(),
        P("dp", None, None),
        P("dp", None, None),
        P("dp", None, None),
    )
    return jax.shard_map(
        partial(layer, mesh.shape["dp"], mesh.shape["tensor"]),
        mesh=mesh,
        in_specs=in_specs,
        out_specs=out_specs,
        check_vma=False,
    )
```

```python
from functools import partial

import jax
import jax.numpy as jnp
from jax import lax
from jax.experimental import pallas as pl
from jax.experimental.pallas import tpu as pltpu
from jax.sharding import PartitionSpec as P

D = 1024
FF = 4096
ADAM_STEP = 10
HEAD_DIM = 64
SHARE = 8


f32, bf16 = jnp.float32, jnp.bfloat16
beta_one = 0.9
beta_two = 0.999
learn_rate = 0.02
weight_decay = 0.1
adam_eps = 1e-08
norm_eps = 1e-05
masked_score = -1e30
AXES = ("dp", "tensor")


def contract(a, b, ca, cb):
    return lax.dot_general(a, b, (((ca,), (cb,)), ((), ())), preferred_element_type=f32)


def norm_parts(value, gain, shift):
    average = jnp.mean(value, axis=-1, keepdims=True)
    centred = value - average
    variance = jnp.mean(centred * centred, axis=-1, keepdims=True)
    inverse = lax.rsqrt(variance + norm_eps)
    normed = centred * inverse
    return normed * gain + shift, normed, inverse


def norm_back(upstream, normed, inverse, gain):
    scaled = upstream * gain
    inner = (
        scaled
        - jnp.mean(scaled, axis=-1, keepdims=True)
        - normed * jnp.mean(scaled * normed, axis=-1, keepdims=True)
    )
    return inner * inverse


def slot_table(owners):
    repeat = FF // D
    tile_matrix = jnp.array([0, 1, 2, 3] + [4] * repeat + [5] * repeat, dtype=jnp.int32)
    choose = (tile_matrix[:, None] == jnp.arange(7, dtype=jnp.int32)[None, :]).astype(jnp.int32)
    tile_owner = jnp.sum(choose * owners[None, :], axis=1)
    position = jnp.arange(tile_matrix.shape[0], dtype=jnp.int32)
    before = (tile_owner[None, :] == tile_owner[:, None]) & (position[None, :] < position[:, None])
    slot_index = jnp.sum(before.astype(jnp.int32), axis=1)
    return (tile_owner, slot_index)


def adam_update(grad, param, first, second, occupied, decay_rate):
    first_new = occupied * (beta_one * first + (1.0 - beta_one) * grad)
    second_new = occupied * (beta_two * second + (1.0 - beta_two) * grad * grad)
    correct_one = 1.0 - beta_one**ADAM_STEP
    correct_two = 1.0 - beta_two**ADAM_STEP
    direction = first_new / correct_one / (jnp.sqrt(second_new / correct_two) + adam_eps)
    param_new = occupied * (param - learn_rate * (direction + decay_rate * param))
    return (param_new, first_new, second_new)


def head_keys(keys, half, start, length):
    lane = lax.broadcasted_iota(jnp.int32, keys.shape, 1)
    row = lax.broadcasted_iota(jnp.int32, keys.shape, 0)
    bias = jnp.where(start + row < length, 0.0, masked_score).astype(f32)
    extra = jnp.where(lane == (1 - half) * HEAD_DIM, bias, 0.0)
    return jnp.where(lane // HEAD_DIM == half, keys.astype(f32), extra).astype(bf16)


def head_half(rows, half):
    lane = lax.broadcasted_iota(jnp.int32, rows.shape, 1)
    return jnp.where(lane // HEAD_DIM == half, rows, jnp.zeros_like(rows))


def head_queries(rows, half):
    lane = lax.broadcasted_iota(jnp.int32, rows.shape, 1)
    scaled = rows.astype(f32) * HEAD_DIM ** (-0.5)
    extra = jnp.where(lane == (1 - half) * HEAD_DIM, 1.0, 0.0)
    return jnp.where(lane // HEAD_DIM == half, scaled, extra).astype(bf16)


def peer_of(bit, turn):
    device, z = lax.axis_index("dp"), lax.axis_index("tensor")
    for one in (1, 2, 4):
        if bit & one:
            device = device + one - 2 * one * ((device // one) % 2)
    if turn == 1:
        z = z + 1 - 2 * (z % 2)
    elif turn == 2:
        z = z + 2 - 4 * (z // 2)
    elif turn == 3:
        z = 3 - z
    return (device, z)


def greet(peers):
    barrier = pltpu.get_barrier_semaphore()
    for peer in peers:
        pl.semaphore_signal(barrier, inc=1, device_id=peer, device_id_type=pl.DeviceIdType.MESH)
    pl.semaphore_wait(barrier, len(peers))


def sender(send_sems, recv_sems):
    def send(source, target, k, peer):
        return pltpu.make_async_remote_copy(
            source, target, send_sems.at[k], recv_sems.at[k], device_id=peer,
            device_id_type=pl.DeviceIdType.MESH,
        )

    return send


def bits():
    device = lax.axis_index("dp")
    return (device // 4) % 2, (device // 2) % 2, device % 2


def block_of(y, x, c):
    return 4 * y + 2 * x + c


def row_block(index, count=1):
    rows = D // SHARE
    return pl.ds(pl.multiple_of(index * rows, rows), count * rows)


class Gather:
    def __init__(self, send, view, first_sem, x_first):
        self.send, self.view, self.sem = send, view, first_sem
        self.y, self.x, self.c = bits()
        self.one, self.two = (2, 4) if x_first else (4, 2)

    def block(self, turn):
        y, x, c = self.y, self.x, self.c
        y = 1 - y if turn & 4 else y
        x = 1 - x if turn & 2 else x
        c = 1 - c if turn & 1 else c
        return block_of(y, x, c)

    def copy(self, turn, over, k):
        place = self.view(self.block(turn))
        return self.send(place, place, self.sem + k, peer_of(over, 0))

    def start(self):
        self.copy(0, self.one, 0).start()
        self.copy(0, self.two, 1).start()
        self.copy(0, 1, 3).start()

    def relay(self):
        self.copy(0, self.one, 0).wait()
        self.copy(self.one, self.two, 2).start()
        self.copy(self.one, 1, 4).start()
        self.copy(0, self.two, 1).wait()
        self.copy(self.two, 1, 5).start()

    def last(self):
        self.copy(self.one, self.two, 2).wait()
        self.copy(6, 1, 6).start()

    def finish(self):
        for turn, k in ((0, 3), (self.one, 4), (self.two, 5), (6, 6)):
            self.copy(turn, 1, k).wait()


GATHER_SEMS = 7


class RowSums:
    def __init__(self, send, ref, place, height, got_one, got_two, first_sem):
        self.send, self.ref, self.place, self.height = send, ref, place, height
        self.got_one, self.got_two, self.sem = got_one, got_two, first_sem
        self.y, self.x, _ = bits()
        self.half = ref.shape[-1] // 2

    def at(self, y, x, side):
        rows = pl.ds(pl.multiple_of(self.place(y, x), 128), self.height)
        return (rows, slice(side * self.half, (side + 1) * self.half))

    def pairs(self, k, mine):
        y, x = self.y, self.x
        return [
            (y if mine else 1 - y, k, 0),
            (k, x if mine else 1 - x, 1),
        ]

    def first(self, k, side):
        y, x, _ = self.pairs(k, False)[side]
        return self.send(
            self.ref.at[self.at(y, x, side)], self.got_one.at[side, k], self.sem + 2 * side + k,
            peer_of((4, 2)[side], 0),
        )

    def second(self, side):
        y, x = ((self.y, 1 - self.x), (1 - self.y, self.x))[side]
        return self.send(
            self.ref.at[self.at(y, x, side)], self.got_two.at[side], self.sem + 4 + side,
            peer_of((2, 4)[side], 0),
        )

    def start(self):
        for side in range(2):
            for k in range(2):
                self.first(k, side).start()

    def relay(self):
        for side in range(2):
            for k in range(2):
                self.first(k, side).wait()
        for side in range(2):
            for k in range(2):
                y, x, _ = self.pairs(k, True)[side]
                at = self.at(y, x, side)
                self.ref[at] = (
                    self.ref[at].astype(f32) + self.got_one[side, k].astype(f32)
                ).astype(bf16)
        for side in range(2):
            self.second(side).start()

    def finish(self):
        for side in range(2):
            self.second(side).wait()
            at = self.at(self.y, self.x, side)
            self.ref[at] = (
                self.ref[at].astype(f32) + self.got_two[side].astype(f32)
            ).astype(bf16)


ROW_SEMS = 6


def start_body(
    lengths, tokens_ref, weights_ref,
    gathered_ref, mixed_ref, context_ref, parts_ref, lse_ref, heads_ref, out_ref, up_ref, down_ref,
    keys, values, length_buf, out_here, out_far, local_sems, send_sems, recv_sems,
):
    chunks, rows, _ = gathered_ref.shape
    width = context_ref.shape[-1]
    lanes = up_ref.shape[-1]
    hidden_width = SHARE * lanes
    piece = rows // 4
    quarter_rows = D // 4
    y, x, c = bits()
    z = lax.axis_index("tensor")
    matched = c == z // 2
    unmatched = jnp.logical_not(matched)
    own_block = block_of(y, x, c)
    send = sender(send_sems, recv_sems)
    core, near_z, diagonal, swapped = peer_of(1, 0), peer_of(0, 1), peer_of(1, 1), peer_of(1, 2)
    across_x, across_y, across_xy = peer_of(2, 0), peer_of(4, 0), peer_of(6, 0)

    def part_of(k):
        return slice(k * piece, (k + 1) * piece)

    def swap_copy(k):
        return send(tokens_ref.at[part_of(k), :], gathered_ref.at[0, part_of(k), :], k, swapped)

    def far_copy(k, source):
        return send(source.at[part_of(k), :], gathered_ref.at[2, part_of(k), :], 4 + k, near_z)

    def near_copy(k, source):
        return send(source.at[part_of(k), :], gathered_ref.at[1, part_of(k), :], 8 + k, core)

    def diagonal_copy(k):
        return send(gathered_ref.at[2, part_of(k), :], gathered_ref.at[3, part_of(k), :], 12 + k, core)

    column = 2 * y + x

    def quarter(k):
        return pl.ds(pl.multiple_of(k * quarter_rows, quarter_rows), quarter_rows)

    def heads_swap():
        return send(
            weights_ref.at[quarter(column), : 3 * width], heads_ref.at[quarter(column), :], 16, swapped
        )

    def heads_share(k, peer):
        return send(heads_ref.at[quarter(column), :], heads_ref.at[quarter(column), :], 17 + k, peer)

    heads_peers = (across_x, across_y, across_xy)
    heads_local = pltpu.make_async_copy(weights_ref.at[:, : 3 * width], heads_ref, local_sems.at[0])

    def out_copy(e):
        return send(out_here, out_far.at[e - 1], 19 + e, peer_of(0, e))

    out_local = pltpu.make_async_copy(
        weights_ref.at[row_block(own_block), 3 * width : 4 * width], out_here, local_sems.at[1]
    )
    outs = [
        Gather(
            send, lambda k, side=side: out_ref.at[row_block(k), side * 2 * width : (side + 1) * 2 * width],
            23 + side * GATHER_SEMS, side == 0,
        )
        for side in range(2)
    ]
    base = 23 + 2 * GATHER_SEMS
    targets = (up_ref, down_ref)

    def feed_source(kind):
        at = 4 * width + kind * hidden_width + own_block * lanes
        return weights_ref.at[:, pl.ds(pl.multiple_of(at, 128), lanes)]

    def feed_copy(kind, e):
        return send(feed_source(kind), targets[kind].at[e - 1, 0, 0], base + 3 * kind + e - 1, peer_of(0, e))

    half = slice(0, D // 2), slice(D // 2, D)

    def feed_one(kind, side):
        source = targets[kind].at[:, 0, 0, half[side], :]
        target = (
            targets[kind].at[:, 0, 1, half[0], :] if side == 0 else targets[kind].at[:, 1, 0, half[1], :]
        )
        return send(source, target, base + 6 + 2 * kind + side, (across_x, across_y)[side])

    def feed_two(kind, side):
        if side == 0:
            source, target = (targets[kind].at[:, dy, 0:2, half[0], :] for dy in range(2))
        else:
            source, target = (targets[kind].at[:, 0:2, dx, half[1], :] for dx in range(2))
        return send(source, target, base + 10 + side, (across_y, across_x)[side])

    def length_copy():
        return send(length_buf.at[0], length_buf.at[1], base + 12, core)

    def part_copy(j):
        return send(
            context_ref.at[j], parts_ref.at[j], base + 12 + j, (None, core, near_z, diagonal)[j]
        )

    def send_weights():
        for e in (3, 2, 1):
            feed_copy(0, e).start()
        for e in (3, 2, 1):
            feed_copy(1, e).start()

    out_local.start()
    length_buf[0] = jnp.full(length_buf.shape[1:], lengths[0], jnp.int32)
    greet(
        [core, near_z, diagonal, swapped, across_x, across_y, across_xy, peer_of(0, 2), peer_of(0, 3)]
    )

    @pl.when(matched)
    def _():
        for k in range(4):
            far_copy(k, tokens_ref).start()
            near_copy(k, tokens_ref).start()
        heads_local.start()
        gathered_ref[0] = tokens_ref[...]

    @pl.when(unmatched)
    def _():
        for k in range(4):
            swap_copy(k).start()
        heads_swap().start()

    length_copy().start()
    out_local.wait()
    for e in (1, 2, 3):
        out_copy(e).start()
    out_ref[row_block(own_block), :width] = out_here[...]

    @pl.when(matched)
    def _():
        send_weights()

    @pl.when(unmatched)
    def _():
        for k in range(4):
            swap_copy(k).wait()
            far_copy(k, gathered_ref.at[0]).start()
            near_copy(k, gathered_ref.at[0]).start()
        heads_swap().wait()
        for k, peer in enumerate(heads_peers):
            heads_share(k, peer).start()
        send_weights()

    for k in range(4):
        far_copy(k, tokens_ref).wait()
        diagonal_copy(k).start()

    @pl.when(matched)
    def _():
        heads_local.wait()

    @pl.when(unmatched)
    def _():
        for k, peer in enumerate(heads_peers):
            heads_share(k, peer).wait()

    length_copy().wait()
    length = jnp.where(matched, length_buf[0][:1, :], length_buf[1][:1, :])
    own_quarter = jnp.where(matched, z, z + 2 - 4 * (z // 2))
    wide = 256

    def project(j):
        def columns(n, carry):
            at = pl.ds(pl.multiple_of(n * wide, wide), wide)
            mixed_ref[j, :, at] = jnp.dot(
                gathered_ref[j], heads_ref[:, at], preferred_element_type=f32
            ).astype(bf16)
            return carry

        lax.fori_loop(0, 3 * width // wide, columns, 0)

    def arrange(j):
        at_quarter = own_quarter
        if j in (1, 3):
            at_quarter = at_quarter + 2 - 4 * (at_quarter // 2)
        if j in (2, 3):
            at_quarter = at_quarter + 1 - 2 * (at_quarter % 2)
        for h in range(width // HEAD_DIM):
            at = width + (h // 2) * 128
            keys[h, j * rows : (j + 1) * rows, :] = head_keys(
                mixed_ref[j, :, at : at + 128], h % 2, at_quarter * rows, length
            )
        values[j * rows : (j + 1) * rows, :] = mixed_ref[j, :, 2 * width :]

    for j in (0, 2, 1, 3):
        if j == 1:
            for k in range(4):
                near_copy(k, tokens_ref).wait()
        if j == 3:
            for k in range(4):
                diagonal_copy(k).wait()
        project(j)
        arrange(j)

    for e in (1, 2, 3):
        out_copy(e).wait()
        out_ref[row_block(own_block), e * width : (e + 1) * width] = out_far[e - 1]
    for e in (3, 2, 1):
        feed_copy(0, e).wait()
    for side in range(2):
        feed_one(0, side).start()
    for gather in outs:
        gather.start()

    lane = lax.broadcasted_iota(jnp.int32, (rows, 128), 1)

    def attend(step, carry):
        chunk = chunks - 1 - step
        logs = jnp.zeros((rows, 128), f32)
        for pair in range(width // 128):
            queries = mixed_ref[chunk, :, pair * 128 : pair * 128 + 128]
            both = []
            for side in range(2):
                h = pair * 2 + side
                scores = contract(head_queries(queries, side), keys[h], 1, 1)
                top = jnp.max(scores, axis=1, keepdims=True)
                weight = jnp.exp(scores - top)
                total = jnp.sum(weight, axis=1, keepdims=True)
                out = contract(weight.astype(bf16), values[:, pair * 128 : pair * 128 + 128], 1, 0)
                both.append(out / total)
                logs = jnp.where(lane == h, top + jnp.log(total), logs)
            context_ref[chunk, :, pair * 128 : pair * 128 + 128] = jnp.where(
                lane < HEAD_DIM, both[0], both[1]
            ).astype(bf16)
        lse_ref[chunk] = jnp.transpose(logs)[:8, :]

        @pl.when(step == 0)
        def _():
            part_copy(3).start()
            for side in range(2):
                feed_one(0, side).wait()
            for side in range(2):
                feed_two(0, side).start()
            for gather in outs:
                gather.relay()

        @pl.when(step == 1)
        def _():
            part_copy(2).start()
            for e in (3, 2, 1):
                feed_copy(1, e).wait()
            for side in range(2):
                feed_one(1, side).start()
            for gather in outs:
                gather.last()

        @pl.when(step == 2)
        def _():
            part_copy(1).start()

        return carry

    lax.fori_loop(0, chunks, attend, 0)
    parts_ref[0] = context_ref[0]
    for gather in outs:
        gather.finish()
    for j in (3, 2, 1):
        part_copy(j).wait()
    for side in range(2):
        feed_two(0, side).wait()
        feed_one(1, side).wait()


def start_block(lengths, tokens, weights):
    rows = tokens.shape[0]
    chunks = 4
    tile = D // 4
    seq = chunks * rows
    lanes = FF // 4 // SHARE
    heads = tile // HEAD_DIM
    sems = 23 + 2 * GATHER_SEMS + 16
    share_rows = D // SHARE
    vmem, anywhere = pl.BlockSpec(memory_space=pltpu.VMEM), pl.BlockSpec(memory_space=pl.ANY)
    return pl.pallas_call(
        start_body,
        name="start_block",
        in_specs=[pl.BlockSpec(memory_space=pltpu.SMEM), vmem, anywhere],
        out_specs=[vmem] * 7 + [anywhere] * 2,
        out_shape=[
            jax.ShapeDtypeStruct((chunks, rows, D), bf16),
            jax.ShapeDtypeStruct((chunks, rows, 3 * tile), bf16),
            jax.ShapeDtypeStruct((chunks, rows, tile), bf16),
            jax.ShapeDtypeStruct((chunks, rows, tile), bf16),
            jax.ShapeDtypeStruct((chunks, 8, rows), f32),
            jax.ShapeDtypeStruct((D, 3 * tile), bf16),
            jax.ShapeDtypeStruct((D, D), bf16),
            jax.ShapeDtypeStruct((3, 2, 2, D, lanes), bf16),
            jax.ShapeDtypeStruct((3, 2, 2, D, lanes), bf16),
        ],
        scratch_shapes=[
            pltpu.VMEM((heads, seq, 128), bf16),
            pltpu.VMEM((seq, tile), bf16),
            pltpu.VMEM((2, 8, 128), jnp.int32),
            pltpu.VMEM((share_rows, tile), bf16),
            pltpu.VMEM((3, share_rows, tile), bf16),
            pltpu.SemaphoreType.DMA((2,)),
            pltpu.SemaphoreType.DMA((sems,)),
            pltpu.SemaphoreType.DMA((sems,)),
        ],
        compiler_params=pltpu.CompilerParams(
            vmem_limit_bytes=60 << 20, collective_id=0, has_side_effects=True
        ),
        cost_estimate=pl.CostEstimate(
            flops=24 * heads * seq * seq * HEAD_DIM, bytes_accessed=20 << 20, transcendentals=0
        ),
    )(lengths, tokens, weights)


def back_body(
    info, mixed_ref, context_ref, upstream_ref, lse_ref, weight_ref, branch_ref, norm_ref, outputs_ref, gathered,
    up_grads, down_grads, out_grads,
    input_out, outputs_out, norm_out, attention_out, feed_out,
    keys, turned, key_sum, value_sum, query_t, grad, rows_held, heads_sum, kept, got_one, got_two, got_three,
    leaving, landed, share, heads, heads_one, heads_two, heads_mine, heads_far, out_held, out_core, out_one, out_two, out_z,
    norm_here, norm_there, input_ref, local_sems, send_sems, recv_sems,
):
    chunks, rows, _ = mixed_ref.shape
    width = context_ref.shape[-1]
    scale = HEAD_DIM ** (-0.5)
    part = 256
    core, near_z = peer_of(1, 0), peer_of(0, 1)
    across = (peer_of(2, 0), peer_of(4, 0))
    send = sender(send_sems, recv_sems)
    sources = (up_grads, down_grads)
    y, x, c = bits()
    z = lax.axis_index("tensor")
    matched = c == z // 2
    own_block = block_of(y, x, c)

    def stage_one(b, kind):
        return send(sources[kind].at[b, 1], got_one.at[b, kind], 2 * b + kind, across[kind])

    def stage_two(b, kind):
        return send(kept.at[b, kind, 1], got_two.at[b, kind], 8 + 2 * b + kind, across[1 - kind])

    def stage_three(b):
        return send(kept.at[b, :, 0], got_three.at[b - 1], 15 + b, peer_of(0, b))

    def load(b, kind):
        return pltpu.make_async_copy(
            sources[kind].at[b, 0], kept.at[b, kind], local_sems.at[2 * b + kind]
        )

    def start_one(b):
        for kind in range(2):
            stage_one(b, kind).start()

    def start_two(b):
        for kind in range(2):
            load(b, kind).wait()
            stage_one(b, kind).wait()
            for k in (1, 0):
                kept[b, kind, k] = (
                    kept[b, kind, k].astype(f32) + got_one[b, kind, k].astype(f32)
                ).astype(bf16)
        for kind in range(2):
            stage_two(b, kind).start()

    def start_three(b):
        for kind in range(2):
            stage_two(b, kind).wait()
            kept[b, kind, 0] = (
                kept[b, kind, 0].astype(f32) + got_two[b, kind].astype(f32)
            ).astype(bf16)
        if b:
            stage_three(b).start()

    def load_rows(j):
        return pltpu.make_async_copy(gathered.at[j], rows_held.at[j], local_sems.at[8 + j])

    def out_load():
        return pltpu.make_async_copy(out_grads, out_held, local_sems.at[12])

    def out_core_copy(k):
        at = row_block(block_of(k // 2, k % 2, 1 - c))
        return send(out_grads.at[at, :], out_core.at[k], 22 + k, core)

    out_sums = RowSums(
        send, out_held, lambda yy, xx: block_of(yy, xx, c) * 128, 128, out_one, out_two, 26
    )

    def out_z_copy(e):
        at = (row_block(own_block), slice(e * width, (e + 1) * width))
        return send(out_held.at[at], out_z.at[e - 1], 31 + e, peer_of(0, e))

    def out_start():
        out_load().wait()
        for k in range(4):
            out_core_copy(k).wait()
        for k in range(4):
            at = row_block(block_of(k // 2, k % 2, c))
            out_held[at, :] = (out_held[at, :].astype(f32) + out_core[k].astype(f32)).astype(bf16)
        out_sums.start()

    def out_last():
        out_sums.finish()
        for e in (1, 2, 3):
            out_z_copy(e).start()

    norm_turns = ((1, 0), (2, 0), (4, 0), (0, 1), (0, 2))

    def norm_copy(k):
        return send(norm_here.at[k], norm_there.at[k], 35 + k, peer_of(*norm_turns[k]))

    def norm_step(k):
        norm_copy(k).wait()
        total = norm_here[k] + norm_there[k]
        if k + 1 < len(norm_turns):
            norm_here[k + 1] = total
            norm_copy(k + 1).start()
        else:
            norm_out[...] = total

    for b in (3, 2, 1, 0):
        for kind in range(2):
            load(b, kind).start()
    for j in range(chunks):
        load_rows(j).start()
    out_load().start()
    norm_here[0] = norm_ref[...]
    greet([core, near_z, across[0], across[1], peer_of(0, 2), peer_of(0, 3), peer_of(1, 2)])
    for k in range(4):
        out_core_copy(k).start()
    norm_copy(0).start()
    start_one(3)

    def return_copy(source, target, k):
        return send(source, target, 49 + 4 * GATHER_SEMS + k, peer_of(1, 2))

    outputs_local = pltpu.make_async_copy(outputs_ref, outputs_out, local_sems.at[15])

    @pl.when(matched)
    def _():
        outputs_local.start()

    @pl.when(jnp.logical_not(matched))
    def _():
        return_copy(outputs_ref, outputs_out, 0).start()

    key_sum[...] = jnp.zeros_like(key_sum)
    value_sum[...] = jnp.zeros_like(value_sum)
    for j in range(chunks):
        for h in range(width // HEAD_DIM):
            at = width + (h // 2) * 128
            keys[h, j * rows : (j + 1) * rows, :] = head_keys(
                mixed_ref[j, :, at : at + 128], h % 2, info[1 + j], info[0]
            )
        turned[:, j * rows : (j + 1) * rows] = jnp.transpose(
            mixed_ref[j, :, width : 2 * width].astype(f32)
        ).astype(bf16)
    feature = lax.broadcasted_iota(jnp.int32, (8, width), 1) // HEAD_DIM
    picks = (feature == lax.broadcasted_iota(jnp.int32, (8, width), 0)).astype(f32)
    per_chunk = rows // part

    def attend(step, carry):
        chunk = step // per_chunk
        at = pl.ds(pl.multiple_of((step % per_chunk) * part, part), part)
        upstream = upstream_ref[chunk, at, :]
        product = upstream.astype(f32) * context_ref[chunk, at, :].astype(f32)
        delta = lax.dot_general(
            picks, product, (((1,), (1,)), ((), ())), precision=lax.Precision.HIGHEST,
            preferred_element_type=f32,
        )
        lse = lse_ref[chunk, :, at]
        for pair in range(width // 128):
            lanes = slice(pair * 128, pair * 128 + 128)
            queries = mixed_ref[chunk, at, lanes]
            value_rows = mixed_ref[:, :, 2 * width + pair * 128 : 2 * width + pair * 128 + 128]
            value_rows = value_rows.reshape(chunks * rows, 128)
            for half in range(2):
                h = pair * 2 + half
                scores = contract(keys[h], head_queries(queries, half), 1, 1)
                weight = jnp.exp(scores - lse[h : h + 1, :])
                up_half = head_half(upstream[:, lanes], half)
                back = contract(value_rows, up_half, 1, 1)
                score_grad = (weight * (back - delta[h : h + 1, :])).astype(bf16)
                value_sum[pair] += contract(weight.astype(bf16), up_half, 1, 0)
                key_sum[pair] += contract(score_grad, head_half(queries, half), 1, 0)
                query_t[h * HEAD_DIM : (h + 1) * HEAD_DIM, :] = (
                    contract(turned[h * HEAD_DIM : (h + 1) * HEAD_DIM, :], score_grad, 1, 0) * scale
                )
        grad[chunk, at, :width] = jnp.transpose(query_t[...]).astype(bf16)

        @pl.when(step == 0)
        def _():
            norm_step(0)
            out_start()

        @pl.when(step == 1)
        def _():
            norm_step(1)
            start_two(3)
            start_one(2)

        @pl.when(step == 2)
        def _():
            norm_step(2)
            out_sums.relay()

        @pl.when(step == 3)
        def _():
            norm_step(3)
            out_last()

        @pl.when(step == 4)
        def _():
            norm_step(4)
            start_two(2)
            start_one(1)
            start_three(3)

        return carry

    lax.fori_loop(0, chunks * per_chunk, attend, 0)
    for j in range(chunks):
        at = slice(j * rows, (j + 1) * rows)
        for pair in range(width // 128):
            left = width + pair * 128
            grad[j, :, left : left + 128] = (key_sum[pair, at, :] * scale).astype(bf16)
            grad[j, :, left + width : left + width + 128] = value_sum[pair, at, :].astype(bf16)
    start_two(1)
    start_one(0)
    start_three(2)

    def rows_back(j):
        return contract(grad[j], weight_ref[...], 1, 1)

    core_copies = {}
    for k, j in enumerate((3, 1)):
        leaving[k] = rows_back(j).astype(bf16)
        core_copies[j] = send(leaving.at[k], landed.at[k], 19 + k, core)
        core_copies[j].start()
    far = rows_back(2)
    core_copies[3].wait()
    leaving[2] = (far + landed[0].astype(f32)).astype(bf16)
    far_copy = send(leaving.at[2], landed.at[2], 21, near_z)
    branch_ref_value = branch_ref[...] + rows_back(0)
    far_copy.start()
    core_copies[1].wait()
    own_rows = branch_ref_value + landed[1].astype(f32)

    heads_sum[...] = jnp.zeros_like(heads_sum)
    for j in range(chunks):
        load_rows(j).wait()

    def weigh(j, carry):
        heads_sum[...] += contract(rows_held[j], grad[j], 0, 0)
        return carry

    lax.fori_loop(0, chunks, weigh, 0)
    heads[...] = heads_sum[...].astype(bf16)
    start_two(0)
    head_sums = RowSums(
        send, heads, lambda yy, xx: block_of(yy, xx, 0) * 128, 256, heads_one, heads_two, 40
    )
    head_sums.start()
    start_three(1)
    far_copy.wait()
    input_ref[...] = (own_rows + landed[2].astype(f32)).astype(bf16)
    start_three(0)
    head_sums.relay()

    @pl.when(matched)
    def _():
        input_out[...] = input_ref[...]

    @pl.when(jnp.logical_not(matched))
    def _():
        return_copy(input_ref, input_out, 1).start()

    total = kept[0, :, 0].astype(f32)
    for b in (3, 2, 1):
        stage_three(b).wait()
        total = total + got_three[b - 1].astype(f32)
    share[...] = total.astype(bf16)
    own_feed = [
        pltpu.make_async_copy(share.at[kind], feed_out.at[own_block, kind], local_sems.at[13 + kind])
        for kind in range(2)
    ]
    for copy in own_feed:
        copy.start()
    head_sums.finish()

    def half_rows(k):
        return row_block(block_of(y, x, k))

    @pl.when(matched)
    def _():
        send(heads.at[half_rows(1 - c), :], heads_mine, 46, core).start()

    @pl.when(jnp.logical_not(matched))
    def _():
        send(heads.at[half_rows(c), :], heads_far, 47, peer_of(0, 2)).start()
        send(heads.at[half_rows(1 - c), :], heads_far, 48, peer_of(1, 2)).start()

    feeds = [
        Gather(send, lambda k, kind=kind: feed_out.at[k, kind], 49 + kind * GATHER_SEMS, kind == 0)
        for kind in range(2)
    ]
    for copy in own_feed:
        copy.wait()
    for feed in feeds:
        feed.start()
    sum_out = out_held[row_block(own_block), :width].astype(f32)
    for e in (1, 2, 3):
        out_z_copy(e).wait()
        sum_out = sum_out + out_z[e - 1].astype(f32)
    attention_out[row_block(own_block), 3 * width :] = sum_out.astype(bf16)

    @pl.when(matched)
    def _():
        send(heads.at[half_rows(1 - c), :], heads_mine, 46, core).wait_send()
        heads_mine[...] = heads[half_rows(c), :]

    @pl.when(jnp.logical_not(matched))
    def _():
        send(heads.at[half_rows(c), :], heads_far, 47, peer_of(0, 2)).wait_send()
        send(heads.at[half_rows(1 - c), :], heads_far, 48, peer_of(1, 2)).wait_send()
        send(heads.at[half_rows(c), :], heads_mine, 46, core).wait_recv()

    @pl.when(matched)
    def _():
        send(heads.at[half_rows(c), :], heads_far, 47, peer_of(0, 2)).wait_recv()

    @pl.when(jnp.logical_not(matched))
    def _():
        send(heads.at[half_rows(c), :], heads_far, 48, peer_of(1, 2)).wait_recv()

    attention_out[row_block(own_block), : 3 * width] = (
        heads_mine[...].astype(f32) + heads_far[...].astype(f32)
    ).astype(bf16)
    sides = [
        Gather(
            send,
            lambda k, side=side: attention_out.at[row_block(k), side * 2 * width : (side + 1) * 2 * width],
            49 + (2 + side) * GATHER_SEMS, side == 0,
        )
        for side in range(2)
    ]
    for side in sides:
        side.start()
    for gather in feeds + sides:
        gather.relay()
    for gather in feeds + sides:
        gather.last()
    for gather in feeds + sides:
        gather.finish()
    @pl.when(matched)
    def _():
        outputs_local.wait()

    @pl.when(jnp.logical_not(matched))
    def _():
        return_copy(outputs_ref, outputs_out, 0).wait()
        return_copy(input_ref, input_out, 1).wait()


def back_block(info, mixed, context, upstream, lse, weight, branch, norm_sums, outputs, gathered, up_grads,
               down_grads, out_grads):
    chunks, rows, width3 = mixed.shape
    width = width3 // 3
    seq = chunks * rows
    heads = width // HEAD_DIM
    lanes = up_grads.shape[-1]
    share_rows = D // SHARE
    sems = 51 + 4 * GATHER_SEMS
    vmem, anywhere = pl.BlockSpec(memory_space=pltpu.VMEM), pl.BlockSpec(memory_space=pl.ANY)
    return pl.pallas_call(
        back_body,
        name="back_block",
        in_specs=[pl.BlockSpec(memory_space=pltpu.SMEM)] + [vmem] * 7 + [anywhere] * 5,
        out_specs=[vmem, vmem, vmem, vmem, anywhere],
        out_shape=[
            jax.ShapeDtypeStruct((rows, D), bf16),
            jax.ShapeDtypeStruct((rows, D), bf16),
            jax.ShapeDtypeStruct((4, D), f32),
            jax.ShapeDtypeStruct((D, 4 * width), bf16),
            jax.ShapeDtypeStruct((SHARE, 2, D, lanes), bf16),
        ],
        scratch_shapes=[
            pltpu.VMEM((heads, seq, 128), bf16),
            pltpu.VMEM((width, seq), bf16),
            pltpu.VMEM((width // 128, seq, 128), f32),
            pltpu.VMEM((width // 128, seq, 128), f32),
            pltpu.VMEM((width, 256), f32),
            pltpu.VMEM((chunks, rows, width3), bf16),
            pltpu.VMEM((chunks, rows, D), bf16),
            pltpu.VMEM((D, width3), f32),
            pltpu.VMEM((4, 2, 2, D, lanes), bf16),
            pltpu.VMEM((4, 2, 2, D, lanes), bf16),
            pltpu.VMEM((4, 2, D, lanes), bf16),
            pltpu.VMEM((3, 2, D, lanes), bf16),
            pltpu.VMEM((3, rows, D), bf16),
            pltpu.VMEM((3, rows, D), bf16),
            pltpu.VMEM((2, D, lanes), bf16),
            pltpu.VMEM((D, width3), bf16),
            pltpu.VMEM((2, 2, 2 * share_rows, width3 // 2), bf16),
            pltpu.VMEM((2, 2 * share_rows, width3 // 2), bf16),
            pltpu.VMEM((share_rows, width3), bf16),
            pltpu.VMEM((share_rows, width3), bf16),
            pltpu.VMEM((D, 4 * width), bf16),
            pltpu.VMEM((4, share_rows, 4 * width), bf16),
            pltpu.VMEM((2, 2, share_rows, 2 * width), bf16),
            pltpu.VMEM((2, share_rows, 2 * width), bf16),
            pltpu.VMEM((3, share_rows, width), bf16),
            pltpu.VMEM((5, 4, D), f32),
            pltpu.VMEM((5, 4, D), f32),
            pltpu.VMEM((rows, D), bf16),
            pltpu.SemaphoreType.DMA((16,)),
            pltpu.SemaphoreType.DMA((sems,)),
            pltpu.SemaphoreType.DMA((sems,)),
        ],
        compiler_params=pltpu.CompilerParams(
            vmem_limit_bytes=67043328, collective_id=2, has_side_effects=True
        ),
        cost_estimate=pl.CostEstimate(
            flops=40 * heads * seq * seq * HEAD_DIM, bytes_accessed=40 << 20, transcendentals=0
        ),
    )(
        info, mixed, context, upstream, lse, weight, branch, norm_sums, outputs, gathered, up_grads, down_grads,
        out_grads,
    )


def adam_body(owned, attention_ref, feed_ref, master_ref, one_ref, two_ref,
              grad_out, master_out, one_out, two_out, tiles_out, up_out, down_out):
    tile = grad_out.shape[-1] // 4
    for s in range(4):
        at = slice(s * tile, (s + 1) * tile)
        grad = jnp.zeros((grad_out.shape[0], tile), f32)
        for i in range(4):
            value = attention_ref[:, i * tile : (i + 1) * tile].astype(f32)
            grad = jnp.where(owned[s, i] > 0, value, grad)
        for kind in range(2):
            value = jnp.concatenate([feed_ref[2 * s + k, kind] for k in range(2)], axis=-1)
            grad = jnp.where(owned[s, 4 + 4 * kind + s] > 0, value.astype(f32), grad)
        occupied = (owned[s, 12] > 0).astype(f32)
        param, first, second = adam_update(
            grad, master_ref[:, at], one_ref[:, at], two_ref[:, at], occupied, weight_decay
        )
        grad_out[:, at] = grad
        master_out[:, at] = param
        one_out[:, at] = first
        two_out[:, at] = second
        low = param.astype(bf16)
        none = jnp.zeros_like(low)
        for i in range(4):
            mine = jnp.where(owned[s, i] > 0, low, none)
            there = slice(i * tile, (i + 1) * tile)
            tiles_out[:, there] = mine if s == 0 else tiles_out[:, there] + mine
        for kind, target in ((0, up_out), (1, down_out)):
            mine = jnp.where(owned[s, 4 + 4 * kind + s] > 0, low, none)
            for k in range(2):
                target[2 * s + k] = mine[:, k * tile // 2 : (k + 1) * tile // 2]


def adam_block(owned, attention_grad, feed_grad, master, one, two):
    part = 128
    wide = pl.BlockSpec((part, D), lambda i: (i, 0))
    lanes = feed_grad.shape[-1]
    split = pl.BlockSpec((SHARE, part, lanes), lambda i: (0, i, 0))
    return pl.pallas_call(
        adam_body,
        grid=(D // part,),
        name="adam_block",
        in_specs=[
            pl.BlockSpec(memory_space=pltpu.SMEM), wide,
            pl.BlockSpec((SHARE, 2, part, lanes), lambda i: (0, 0, i, 0)), wide, wide, wide,
        ],
        out_specs=[wide] * 5 + [split] * 2,
        out_shape=[jax.ShapeDtypeStruct((D, D), f32)] * 4
        + [jax.ShapeDtypeStruct((D, D), bf16)]
        + [jax.ShapeDtypeStruct((SHARE, D, lanes), bf16)] * 2,
        compiler_params=pltpu.CompilerParams(vmem_limit_bytes=32 << 20),
        cost_estimate=pl.CostEstimate(flops=40 * D * D, bytes_accessed=40 << 20, transcendentals=0),
    )(owned, attention_grad, feed_grad, master, one, two)


def tiles_body(tiles_ref, up_ref, down_ref, tiles_out, up_out, down_out, *scratch):
    core_got = scratch[:3]
    one_got, two_got = scratch[3:5], scratch[5:7]
    work = scratch[7:10]
    row_one, row_two, send_sems, recv_sems = scratch[10:]
    send = sender(send_sems, recv_sems)
    y, x, c = bits()
    core = peer_of(1, 0)
    own_block = block_of(y, x, c)
    greet([core, peer_of(2, 0), peer_of(4, 0)])
    arrays = ((up_ref, up_out), (down_ref, down_out), (tiles_ref, tiles_out))

    def place(n, ref, block):
        return ref.at[row_block(block), :] if n == 2 else ref.at[block]

    def core_copy(n, k):
        return send(
            place(n, arrays[n][0], block_of(k // 2, k % 2, 1 - c)), core_got[n].at[k], 4 * n + k, core
        )

    def core_add(n):
        source, target = arrays[n][0], work[n]
        for k in range(4):
            core_copy(n, k).wait()
        for k in range(4):
            block = block_of(k // 2, k % 2, c)
            if n == 2:
                at = row_block(block)
                target[at, :] = source[at, :] + core_got[n][k]
            else:
                target[k] = source[block] + core_got[n][k]

    def first(n, k):
        y_, x_ = ((k, 1 - x), (1 - y, k))[n]
        return send(
            work[n].at[2 * y_ + x_], one_got[n].at[k], 12 + 2 * n + k,
            peer_of((2, 4)[n], 0),
        )

    def second(n):
        y_, x_ = ((1 - y, x), (y, 1 - x))[n]
        return send(
            work[n].at[2 * y_ + x_], two_got[n], 16 + n, peer_of((4, 2)[n], 0)
        )

    def relay(n):
        target = work[n]
        for k in range(2):
            first(n, k).wait()
        for k in range(2):
            y_, x_ = ((k, x), (y, k))[n]
            block = 2 * y_ + x_
            target[block] = target[block] + one_got[n][k]
        second(n).start()

    def settle(n):
        second(n).wait()
        arrays[n][1][own_block] = work[n][2 * y + x] + two_got[n][...]

    for n in range(3):
        for k in range(4):
            core_copy(n, k).start()
    for n in range(2):
        core_add(n)
        for k in range(2):
            first(n, k).start()
    core_add(2)
    rows = RowSums(
        send, work[2], lambda yy, xx: block_of(yy, xx, c) * 128, 128, row_one, row_two, 18
    )
    rows.start()
    for n in range(2):
        relay(n)
    rows.relay()
    gathers = []
    for n in range(2):
        settle(n)
        gathers.append(
            Gather(send, lambda k, n=n: arrays[n][1].at[k], 24 + n * GATHER_SEMS, n == 0)
        )
        gathers[-1].start()
    rows.finish()
    tiles_out[row_block(own_block), :] = work[2][row_block(own_block), :]
    half = tiles_out.shape[-1] // 2
    for side in range(2):
        gathers.append(
            Gather(
                send,
                lambda k, side=side: tiles_out.at[row_block(k), side * half : (side + 1) * half],
                24 + (2 + side) * GATHER_SEMS, side == 0,
            )
        )
        gathers[-1].start()
    for gather in gathers:
        gather.relay()
    for gather in gathers:
        gather.last()
    for gather in gathers:
        gather.finish()


def spread_tiles(tiles, up, down):
    share_rows = D // SHARE
    lanes = up.shape[-1]
    sems = 24 + 4 * GATHER_SEMS
    piece = (D, lanes)
    vmem = pl.BlockSpec(memory_space=pltpu.VMEM)
    return pl.pallas_call(
        tiles_body,
        name="spread_tiles",
        in_specs=[vmem] * 3,
        out_specs=[vmem] * 3,
        out_shape=[jax.ShapeDtypeStruct(v.shape, bf16) for v in (tiles, up, down)],
        scratch_shapes=[
            pltpu.VMEM((4,) + piece, bf16),
            pltpu.VMEM((4,) + piece, bf16),
            pltpu.VMEM((4, share_rows, D), bf16),
            pltpu.VMEM((2,) + piece, bf16),
            pltpu.VMEM((2,) + piece, bf16),
            pltpu.VMEM(piece, bf16),
            pltpu.VMEM(piece, bf16),
            pltpu.VMEM((4,) + piece, bf16),
            pltpu.VMEM((4,) + piece, bf16),
            pltpu.VMEM((D, D), bf16),
            pltpu.VMEM((2, 2, share_rows, D // 2), bf16),
            pltpu.VMEM((2, share_rows, D // 2), bf16),
            pltpu.SemaphoreType.DMA((sems,)),
            pltpu.SemaphoreType.DMA((sems,)),
        ],
        compiler_params=pltpu.CompilerParams(
            vmem_limit_bytes=48 << 20, collective_id=3, has_side_effects=True
        ),
        cost_estimate=pl.CostEstimate(flops=D * D, bytes_accessed=12 << 20, transcendentals=0),
    )(tiles, up, down)


def joined(held, i, kind):
    return jnp.concatenate(
        [held[kind, 2 * (i // 2) + m, i % 2, k] for k in range(2) for m in range(2)], axis=-1
    )


def gelu_parts(value):
    bell = jnp.exp(-0.5 * value * value)
    t = 1.0 / (1.0 + (0.3275911 * 0.5**0.5) * jnp.abs(value))
    tail = 0.5 * 1.061405429
    for c in (-1.453152027, 1.421413741, -0.284496736, 0.254829592):
        tail = tail * t + 0.5 * c
    tail = tail * t * bell
    area = jnp.where(value > 0, 1.0 - tail, tail)
    return value * area, area + value * bell * (0.5 / jnp.pi) ** 0.5


def feed_body(
    info, first_ref, cotangent_ref, norms_ref, weights_ref, up_ref, down_ref,
    out_ref, low_ref, both_ref, hidden_ref, pre_ref, grad_ref, sums_ref,
    held, slope, total, leaving, landed, local_sems, send_sems, recv_sems,
):
    rows = first_ref.shape[0]
    steps = hidden_ref.shape[0]
    lanes = held.shape[-1]
    y, x, c = bits()
    peer = peer_of(1, 0)
    send = sender(send_sems, recv_sems)
    half = slice(0, D // 2), slice(D // 2, D)
    loads = []
    for kind in range(2):
        for dy in range(2):
            for dx in range(2):
                block = block_of(1 - y if dy else y, 1 - x if dx else x, c)
                at = D + kind * SHARE * lanes + block * lanes
                loads.append(
                    (weights_ref.at[:, pl.ds(pl.multiple_of(at, 128), lanes)], held.at[kind, 0, dy, dx])
                )
    loads.append((up_ref, held.at[0, 1:4]))
    loads.append((down_ref.at[:, 0, 0:2, half[0], :], held.at[1, 1:4, 0, 0:2, half[0], :]))
    loads.append((down_ref.at[:, 0:2, 0, half[1], :], held.at[1, 1:4, 0:2, 0, half[1], :]))
    loads = [pltpu.make_async_copy(a, b, local_sems.at[k]) for k, (a, b) in enumerate(loads)]
    for load in loads:
        load.start()
    greet([peer, peer_of(2, 0), peer_of(4, 0)])
    hops = [
        send(
            down_ref.at[:, 0, 0:2, half[0], :], held.at[1, 1:4, 1, 0:2, half[0], :], 4, peer_of(4, 0)
        ),
        send(
            down_ref.at[:, 0:2, 0, half[1], :], held.at[1, 1:4, 0:2, 1, half[1], :], 5, peer_of(2, 0)
        ),
    ]
    for hop in hops:
        hop.start()

    def across(source, target, k):
        return send(source, target, k, peer)

    middle_row = rows // 2
    both_ref[0] = first_ref[...].astype(bf16)
    first_copy = across(both_ref.at[0], both_ref.at[1], 0)
    first_copy.start()

    def up(i, slot):
        weight = joined(held, i, 0)
        for r in range(0, rows, middle_row):
            at = slice(r, r + middle_row)
            value = jnp.dot(both_ref[slot, at, :], weight, preferred_element_type=f32)
            hidden, steep = gelu_parts(value)
            hidden_ref[i, slot, at, :] = hidden.astype(bf16)
            slope[i, slot, at, :] = steep.astype(bf16)

    def down(i, slot):
        total[slot] += contract(hidden_ref[i, slot], joined(held, i, 1), 1, 1)

    def back(i, slot):
        weight = joined(held, i, 1)
        for r in range(0, rows, middle_row):
            at = slice(r, r + middle_row)
            value = jnp.dot(low_ref[slot, at, :], weight, preferred_element_type=f32)
            pre_ref[i, slot, at, :] = (value * slope[i, slot, at, :].astype(f32)).astype(bf16)

    def back_up(i, slot):
        total[slot] += contract(pre_ref[i, slot], joined(held, i, 0), 1, 1)

    def loop(*works):
        def body(i, carry):
            for work in works:
                work(i)
            return carry

        lax.fori_loop(0, steps, body, 0)

    total[...] = jnp.zeros_like(total)
    for load in loads:
        load.wait()
    loop(lambda i: up(i, 0))
    first_copy.wait()
    for hop in hops:
        hop.wait()
    loop(lambda i: up(i, 1), lambda i: down(i, 1))
    leaving[...] = total[1].astype(bf16)
    feed_copy = across(leaving, landed.at[0], 1)
    feed_copy.start()
    loop(lambda i: down(i, 0))
    feed_copy.wait()

    sums_ref[...] = jnp.zeros_like(sums_ref)
    part = 128

    def middle(r, carry):
        at = pl.ds(pl.multiple_of(r * part, part), part)
        second, normed, inverse = norm_parts(
            first_ref[at, :] + (total[0, at, :] + landed[0, at, :].astype(f32)),
            norms_ref[2:3, :], norms_ref[3:4, :],
        )
        out_ref[at, :] = second.astype(bf16)
        row = lax.broadcasted_iota(jnp.int32, (part, 1), 0) + r * part + info[1]
        seed = cotangent_ref[at, :].astype(f32) * (row < info[0]).astype(f32)
        grad = norm_back(seed, normed, inverse, norms_ref[2:3, :])
        sums_ref[0:1, :] += jnp.sum(seed * normed, axis=0, keepdims=True)
        sums_ref[1:2, :] += jnp.sum(seed, axis=0, keepdims=True)
        total[0, at, :] = grad
        low_ref[0, at, :] = grad.astype(bf16)
        return carry

    lax.fori_loop(0, rows // part, middle, 0)
    low_copy = across(low_ref.at[0], low_ref.at[1], 2)
    low_copy.start()
    total[1] = jnp.zeros_like(total[1])
    loop(lambda i: back(i, 0))
    low_copy.wait()
    loop(lambda i: back(i, 1), lambda i: back_up(i, 1))
    leaving[...] = total[1].astype(bf16)
    grad_copy = across(leaving, landed.at[1], 3)
    grad_copy.start()
    loop(lambda i: back_up(i, 0))
    grad_copy.wait()
    grad_ref[...] = total[0] + landed[1].astype(f32)


def feed_block(info, first, cotangent, norms, weights, up, down):
    rows = first.shape[0]
    lanes = up.shape[-1]
    width = 4 * lanes
    vmem, anywhere = pl.BlockSpec(memory_space=pltpu.VMEM), pl.BlockSpec(memory_space=pl.ANY)
    return pl.pallas_call(
        feed_body,
        name="feed_block",
        in_specs=[pl.BlockSpec(memory_space=pltpu.SMEM)] + [vmem] * 3 + [anywhere] * 3,
        out_specs=[vmem] * 7,
        out_shape=[
            jax.ShapeDtypeStruct((rows, D), bf16),
            jax.ShapeDtypeStruct((2, rows, D), bf16),
            jax.ShapeDtypeStruct((2, rows, D), bf16),
            jax.ShapeDtypeStruct((4, 2, rows, width), bf16),
            jax.ShapeDtypeStruct((4, 2, rows, width), bf16),
            jax.ShapeDtypeStruct((rows, D), f32),
            jax.ShapeDtypeStruct((2, D), f32),
        ],
        scratch_shapes=[
            pltpu.VMEM((2, 4, 2, 2, D, lanes), bf16),
            pltpu.VMEM((4, 2, rows, width), bf16),
            pltpu.VMEM((2, rows, D), f32),
            pltpu.VMEM((rows, D), bf16),
            pltpu.VMEM((2, rows, D), bf16),
            pltpu.SemaphoreType.DMA((11,)),
            pltpu.SemaphoreType.DMA((6,)),
            pltpu.SemaphoreType.DMA((6,)),
        ],
        compiler_params=pltpu.CompilerParams(
            vmem_limit_bytes=60 << 20, collective_id=1, has_side_effects=True
        ),
        cost_estimate=pl.CostEstimate(
            flops=64 * rows * D * width, bytes_accessed=30 << 20, transcendentals=0
        ),
    )(info, first, cotangent, norms, weights, up, down)


def feed_grads_body(first_ref, low_ref, hidden_ref, pre_ref, up_ref, down_ref, first_t, low_t):
    rows = first_ref.shape[1]

    @pl.when(pl.program_id(0) == 0)
    def _():
        for slot in range(2):
            at = slice(slot * rows, (slot + 1) * rows)
            first_t[:, at] = jnp.transpose(first_ref[slot].astype(f32)).astype(bf16)
            low_t[:, at] = jnp.transpose(low_ref[slot].astype(f32)).astype(bf16)

    lanes = up_ref.shape[-1]
    width = pre_ref.shape[-1]
    for target, source, turned in ((up_ref, pre_ref, first_t), (down_ref, hidden_ref, low_t)):
        grad = jnp.dot(
            turned[...], source[0].reshape(2 * rows, width), preferred_element_type=f32
        ).astype(bf16)
        for k in range(2):
            for m in range(2):
                at = (2 * k + m) * lanes
                if target is up_ref:
                    target[m, k, 0] = grad[:, at : at + lanes]
                else:
                    target[m, 0, k] = grad[:, at : at + lanes]


def feed_grads(first, low, hidden, pre):
    count, _, rows, width = hidden.shape
    full = pl.BlockSpec((2, rows, D), lambda i: (0, 0, 0))
    piece = pl.BlockSpec((1, 2, rows, width), lambda i: (i, 0, 0, 0))
    lanes = width // 4
    return pl.pallas_call(
        feed_grads_body,
        grid=(count,),
        name="feed_grads",
        in_specs=[full, full, piece, piece],
        out_specs=[
            pl.BlockSpec((2, 2, 1, D, lanes), lambda i: (i // 2, 0, i % 2, 0, 0)),
            pl.BlockSpec((2, 1, 2, D, lanes), lambda i: (i // 2, i % 2, 0, 0, 0)),
        ],
        out_shape=[jax.ShapeDtypeStruct((count, 2, 2, D, lanes), bf16)] * 2,
        scratch_shapes=[pltpu.VMEM((D, 2 * rows), bf16), pltpu.VMEM((D, 2 * rows), bf16)],
        compiler_params=pltpu.CompilerParams(vmem_limit_bytes=48 << 20),
        cost_estimate=pl.CostEstimate(
            flops=8 * rows * D * width * count, bytes_accessed=20 << 20, transcendentals=0
        ),
    )(first, low, hidden, pre)


def layer(n_dp, n_tensor, tokens, weights, norms, cotangent, lengths, owners, master, moment_one,
          moment_two, norm_master, norm_one, norm_two):
    tile = D // n_tensor
    rows = tokens.shape[0]
    device = lax.axis_index("dp")
    z = lax.axis_index("tensor")
    core = device % 2
    matched = core == z // 2
    quarter = jnp.where(matched, z, z ^ 2)

    def flip(x, dd, dz):
        pairs = [
            (d * n_tensor + t, (d ^ dd) * n_tensor + (t ^ dz))
            for d in range(n_dp)
            for t in range(n_tensor)
        ]
        return lax.ppermute(x, AXES, pairs)

    def some(x, dd, dz, want):
        pairs = [
            (d * n_tensor + t, (d ^ dd) * n_tensor + (t ^ dz))
            for d in range(n_dp)
            for t in range(n_tensor)
            if (t // 2 == d % 2) == want
        ]
        return lax.ppermute(x, AXES, pairs)

    def swap(x):
        return jnp.where(matched, x, some(x, 1, 2, False))

    length = jnp.where(matched, lengths, flip(lengths, 1, 0))[0]
    base = jnp.stack([quarter ^ k for k in (0, 2, 1, 3)]) * rows
    info = jnp.concatenate([length[None], base]).astype(jnp.int32)

    gathered, mixed, context, parts, lse, w_heads, w_out_all, up_all, down_all = start_block(
        lengths, tokens[:, 0, :], weights
    )
    own = gathered[0]

    context_all = jnp.where(
        matched,
        jnp.concatenate([parts[k] for k in (0, 2, 1, 3)], axis=1),
        jnp.concatenate([parts[k] for k in (1, 3, 0, 2)], axis=1),
    )
    branch = contract(context_all, w_out_all, 1, 1)
    first, first_normed, first_inverse = norm_parts(
        own.astype(f32) + branch, norms[0], norms[1]
    )
    seed = swap(cotangent[:, 0, :])
    outputs, both_low, both_first, hidden, pre_grad, first_grad, sums_two = feed_block(
        info, first, seed, norms, weights, up_all, down_all
    )
    branch_grad = norm_back(first_grad, first_normed, first_inverse, norms[0])
    gain_one = jnp.sum(first_grad * first_normed, axis=0)
    shift_one = jnp.sum(first_grad, axis=0)
    branch_low = branch_grad.astype(bf16)
    context_grad = jnp.dot(branch_low, w_out_all, preferred_element_type=f32).astype(bf16)
    blocks = [context_grad[:, k * tile : (k + 1) * tile] for k in range(4)]
    blocks = [
        jnp.where(matched, blocks[a], blocks[b]) for a, b in ((0, 2), (2, 0), (1, 3), (3, 1))
    ]
    upstream = jnp.stack(
        [blocks[0], flip(blocks[1], 1, 0), flip(blocks[2], 0, 1), flip(blocks[3], 1, 1)]
    )

    def add(a, b):
        return (a.astype(f32) + b.astype(f32)).astype(bf16)

    up_grads, down_grads = feed_grads(both_first, both_low, hidden, pre_grad)
    out_grad = contract(branch_low, context_all, 0, 0).astype(bf16)
    norm_sums = jnp.concatenate([jnp.stack([gain_one, shift_one]), sums_two])
    input_grad, outputs, norm_grads, attention_grad, feed_grad = back_block(
        info, mixed, context, upstream, lse, w_heads, branch_grad, norm_sums, outputs, gathered, up_grads, down_grads,
        out_grad,
    )

    def over_groups(value, combine):
        bit = SHARE
        while bit < n_dp:
            value = combine(value, flip(value, bit, 0))
            bit *= 2
        return value

    def plus(a, b):
        return a + b

    norm_grads = over_groups(norm_grads, plus)
    attention_grad = over_groups(attention_grad, add)
    feed_grad = over_groups(feed_grad, add)

    tile_owner, slot_index = slot_table(owners)
    slot_ids = jnp.arange(FF // D, dtype=jnp.int32)
    owned = (
        (tile_owner[None, :] == device) & (slot_index[None, :] == slot_ids[:, None])
    ).astype(jnp.int32)
    owned = jnp.concatenate([owned, jnp.sum(owned, axis=1, keepdims=True)], axis=1)
    slot_grad, new_master, new_one, new_two, tiles, up_tiles, down_tiles = adam_block(
        owned, attention_grad, feed_grad, master[0], moment_one[0], moment_two[0]
    )
    tiles, up_tiles, down_tiles = (
        over_groups(v, plus) for v in spread_tiles(tiles, up_tiles, down_tiles)
    )
    new_weights = jnp.concatenate(
        [tiles] + [up_tiles[k] for k in range(SHARE)] + [down_tiles[k] for k in range(SHARE)], axis=1
    )
    norm_owner = (device == owners[6]).astype(f32)
    new_norm_master, new_norm_one, new_norm_two = adam_update(
        norm_grads, norm_master[0], norm_one[0], norm_two[0], norm_owner, 0.0
    )
    return (
        outputs[:, None, :],
        input_grad[:, None, :],
        slot_grad[None],
        new_master[None],
        new_one[None],
        new_two[None],
        new_weights,
        norm_grads,
        new_norm_master[None],
        new_norm_one[None],
        new_norm_two[None],
    )


def solution(mesh):
    in_specs = (
        P("tensor", "dp", None),
        P(None, "tensor"),
        P(),
        P("tensor", "dp", None),
        P("dp"),
        P(),
        P("dp", None, "tensor"),
        P("dp", None, "tensor"),
        P("dp", None, "tensor"),
        P("dp", None, None),
        P("dp", None, None),
        P("dp", None, None),
    )
    out_specs = (
        P("tensor", "dp", None),
        P("tensor", "dp", None),
        P("dp", None, "tensor"),
        P("dp", None, "tensor"),
        P("dp", None, "tensor"),
        P("dp", None, "tensor"),
        P(None, "tensor"),
        P(),
        P("dp", None, None),
        P("dp", None, None),
        P("dp", None, None),
    )
    return jax.shard_map(
        partial(layer, mesh.shape["dp"], mesh.shape["tensor"]),
        mesh=mesh,
        in_specs=in_specs,
        out_specs=out_specs,
        check_vma=False,
    )
```

```python
from functools import partial

import jax
import jax.numpy as jnp
from jax import lax
from jax.experimental import pallas as pl
from jax.experimental.pallas import tpu as pltpu
from jax.sharding import PartitionSpec as P

D = 1024
FF = 4096
ADAM_STEP = 10
HEAD_DIM = 64
SHARE = 8


f32, bf16 = jnp.float32, jnp.bfloat16
beta_one = 0.9
beta_two = 0.999
learn_rate = 0.02
weight_decay = 0.1
adam_eps = 1e-08
norm_eps = 1e-05
masked_score = -1e30
AXES = ("dp", "tensor")


def contract(a, b, ca, cb):
    return lax.dot_general(a, b, (((ca,), (cb,)), ((), ())), preferred_element_type=f32)


def norm_parts(value, gain, shift):
    average = jnp.mean(value, axis=-1, keepdims=True)
    centred = value - average
    variance = jnp.mean(centred * centred, axis=-1, keepdims=True)
    inverse = lax.rsqrt(variance + norm_eps)
    normed = centred * inverse
    return normed * gain + shift, normed, inverse


def norm_back(upstream, normed, inverse, gain):
    scaled = upstream * gain
    inner = (
        scaled
        - jnp.mean(scaled, axis=-1, keepdims=True)
        - normed * jnp.mean(scaled * normed, axis=-1, keepdims=True)
    )
    return inner * inverse


def slot_table(owners):
    repeat = FF // D
    tile_matrix = jnp.array([0, 1, 2, 3] + [4] * repeat + [5] * repeat, dtype=jnp.int32)
    choose = (tile_matrix[:, None] == jnp.arange(7, dtype=jnp.int32)[None, :]).astype(jnp.int32)
    tile_owner = jnp.sum(choose * owners[None, :], axis=1)
    position = jnp.arange(tile_matrix.shape[0], dtype=jnp.int32)
    before = (tile_owner[None, :] == tile_owner[:, None]) & (position[None, :] < position[:, None])
    slot_index = jnp.sum(before.astype(jnp.int32), axis=1)
    return (tile_owner, slot_index)


def adam_update(grad, param, first, second, occupied, decay_rate):
    first_new = occupied * (beta_one * first + (1.0 - beta_one) * grad)
    second_new = occupied * (beta_two * second + (1.0 - beta_two) * grad * grad)
    correct_one = 1.0 - beta_one**ADAM_STEP
    correct_two = 1.0 - beta_two**ADAM_STEP
    direction = first_new / correct_one / (jnp.sqrt(second_new / correct_two) + adam_eps)
    param_new = occupied * (param - learn_rate * (direction + decay_rate * param))
    return (param_new, first_new, second_new)


def head_keys(keys, half, start, length):
    lane = lax.broadcasted_iota(jnp.int32, keys.shape, 1)
    row = lax.broadcasted_iota(jnp.int32, keys.shape, 0)
    bias = jnp.where(start + row < length, 0.0, masked_score).astype(f32)
    extra = jnp.where(lane == (1 - half) * HEAD_DIM, bias, 0.0)
    return jnp.where(lane // HEAD_DIM == half, keys.astype(f32), extra).astype(bf16)


def head_half(rows, half):
    lane = lax.broadcasted_iota(jnp.int32, rows.shape, 1)
    return jnp.where(lane // HEAD_DIM == half, rows, jnp.zeros_like(rows))


def head_queries(rows, half):
    lane = lax.broadcasted_iota(jnp.int32, rows.shape, 1)
    scaled = rows.astype(f32) * HEAD_DIM ** (-0.5)
    extra = jnp.where(lane == (1 - half) * HEAD_DIM, 1.0, 0.0)
    return jnp.where(lane // HEAD_DIM == half, scaled, extra).astype(bf16)


def peer_of(bit, turn):
    device, z = lax.axis_index("dp"), lax.axis_index("tensor")
    for one in (1, 2, 4):
        if bit & one:
            device = device + one - 2 * one * ((device // one) % 2)
    if turn == 1:
        z = z + 1 - 2 * (z % 2)
    elif turn == 2:
        z = z + 2 - 4 * (z // 2)
    elif turn == 3:
        z = 3 - z
    return (device, z)


def greet(peers):
    barrier = pltpu.get_barrier_semaphore()
    for peer in peers:
        pl.semaphore_signal(barrier, inc=1, device_id=peer, device_id_type=pl.DeviceIdType.MESH)
    pl.semaphore_wait(barrier, len(peers))


def sender(send_sems, recv_sems):
    def send(source, target, k, peer):
        return pltpu.make_async_remote_copy(
            source, target, send_sems.at[k], recv_sems.at[k], device_id=peer,
            device_id_type=pl.DeviceIdType.MESH,
        )

    return send


def bits():
    device = lax.axis_index("dp")
    return (device // 4) % 2, (device // 2) % 2, device % 2


def block_of(y, x, c):
    return 4 * y + 2 * x + c


def row_block(index, count=1):
    rows = D // SHARE
    return pl.ds(pl.multiple_of(index * rows, rows), count * rows)


class Gather:
    def __init__(self, send, view, first_sem, x_first):
        self.send, self.view, self.sem = send, view, first_sem
        self.y, self.x, self.c = bits()
        self.one, self.two = (2, 4) if x_first else (4, 2)

    def block(self, turn):
        y, x, c = self.y, self.x, self.c
        y = 1 - y if turn & 4 else y
        x = 1 - x if turn & 2 else x
        c = 1 - c if turn & 1 else c
        return block_of(y, x, c)

    def copy(self, turn, over, k):
        place = self.view(self.block(turn))
        return self.send(place, place, self.sem + k, peer_of(over, 0))

    def start(self):
        self.copy(0, self.one, 0).start()
        self.copy(0, self.two, 1).start()
        self.copy(0, 1, 3).start()

    def relay(self):
        self.copy(0, self.one, 0).wait()
        self.copy(self.one, self.two, 2).start()
        self.copy(self.one, 1, 4).start()
        self.copy(0, self.two, 1).wait()
        self.copy(self.two, 1, 5).start()

    def last(self):
        self.copy(self.one, self.two, 2).wait()
        self.copy(6, 1, 6).start()

    def finish(self):
        for turn, k in ((0, 3), (self.one, 4), (self.two, 5), (6, 6)):
            self.copy(turn, 1, k).wait()


GATHER_SEMS = 7


class RowSums:
    def __init__(self, send, ref, place, height, got_one, got_two, first_sem):
        self.send, self.ref, self.place, self.height = send, ref, place, height
        self.got_one, self.got_two, self.sem = got_one, got_two, first_sem
        self.y, self.x, _ = bits()
        self.half = ref.shape[-1] // 2

    def at(self, y, x, side):
        rows = pl.ds(pl.multiple_of(self.place(y, x), 128), self.height)
        return (rows, slice(side * self.half, (side + 1) * self.half))

    def pairs(self, k, mine):
        y, x = self.y, self.x
        return [
            (y if mine else 1 - y, k, 0),
            (k, x if mine else 1 - x, 1),
        ]

    def first(self, k, side):
        y, x, _ = self.pairs(k, False)[side]
        return self.send(
            self.ref.at[self.at(y, x, side)], self.got_one.at[side, k], self.sem + 2 * side + k,
            peer_of((4, 2)[side], 0),
        )

    def second(self, side):
        y, x = ((self.y, 1 - self.x), (1 - self.y, self.x))[side]
        return self.send(
            self.ref.at[self.at(y, x, side)], self.got_two.at[side], self.sem + 4 + side,
            peer_of((2, 4)[side], 0),
        )

    def start(self):
        for side in range(2):
            for k in range(2):
                self.first(k, side).start()

    def relay(self):
        for side in range(2):
            for k in range(2):
                self.first(k, side).wait()
        for side in range(2):
            for k in range(2):
                y, x, _ = self.pairs(k, True)[side]
                at = self.at(y, x, side)
                self.ref[at] = (
                    self.ref[at].astype(f32) + self.got_one[side, k].astype(f32)
                ).astype(bf16)
        for side in range(2):
            self.second(side).start()

    def finish(self):
        for side in range(2):
            self.second(side).wait()
            at = self.at(self.y, self.x, side)
            self.ref[at] = (
                self.ref[at].astype(f32) + self.got_two[side].astype(f32)
            ).astype(bf16)


ROW_SEMS = 6


def start_body(
    lengths, tokens_ref, weights_ref,
    gathered_ref, mixed_ref, context_ref, parts_ref, lse_ref, heads_ref, out_ref, length_ref, up_ref, down_ref,
    keys, values, length_buf, out_here, out_far, local_sems, send_sems, recv_sems,
):
    chunks, rows, _ = gathered_ref.shape
    width = context_ref.shape[-1]
    lanes = up_ref.shape[-1]
    hidden_width = SHARE * lanes
    piece = rows // 4
    quarter_rows = D // 4
    y, x, c = bits()
    z = lax.axis_index("tensor")
    matched = c == z // 2
    unmatched = jnp.logical_not(matched)
    own_block = block_of(y, x, c)
    send = sender(send_sems, recv_sems)
    core, near_z, diagonal, swapped = peer_of(1, 0), peer_of(0, 1), peer_of(1, 1), peer_of(1, 2)
    across_x, across_y, across_xy = peer_of(2, 0), peer_of(4, 0), peer_of(6, 0)

    def part_of(k):
        return slice(k * piece, (k + 1) * piece)

    def swap_copy(k):
        return send(tokens_ref.at[part_of(k), :], gathered_ref.at[0, part_of(k), :], k, swapped)

    def far_copy(k, source):
        return send(source.at[part_of(k), :], gathered_ref.at[2, part_of(k), :], 4 + k, near_z)

    def near_copy(k, source):
        return send(source.at[part_of(k), :], gathered_ref.at[1, part_of(k), :], 8 + k, core)

    def diagonal_copy(k):
        return send(gathered_ref.at[2, part_of(k), :], gathered_ref.at[3, part_of(k), :], 12 + k, core)

    column = 2 * y + x

    def quarter(k):
        return pl.ds(pl.multiple_of(k * quarter_rows, quarter_rows), quarter_rows)

    def heads_swap():
        return send(
            weights_ref.at[quarter(column), : 3 * width], heads_ref.at[quarter(column), :], 16, swapped
        )

    def heads_share(k, peer):
        return send(heads_ref.at[quarter(column), :], heads_ref.at[quarter(column), :], 17 + k, peer)

    heads_peers = (across_x, across_y, across_xy)
    heads_local = pltpu.make_async_copy(weights_ref.at[:, : 3 * width], heads_ref, local_sems.at[0])

    def out_copy(e):
        return send(out_here, out_far.at[e - 1], 19 + e, peer_of(0, e))

    out_local = pltpu.make_async_copy(
        weights_ref.at[row_block(own_block), 3 * width : 4 * width], out_here, local_sems.at[1]
    )
    outs = [
        Gather(
            send, lambda k, side=side: out_ref.at[row_block(k), side * 2 * width : (side + 1) * 2 * width],
            23 + side * GATHER_SEMS, side == 0,
        )
        for side in range(2)
    ]
    base = 23 + 2 * GATHER_SEMS
    targets = (up_ref, down_ref)

    def feed_source(kind):
        at = 4 * width + kind * hidden_width + own_block * lanes
        return weights_ref.at[:, pl.ds(pl.multiple_of(at, 128), lanes)]

    def feed_copy(kind, e):
        return send(feed_source(kind), targets[kind].at[e - 1, 0, 0], base + 3 * kind + e - 1, peer_of(0, e))

    half = slice(0, D // 2), slice(D // 2, D)

    def feed_one(kind, e, side):
        source = targets[kind].at[e - 1, 0, 0, half[side], :]
        target = targets[kind].at[e - 1, side, 1 - side, half[side], :]
        return send(
            source, target, base + 6 + 6 * kind + 2 * (e - 1) + side, (across_x, across_y)[side]
        )

    def feed_two(e, side):
        if side == 0:
            source, target = (up_ref.at[e - 1, dy, 0:2, half[0], :] for dy in range(2))
        else:
            source, target = (up_ref.at[e - 1, 0:2, dx, half[1], :] for dx in range(2))
        return send(source, target, base + 18 + 2 * (e - 1) + side, (across_y, across_x)[side])

    def first_hop(kind, e):
        feed_copy(kind, e).wait()
        for side in range(2):
            feed_one(kind, e, side).start()

    def second_hop(e):
        for side in range(2):
            feed_one(0, e, side).wait()
        for side in range(2):
            feed_two(e, side).start()

    def length_copy():
        return send(length_buf.at[0], length_buf.at[1], base + 24, core)

    def part_copy(j):
        return send(
            context_ref.at[j], parts_ref.at[j], base + 24 + j, (None, core, near_z, diagonal)[j]
        )

    def send_weights():
        for e in (3, 2, 1):
            feed_copy(0, e).start()
        for e in (3, 2, 1):
            feed_copy(1, e).start()

    out_local.start()
    length_buf[0] = jnp.full(length_buf.shape[1:], lengths[0], jnp.int32)
    greet(
        [core, near_z, diagonal, swapped, across_x, across_y, across_xy, peer_of(0, 2), peer_of(0, 3)]
    )

    @pl.when(matched)
    def _():
        for k in range(4):
            far_copy(k, tokens_ref).start()
            near_copy(k, tokens_ref).start()
        heads_local.start()
        gathered_ref[0] = tokens_ref[...]

    @pl.when(unmatched)
    def _():
        for k in range(4):
            swap_copy(k).start()
        heads_swap().start()

    length_copy().start()
    out_local.wait()
    for e in (1, 2, 3):
        out_copy(e).start()
    out_ref[row_block(own_block), :width] = out_here[...]

    @pl.when(matched)
    def _():
        send_weights()

    @pl.when(unmatched)
    def _():
        for k in range(4):
            swap_copy(k).wait()
            far_copy(k, gathered_ref.at[0]).start()
            near_copy(k, gathered_ref.at[0]).start()
        heads_swap().wait()
        for k, peer in enumerate(heads_peers):
            heads_share(k, peer).start()
        send_weights()

    for k in range(4):
        far_copy(k, tokens_ref).wait()
        diagonal_copy(k).start()

    @pl.when(matched)
    def _():
        heads_local.wait()

    @pl.when(unmatched)
    def _():
        for k, peer in enumerate(heads_peers):
            heads_share(k, peer).wait()

    length_copy().wait()
    length_ref[...] = jnp.where(matched, length_buf[0], length_buf[1])
    length = length_ref[:1, :]
    own_quarter = jnp.where(matched, z, z + 2 - 4 * (z // 2))
    wide = 256

    def project(j):
        def columns(n, carry):
            at = pl.ds(pl.multiple_of(n * wide, wide), wide)
            mixed_ref[j, :, at] = jnp.dot(
                gathered_ref[j], heads_ref[:, at], preferred_element_type=f32
            ).astype(bf16)
            return carry

        lax.fori_loop(0, 3 * width // wide, columns, 0)

    def arrange(j):
        at_quarter = own_quarter
        if j in (1, 3):
            at_quarter = at_quarter + 2 - 4 * (at_quarter // 2)
        if j in (2, 3):
            at_quarter = at_quarter + 1 - 2 * (at_quarter % 2)
        for h in range(width // HEAD_DIM):
            at = width + (h // 2) * 128
            keys[h, j * rows : (j + 1) * rows, :] = head_keys(
                mixed_ref[j, :, at : at + 128], h % 2, at_quarter * rows, length
            )
        values[j * rows : (j + 1) * rows, :] = mixed_ref[j, :, 2 * width :]

    for j in (0, 2, 1, 3):
        if j == 1:
            for k in range(4):
                near_copy(k, tokens_ref).wait()
        if j == 3:
            for k in range(4):
                diagonal_copy(k).wait()
        project(j)
        arrange(j)

    lane = lax.broadcasted_iota(jnp.int32, (rows, 128), 1)

    def attend(step, carry):
        chunk = chunks - 1 - step
        logs = jnp.zeros((rows, 128), f32)
        for pair in range(width // 128):
            queries = mixed_ref[chunk, :, pair * 128 : pair * 128 + 128]
            both = []
            for side in range(2):
                h = pair * 2 + side
                scores = contract(head_queries(queries, side), keys[h], 1, 1)
                top = jnp.max(scores, axis=1, keepdims=True)
                weight = jnp.exp(scores - top)
                total = jnp.sum(weight, axis=1, keepdims=True)
                out = contract(weight.astype(bf16), values[:, pair * 128 : pair * 128 + 128], 1, 0)
                both.append(out / total)
                logs = jnp.where(lane == h, top + jnp.log(total), logs)
            context_ref[chunk, :, pair * 128 : pair * 128 + 128] = jnp.where(
                lane < HEAD_DIM, both[0], both[1]
            ).astype(bf16)
        lse_ref[chunk] = jnp.transpose(logs)[:8, :]

        @pl.when(step == 0)
        def _():
            part_copy(3).start()
            for e in (1, 2, 3):
                out_copy(e).wait()
                out_ref[row_block(own_block), e * width : (e + 1) * width] = out_far[e - 1]
            for gather in outs:
                gather.start()
            first_hop(0, 3)

        @pl.when(step == 1)
        def _():
            part_copy(2).start()
            for gather in outs:
                gather.relay()
            first_hop(0, 2)
            second_hop(3)

        @pl.when(step == 2)
        def _():
            part_copy(1).start()
            for gather in outs:
                gather.last()
            first_hop(0, 1)
            second_hop(2)

        return carry

    lax.fori_loop(0, chunks, attend, 0)
    parts_ref[0] = context_ref[0]
    for gather in outs:
        gather.finish()
    second_hop(1)
    for e in (3, 2, 1):
        first_hop(1, e)
    for j in (3, 2, 1):
        part_copy(j).wait()
    for e in (3, 2, 1):
        for side in range(2):
            feed_two(e, side).wait()
            feed_one(1, e, side).wait()


def start_block(lengths, tokens, weights):
    rows = tokens.shape[0]
    chunks = 4
    tile = D // 4
    seq = chunks * rows
    lanes = FF // 4 // SHARE
    heads = tile // HEAD_DIM
    sems = 23 + 2 * GATHER_SEMS + 28
    share_rows = D // SHARE
    vmem, anywhere = pl.BlockSpec(memory_space=pltpu.VMEM), pl.BlockSpec(memory_space=pl.ANY)
    return pl.pallas_call(
        start_body,
        name="start_block",
        in_specs=[pl.BlockSpec(memory_space=pltpu.SMEM), vmem, anywhere],
        out_specs=[vmem] * 8 + [anywhere] * 2,
        out_shape=[
            jax.ShapeDtypeStruct((chunks, rows, D), bf16),
            jax.ShapeDtypeStruct((chunks, rows, 3 * tile), bf16),
            jax.ShapeDtypeStruct((chunks, rows, tile), bf16),
            jax.ShapeDtypeStruct((chunks, rows, tile), bf16),
            jax.ShapeDtypeStruct((chunks, 8, rows), f32),
            jax.ShapeDtypeStruct((D, 3 * tile), bf16),
            jax.ShapeDtypeStruct((D, D), bf16),
            jax.ShapeDtypeStruct((8, 128), jnp.int32),
            jax.ShapeDtypeStruct((3, 2, 2, D, lanes), bf16),
            jax.ShapeDtypeStruct((3, 2, 2, D, lanes), bf16),
        ],
        scratch_shapes=[
            pltpu.VMEM((heads, seq, 128), bf16),
            pltpu.VMEM((seq, tile), bf16),
            pltpu.VMEM((2, 8, 128), jnp.int32),
            pltpu.VMEM((share_rows, tile), bf16),
            pltpu.VMEM((3, share_rows, tile), bf16),
            pltpu.SemaphoreType.DMA((2,)),
            pltpu.SemaphoreType.DMA((sems,)),
            pltpu.SemaphoreType.DMA((sems,)),
        ],
        compiler_params=pltpu.CompilerParams(
            vmem_limit_bytes=60 << 20, collective_id=0, has_side_effects=True
        ),
        cost_estimate=pl.CostEstimate(
            flops=24 * heads * seq * seq * HEAD_DIM, bytes_accessed=20 << 20, transcendentals=0
        ),
    )(lengths, tokens, weights)


def back_body(
    info, mixed_ref, context_ref, upstream_ref, lse_ref, weight_ref, branch_ref, norm_ref, outputs_ref, gathered,
    up_grads, down_grads, out_grads,
    input_out, outputs_out, norm_out, attention_out, feed_out,
    keys, turned, key_sum, value_sum, query_t, grad, rows_held, heads_sum, kept, got_one, got_two, got_three,
    leaving, landed, share, heads, heads_one, heads_two, heads_mine, heads_far, out_held, out_core, out_one, out_two, out_z,
    norm_here, norm_there, input_ref, local_sems, send_sems, recv_sems,
):
    chunks, rows, _ = mixed_ref.shape
    width = context_ref.shape[-1]
    scale = HEAD_DIM ** (-0.5)
    part = 256
    core, near_z = peer_of(1, 0), peer_of(0, 1)
    across = (peer_of(2, 0), peer_of(4, 0))
    send = sender(send_sems, recv_sems)
    sources = (up_grads, down_grads)
    y, x, c = bits()
    z = lax.axis_index("tensor")
    matched = c == z // 2
    own_block = block_of(y, x, c)

    def stage_one(b, kind):
        return send(sources[kind].at[b, 1], got_one.at[b, kind], 2 * b + kind, across[kind])

    def stage_two(b, kind):
        return send(kept.at[b, kind, 1], got_two.at[b, kind], 8 + 2 * b + kind, across[1 - kind])

    def stage_three(b):
        return send(kept.at[b, :, 0], got_three.at[b - 1], 15 + b, peer_of(0, b))

    def load(b, kind):
        return pltpu.make_async_copy(
            sources[kind].at[b, 0], kept.at[b, kind], local_sems.at[2 * b + kind]
        )

    def start_one(b):
        for kind in range(2):
            stage_one(b, kind).start()

    def start_two(b):
        for kind in range(2):
            load(b, kind).wait()
            stage_one(b, kind).wait()
            for k in (1, 0):
                kept[b, kind, k] = (
                    kept[b, kind, k].astype(f32) + got_one[b, kind, k].astype(f32)
                ).astype(bf16)
        for kind in range(2):
            stage_two(b, kind).start()

    def start_three(b):
        for kind in range(2):
            stage_two(b, kind).wait()
            kept[b, kind, 0] = (
                kept[b, kind, 0].astype(f32) + got_two[b, kind].astype(f32)
            ).astype(bf16)
        if b:
            stage_three(b).start()

    def load_rows(j):
        return pltpu.make_async_copy(gathered.at[j], rows_held.at[j], local_sems.at[8 + j])

    def out_load():
        return pltpu.make_async_copy(out_grads, out_held, local_sems.at[12])

    def out_core_copy(k):
        at = row_block(block_of(k // 2, k % 2, 1 - c))
        return send(out_grads.at[at, :], out_core.at[k], 22 + k, core)

    out_sums = RowSums(
        send, out_held, lambda yy, xx: block_of(yy, xx, c) * 128, 128, out_one, out_two, 26
    )

    def out_z_copy(e):
        at = (row_block(own_block), slice(e * width, (e + 1) * width))
        return send(out_held.at[at], out_z.at[e - 1], 31 + e, peer_of(0, e))

    def out_start():
        out_load().wait()
        for k in range(4):
            out_core_copy(k).wait()
        for k in range(4):
            at = row_block(block_of(k // 2, k % 2, c))
            out_held[at, :] = (out_held[at, :].astype(f32) + out_core[k].astype(f32)).astype(bf16)
        out_sums.start()

    def out_last():
        out_sums.finish()
        for e in (1, 2, 3):
            out_z_copy(e).start()

    norm_turns = ((1, 0), (2, 0), (4, 0), (0, 1), (0, 2))

    def norm_copy(k):
        return send(norm_here.at[k], norm_there.at[k], 35 + k, peer_of(*norm_turns[k]))

    def norm_step(k):
        norm_copy(k).wait()
        total = norm_here[k] + norm_there[k]
        if k + 1 < len(norm_turns):
            norm_here[k + 1] = total
            norm_copy(k + 1).start()
        else:
            norm_out[...] = total

    for b in (3, 2, 1, 0):
        for kind in range(2):
            load(b, kind).start()
    for j in range(chunks):
        load_rows(j).start()
    out_load().start()
    norm_here[0] = norm_ref[...]
    greet([core, near_z, across[0], across[1], peer_of(0, 2), peer_of(0, 3), peer_of(1, 2)])
    for k in range(4):
        out_core_copy(k).start()
    norm_copy(0).start()
    start_one(3)
    start_one(2)

    def return_copy(source, target, k):
        return send(source, target, 49 + 4 * GATHER_SEMS + k, peer_of(1, 2))

    outputs_local = pltpu.make_async_copy(outputs_ref, outputs_out, local_sems.at[15])

    @pl.when(matched)
    def _():
        outputs_local.start()

    @pl.when(jnp.logical_not(matched))
    def _():
        return_copy(outputs_ref, outputs_out, 0).start()

    key_sum[...] = jnp.zeros_like(key_sum)
    value_sum[...] = jnp.zeros_like(value_sum)
    for j in range(chunks):
        for h in range(width // HEAD_DIM):
            at = width + (h // 2) * 128
            keys[h, j * rows : (j + 1) * rows, :] = head_keys(
                mixed_ref[j, :, at : at + 128], h % 2, info[1 + j], info[0]
            )
        turned[:, j * rows : (j + 1) * rows] = jnp.transpose(
            mixed_ref[j, :, width : 2 * width].astype(f32)
        ).astype(bf16)
    feature = lax.broadcasted_iota(jnp.int32, (8, width), 1) // HEAD_DIM
    picks = (feature == lax.broadcasted_iota(jnp.int32, (8, width), 0)).astype(f32)
    per_chunk = rows // part

    def attend(step, carry):
        chunk = step // per_chunk
        at = pl.ds(pl.multiple_of((step % per_chunk) * part, part), part)
        upstream = upstream_ref[chunk, at, :]
        product = upstream.astype(f32) * context_ref[chunk, at, :].astype(f32)
        delta = lax.dot_general(
            picks, product, (((1,), (1,)), ((), ())), precision=lax.Precision.HIGHEST,
            preferred_element_type=f32,
        )
        lse = lse_ref[chunk, :, at]
        for pair in range(width // 128):
            lanes = slice(pair * 128, pair * 128 + 128)
            queries = mixed_ref[chunk, at, lanes]
            value_rows = mixed_ref[:, :, 2 * width + pair * 128 : 2 * width + pair * 128 + 128]
            value_rows = value_rows.reshape(chunks * rows, 128)
            for half in range(2):
                h = pair * 2 + half
                scores = contract(keys[h], head_queries(queries, half), 1, 1)
                weight = jnp.exp(scores - lse[h : h + 1, :])
                up_half = head_half(upstream[:, lanes], half)
                back = contract(value_rows, up_half, 1, 1)
                score_grad = (weight * (back - delta[h : h + 1, :])).astype(bf16)
                value_sum[pair] += contract(weight.astype(bf16), up_half, 1, 0)
                key_sum[pair] += contract(score_grad, head_half(queries, half), 1, 0)
                query_t[h * HEAD_DIM : (h + 1) * HEAD_DIM, :] = (
                    contract(turned[h * HEAD_DIM : (h + 1) * HEAD_DIM, :], score_grad, 1, 0) * scale
                )
        grad[chunk, at, :width] = jnp.transpose(query_t[...]).astype(bf16)

        @pl.when(step == 0)
        def _():
            norm_step(0)
            out_start()

        @pl.when(step == 1)
        def _():
            norm_step(1)
            start_two(3)
            start_one(1)

        @pl.when(step == 2)
        def _():
            norm_step(2)
            out_sums.relay()

        @pl.when(step == 3)
        def _():
            norm_step(3)
            start_two(2)
            start_one(0)
            start_three(3)

        @pl.when(step == 4)
        def _():
            norm_step(4)
            out_last()

        @pl.when(step == 6)
        def _():
            start_two(1)

        return carry

    lax.fori_loop(0, chunks * per_chunk, attend, 0)
    for j in range(chunks):
        at = slice(j * rows, (j + 1) * rows)
        for pair in range(width // 128):
            left = width + pair * 128
            grad[j, :, left : left + 128] = (key_sum[pair, at, :] * scale).astype(bf16)
            grad[j, :, left + width : left + width + 128] = value_sum[pair, at, :].astype(bf16)
    start_three(2)

    def rows_back(j):
        return contract(grad[j], weight_ref[...], 1, 1)

    core_copies = {}
    for k, j in enumerate((3, 1)):
        leaving[k] = rows_back(j).astype(bf16)
        core_copies[j] = send(leaving.at[k], landed.at[k], 19 + k, core)
        core_copies[j].start()
    far = rows_back(2)
    core_copies[3].wait()
    leaving[2] = (far + landed[0].astype(f32)).astype(bf16)
    far_copy = send(leaving.at[2], landed.at[2], 21, near_z)
    branch_ref_value = branch_ref[...] + rows_back(0)
    far_copy.start()
    core_copies[1].wait()
    own_rows = branch_ref_value + landed[1].astype(f32)

    heads_sum[...] = jnp.zeros_like(heads_sum)
    for j in range(chunks):
        load_rows(j).wait()

    def weigh(j, carry):
        heads_sum[...] += contract(rows_held[j], grad[j], 0, 0)
        return carry

    lax.fori_loop(0, chunks, weigh, 0)
    heads[...] = heads_sum[...].astype(bf16)
    start_two(0)
    head_sums = RowSums(
        send, heads, lambda yy, xx: block_of(yy, xx, 0) * 128, 256, heads_one, heads_two, 40
    )
    head_sums.start()
    start_three(1)
    far_copy.wait()
    input_ref[...] = (own_rows + landed[2].astype(f32)).astype(bf16)
    start_three(0)
    head_sums.relay()

    @pl.when(matched)
    def _():
        input_out[...] = input_ref[...]

    @pl.when(jnp.logical_not(matched))
    def _():
        return_copy(input_ref, input_out, 1).start()

    total = kept[0, :, 0].astype(f32)
    for b in (3, 2, 1):
        stage_three(b).wait()
        total = total + got_three[b - 1].astype(f32)
    share[...] = total.astype(bf16)
    own_feed = [
        pltpu.make_async_copy(share.at[kind], feed_out.at[own_block, kind], local_sems.at[13 + kind])
        for kind in range(2)
    ]
    for copy in own_feed:
        copy.start()
    head_sums.finish()

    def half_rows(k):
        return row_block(block_of(y, x, k))

    @pl.when(matched)
    def _():
        send(heads.at[half_rows(1 - c), :], heads_mine, 46, core).start()

    @pl.when(jnp.logical_not(matched))
    def _():
        send(heads.at[half_rows(c), :], heads_far, 47, peer_of(0, 2)).start()
        send(heads.at[half_rows(1 - c), :], heads_far, 48, peer_of(1, 2)).start()

    feeds = [
        Gather(send, lambda k, kind=kind: feed_out.at[k, kind], 49 + kind * GATHER_SEMS, kind == 0)
        for kind in range(2)
    ]
    for copy in own_feed:
        copy.wait()
    for feed in feeds:
        feed.start()
    sum_out = out_held[row_block(own_block), :width].astype(f32)
    for e in (1, 2, 3):
        out_z_copy(e).wait()
        sum_out = sum_out + out_z[e - 1].astype(f32)
    attention_out[row_block(own_block), 3 * width :] = sum_out.astype(bf16)

    @pl.when(matched)
    def _():
        send(heads.at[half_rows(1 - c), :], heads_mine, 46, core).wait_send()
        heads_mine[...] = heads[half_rows(c), :]

    @pl.when(jnp.logical_not(matched))
    def _():
        send(heads.at[half_rows(c), :], heads_far, 47, peer_of(0, 2)).wait_send()
        send(heads.at[half_rows(1 - c), :], heads_far, 48, peer_of(1, 2)).wait_send()
        send(heads.at[half_rows(c), :], heads_mine, 46, core).wait_recv()

    @pl.when(matched)
    def _():
        send(heads.at[half_rows(c), :], heads_far, 47, peer_of(0, 2)).wait_recv()

    @pl.when(jnp.logical_not(matched))
    def _():
        send(heads.at[half_rows(c), :], heads_far, 48, peer_of(1, 2)).wait_recv()

    attention_out[row_block(own_block), : 3 * width] = (
        heads_mine[...].astype(f32) + heads_far[...].astype(f32)
    ).astype(bf16)
    sides = [
        Gather(
            send,
            lambda k, side=side: attention_out.at[row_block(k), side * 2 * width : (side + 1) * 2 * width],
            49 + (2 + side) * GATHER_SEMS, side == 0,
        )
        for side in range(2)
    ]
    for side in sides:
        side.start()
    for gather in feeds + sides:
        gather.relay()
    for gather in feeds + sides:
        gather.last()
    for gather in feeds + sides:
        gather.finish()
    @pl.when(matched)
    def _():
        outputs_local.wait()

    @pl.when(jnp.logical_not(matched))
    def _():
        return_copy(outputs_ref, outputs_out, 0).wait()
        return_copy(input_ref, input_out, 1).wait()


def back_block(info, mixed, context, upstream, lse, weight, branch, norm_sums, outputs, gathered, up_grads,
               down_grads, out_grads):
    chunks, rows, width3 = mixed.shape
    width = width3 // 3
    seq = chunks * rows
    heads = width // HEAD_DIM
    lanes = up_grads.shape[-1]
    share_rows = D // SHARE
    sems = 51 + 4 * GATHER_SEMS
    vmem, anywhere = pl.BlockSpec(memory_space=pltpu.VMEM), pl.BlockSpec(memory_space=pl.ANY)
    return pl.pallas_call(
        back_body,
        name="back_block",
        in_specs=[pl.BlockSpec(memory_space=pltpu.SMEM)] + [vmem] * 7 + [anywhere] * 5,
        out_specs=[vmem, vmem, vmem, vmem, anywhere],
        out_shape=[
            jax.ShapeDtypeStruct((rows, D), bf16),
            jax.ShapeDtypeStruct((rows, D), bf16),
            jax.ShapeDtypeStruct((4, D), f32),
            jax.ShapeDtypeStruct((D, 4 * width), bf16),
            jax.ShapeDtypeStruct((SHARE, 2, D, lanes), bf16),
        ],
        scratch_shapes=[
            pltpu.VMEM((heads, seq, 128), bf16),
            pltpu.VMEM((width, seq), bf16),
            pltpu.VMEM((width // 128, seq, 128), f32),
            pltpu.VMEM((width // 128, seq, 128), f32),
            pltpu.VMEM((width, 256), f32),
            pltpu.VMEM((chunks, rows, width3), bf16),
            pltpu.VMEM((chunks, rows, D), bf16),
            pltpu.VMEM((D, width3), f32),
            pltpu.VMEM((4, 2, 2, D, lanes), bf16),
            pltpu.VMEM((4, 2, 2, D, lanes), bf16),
            pltpu.VMEM((4, 2, D, lanes), bf16),
            pltpu.VMEM((3, 2, D, lanes), bf16),
            pltpu.VMEM((3, rows, D), bf16),
            pltpu.VMEM((3, rows, D), bf16),
            pltpu.VMEM((2, D, lanes), bf16),
            pltpu.VMEM((D, width3), bf16),
            pltpu.VMEM((2, 2, 2 * share_rows, width3 // 2), bf16),
            pltpu.VMEM((2, 2 * share_rows, width3 // 2), bf16),
            pltpu.VMEM((share_rows, width3), bf16),
            pltpu.VMEM((share_rows, width3), bf16),
            pltpu.VMEM((D, 4 * width), bf16),
            pltpu.VMEM((4, share_rows, 4 * width), bf16),
            pltpu.VMEM((2, 2, share_rows, 2 * width), bf16),
            pltpu.VMEM((2, share_rows, 2 * width), bf16),
            pltpu.VMEM((3, share_rows, width), bf16),
            pltpu.VMEM((5, 4, D), f32),
            pltpu.VMEM((5, 4, D), f32),
            pltpu.VMEM((rows, D), bf16),
            pltpu.SemaphoreType.DMA((16,)),
            pltpu.SemaphoreType.DMA((sems,)),
            pltpu.SemaphoreType.DMA((sems,)),
        ],
        compiler_params=pltpu.CompilerParams(
            vmem_limit_bytes=67043328, collective_id=2, has_side_effects=True
        ),
        cost_estimate=pl.CostEstimate(
            flops=40 * heads * seq * seq * HEAD_DIM, bytes_accessed=40 << 20, transcendentals=0
        ),
    )(
        info, mixed, context, upstream, lse, weight, branch, norm_sums, outputs, gathered, up_grads, down_grads,
        out_grads,
    )


def adam_body(owned, attention_ref, feed_ref, master_ref, one_ref, two_ref,
              grad_out, master_out, one_out, two_out, tiles_out, up_out, down_out):
    tile = grad_out.shape[-1] // 4
    for s in range(4):
        at = slice(s * tile, (s + 1) * tile)
        grad = jnp.zeros((grad_out.shape[0], tile), f32)
        for i in range(4):
            value = attention_ref[:, i * tile : (i + 1) * tile].astype(f32)
            grad = jnp.where(owned[s, i] > 0, value, grad)
        for kind in range(2):
            value = jnp.concatenate([feed_ref[2 * s + k, kind] for k in range(2)], axis=-1)
            grad = jnp.where(owned[s, 4 + 4 * kind + s] > 0, value.astype(f32), grad)
        occupied = (owned[s, 12] > 0).astype(f32)
        param, first, second = adam_update(
            grad, master_ref[:, at], one_ref[:, at], two_ref[:, at], occupied, weight_decay
        )
        grad_out[:, at] = grad
        master_out[:, at] = param
        one_out[:, at] = first
        two_out[:, at] = second
        low = param.astype(bf16)
        none = jnp.zeros_like(low)
        for i in range(4):
            mine = jnp.where(owned[s, i] > 0, low, none)
            there = slice(i * tile, (i + 1) * tile)
            tiles_out[:, there] = mine if s == 0 else tiles_out[:, there] + mine
        for kind, target in ((0, up_out), (1, down_out)):
            mine = jnp.where(owned[s, 4 + 4 * kind + s] > 0, low, none)
            for k in range(2):
                target[2 * s + k] = mine[:, k * tile // 2 : (k + 1) * tile // 2]


def adam_block(owned, attention_grad, feed_grad, master, one, two):
    part = 128
    wide = pl.BlockSpec((part, D), lambda i: (i, 0))
    lanes = feed_grad.shape[-1]
    split = pl.BlockSpec((SHARE, part, lanes), lambda i: (0, i, 0))
    return pl.pallas_call(
        adam_body,
        grid=(D // part,),
        name="adam_block",
        in_specs=[
            pl.BlockSpec(memory_space=pltpu.SMEM), wide,
            pl.BlockSpec((SHARE, 2, part, lanes), lambda i: (0, 0, i, 0)), wide, wide, wide,
        ],
        out_specs=[wide] * 5 + [split] * 2,
        out_shape=[jax.ShapeDtypeStruct((D, D), f32)] * 4
        + [jax.ShapeDtypeStruct((D, D), bf16)]
        + [jax.ShapeDtypeStruct((SHARE, D, lanes), bf16)] * 2,
        compiler_params=pltpu.CompilerParams(vmem_limit_bytes=62 << 20),
        cost_estimate=pl.CostEstimate(flops=40 * D * D, bytes_accessed=40 << 20, transcendentals=0),
    )(owned, attention_grad, feed_grad, master, one, two)


def tiles_body(tiles_ref, up_ref, down_ref, tiles_out, up_out, down_out, *scratch):
    core_got = scratch[:3]
    one_got, two_got = scratch[3:5], scratch[5:7]
    work = scratch[7:10]
    row_one, row_two, send_sems, recv_sems = scratch[10:]
    send = sender(send_sems, recv_sems)
    y, x, c = bits()
    core = peer_of(1, 0)
    own_block = block_of(y, x, c)
    greet([core, peer_of(2, 0), peer_of(4, 0)])
    arrays = ((up_ref, up_out), (down_ref, down_out), (tiles_ref, tiles_out))

    def place(n, ref, block):
        return ref.at[row_block(block), :] if n == 2 else ref.at[block]

    def core_copy(n, k):
        return send(
            place(n, arrays[n][0], block_of(k // 2, k % 2, 1 - c)), core_got[n].at[k], 4 * n + k, core
        )

    def core_add(n):
        source, target = arrays[n][0], work[n]
        for k in range(4):
            core_copy(n, k).wait()
        for k in range(4):
            block = block_of(k // 2, k % 2, c)
            if n == 2:
                at = row_block(block)
                target[at, :] = source[at, :] + core_got[n][k]
            else:
                target[k] = source[block] + core_got[n][k]

    def first(n, k):
        y_, x_ = ((k, 1 - x), (1 - y, k))[n]
        return send(
            work[n].at[2 * y_ + x_], one_got[n].at[k], 12 + 2 * n + k,
            peer_of((2, 4)[n], 0),
        )

    def second(n):
        y_, x_ = ((1 - y, x), (y, 1 - x))[n]
        return send(
            work[n].at[2 * y_ + x_], two_got[n], 16 + n, peer_of((4, 2)[n], 0)
        )

    def relay(n):
        target = work[n]
        for k in range(2):
            first(n, k).wait()
        for k in range(2):
            y_, x_ = ((k, x), (y, k))[n]
            block = 2 * y_ + x_
            target[block] = target[block] + one_got[n][k]
        second(n).start()

    def settle(n):
        second(n).wait()
        arrays[n][1][own_block] = work[n][2 * y + x] + two_got[n][...]

    for n in range(3):
        for k in range(4):
            core_copy(n, k).start()
    for n in range(2):
        core_add(n)
        for k in range(2):
            first(n, k).start()
    core_add(2)
    rows = RowSums(
        send, work[2], lambda yy, xx: block_of(yy, xx, c) * 128, 128, row_one, row_two, 18
    )
    rows.start()
    for n in range(2):
        relay(n)
    rows.relay()
    gathers = []
    for n in range(2):
        settle(n)
        gathers.append(
            Gather(send, lambda k, n=n: arrays[n][1].at[k], 24 + n * GATHER_SEMS, n == 0)
        )
        gathers[-1].start()
    rows.finish()
    tiles_out[row_block(own_block), :] = work[2][row_block(own_block), :]
    half = tiles_out.shape[-1] // 2
    for side in range(2):
        gathers.append(
            Gather(
                send,
                lambda k, side=side: tiles_out.at[row_block(k), side * half : (side + 1) * half],
                24 + (2 + side) * GATHER_SEMS, side == 0,
            )
        )
        gathers[-1].start()
    for gather in gathers:
        gather.relay()
    for gather in gathers:
        gather.last()
    for gather in gathers:
        gather.finish()


def spread_tiles(tiles, up, down):
    share_rows = D // SHARE
    lanes = up.shape[-1]
    sems = 24 + 4 * GATHER_SEMS
    piece = (D, lanes)
    vmem = pl.BlockSpec(memory_space=pltpu.VMEM)
    return pl.pallas_call(
        tiles_body,
        name="spread_tiles",
        in_specs=[vmem] * 3,
        out_specs=[vmem] * 3,
        out_shape=[jax.ShapeDtypeStruct(v.shape, bf16) for v in (tiles, up, down)],
        scratch_shapes=[
            pltpu.VMEM((4,) + piece, bf16),
            pltpu.VMEM((4,) + piece, bf16),
            pltpu.VMEM((4, share_rows, D), bf16),
            pltpu.VMEM((2,) + piece, bf16),
            pltpu.VMEM((2,) + piece, bf16),
            pltpu.VMEM(piece, bf16),
            pltpu.VMEM(piece, bf16),
            pltpu.VMEM((4,) + piece, bf16),
            pltpu.VMEM((4,) + piece, bf16),
            pltpu.VMEM((D, D), bf16),
            pltpu.VMEM((2, 2, share_rows, D // 2), bf16),
            pltpu.VMEM((2, share_rows, D // 2), bf16),
            pltpu.SemaphoreType.DMA((sems,)),
            pltpu.SemaphoreType.DMA((sems,)),
        ],
        compiler_params=pltpu.CompilerParams(
            vmem_limit_bytes=48 << 20, collective_id=3, has_side_effects=True
        ),
        cost_estimate=pl.CostEstimate(flops=D * D, bytes_accessed=12 << 20, transcendentals=0),
    )(tiles, up, down)


def joined(held, i, kind):
    return jnp.concatenate(
        [held[kind, 2 * (i // 2) + m, i % 2, k] for k in range(2) for m in range(2)], axis=-1
    )


def gelu_parts(value):
    bell = jnp.exp(-0.5 * value * value)
    t = 1.0 / (1.0 + (0.3275911 * 0.5**0.5) * jnp.abs(value))
    tail = 0.5 * 1.061405429
    for c in (-1.453152027, 1.421413741, -0.284496736, 0.254829592):
        tail = tail * t + 0.5 * c
    tail = tail * t * bell
    area = jnp.where(value > 0, 1.0 - tail, tail)
    return value * area, area + value * bell * (0.5 / jnp.pi) ** 0.5


def feed_body(
    info, first_ref, cotangent_ref, norms_ref, weights_ref, up_ref, down_ref,
    out_ref, low_ref, both_ref, hidden_ref, pre_ref, grad_ref, sums_ref,
    held, slope, total, leaving, landed, seed_held, local_sems, send_sems, recv_sems,
):
    rows = first_ref.shape[0]
    steps = hidden_ref.shape[0]
    lanes = held.shape[-1]
    y, x, c = bits()
    peer = peer_of(1, 0)
    send = sender(send_sems, recv_sems)
    half = slice(0, D // 2), slice(D // 2, D)
    loads = []
    for kind in range(2):
        for dy in range(2):
            for dx in range(2):
                block = block_of(1 - y if dy else y, 1 - x if dx else x, c)
                at = D + kind * SHARE * lanes + block * lanes
                loads.append(
                    (weights_ref.at[:, pl.ds(pl.multiple_of(at, 128), lanes)], held.at[kind, 0, dy, dx])
                )
    loads.append((up_ref, held.at[0, 1:4]))
    loads.append((down_ref.at[:, 0, 0:2, half[0], :], held.at[1, 1:4, 0, 0:2, half[0], :]))
    loads.append((down_ref.at[:, 0:2, 0, half[1], :], held.at[1, 1:4, 0:2, 0, half[1], :]))
    loads = [pltpu.make_async_copy(a, b, local_sems.at[k]) for k, (a, b) in enumerate(loads)]
    for load in loads:
        load.start()
    greet([peer, peer_of(2, 0), peer_of(4, 0), peer_of(1, 2)])
    matched = c == lax.axis_index("tensor") // 2
    seed_local = pltpu.make_async_copy(cotangent_ref, seed_held, local_sems.at[len(loads)])
    seed_swap = send(cotangent_ref, seed_held, 6, peer_of(1, 2))
    hops = [
        send(
            down_ref.at[:, 0, 0:2, half[0], :], held.at[1, 1:4, 1, 0:2, half[0], :], 4, peer_of(4, 0)
        ),
        send(
            down_ref.at[:, 0:2, 0, half[1], :], held.at[1, 1:4, 0:2, 1, half[1], :], 5, peer_of(2, 0)
        ),
    ]
    for hop in hops:
        hop.start()

    @pl.when(matched)
    def _():
        seed_local.start()

    @pl.when(jnp.logical_not(matched))
    def _():
        seed_swap.start()

    def across(source, target, k):
        return send(source, target, k, peer)

    middle_row = rows // 2
    both_ref[0] = first_ref[...].astype(bf16)
    first_copy = across(both_ref.at[0], both_ref.at[1], 0)
    first_copy.start()

    def up(i, slot):
        weight = joined(held, i, 0)
        for r in range(0, rows, middle_row):
            at = slice(r, r + middle_row)
            value = jnp.dot(both_ref[slot, at, :], weight, preferred_element_type=f32)
            hidden, steep = gelu_parts(value)
            hidden_ref[i, slot, at, :] = hidden.astype(bf16)
            slope[i, slot, at, :] = steep.astype(bf16)

    def down(i, slot):
        total[slot] += contract(hidden_ref[i, slot], joined(held, i, 1), 1, 1)

    def back(i, slot):
        weight = joined(held, i, 1)
        for r in range(0, rows, middle_row):
            at = slice(r, r + middle_row)
            value = jnp.dot(low_ref[slot, at, :], weight, preferred_element_type=f32)
            pre_ref[i, slot, at, :] = (value * slope[i, slot, at, :].astype(f32)).astype(bf16)

    def back_up(i, slot):
        total[slot] += contract(pre_ref[i, slot], joined(held, i, 0), 1, 1)

    def loop(*works):
        def body(i, carry):
            for work in works:
                work(i)
            return carry

        lax.fori_loop(0, steps, body, 0)

    total[...] = jnp.zeros_like(total)
    for load in loads:
        load.wait()
    loop(lambda i: up(i, 0))
    first_copy.wait()
    for hop in hops:
        hop.wait()
    loop(lambda i: up(i, 1), lambda i: down(i, 1))
    leaving[...] = total[1].astype(bf16)
    feed_copy = across(leaving, landed.at[0], 1)
    feed_copy.start()
    loop(lambda i: down(i, 0))
    feed_copy.wait()

    @pl.when(matched)
    def _():
        seed_local.wait()

    @pl.when(jnp.logical_not(matched))
    def _():
        seed_swap.wait()

    sums_ref[...] = jnp.zeros_like(sums_ref)
    part = 128

    def middle(r, carry):
        at = pl.ds(pl.multiple_of(r * part, part), part)
        second, normed, inverse = norm_parts(
            first_ref[at, :] + (total[0, at, :] + landed[0, at, :].astype(f32)),
            norms_ref[2:3, :], norms_ref[3:4, :],
        )
        out_ref[at, :] = second.astype(bf16)
        row = lax.broadcasted_iota(jnp.int32, (part, 1), 0) + r * part + info[1]
        seed = seed_held[at, :].astype(f32) * (row < info[0]).astype(f32)
        grad = norm_back(seed, normed, inverse, norms_ref[2:3, :])
        sums_ref[0:1, :] += jnp.sum(seed * normed, axis=0, keepdims=True)
        sums_ref[1:2, :] += jnp.sum(seed, axis=0, keepdims=True)
        total[0, at, :] = grad
        low_ref[0, at, :] = grad.astype(bf16)
        return carry

    lax.fori_loop(0, rows // part, middle, 0)
    low_copy = across(low_ref.at[0], low_ref.at[1], 2)
    low_copy.start()
    total[1] = jnp.zeros_like(total[1])
    loop(lambda i: back(i, 0))
    low_copy.wait()
    loop(lambda i: back(i, 1), lambda i: back_up(i, 1))
    leaving[...] = total[1].astype(bf16)
    grad_copy = across(leaving, landed.at[1], 3)
    grad_copy.start()
    loop(lambda i: back_up(i, 0))
    grad_copy.wait()
    grad_ref[...] = total[0] + landed[1].astype(f32)


def feed_block(info, first, cotangent, norms, weights, up, down):
    rows = first.shape[0]
    lanes = up.shape[-1]
    width = 4 * lanes
    vmem, anywhere = pl.BlockSpec(memory_space=pltpu.VMEM), pl.BlockSpec(memory_space=pl.ANY)
    return pl.pallas_call(
        feed_body,
        name="feed_block",
        in_specs=[pl.BlockSpec(memory_space=pltpu.SMEM), vmem, anywhere, vmem] + [anywhere] * 3,
        out_specs=[vmem] * 7,
        out_shape=[
            jax.ShapeDtypeStruct((rows, D), bf16),
            jax.ShapeDtypeStruct((2, rows, D), bf16),
            jax.ShapeDtypeStruct((2, rows, D), bf16),
            jax.ShapeDtypeStruct((4, 2, rows, width), bf16),
            jax.ShapeDtypeStruct((4, 2, rows, width), bf16),
            jax.ShapeDtypeStruct((rows, D), f32),
            jax.ShapeDtypeStruct((2, D), f32),
        ],
        scratch_shapes=[
            pltpu.VMEM((2, 4, 2, 2, D, lanes), bf16),
            pltpu.VMEM((4, 2, rows, width), bf16),
            pltpu.VMEM((2, rows, D), f32),
            pltpu.VMEM((rows, D), bf16),
            pltpu.VMEM((2, rows, D), bf16),
            pltpu.VMEM((rows, D), bf16),
            pltpu.SemaphoreType.DMA((12,)),
            pltpu.SemaphoreType.DMA((7,)),
            pltpu.SemaphoreType.DMA((7,)),
        ],
        compiler_params=pltpu.CompilerParams(
            vmem_limit_bytes=60 << 20, collective_id=1, has_side_effects=True
        ),
        cost_estimate=pl.CostEstimate(
            flops=64 * rows * D * width, bytes_accessed=30 << 20, transcendentals=0
        ),
    )(info, first, cotangent, norms, weights, up, down)


def feed_grads_body(first_ref, low_ref, hidden_ref, pre_ref, up_ref, down_ref, first_t, low_t):
    rows = first_ref.shape[1]

    @pl.when(pl.program_id(0) == 0)
    def _():
        for slot in range(2):
            at = slice(slot * rows, (slot + 1) * rows)
            first_t[:, at] = jnp.transpose(first_ref[slot].astype(f32)).astype(bf16)
            low_t[:, at] = jnp.transpose(low_ref[slot].astype(f32)).astype(bf16)

    lanes = up_ref.shape[-1]
    width = pre_ref.shape[-1]
    for target, source, turned in ((up_ref, pre_ref, first_t), (down_ref, hidden_ref, low_t)):
        grad = jnp.dot(
            turned[...], source[0].reshape(2 * rows, width), preferred_element_type=f32
        ).astype(bf16)
        for k in range(2):
            for m in range(2):
                at = (2 * k + m) * lanes
                if target is up_ref:
                    target[m, k, 0] = grad[:, at : at + lanes]
                else:
                    target[m, 0, k] = grad[:, at : at + lanes]


def feed_grads(first, low, hidden, pre):
    count, _, rows, width = hidden.shape
    full = pl.BlockSpec((2, rows, D), lambda i: (0, 0, 0))
    piece = pl.BlockSpec((1, 2, rows, width), lambda i: (i, 0, 0, 0))
    lanes = width // 4
    return pl.pallas_call(
        feed_grads_body,
        grid=(count,),
        name="feed_grads",
        in_specs=[full, full, piece, piece],
        out_specs=[
            pl.BlockSpec((2, 2, 1, D, lanes), lambda i: (i // 2, 0, i % 2, 0, 0)),
            pl.BlockSpec((2, 1, 2, D, lanes), lambda i: (i // 2, i % 2, 0, 0, 0)),
        ],
        out_shape=[jax.ShapeDtypeStruct((count, 2, 2, D, lanes), bf16)] * 2,
        scratch_shapes=[pltpu.VMEM((D, 2 * rows), bf16), pltpu.VMEM((D, 2 * rows), bf16)],
        compiler_params=pltpu.CompilerParams(vmem_limit_bytes=48 << 20),
        cost_estimate=pl.CostEstimate(
            flops=8 * rows * D * width * count, bytes_accessed=20 << 20, transcendentals=0
        ),
    )(first, low, hidden, pre)


def layer(n_dp, n_tensor, tokens, weights, norms, cotangent, lengths, owners, master, moment_one,
          moment_two, norm_master, norm_one, norm_two):
    tile = D // n_tensor
    rows = tokens.shape[0]
    device = lax.axis_index("dp")
    z = lax.axis_index("tensor")
    core = device % 2
    matched = core == z // 2
    quarter = jnp.where(matched, z, z ^ 2)

    def flip(x, dd, dz):
        pairs = [
            (d * n_tensor + t, (d ^ dd) * n_tensor + (t ^ dz))
            for d in range(n_dp)
            for t in range(n_tensor)
        ]
        return lax.ppermute(x, AXES, pairs)

    gathered, mixed, context, parts, lse, w_heads, w_out_all, length, up_all, down_all = start_block(
        lengths, tokens[:, 0, :], weights
    )
    own = gathered[0]
    base = jnp.stack([quarter ^ k for k in (0, 2, 1, 3)]) * rows
    info = jnp.concatenate([length[0, :1], base]).astype(jnp.int32)

    context_all = jnp.where(
        matched,
        jnp.concatenate([parts[k] for k in (0, 2, 1, 3)], axis=1),
        jnp.concatenate([parts[k] for k in (1, 3, 0, 2)], axis=1),
    )
    branch = contract(context_all, w_out_all, 1, 1)
    first, first_normed, first_inverse = norm_parts(
        own.astype(f32) + branch, norms[0], norms[1]
    )
    outputs, both_low, both_first, hidden, pre_grad, first_grad, sums_two = feed_block(
        info, first, cotangent[:, 0, :], norms, weights, up_all, down_all
    )
    branch_grad = norm_back(first_grad, first_normed, first_inverse, norms[0])
    gain_one = jnp.sum(first_grad * first_normed, axis=0)
    shift_one = jnp.sum(first_grad, axis=0)
    branch_low = branch_grad.astype(bf16)
    context_grad = jnp.dot(branch_low, w_out_all, preferred_element_type=f32).astype(bf16)
    blocks = [context_grad[:, k * tile : (k + 1) * tile] for k in range(4)]
    blocks = [
        jnp.where(matched, blocks[a], blocks[b]) for a, b in ((0, 2), (2, 0), (1, 3), (3, 1))
    ]
    upstream = jnp.stack(
        [blocks[0], flip(blocks[1], 1, 0), flip(blocks[2], 0, 1), flip(blocks[3], 1, 1)]
    )

    def add(a, b):
        return (a.astype(f32) + b.astype(f32)).astype(bf16)

    up_grads, down_grads = feed_grads(both_first, both_low, hidden, pre_grad)
    out_grad = contract(branch_low, context_all, 0, 0).astype(bf16)
    norm_sums = jnp.concatenate([jnp.stack([gain_one, shift_one]), sums_two])
    input_grad, outputs, norm_grads, attention_grad, feed_grad = back_block(
        info, mixed, context, upstream, lse, w_heads, branch_grad, norm_sums, outputs, gathered, up_grads, down_grads,
        out_grad,
    )

    def over_groups(value, combine):
        bit = SHARE
        while bit < n_dp:
            value = combine(value, flip(value, bit, 0))
            bit *= 2
        return value

    def plus(a, b):
        return a + b

    norm_grads = over_groups(norm_grads, plus)
    attention_grad = over_groups(attention_grad, add)
    feed_grad = over_groups(feed_grad, add)

    tile_owner, slot_index = slot_table(owners)
    slot_ids = jnp.arange(FF // D, dtype=jnp.int32)
    owned = (
        (tile_owner[None, :] == device) & (slot_index[None, :] == slot_ids[:, None])
    ).astype(jnp.int32)
    owned = jnp.concatenate([owned, jnp.sum(owned, axis=1, keepdims=True)], axis=1)
    slot_grad, new_master, new_one, new_two, tiles, up_tiles, down_tiles = adam_block(
        owned, attention_grad, feed_grad, master[0], moment_one[0], moment_two[0]
    )
    tiles, up_tiles, down_tiles = (
        over_groups(v, plus) for v in spread_tiles(tiles, up_tiles, down_tiles)
    )
    new_weights = jnp.concatenate(
        [tiles] + [up_tiles[k] for k in range(SHARE)] + [down_tiles[k] for k in range(SHARE)], axis=1
    )
    norm_owner = (device == owners[6]).astype(f32)
    new_norm_master, new_norm_one, new_norm_two = adam_update(
        norm_grads, norm_master[0], norm_one[0], norm_two[0], norm_owner, 0.0
    )
    return (
        outputs[:, None, :],
        input_grad[:, None, :],
        slot_grad[None],
        new_master[None],
        new_one[None],
        new_two[None],
        new_weights,
        norm_grads,
        new_norm_master[None],
        new_norm_one[None],
        new_norm_two[None],
    )


def solution(mesh):
    in_specs = (
        P("tensor", "dp", None),
        P(None, "tensor"),
        P(),
        P("tensor", "dp", None),
        P("dp"),
        P(),
        P("dp", None, "tensor"),
        P("dp", None, "tensor"),
        P("dp", None, "tensor"),
        P("dp", None, None),
        P("dp", None, None),
        P("dp", None, None),
    )
    out_specs = (
        P("tensor", "dp", None),
        P("tensor", "dp", None),
        P("dp", None, "tensor"),
        P("dp", None, "tensor"),
        P("dp", None, "tensor"),
        P("dp", None, "tensor"),
        P(None, "tensor"),
        P(),
        P("dp", None, None),
        P("dp", None, None),
        P("dp", None, None),
    )
    return jax.shard_map(
        partial(layer, mesh.shape["dp"], mesh.shape["tensor"]),
        mesh=mesh,
        in_specs=in_specs,
        out_specs=out_specs,
        check_vma=False,
    )
```

```python
from functools import partial

import jax
import jax.numpy as jnp
from jax import lax
from jax.experimental import pallas as pl
from jax.experimental.pallas import tpu as pltpu
from jax.sharding import PartitionSpec as P

D = 1024
FF = 4096
ADAM_STEP = 10
HEAD_DIM = 64
SHARE = 8


f32, bf16 = jnp.float32, jnp.bfloat16
beta_one = 0.9
beta_two = 0.999
learn_rate = 0.02
weight_decay = 0.1
adam_eps = 1e-08
norm_eps = 1e-05
masked_score = -1e30
AXES = ("dp", "tensor")


def contract(a, b, ca, cb):
    return lax.dot_general(a, b, (((ca,), (cb,)), ((), ())), preferred_element_type=f32)


def norm_parts(value, gain, shift):
    average = jnp.mean(value, axis=-1, keepdims=True)
    centred = value - average
    variance = jnp.mean(centred * centred, axis=-1, keepdims=True)
    inverse = lax.rsqrt(variance + norm_eps)
    normed = centred * inverse
    return normed * gain + shift, normed, inverse


def norm_back(upstream, normed, inverse, gain):
    scaled = upstream * gain
    inner = (
        scaled
        - jnp.mean(scaled, axis=-1, keepdims=True)
        - normed * jnp.mean(scaled * normed, axis=-1, keepdims=True)
    )
    return inner * inverse


def slot_table(owners):
    repeat = FF // D
    tile_matrix = jnp.array([0, 1, 2, 3] + [4] * repeat + [5] * repeat, dtype=jnp.int32)
    choose = (tile_matrix[:, None] == jnp.arange(7, dtype=jnp.int32)[None, :]).astype(jnp.int32)
    tile_owner = jnp.sum(choose * owners[None, :], axis=1)
    position = jnp.arange(tile_matrix.shape[0], dtype=jnp.int32)
    before = (tile_owner[None, :] == tile_owner[:, None]) & (position[None, :] < position[:, None])
    slot_index = jnp.sum(before.astype(jnp.int32), axis=1)
    return (tile_owner, slot_index)


def adam_update(grad, param, first, second, occupied, decay_rate):
    first_new = occupied * (beta_one * first + (1.0 - beta_one) * grad)
    second_new = occupied * (beta_two * second + (1.0 - beta_two) * grad * grad)
    correct_one = 1.0 - beta_one**ADAM_STEP
    correct_two = 1.0 - beta_two**ADAM_STEP
    direction = first_new / correct_one / (jnp.sqrt(second_new / correct_two) + adam_eps)
    param_new = occupied * (param - learn_rate * (direction + decay_rate * param))
    return (param_new, first_new, second_new)


def head_keys(keys, half, start, length):
    lane = lax.broadcasted_iota(jnp.int32, keys.shape, 1)
    row = lax.broadcasted_iota(jnp.int32, keys.shape, 0)
    bias = jnp.where(start + row < length, 0.0, masked_score).astype(f32)
    extra = jnp.where(lane == (1 - half) * HEAD_DIM, bias, 0.0)
    return jnp.where(lane // HEAD_DIM == half, keys.astype(f32), extra).astype(bf16)


def head_half(rows, half):
    lane = lax.broadcasted_iota(jnp.int32, rows.shape, 1)
    return jnp.where(lane // HEAD_DIM == half, rows, jnp.zeros_like(rows))


def head_queries(rows, half):
    lane = lax.broadcasted_iota(jnp.int32, rows.shape, 1)
    scaled = rows.astype(f32) * HEAD_DIM ** (-0.5)
    extra = jnp.where(lane == (1 - half) * HEAD_DIM, 1.0, 0.0)
    return jnp.where(lane // HEAD_DIM == half, scaled, extra).astype(bf16)


def peer_of(bit, turn):
    device, z = lax.axis_index("dp"), lax.axis_index("tensor")
    for one in (1, 2, 4):
        if bit & one:
            device = device + one - 2 * one * ((device // one) % 2)
    if turn == 1:
        z = z + 1 - 2 * (z % 2)
    elif turn == 2:
        z = z + 2 - 4 * (z // 2)
    elif turn == 3:
        z = 3 - z
    return (device, z)


def greet(peers):
    barrier = pltpu.get_barrier_semaphore()
    for peer in peers:
        pl.semaphore_signal(barrier, inc=1, device_id=peer, device_id_type=pl.DeviceIdType.MESH)
    pl.semaphore_wait(barrier, len(peers))


def sender(send_sems, recv_sems):
    def send(source, target, k, peer):
        return pltpu.make_async_remote_copy(
            source, target, send_sems.at[k], recv_sems.at[k], device_id=peer,
            device_id_type=pl.DeviceIdType.MESH,
        )

    return send


def bits():
    device = lax.axis_index("dp")
    return (device // 4) % 2, (device // 2) % 2, device % 2


def block_of(y, x, c):
    return 4 * y + 2 * x + c


def row_block(index, count=1):
    rows = D // SHARE
    return pl.ds(pl.multiple_of(index * rows, rows), count * rows)


class Gather:
    def __init__(self, send, view, first_sem, x_first):
        self.send, self.view, self.sem = send, view, first_sem
        self.y, self.x, self.c = bits()
        self.one, self.two = (2, 4) if x_first else (4, 2)

    def block(self, turn):
        y, x, c = self.y, self.x, self.c
        y = 1 - y if turn & 4 else y
        x = 1 - x if turn & 2 else x
        c = 1 - c if turn & 1 else c
        return block_of(y, x, c)

    def copy(self, turn, over, k):
        place = self.view(self.block(turn))
        return self.send(place, place, self.sem + k, peer_of(over, 0))

    def start(self):
        self.copy(0, self.one, 0).start()
        self.copy(0, self.two, 1).start()
        self.copy(0, 1, 3).start()

    def relay(self):
        self.copy(0, self.one, 0).wait()
        self.copy(self.one, self.two, 2).start()
        self.copy(self.one, 1, 4).start()
        self.copy(0, self.two, 1).wait()
        self.copy(self.two, 1, 5).start()

    def last(self):
        self.copy(self.one, self.two, 2).wait()
        self.copy(6, 1, 6).start()

    def finish(self):
        for turn, k in ((0, 3), (self.one, 4), (self.two, 5), (6, 6)):
            self.copy(turn, 1, k).wait()


GATHER_SEMS = 7


class RowSums:
    def __init__(self, send, ref, place, height, got_one, got_two, first_sem):
        self.send, self.ref, self.place, self.height = send, ref, place, height
        self.got_one, self.got_two, self.sem = got_one, got_two, first_sem
        self.y, self.x, _ = bits()
        self.half = ref.shape[-1] // 2

    def at(self, y, x, side):
        rows = pl.ds(pl.multiple_of(self.place(y, x), 128), self.height)
        return (rows, slice(side * self.half, (side + 1) * self.half))

    def pairs(self, k, mine):
        y, x = self.y, self.x
        return [
            (y if mine else 1 - y, k, 0),
            (k, x if mine else 1 - x, 1),
        ]

    def first(self, k, side):
        y, x, _ = self.pairs(k, False)[side]
        return self.send(
            self.ref.at[self.at(y, x, side)], self.got_one.at[side, k], self.sem + 2 * side + k,
            peer_of((4, 2)[side], 0),
        )

    def second(self, side):
        y, x = ((self.y, 1 - self.x), (1 - self.y, self.x))[side]
        return self.send(
            self.ref.at[self.at(y, x, side)], self.got_two.at[side], self.sem + 4 + side,
            peer_of((2, 4)[side], 0),
        )

    def start(self):
        for side in range(2):
            for k in range(2):
                self.first(k, side).start()

    def relay(self):
        for side in range(2):
            for k in range(2):
                self.first(k, side).wait()
        for side in range(2):
            for k in range(2):
                y, x, _ = self.pairs(k, True)[side]
                at = self.at(y, x, side)
                self.ref[at] = (
                    self.ref[at].astype(f32) + self.got_one[side, k].astype(f32)
                ).astype(bf16)
        for side in range(2):
            self.second(side).start()

    def finish(self):
        for side in range(2):
            self.second(side).wait()
            at = self.at(self.y, self.x, side)
            self.ref[at] = (
                self.ref[at].astype(f32) + self.got_two[side].astype(f32)
            ).astype(bf16)


ROW_SEMS = 6


def start_body(
    lengths, tokens_ref, weights_ref,
    gathered_ref, mixed_ref, context_ref, parts_ref, lse_ref, heads_ref, out_ref, length_ref, up_ref, down_ref,
    keys, values, length_buf, out_here, out_far, local_sems, send_sems, recv_sems,
):
    chunks, rows, _ = gathered_ref.shape
    width = context_ref.shape[-1]
    lanes = up_ref.shape[-1]
    hidden_width = SHARE * lanes
    piece = rows // 4
    quarter_rows = D // 4
    y, x, c = bits()
    z = lax.axis_index("tensor")
    matched = c == z // 2
    unmatched = jnp.logical_not(matched)
    own_block = block_of(y, x, c)
    send = sender(send_sems, recv_sems)
    core, near_z, diagonal, swapped = peer_of(1, 0), peer_of(0, 1), peer_of(1, 1), peer_of(1, 2)
    across_x, across_y, across_xy = peer_of(2, 0), peer_of(4, 0), peer_of(6, 0)

    def part_of(k):
        return slice(k * piece, (k + 1) * piece)

    def swap_copy(k):
        return send(tokens_ref.at[part_of(k), :], gathered_ref.at[0, part_of(k), :], k, swapped)

    def far_copy(k, source):
        return send(source.at[part_of(k), :], gathered_ref.at[2, part_of(k), :], 4 + k, near_z)

    def near_copy(k, source):
        return send(source.at[part_of(k), :], gathered_ref.at[1, part_of(k), :], 8 + k, core)

    def diagonal_copy(k):
        return send(gathered_ref.at[2, part_of(k), :], gathered_ref.at[3, part_of(k), :], 12 + k, core)

    column = 2 * y + x

    def quarter(k):
        return pl.ds(pl.multiple_of(k * quarter_rows, quarter_rows), quarter_rows)

    def heads_swap():
        return send(
            weights_ref.at[quarter(column), : 3 * width], heads_ref.at[quarter(column), :], 16, swapped
        )

    def heads_share(k, peer):
        return send(heads_ref.at[quarter(column), :], heads_ref.at[quarter(column), :], 17 + k, peer)

    heads_peers = (across_x, across_y, across_xy)
    heads_local = pltpu.make_async_copy(weights_ref.at[:, : 3 * width], heads_ref, local_sems.at[0])

    def out_copy(e):
        return send(out_here, out_far.at[e - 1], 19 + e, peer_of(0, e))

    out_local = pltpu.make_async_copy(
        weights_ref.at[row_block(own_block), 3 * width : 4 * width], out_here, local_sems.at[1]
    )
    outs = [
        Gather(
            send, lambda k, side=side: out_ref.at[row_block(k), side * 2 * width : (side + 1) * 2 * width],
            23 + side * GATHER_SEMS, side == 0,
        )
        for side in range(2)
    ]
    base = 23 + 2 * GATHER_SEMS
    targets = (up_ref, down_ref)

    def feed_source(kind):
        at = 4 * width + kind * hidden_width + own_block * lanes
        return weights_ref.at[:, pl.ds(pl.multiple_of(at, 128), lanes)]

    def feed_copy(kind, e):
        return send(feed_source(kind), targets[kind].at[e - 1, 0, 0], base + 3 * kind + e - 1, peer_of(0, e))

    half = slice(0, D // 2), slice(D // 2, D)

    def feed_one(kind, e, side):
        source = targets[kind].at[e - 1, 0, 0, half[side], :]
        target = targets[kind].at[e - 1, side, 1 - side, half[side], :]
        return send(
            source, target, base + 6 + 6 * kind + 2 * (e - 1) + side, (across_x, across_y)[side]
        )

    def feed_two(e, side):
        if side == 0:
            source, target = (up_ref.at[e - 1, dy, 0:2, half[0], :] for dy in range(2))
        else:
            source, target = (up_ref.at[e - 1, 0:2, dx, half[1], :] for dx in range(2))
        return send(source, target, base + 18 + 2 * (e - 1) + side, (across_y, across_x)[side])

    def first_hop(kind, e):
        feed_copy(kind, e).wait()
        for side in range(2):
            feed_one(kind, e, side).start()

    def second_hop(e):
        for side in range(2):
            feed_one(0, e, side).wait()
        for side in range(2):
            feed_two(e, side).start()

    def length_copy():
        return send(length_buf.at[0], length_buf.at[1], base + 24, core)

    def part_copy(j):
        return send(
            context_ref.at[j], parts_ref.at[j], base + 24 + j, (None, core, near_z, diagonal)[j]
        )

    def send_weights():
        for e in (3, 2, 1):
            feed_copy(0, e).start()
        for e in (3, 2, 1):
            feed_copy(1, e).start()

    out_local.start()
    length_buf[0] = jnp.full(length_buf.shape[1:], lengths[0], jnp.int32)
    greet(
        [core, near_z, diagonal, swapped, across_x, across_y, across_xy, peer_of(0, 2), peer_of(0, 3)]
    )

    @pl.when(matched)
    def _():
        for k in range(4):
            far_copy(k, tokens_ref).start()
            near_copy(k, tokens_ref).start()
        heads_local.start()
        gathered_ref[0] = tokens_ref[...]

    @pl.when(unmatched)
    def _():
        for k in range(4):
            swap_copy(k).start()
        heads_swap().start()

    length_copy().start()

    @pl.when(unmatched)
    def _():
        for k in range(4):
            swap_copy(k).wait()
            far_copy(k, gathered_ref.at[0]).start()
            near_copy(k, gathered_ref.at[0]).start()
        heads_swap().wait()
        for k, peer in enumerate(heads_peers):
            heads_share(k, peer).start()

    for k in range(4):
        far_copy(k, tokens_ref).wait()
        diagonal_copy(k).start()
    out_local.wait()
    for e in (1, 2, 3):
        out_copy(e).start()
    send_weights()
    out_ref[row_block(own_block), :width] = out_here[...]

    @pl.when(matched)
    def _():
        heads_local.wait()

    @pl.when(unmatched)
    def _():
        for k, peer in enumerate(heads_peers):
            heads_share(k, peer).wait()

    length_copy().wait()
    length_ref[...] = jnp.where(matched, length_buf[0], length_buf[1])
    length = length_ref[:1, :]
    own_quarter = jnp.where(matched, z, z + 2 - 4 * (z // 2))
    wide = 256

    def project(j):
        def columns(n, carry):
            at = pl.ds(pl.multiple_of(n * wide, wide), wide)
            mixed_ref[j, :, at] = jnp.dot(
                gathered_ref[j], heads_ref[:, at], preferred_element_type=f32
            ).astype(bf16)
            return carry

        lax.fori_loop(0, 3 * width // wide, columns, 0)

    def arrange(j):
        at_quarter = own_quarter
        if j in (1, 3):
            at_quarter = at_quarter + 2 - 4 * (at_quarter // 2)
        if j in (2, 3):
            at_quarter = at_quarter + 1 - 2 * (at_quarter % 2)
        for h in range(width // HEAD_DIM):
            at = width + (h // 2) * 128
            keys[h, j * rows : (j + 1) * rows, :] = head_keys(
                mixed_ref[j, :, at : at + 128], h % 2, at_quarter * rows, length
            )
        values[j * rows : (j + 1) * rows, :] = mixed_ref[j, :, 2 * width :]

    for j in (0, 2, 1, 3):
        if j == 1:
            for k in range(4):
                near_copy(k, tokens_ref).wait()
        if j == 3:
            for k in range(4):
                diagonal_copy(k).wait()
        project(j)
        arrange(j)

    lane = lax.broadcasted_iota(jnp.int32, (rows, 128), 1)

    def attend(step, carry):
        chunk = chunks - 1 - step
        logs = jnp.zeros((rows, 128), f32)
        for pair in range(width // 128):
            queries = mixed_ref[chunk, :, pair * 128 : pair * 128 + 128]
            both = []
            for side in range(2):
                h = pair * 2 + side
                scores = contract(head_queries(queries, side), keys[h], 1, 1)
                top = jnp.max(scores, axis=1, keepdims=True)
                weight = jnp.exp(scores - top)
                total = jnp.sum(weight, axis=1, keepdims=True)
                out = contract(weight.astype(bf16), values[:, pair * 128 : pair * 128 + 128], 1, 0)
                both.append(out / total)
                logs = jnp.where(lane == h, top + jnp.log(total), logs)
            context_ref[chunk, :, pair * 128 : pair * 128 + 128] = jnp.where(
                lane < HEAD_DIM, both[0], both[1]
            ).astype(bf16)
        lse_ref[chunk] = jnp.transpose(logs)[:8, :]

        @pl.when(step == 0)
        def _():
            part_copy(3).start()
            for e in (1, 2, 3):
                out_copy(e).wait()
                out_ref[row_block(own_block), e * width : (e + 1) * width] = out_far[e - 1]
            for gather in outs:
                gather.start()
            first_hop(0, 3)

        @pl.when(step == 1)
        def _():
            part_copy(2).start()
            for gather in outs:
                gather.relay()
            first_hop(0, 2)
            second_hop(3)

        @pl.when(step == 2)
        def _():
            part_copy(1).start()
            for gather in outs:
                gather.last()
            first_hop(0, 1)
            second_hop(2)

        return carry

    lax.fori_loop(0, chunks, attend, 0)
    parts_ref[0] = context_ref[0]
    for gather in outs:
        gather.finish()
    second_hop(1)
    for e in (3, 2, 1):
        first_hop(1, e)
    for j in (3, 2, 1):
        part_copy(j).wait()
    for e in (3, 2, 1):
        for side in range(2):
            feed_two(e, side).wait()
            feed_one(1, e, side).wait()


def start_block(lengths, tokens, weights):
    rows = tokens.shape[0]
    chunks = 4
    tile = D // 4
    seq = chunks * rows
    lanes = FF // 4 // SHARE
    heads = tile // HEAD_DIM
    sems = 23 + 2 * GATHER_SEMS + 28
    share_rows = D // SHARE
    vmem, anywhere = pl.BlockSpec(memory_space=pltpu.VMEM), pl.BlockSpec(memory_space=pl.ANY)
    return pl.pallas_call(
        start_body,
        name="start_block",
        in_specs=[pl.BlockSpec(memory_space=pltpu.SMEM), vmem, anywhere],
        out_specs=[vmem] * 8 + [anywhere] * 2,
        out_shape=[
            jax.ShapeDtypeStruct((chunks, rows, D), bf16),
            jax.ShapeDtypeStruct((chunks, rows, 3 * tile), bf16),
            jax.ShapeDtypeStruct((chunks, rows, tile), bf16),
            jax.ShapeDtypeStruct((chunks, rows, tile), bf16),
            jax.ShapeDtypeStruct((chunks, 8, rows), f32),
            jax.ShapeDtypeStruct((D, 3 * tile), bf16),
            jax.ShapeDtypeStruct((D, D), bf16),
            jax.ShapeDtypeStruct((8, 128), jnp.int32),
            jax.ShapeDtypeStruct((3, 2, 2, D, lanes), bf16),
            jax.ShapeDtypeStruct((3, 2, 2, D, lanes), bf16),
        ],
        scratch_shapes=[
            pltpu.VMEM((heads, seq, 128), bf16),
            pltpu.VMEM((seq, tile), bf16),
            pltpu.VMEM((2, 8, 128), jnp.int32),
            pltpu.VMEM((share_rows, tile), bf16),
            pltpu.VMEM((3, share_rows, tile), bf16),
            pltpu.SemaphoreType.DMA((2,)),
            pltpu.SemaphoreType.DMA((sems,)),
            pltpu.SemaphoreType.DMA((sems,)),
        ],
        compiler_params=pltpu.CompilerParams(
            vmem_limit_bytes=60 << 20, collective_id=0, has_side_effects=True
        ),
        cost_estimate=pl.CostEstimate(
            flops=24 * heads * seq * seq * HEAD_DIM, bytes_accessed=20 << 20, transcendentals=0
        ),
    )(lengths, tokens, weights)


def back_body(
    info, mixed_ref, context_ref, upstream_ref, lse_ref, weight_ref, branch_ref, norm_ref, outputs_ref, gathered,
    up_grads, down_grads, out_grads,
    input_out, outputs_out, norm_out, attention_out, feed_out,
    keys, turned, key_sum, value_sum, query_t, grad, rows_held, heads_sum, kept, got_one, got_two, got_three,
    leaving, landed, share, heads, heads_one, heads_two, heads_mine, heads_far, out_held, out_core, out_one, out_two, out_z,
    norm_here, norm_there, input_ref, local_sems, send_sems, recv_sems,
):
    chunks, rows, _ = mixed_ref.shape
    width = context_ref.shape[-1]
    scale = HEAD_DIM ** (-0.5)
    part = 256
    core, near_z = peer_of(1, 0), peer_of(0, 1)
    across = (peer_of(2, 0), peer_of(4, 0))
    send = sender(send_sems, recv_sems)
    sources = (up_grads, down_grads)
    y, x, c = bits()
    z = lax.axis_index("tensor")
    matched = c == z // 2
    own_block = block_of(y, x, c)

    def stage_one(b, kind):
        return send(sources[kind].at[b, 1], got_one.at[b, kind], 2 * b + kind, across[kind])

    def stage_two(b, kind):
        return send(kept.at[b, kind, 1], got_two.at[b, kind], 8 + 2 * b + kind, across[1 - kind])

    def stage_three(b):
        return send(kept.at[b, :, 0], got_three.at[b - 1], 15 + b, peer_of(0, b))

    def load(b, kind):
        return pltpu.make_async_copy(
            sources[kind].at[b, 0], kept.at[b, kind], local_sems.at[2 * b + kind]
        )

    def start_one(b):
        for kind in range(2):
            stage_one(b, kind).start()

    def start_two(b):
        for kind in range(2):
            load(b, kind).wait()
            stage_one(b, kind).wait()
            for k in (1, 0):
                kept[b, kind, k] = (
                    kept[b, kind, k].astype(f32) + got_one[b, kind, k].astype(f32)
                ).astype(bf16)
        for kind in range(2):
            stage_two(b, kind).start()

    def start_three(b):
        for kind in range(2):
            stage_two(b, kind).wait()
            kept[b, kind, 0] = (
                kept[b, kind, 0].astype(f32) + got_two[b, kind].astype(f32)
            ).astype(bf16)
        if b:
            stage_three(b).start()

    def load_rows(j):
        return pltpu.make_async_copy(gathered.at[j], rows_held.at[j], local_sems.at[8 + j])

    def out_load():
        return pltpu.make_async_copy(out_grads, out_held, local_sems.at[12])

    def out_core_copy(k):
        at = row_block(block_of(k // 2, k % 2, 1 - c))
        return send(out_grads.at[at, :], out_core.at[k], 22 + k, core)

    out_sums = RowSums(
        send, out_held, lambda yy, xx: block_of(yy, xx, c) * 128, 128, out_one, out_two, 26
    )

    def out_z_copy(e):
        at = (row_block(own_block), slice(e * width, (e + 1) * width))
        return send(out_held.at[at], out_z.at[e - 1], 31 + e, peer_of(0, e))

    def out_start():
        out_load().wait()
        for k in range(4):
            out_core_copy(k).wait()
        for k in range(4):
            at = row_block(block_of(k // 2, k % 2, c))
            out_held[at, :] = (out_held[at, :].astype(f32) + out_core[k].astype(f32)).astype(bf16)
        out_sums.start()

    def out_last():
        out_sums.finish()
        for e in (1, 2, 3):
            out_z_copy(e).start()

    norm_turns = ((1, 0), (2, 0), (4, 0), (0, 1), (0, 2))

    def norm_copy(k):
        return send(norm_here.at[k], norm_there.at[k], 35 + k, peer_of(*norm_turns[k]))

    def norm_step(k):
        norm_copy(k).wait()
        total = norm_here[k] + norm_there[k]
        if k + 1 < len(norm_turns):
            norm_here[k + 1] = total
            norm_copy(k + 1).start()
        else:
            norm_out[...] = total

    for b in (3, 2, 1, 0):
        for kind in range(2):
            load(b, kind).start()
    for j in range(chunks):
        load_rows(j).start()
    out_load().start()
    norm_here[0] = norm_ref[...]
    greet([core, near_z, across[0], across[1], peer_of(0, 2), peer_of(0, 3), peer_of(1, 2)])
    for k in range(4):
        out_core_copy(k).start()
    norm_copy(0).start()
    start_one(3)
    start_one(2)

    def return_copy(source, target, k):
        return send(source, target, 49 + 4 * GATHER_SEMS + k, peer_of(1, 2))

    outputs_local = pltpu.make_async_copy(outputs_ref, outputs_out, local_sems.at[15])

    @pl.when(matched)
    def _():
        outputs_local.start()

    @pl.when(jnp.logical_not(matched))
    def _():
        return_copy(outputs_ref, outputs_out, 0).start()

    key_sum[...] = jnp.zeros_like(key_sum)
    value_sum[...] = jnp.zeros_like(value_sum)
    for j in range(chunks):
        for h in range(width // HEAD_DIM):
            at = width + (h // 2) * 128
            keys[h, j * rows : (j + 1) * rows, :] = head_keys(
                mixed_ref[j, :, at : at + 128], h % 2, info[1 + j], info[0]
            )
        turned[:, j * rows : (j + 1) * rows] = jnp.transpose(
            mixed_ref[j, :, width : 2 * width].astype(f32)
        ).astype(bf16)
    feature = lax.broadcasted_iota(jnp.int32, (8, width), 1) // HEAD_DIM
    picks = (feature == lax.broadcasted_iota(jnp.int32, (8, width), 0)).astype(f32)
    per_chunk = rows // part

    def attend(step, carry):
        chunk = step // per_chunk
        at = pl.ds(pl.multiple_of((step % per_chunk) * part, part), part)
        upstream = upstream_ref[chunk, at, :]
        product = upstream.astype(f32) * context_ref[chunk, at, :].astype(f32)
        delta = lax.dot_general(
            picks, product, (((1,), (1,)), ((), ())), precision=lax.Precision.HIGHEST,
            preferred_element_type=f32,
        )
        lse = lse_ref[chunk, :, at]
        for pair in range(width // 128):
            lanes = slice(pair * 128, pair * 128 + 128)
            queries = mixed_ref[chunk, at, lanes]
            value_rows = mixed_ref[:, :, 2 * width + pair * 128 : 2 * width + pair * 128 + 128]
            value_rows = value_rows.reshape(chunks * rows, 128)
            for half in range(2):
                h = pair * 2 + half
                scores = contract(keys[h], head_queries(queries, half), 1, 1)
                weight = jnp.exp(scores - lse[h : h + 1, :])
                up_half = head_half(upstream[:, lanes], half)
                back = contract(value_rows, up_half, 1, 1)
                score_grad = (weight * (back - delta[h : h + 1, :])).astype(bf16)
                value_sum[pair] += contract(weight.astype(bf16), up_half, 1, 0)
                key_sum[pair] += contract(score_grad, head_half(queries, half), 1, 0)
                query_t[h * HEAD_DIM : (h + 1) * HEAD_DIM, :] = (
                    contract(turned[h * HEAD_DIM : (h + 1) * HEAD_DIM, :], score_grad, 1, 0) * scale
                )
        grad[chunk, at, :width] = jnp.transpose(query_t[...]).astype(bf16)

        @pl.when(step == 0)
        def _():
            norm_step(0)
            out_start()

        @pl.when(step == 1)
        def _():
            norm_step(1)
            start_two(3)
            start_one(1)

        @pl.when(step == 2)
        def _():
            norm_step(2)
            out_sums.relay()

        @pl.when(step == 3)
        def _():
            norm_step(3)
            start_two(2)
            start_one(0)
            start_three(3)

        @pl.when(step == 4)
        def _():
            norm_step(4)
            out_last()

        @pl.when(step == 6)
        def _():
            start_two(1)

        return carry

    lax.fori_loop(0, chunks * per_chunk, attend, 0)
    for j in range(chunks):
        at = slice(j * rows, (j + 1) * rows)
        for pair in range(width // 128):
            left = width + pair * 128
            grad[j, :, left : left + 128] = (key_sum[pair, at, :] * scale).astype(bf16)
            grad[j, :, left + width : left + width + 128] = value_sum[pair, at, :].astype(bf16)
    start_three(2)

    def rows_back(j):
        return contract(grad[j], weight_ref[...], 1, 1)

    core_copies = {}
    for k, j in enumerate((3, 1)):
        leaving[k] = rows_back(j).astype(bf16)
        core_copies[j] = send(leaving.at[k], landed.at[k], 19 + k, core)
        core_copies[j].start()
    far = rows_back(2)
    core_copies[3].wait()
    leaving[2] = (far + landed[0].astype(f32)).astype(bf16)
    far_copy = send(leaving.at[2], landed.at[2], 21, near_z)
    branch_ref_value = branch_ref[...] + rows_back(0)
    core_copies[1].wait()
    own_rows = branch_ref_value + landed[1].astype(f32)

    heads_sum[...] = jnp.zeros_like(heads_sum)
    for j in range(chunks):
        load_rows(j).wait()

    def weigh(j, carry):
        heads_sum[...] += contract(rows_held[j], grad[j], 0, 0)
        return carry

    lax.fori_loop(0, chunks, weigh, 0)
    heads[...] = heads_sum[...].astype(bf16)
    head_sums = RowSums(
        send, heads, lambda yy, xx: block_of(yy, xx, 0) * 128, 256, heads_one, heads_two, 40
    )
    head_sums.start()
    start_three(1)
    far_copy.start()
    start_two(0)
    head_sums.relay()
    start_three(0)
    head_sums.finish()

    def half_rows(k):
        return row_block(block_of(y, x, k))

    @pl.when(matched)
    def _():
        send(heads.at[half_rows(1 - c), :], heads_mine, 46, core).start()

    @pl.when(jnp.logical_not(matched))
    def _():
        send(heads.at[half_rows(c), :], heads_far, 47, peer_of(0, 2)).start()
        send(heads.at[half_rows(1 - c), :], heads_far, 48, peer_of(1, 2)).start()

    total = kept[0, :, 0].astype(f32)
    for b in (3, 2, 1):
        stage_three(b).wait()
        total = total + got_three[b - 1].astype(f32)
    share[...] = total.astype(bf16)
    own_feed = [
        pltpu.make_async_copy(share.at[kind], feed_out.at[own_block, kind], local_sems.at[13 + kind])
        for kind in range(2)
    ]
    for copy in own_feed:
        copy.start()
    feeds = [
        Gather(send, lambda k, kind=kind: feed_out.at[k, kind], 49 + kind * GATHER_SEMS, kind == 0)
        for kind in range(2)
    ]
    for copy in own_feed:
        copy.wait()
    for feed in feeds:
        feed.start()
    sum_out = out_held[row_block(own_block), :width].astype(f32)
    for e in (1, 2, 3):
        out_z_copy(e).wait()
        sum_out = sum_out + out_z[e - 1].astype(f32)
    attention_out[row_block(own_block), 3 * width :] = sum_out.astype(bf16)

    @pl.when(matched)
    def _():
        send(heads.at[half_rows(1 - c), :], heads_mine, 46, core).wait_send()
        heads_mine[...] = heads[half_rows(c), :]

    @pl.when(jnp.logical_not(matched))
    def _():
        send(heads.at[half_rows(c), :], heads_far, 47, peer_of(0, 2)).wait_send()
        send(heads.at[half_rows(1 - c), :], heads_far, 48, peer_of(1, 2)).wait_send()
        send(heads.at[half_rows(c), :], heads_mine, 46, core).wait_recv()

    @pl.when(matched)
    def _():
        send(heads.at[half_rows(c), :], heads_far, 47, peer_of(0, 2)).wait_recv()

    @pl.when(jnp.logical_not(matched))
    def _():
        send(heads.at[half_rows(c), :], heads_far, 48, peer_of(1, 2)).wait_recv()

    attention_out[row_block(own_block), : 3 * width] = (
        heads_mine[...].astype(f32) + heads_far[...].astype(f32)
    ).astype(bf16)
    sides = [
        Gather(
            send,
            lambda k, side=side: attention_out.at[row_block(k), side * 2 * width : (side + 1) * 2 * width],
            49 + (2 + side) * GATHER_SEMS, side == 0,
        )
        for side in range(2)
    ]
    for side in sides:
        side.start()
    far_copy.wait()
    input_ref[...] = (own_rows + landed[2].astype(f32)).astype(bf16)

    @pl.when(matched)
    def _():
        input_out[...] = input_ref[...]

    @pl.when(jnp.logical_not(matched))
    def _():
        return_copy(input_ref, input_out, 1).start()

    for gather in feeds + sides:
        gather.relay()
    for gather in feeds + sides:
        gather.last()
    for gather in feeds + sides:
        gather.finish()
    @pl.when(matched)
    def _():
        outputs_local.wait()

    @pl.when(jnp.logical_not(matched))
    def _():
        return_copy(outputs_ref, outputs_out, 0).wait()
        return_copy(input_ref, input_out, 1).wait()


def back_block(info, mixed, context, upstream, lse, weight, branch, norm_sums, outputs, gathered, up_grads,
               down_grads, out_grads):
    chunks, rows, width3 = mixed.shape
    width = width3 // 3
    seq = chunks * rows
    heads = width // HEAD_DIM
    lanes = up_grads.shape[-1]
    share_rows = D // SHARE
    sems = 51 + 4 * GATHER_SEMS
    vmem, anywhere = pl.BlockSpec(memory_space=pltpu.VMEM), pl.BlockSpec(memory_space=pl.ANY)
    return pl.pallas_call(
        back_body,
        name="back_block",
        in_specs=[pl.BlockSpec(memory_space=pltpu.SMEM)] + [vmem] * 7 + [anywhere] * 5,
        out_specs=[vmem, vmem, vmem, vmem, anywhere],
        out_shape=[
            jax.ShapeDtypeStruct((rows, D), bf16),
            jax.ShapeDtypeStruct((rows, D), bf16),
            jax.ShapeDtypeStruct((4, D), f32),
            jax.ShapeDtypeStruct((D, 4 * width), bf16),
            jax.ShapeDtypeStruct((SHARE, 2, D, lanes), bf16),
        ],
        scratch_shapes=[
            pltpu.VMEM((heads, seq, 128), bf16),
            pltpu.VMEM((width, seq), bf16),
            pltpu.VMEM((width // 128, seq, 128), f32),
            pltpu.VMEM((width // 128, seq, 128), f32),
            pltpu.VMEM((width, 256), f32),
            pltpu.VMEM((chunks, rows, width3), bf16),
            pltpu.VMEM((chunks, rows, D), bf16),
            pltpu.VMEM((D, width3), f32),
            pltpu.VMEM((4, 2, 2, D, lanes), bf16),
            pltpu.VMEM((4, 2, 2, D, lanes), bf16),
            pltpu.VMEM((4, 2, D, lanes), bf16),
            pltpu.VMEM((3, 2, D, lanes), bf16),
            pltpu.VMEM((3, rows, D), bf16),
            pltpu.VMEM((3, rows, D), bf16),
            pltpu.VMEM((2, D, lanes), bf16),
            pltpu.VMEM((D, width3), bf16),
            pltpu.VMEM((2, 2, 2 * share_rows, width3 // 2), bf16),
            pltpu.VMEM((2, 2 * share_rows, width3 // 2), bf16),
            pltpu.VMEM((share_rows, width3), bf16),
            pltpu.VMEM((share_rows, width3), bf16),
            pltpu.VMEM((D, 4 * width), bf16),
            pltpu.VMEM((4, share_rows, 4 * width), bf16),
            pltpu.VMEM((2, 2, share_rows, 2 * width), bf16),
            pltpu.VMEM((2, share_rows, 2 * width), bf16),
            pltpu.VMEM((3, share_rows, width), bf16),
            pltpu.VMEM((5, 4, D), f32),
            pltpu.VMEM((5, 4, D), f32),
            pltpu.VMEM((rows, D), bf16),
            pltpu.SemaphoreType.DMA((16,)),
            pltpu.SemaphoreType.DMA((sems,)),
            pltpu.SemaphoreType.DMA((sems,)),
        ],
        compiler_params=pltpu.CompilerParams(
            vmem_limit_bytes=67043328, collective_id=2, has_side_effects=True
        ),
        cost_estimate=pl.CostEstimate(
            flops=40 * heads * seq * seq * HEAD_DIM, bytes_accessed=40 << 20, transcendentals=0
        ),
    )(
        info, mixed, context, upstream, lse, weight, branch, norm_sums, outputs, gathered, up_grads, down_grads,
        out_grads,
    )


def adam_body(owned, attention_ref, feed_ref, master_ref, one_ref, two_ref,
              grad_out, master_out, one_out, two_out, tiles_out, up_out, down_out):
    tile = grad_out.shape[-1] // 4
    for s in range(4):
        at = slice(s * tile, (s + 1) * tile)
        grad = jnp.zeros((grad_out.shape[0], tile), f32)
        for i in range(4):
            value = attention_ref[:, i * tile : (i + 1) * tile].astype(f32)
            grad = jnp.where(owned[s, i] > 0, value, grad)
        for kind in range(2):
            value = jnp.concatenate([feed_ref[2 * s + k, kind] for k in range(2)], axis=-1)
            grad = jnp.where(owned[s, 4 + 4 * kind + s] > 0, value.astype(f32), grad)
        occupied = (owned[s, 12] > 0).astype(f32)
        param, first, second = adam_update(
            grad, master_ref[:, at], one_ref[:, at], two_ref[:, at], occupied, weight_decay
        )
        grad_out[:, at] = grad
        master_out[:, at] = param
        one_out[:, at] = first
        two_out[:, at] = second
        low = param.astype(bf16)
        none = jnp.zeros_like(low)
        for i in range(4):
            mine = jnp.where(owned[s, i] > 0, low, none)
            there = slice(i * tile, (i + 1) * tile)
            tiles_out[:, there] = mine if s == 0 else tiles_out[:, there] + mine
        for kind, target in ((0, up_out), (1, down_out)):
            mine = jnp.where(owned[s, 4 + 4 * kind + s] > 0, low, none)
            for k in range(2):
                target[2 * s + k] = mine[:, k * tile // 2 : (k + 1) * tile // 2]


def adam_block(owned, attention_grad, feed_grad, master, one, two):
    part = 128
    wide = pl.BlockSpec((part, D), lambda i: (i, 0))
    lanes = feed_grad.shape[-1]
    split = pl.BlockSpec((SHARE, part, lanes), lambda i: (0, i, 0))
    return pl.pallas_call(
        adam_body,
        grid=(D // part,),
        name="adam_block",
        in_specs=[
            pl.BlockSpec(memory_space=pltpu.SMEM), wide,
            pl.BlockSpec((SHARE, 2, part, lanes), lambda i: (0, 0, i, 0)), wide, wide, wide,
        ],
        out_specs=[wide] * 5 + [split] * 2,
        out_shape=[jax.ShapeDtypeStruct((D, D), f32)] * 4
        + [jax.ShapeDtypeStruct((D, D), bf16)]
        + [jax.ShapeDtypeStruct((SHARE, D, lanes), bf16)] * 2,
        compiler_params=pltpu.CompilerParams(vmem_limit_bytes=62 << 20),
        cost_estimate=pl.CostEstimate(flops=40 * D * D, bytes_accessed=40 << 20, transcendentals=0),
    )(owned, attention_grad, feed_grad, master, one, two)


def tiles_body(tiles_ref, up_ref, down_ref, tiles_out, up_out, down_out, *scratch):
    core_got = scratch[:3]
    one_got, two_got = scratch[3:5], scratch[5:7]
    work = scratch[7:10]
    row_one, row_two, send_sems, recv_sems = scratch[10:]
    send = sender(send_sems, recv_sems)
    y, x, c = bits()
    core = peer_of(1, 0)
    own_block = block_of(y, x, c)
    greet([core, peer_of(2, 0), peer_of(4, 0)])
    arrays = ((up_ref, up_out), (down_ref, down_out), (tiles_ref, tiles_out))

    def place(n, ref, block):
        return ref.at[row_block(block), :] if n == 2 else ref.at[block]

    def core_copy(n, k):
        return send(
            place(n, arrays[n][0], block_of(k // 2, k % 2, 1 - c)), core_got[n].at[k], 4 * n + k, core
        )

    def core_add(n):
        source, target = arrays[n][0], work[n]
        for k in range(4):
            core_copy(n, k).wait()
        for k in range(4):
            block = block_of(k // 2, k % 2, c)
            if n == 2:
                at = row_block(block)
                target[at, :] = source[at, :] + core_got[n][k]
            else:
                target[k] = source[block] + core_got[n][k]

    def first(n, k):
        y_, x_ = ((k, 1 - x), (1 - y, k))[n]
        return send(
            work[n].at[2 * y_ + x_], one_got[n].at[k], 12 + 2 * n + k,
            peer_of((2, 4)[n], 0),
        )

    def second(n):
        y_, x_ = ((1 - y, x), (y, 1 - x))[n]
        return send(
            work[n].at[2 * y_ + x_], two_got[n], 16 + n, peer_of((4, 2)[n], 0)
        )

    def relay(n):
        target = work[n]
        for k in range(2):
            first(n, k).wait()
        for k in range(2):
            y_, x_ = ((k, x), (y, k))[n]
            block = 2 * y_ + x_
            target[block] = target[block] + one_got[n][k]
        second(n).start()

    def settle(n):
        second(n).wait()
        arrays[n][1][own_block] = work[n][2 * y + x] + two_got[n][...]

    for n in range(3):
        for k in range(4):
            core_copy(n, k).start()
    for n in range(2):
        core_add(n)
        for k in range(2):
            first(n, k).start()
    core_add(2)
    rows = RowSums(
        send, work[2], lambda yy, xx: block_of(yy, xx, c) * 128, 128, row_one, row_two, 18
    )
    rows.start()
    for n in range(2):
        relay(n)
    rows.relay()
    gathers = []
    for n in range(2):
        settle(n)
        gathers.append(
            Gather(send, lambda k, n=n: arrays[n][1].at[k], 24 + n * GATHER_SEMS, n == 0)
        )
        gathers[-1].start()
    rows.finish()
    tiles_out[row_block(own_block), :] = work[2][row_block(own_block), :]
    half = tiles_out.shape[-1] // 2
    for side in range(2):
        gathers.append(
            Gather(
                send,
                lambda k, side=side: tiles_out.at[row_block(k), side * half : (side + 1) * half],
                24 + (2 + side) * GATHER_SEMS, side == 0,
            )
        )
        gathers[-1].start()
    for gather in gathers:
        gather.relay()
    for gather in gathers:
        gather.last()
    for gather in gathers:
        gather.finish()


def spread_tiles(tiles, up, down):
    share_rows = D // SHARE
    lanes = up.shape[-1]
    sems = 24 + 4 * GATHER_SEMS
    piece = (D, lanes)
    vmem = pl.BlockSpec(memory_space=pltpu.VMEM)
    return pl.pallas_call(
        tiles_body,
        name="spread_tiles",
        in_specs=[vmem] * 3,
        out_specs=[vmem] * 3,
        out_shape=[jax.ShapeDtypeStruct(v.shape, bf16) for v in (tiles, up, down)],
        scratch_shapes=[
            pltpu.VMEM((4,) + piece, bf16),
            pltpu.VMEM((4,) + piece, bf16),
            pltpu.VMEM((4, share_rows, D), bf16),
            pltpu.VMEM((2,) + piece, bf16),
            pltpu.VMEM((2,) + piece, bf16),
            pltpu.VMEM(piece, bf16),
            pltpu.VMEM(piece, bf16),
            pltpu.VMEM((4,) + piece, bf16),
            pltpu.VMEM((4,) + piece, bf16),
            pltpu.VMEM((D, D), bf16),
            pltpu.VMEM((2, 2, share_rows, D // 2), bf16),
            pltpu.VMEM((2, share_rows, D // 2), bf16),
            pltpu.SemaphoreType.DMA((sems,)),
            pltpu.SemaphoreType.DMA((sems,)),
        ],
        compiler_params=pltpu.CompilerParams(
            vmem_limit_bytes=48 << 20, collective_id=3, has_side_effects=True
        ),
        cost_estimate=pl.CostEstimate(flops=D * D, bytes_accessed=12 << 20, transcendentals=0),
    )(tiles, up, down)


def joined(held, i, kind):
    return jnp.concatenate(
        [held[kind, 2 * (i // 2) + m, i % 2, k] for k in range(2) for m in range(2)], axis=-1
    )


def gelu_parts(value):
    bell = jnp.exp(-0.5 * value * value)
    t = 1.0 / (1.0 + (0.3275911 * 0.5**0.5) * jnp.abs(value))
    tail = 0.5 * 1.061405429
    for c in (-1.453152027, 1.421413741, -0.284496736, 0.254829592):
        tail = tail * t + 0.5 * c
    tail = tail * t * bell
    area = jnp.where(value > 0, 1.0 - tail, tail)
    return value * area, area + value * bell * (0.5 / jnp.pi) ** 0.5


def feed_body(
    info, first_ref, cotangent_ref, norms_ref, weights_ref, up_ref, down_ref,
    out_ref, low_ref, both_ref, hidden_ref, pre_ref, grad_ref, sums_ref,
    held, slope, total, leaving, landed, seed_held, local_sems, send_sems, recv_sems,
):
    rows = first_ref.shape[0]
    steps = hidden_ref.shape[0]
    lanes = held.shape[-1]
    y, x, c = bits()
    peer = peer_of(1, 0)
    send = sender(send_sems, recv_sems)
    half = slice(0, D // 2), slice(D // 2, D)
    loads = []
    for kind in range(2):
        for dy in range(2):
            for dx in range(2):
                block = block_of(1 - y if dy else y, 1 - x if dx else x, c)
                at = D + kind * SHARE * lanes + block * lanes
                loads.append(
                    (weights_ref.at[:, pl.ds(pl.multiple_of(at, 128), lanes)], held.at[kind, 0, dy, dx])
                )
    loads.append((up_ref, held.at[0, 1:4]))
    loads.append((down_ref.at[:, 0, 0:2, half[0], :], held.at[1, 1:4, 0, 0:2, half[0], :]))
    loads.append((down_ref.at[:, 0:2, 0, half[1], :], held.at[1, 1:4, 0:2, 0, half[1], :]))
    loads = [pltpu.make_async_copy(a, b, local_sems.at[k]) for k, (a, b) in enumerate(loads)]
    for load in loads:
        load.start()
    greet([peer, peer_of(2, 0), peer_of(4, 0), peer_of(1, 2)])
    matched = c == lax.axis_index("tensor") // 2
    seed_local = pltpu.make_async_copy(cotangent_ref, seed_held, local_sems.at[len(loads)])
    seed_swap = send(cotangent_ref, seed_held, 6, peer_of(1, 2))
    hops = [
        send(
            down_ref.at[:, 0, 0:2, half[0], :], held.at[1, 1:4, 1, 0:2, half[0], :], 4, peer_of(4, 0)
        ),
        send(
            down_ref.at[:, 0:2, 0, half[1], :], held.at[1, 1:4, 0:2, 1, half[1], :], 5, peer_of(2, 0)
        ),
    ]
    for hop in hops:
        hop.start()

    @pl.when(matched)
    def _():
        seed_local.start()

    @pl.when(jnp.logical_not(matched))
    def _():
        seed_swap.start()

    def across(source, target, k):
        return send(source, target, k, peer)

    middle_row = rows // 2
    both_ref[0] = first_ref[...].astype(bf16)
    first_copy = across(both_ref.at[0], both_ref.at[1], 0)
    first_copy.start()

    def up(i, slot):
        weight = joined(held, i, 0)
        for r in range(0, rows, middle_row):
            at = slice(r, r + middle_row)
            value = jnp.dot(both_ref[slot, at, :], weight, preferred_element_type=f32)
            hidden, steep = gelu_parts(value)
            hidden_ref[i, slot, at, :] = hidden.astype(bf16)
            slope[i, slot, at, :] = steep.astype(bf16)

    def down(i, slot):
        total[slot] += contract(hidden_ref[i, slot], joined(held, i, 1), 1, 1)

    def back(i, slot):
        weight = joined(held, i, 1)
        for r in range(0, rows, middle_row):
            at = slice(r, r + middle_row)
            value = jnp.dot(low_ref[slot, at, :], weight, preferred_element_type=f32)
            pre_ref[i, slot, at, :] = (value * slope[i, slot, at, :].astype(f32)).astype(bf16)

    def back_up(i, slot):
        total[slot] += contract(pre_ref[i, slot], joined(held, i, 0), 1, 1)

    def loop(*works):
        def body(i, carry):
            for work in works:
                work(i)
            return carry

        lax.fori_loop(0, steps, body, 0)

    total[...] = jnp.zeros_like(total)
    for load in loads:
        load.wait()
    loop(lambda i: up(i, 0))
    first_copy.wait()
    loop(lambda i: up(i, 1))
    for hop in hops:
        hop.wait()
    loop(lambda i: down(i, 1))
    leaving[...] = total[1].astype(bf16)
    feed_copy = across(leaving, landed.at[0], 1)
    feed_copy.start()
    loop(lambda i: down(i, 0))
    feed_copy.wait()

    @pl.when(matched)
    def _():
        seed_local.wait()

    @pl.when(jnp.logical_not(matched))
    def _():
        seed_swap.wait()

    sums_ref[...] = jnp.zeros_like(sums_ref)
    part = 128

    def middle(r, carry):
        at = pl.ds(pl.multiple_of(r * part, part), part)
        second, normed, inverse = norm_parts(
            first_ref[at, :] + (total[0, at, :] + landed[0, at, :].astype(f32)),
            norms_ref[2:3, :], norms_ref[3:4, :],
        )
        out_ref[at, :] = second.astype(bf16)
        row = lax.broadcasted_iota(jnp.int32, (part, 1), 0) + r * part + info[1]
        seed = seed_held[at, :].astype(f32) * (row < info[0]).astype(f32)
        grad = norm_back(seed, normed, inverse, norms_ref[2:3, :])
        sums_ref[0:1, :] += jnp.sum(seed * normed, axis=0, keepdims=True)
        sums_ref[1:2, :] += jnp.sum(seed, axis=0, keepdims=True)
        total[0, at, :] = grad
        low_ref[0, at, :] = grad.astype(bf16)
        return carry

    lax.fori_loop(0, rows // part, middle, 0)
    low_copy = across(low_ref.at[0], low_ref.at[1], 2)
    low_copy.start()
    total[1] = jnp.zeros_like(total[1])
    loop(lambda i: back(i, 0))
    low_copy.wait()
    loop(lambda i: back(i, 1), lambda i: back_up(i, 1))
    leaving[...] = total[1].astype(bf16)
    grad_copy = across(leaving, landed.at[1], 3)
    grad_copy.start()
    loop(lambda i: back_up(i, 0))
    grad_copy.wait()
    grad_ref[...] = total[0] + landed[1].astype(f32)


def feed_block(info, first, cotangent, norms, weights, up, down):
    rows = first.shape[0]
    lanes = up.shape[-1]
    width = 4 * lanes
    vmem, anywhere = pl.BlockSpec(memory_space=pltpu.VMEM), pl.BlockSpec(memory_space=pl.ANY)
    return pl.pallas_call(
        feed_body,
        name="feed_block",
        in_specs=[pl.BlockSpec(memory_space=pltpu.SMEM), vmem, anywhere, vmem] + [anywhere] * 3,
        out_specs=[vmem] * 7,
        out_shape=[
            jax.ShapeDtypeStruct((rows, D), bf16),
            jax.ShapeDtypeStruct((2, rows, D), bf16),
            jax.ShapeDtypeStruct((2, rows, D), bf16),
            jax.ShapeDtypeStruct((4, 2, rows, width), bf16),
            jax.ShapeDtypeStruct((4, 2, rows, width), bf16),
            jax.ShapeDtypeStruct((rows, D), f32),
            jax.ShapeDtypeStruct((2, D), f32),
        ],
        scratch_shapes=[
            pltpu.VMEM((2, 4, 2, 2, D, lanes), bf16),
            pltpu.VMEM((4, 2, rows, width), bf16),
            pltpu.VMEM((2, rows, D), f32),
            pltpu.VMEM((rows, D), bf16),
            pltpu.VMEM((2, rows, D), bf16),
            pltpu.VMEM((rows, D), bf16),
            pltpu.SemaphoreType.DMA((12,)),
            pltpu.SemaphoreType.DMA((7,)),
            pltpu.SemaphoreType.DMA((7,)),
        ],
        compiler_params=pltpu.CompilerParams(
            vmem_limit_bytes=60 << 20, collective_id=1, has_side_effects=True
        ),
        cost_estimate=pl.CostEstimate(
            flops=64 * rows * D * width, bytes_accessed=30 << 20, transcendentals=0
        ),
    )(info, first, cotangent, norms, weights, up, down)


def feed_grads_body(first_ref, low_ref, hidden_ref, pre_ref, up_ref, down_ref, first_t, low_t):
    rows = first_ref.shape[1]

    @pl.when(pl.program_id(0) == 0)
    def _():
        for slot in range(2):
            at = slice(slot * rows, (slot + 1) * rows)
            first_t[:, at] = jnp.transpose(first_ref[slot].astype(f32)).astype(bf16)
            low_t[:, at] = jnp.transpose(low_ref[slot].astype(f32)).astype(bf16)

    lanes = up_ref.shape[-1]
    width = pre_ref.shape[-1]
    for target, source, turned in ((up_ref, pre_ref, first_t), (down_ref, hidden_ref, low_t)):
        grad = jnp.dot(
            turned[...], source[0].reshape(2 * rows, width), preferred_element_type=f32
        ).astype(bf16)
        for k in range(2):
            for m in range(2):
                at = (2 * k + m) * lanes
                if target is up_ref:
                    target[m, k, 0] = grad[:, at : at + lanes]
                else:
                    target[m, 0, k] = grad[:, at : at + lanes]


def feed_grads(first, low, hidden, pre):
    count, _, rows, width = hidden.shape
    full = pl.BlockSpec((2, rows, D), lambda i: (0, 0, 0))
    piece = pl.BlockSpec((1, 2, rows, width), lambda i: (i, 0, 0, 0))
    lanes = width // 4
    return pl.pallas_call(
        feed_grads_body,
        grid=(count,),
        name="feed_grads",
        in_specs=[full, full, piece, piece],
        out_specs=[
            pl.BlockSpec((2, 2, 1, D, lanes), lambda i: (i // 2, 0, i % 2, 0, 0)),
            pl.BlockSpec((2, 1, 2, D, lanes), lambda i: (i // 2, i % 2, 0, 0, 0)),
        ],
        out_shape=[jax.ShapeDtypeStruct((count, 2, 2, D, lanes), bf16)] * 2,
        scratch_shapes=[pltpu.VMEM((D, 2 * rows), bf16), pltpu.VMEM((D, 2 * rows), bf16)],
        compiler_params=pltpu.CompilerParams(vmem_limit_bytes=48 << 20),
        cost_estimate=pl.CostEstimate(
            flops=8 * rows * D * width * count, bytes_accessed=20 << 20, transcendentals=0
        ),
    )(first, low, hidden, pre)


def layer(n_dp, n_tensor, tokens, weights, norms, cotangent, lengths, owners, master, moment_one,
          moment_two, norm_master, norm_one, norm_two):
    tile = D // n_tensor
    rows = tokens.shape[0]
    device = lax.axis_index("dp")
    z = lax.axis_index("tensor")
    core = device % 2
    matched = core == z // 2
    quarter = jnp.where(matched, z, z ^ 2)

    def flip(x, dd, dz):
        pairs = [
            (d * n_tensor + t, (d ^ dd) * n_tensor + (t ^ dz))
            for d in range(n_dp)
            for t in range(n_tensor)
        ]
        return lax.ppermute(x, AXES, pairs)

    gathered, mixed, context, parts, lse, w_heads, w_out_all, length, up_all, down_all = start_block(
        lengths, tokens[:, 0, :], weights
    )
    own = gathered[0]
    base = jnp.stack([quarter ^ k for k in (0, 2, 1, 3)]) * rows
    info = jnp.concatenate([length[0, :1], base]).astype(jnp.int32)

    context_all = jnp.where(
        matched,
        jnp.concatenate([parts[k] for k in (0, 2, 1, 3)], axis=1),
        jnp.concatenate([parts[k] for k in (1, 3, 0, 2)], axis=1),
    )
    branch = contract(context_all, w_out_all, 1, 1)
    first, first_normed, first_inverse = norm_parts(
        own.astype(f32) + branch, norms[0], norms[1]
    )
    outputs, both_low, both_first, hidden, pre_grad, first_grad, sums_two = feed_block(
        info, first, cotangent[:, 0, :], norms, weights, up_all, down_all
    )
    branch_grad = norm_back(first_grad, first_normed, first_inverse, norms[0])
    gain_one = jnp.sum(first_grad * first_normed, axis=0)
    shift_one = jnp.sum(first_grad, axis=0)
    branch_low = branch_grad.astype(bf16)
    context_grad = jnp.dot(branch_low, w_out_all, preferred_element_type=f32).astype(bf16)
    blocks = [context_grad[:, k * tile : (k + 1) * tile] for k in range(4)]
    blocks = [
        jnp.where(matched, blocks[a], blocks[b]) for a, b in ((0, 2), (2, 0), (1, 3), (3, 1))
    ]
    upstream = jnp.stack(
        [blocks[0], flip(blocks[1], 1, 0), flip(blocks[2], 0, 1), flip(blocks[3], 1, 1)]
    )

    def add(a, b):
        return (a.astype(f32) + b.astype(f32)).astype(bf16)

    up_grads, down_grads = feed_grads(both_first, both_low, hidden, pre_grad)
    out_grad = contract(branch_low, context_all, 0, 0).astype(bf16)
    norm_sums = jnp.concatenate([jnp.stack([gain_one, shift_one]), sums_two])
    input_grad, outputs, norm_grads, attention_grad, feed_grad = back_block(
        info, mixed, context, upstream, lse, w_heads, branch_grad, norm_sums, outputs, gathered, up_grads, down_grads,
        out_grad,
    )

    def over_groups(value, combine):
        bit = SHARE
        while bit < n_dp:
            value = combine(value, flip(value, bit, 0))
            bit *= 2
        return value

    def plus(a, b):
        return a + b

    norm_grads = over_groups(norm_grads, plus)
    attention_grad = over_groups(attention_grad, add)
    feed_grad = over_groups(feed_grad, add)

    tile_owner, slot_index = slot_table(owners)
    slot_ids = jnp.arange(FF // D, dtype=jnp.int32)
    owned = (
        (tile_owner[None, :] == device) & (slot_index[None, :] == slot_ids[:, None])
    ).astype(jnp.int32)
    owned = jnp.concatenate([owned, jnp.sum(owned, axis=1, keepdims=True)], axis=1)
    slot_grad, new_master, new_one, new_two, tiles, up_tiles, down_tiles = adam_block(
        owned, attention_grad, feed_grad, master[0], moment_one[0], moment_two[0]
    )
    tiles, up_tiles, down_tiles = (
        over_groups(v, plus) for v in spread_tiles(tiles, up_tiles, down_tiles)
    )
    new_weights = jnp.concatenate(
        [tiles] + [up_tiles[k] for k in range(SHARE)] + [down_tiles[k] for k in range(SHARE)], axis=1
    )
    norm_owner = (device == owners[6]).astype(f32)
    new_norm_master, new_norm_one, new_norm_two = adam_update(
        norm_grads, norm_master[0], norm_one[0], norm_two[0], norm_owner, 0.0
    )
    return (
        outputs[:, None, :],
        input_grad[:, None, :],
        slot_grad[None],
        new_master[None],
        new_one[None],
        new_two[None],
        new_weights,
        norm_grads,
        new_norm_master[None],
        new_norm_one[None],
        new_norm_two[None],
    )


def solution(mesh):
    in_specs = (
        P("tensor", "dp", None),
        P(None, "tensor"),
        P(),
        P("tensor", "dp", None),
        P("dp"),
        P(),
        P("dp", None, "tensor"),
        P("dp", None, "tensor"),
        P("dp", None, "tensor"),
        P("dp", None, None),
        P("dp", None, None),
        P("dp", None, None),
    )
    out_specs = (
        P("tensor", "dp", None),
        P("tensor", "dp", None),
        P("dp", None, "tensor"),
        P("dp", None, "tensor"),
        P("dp", None, "tensor"),
        P("dp", None, "tensor"),
        P(None, "tensor"),
        P(),
        P("dp", None, None),
        P("dp", None, None),
        P("dp", None, None),
    )
    return jax.shard_map(
        partial(layer, mesh.shape["dp"], mesh.shape["tensor"]),
        mesh=mesh,
        in_specs=in_specs,
        out_specs=out_specs,
        check_vma=False,
    )
```

```python
from functools import partial

import jax
import jax.numpy as jnp
from jax import lax
from jax.experimental import pallas as pl
from jax.experimental.pallas import tpu as pltpu
from jax.sharding import PartitionSpec as P

D = 1024
FF = 4096
ADAM_STEP = 10
HEAD_DIM = 64
SHARE = 8


f32, bf16 = jnp.float32, jnp.bfloat16
beta_one = 0.9
beta_two = 0.999
learn_rate = 0.02
weight_decay = 0.1
adam_eps = 1e-08
norm_eps = 1e-05
masked_score = -1e30
AXES = ("dp", "tensor")


def contract(a, b, ca, cb):
    return lax.dot_general(a, b, (((ca,), (cb,)), ((), ())), preferred_element_type=f32)


def norm_parts(value, gain, shift):
    average = jnp.mean(value, axis=-1, keepdims=True)
    centred = value - average
    variance = jnp.mean(centred * centred, axis=-1, keepdims=True)
    inverse = lax.rsqrt(variance + norm_eps)
    normed = centred * inverse
    return normed * gain + shift, normed, inverse


def norm_back(upstream, normed, inverse, gain):
    scaled = upstream * gain
    inner = (
        scaled
        - jnp.mean(scaled, axis=-1, keepdims=True)
        - normed * jnp.mean(scaled * normed, axis=-1, keepdims=True)
    )
    return inner * inverse


def slot_table(owners):
    repeat = FF // D
    tile_matrix = jnp.array([0, 1, 2, 3] + [4] * repeat + [5] * repeat, dtype=jnp.int32)
    choose = (tile_matrix[:, None] == jnp.arange(7, dtype=jnp.int32)[None, :]).astype(jnp.int32)
    tile_owner = jnp.sum(choose * owners[None, :], axis=1)
    position = jnp.arange(tile_matrix.shape[0], dtype=jnp.int32)
    before = (tile_owner[None, :] == tile_owner[:, None]) & (position[None, :] < position[:, None])
    slot_index = jnp.sum(before.astype(jnp.int32), axis=1)
    return (tile_owner, slot_index)


def adam_update(grad, param, first, second, occupied, decay_rate):
    first_new = occupied * (beta_one * first + (1.0 - beta_one) * grad)
    second_new = occupied * (beta_two * second + (1.0 - beta_two) * grad * grad)
    correct_one = 1.0 - beta_one**ADAM_STEP
    correct_two = 1.0 - beta_two**ADAM_STEP
    direction = first_new / correct_one / (jnp.sqrt(second_new / correct_two) + adam_eps)
    param_new = occupied * (param - learn_rate * (direction + decay_rate * param))
    return (param_new, first_new, second_new)


def head_keys(keys, half, start, length):
    lane = lax.broadcasted_iota(jnp.int32, keys.shape, 1)
    row = lax.broadcasted_iota(jnp.int32, keys.shape, 0)
    bias = jnp.where(start + row < length, 0.0, masked_score).astype(f32)
    extra = jnp.where(lane == (1 - half) * HEAD_DIM, bias, 0.0)
    return jnp.where(lane // HEAD_DIM == half, keys.astype(f32), extra).astype(bf16)


def head_half(rows, half):
    lane = lax.broadcasted_iota(jnp.int32, rows.shape, 1)
    return jnp.where(lane // HEAD_DIM == half, rows, jnp.zeros_like(rows))


def head_queries(rows, half):
    lane = lax.broadcasted_iota(jnp.int32, rows.shape, 1)
    scaled = rows.astype(f32) * HEAD_DIM ** (-0.5)
    extra = jnp.where(lane == (1 - half) * HEAD_DIM, 1.0, 0.0)
    return jnp.where(lane // HEAD_DIM == half, scaled, extra).astype(bf16)


def peer_of(bit, turn):
    device, z = lax.axis_index("dp"), lax.axis_index("tensor")
    for one in (1, 2, 4):
        if bit & one:
            device = device + one - 2 * one * ((device // one) % 2)
    if turn == 1:
        z = z + 1 - 2 * (z % 2)
    elif turn == 2:
        z = z + 2 - 4 * (z // 2)
    elif turn == 3:
        z = 3 - z
    return (device, z)


def greet(peers):
    barrier = pltpu.get_barrier_semaphore()
    for peer in peers:
        pl.semaphore_signal(barrier, inc=1, device_id=peer, device_id_type=pl.DeviceIdType.MESH)
    pl.semaphore_wait(barrier, len(peers))


def sender(send_sems, recv_sems):
    def send(source, target, k, peer):
        return pltpu.make_async_remote_copy(
            source, target, send_sems.at[k], recv_sems.at[k], device_id=peer,
            device_id_type=pl.DeviceIdType.MESH,
        )

    return send


def bits():
    device = lax.axis_index("dp")
    return (device // 4) % 2, (device // 2) % 2, device % 2


def block_of(y, x, c):
    return 4 * y + 2 * x + c


def row_block(index, count=1):
    rows = D // SHARE
    return pl.ds(pl.multiple_of(index * rows, rows), count * rows)


class Gather:
    def __init__(self, send, view, first_sem, x_first):
        self.send, self.view, self.sem = send, view, first_sem
        self.y, self.x, self.c = bits()
        self.one, self.two = (2, 4) if x_first else (4, 2)

    def block(self, turn):
        y, x, c = self.y, self.x, self.c
        y = 1 - y if turn & 4 else y
        x = 1 - x if turn & 2 else x
        c = 1 - c if turn & 1 else c
        return block_of(y, x, c)

    def copy(self, turn, over, k):
        place = self.view(self.block(turn))
        return self.send(place, place, self.sem + k, peer_of(over, 0))

    def start(self):
        self.copy(0, self.one, 0).start()
        self.copy(0, self.two, 1).start()
        self.copy(0, 1, 3).start()

    def relay(self):
        self.copy(0, self.one, 0).wait()
        self.copy(self.one, self.two, 2).start()
        self.copy(self.one, 1, 4).start()
        self.copy(0, self.two, 1).wait()
        self.copy(self.two, 1, 5).start()

    def last(self):
        self.copy(self.one, self.two, 2).wait()
        self.copy(6, 1, 6).start()

    def finish(self):
        for turn, k in ((0, 3), (self.one, 4), (self.two, 5), (6, 6)):
            self.copy(turn, 1, k).wait()


GATHER_SEMS = 7


class RowSums:
    def __init__(self, send, ref, place, height, got_one, got_two, first_sem):
        self.send, self.ref, self.place, self.height = send, ref, place, height
        self.got_one, self.got_two, self.sem = got_one, got_two, first_sem
        self.y, self.x, _ = bits()
        self.half = ref.shape[-1] // 2

    def at(self, y, x, side):
        rows = pl.ds(pl.multiple_of(self.place(y, x), 128), self.height)
        return (rows, slice(side * self.half, (side + 1) * self.half))

    def pairs(self, k, mine):
        y, x = self.y, self.x
        return [
            (y if mine else 1 - y, k, 0),
            (k, x if mine else 1 - x, 1),
        ]

    def first(self, k, side):
        y, x, _ = self.pairs(k, False)[side]
        return self.send(
            self.ref.at[self.at(y, x, side)], self.got_one.at[side, k], self.sem + 2 * side + k,
            peer_of((4, 2)[side], 0),
        )

    def second(self, side):
        y, x = ((self.y, 1 - self.x), (1 - self.y, self.x))[side]
        return self.send(
            self.ref.at[self.at(y, x, side)], self.got_two.at[side], self.sem + 4 + side,
            peer_of((2, 4)[side], 0),
        )

    def start(self):
        for side in range(2):
            for k in range(2):
                self.first(k, side).start()

    def relay(self):
        for side in range(2):
            for k in range(2):
                self.first(k, side).wait()
        for side in range(2):
            for k in range(2):
                y, x, _ = self.pairs(k, True)[side]
                at = self.at(y, x, side)
                self.ref[at] = (
                    self.ref[at].astype(f32) + self.got_one[side, k].astype(f32)
                ).astype(bf16)
        for side in range(2):
            self.second(side).start()

    def finish(self):
        for side in range(2):
            self.second(side).wait()
            at = self.at(self.y, self.x, side)
            self.ref[at] = (
                self.ref[at].astype(f32) + self.got_two[side].astype(f32)
            ).astype(bf16)


ROW_SEMS = 6


def start_body(
    lengths, tokens_ref, weights_ref,
    gathered_ref, mixed_ref, context_ref, parts_ref, lse_ref, heads_ref, out_ref, length_ref, up_ref, down_ref,
    keys, values, length_buf, out_here, out_far, local_sems, send_sems, recv_sems,
):
    chunks, rows, _ = gathered_ref.shape
    width = context_ref.shape[-1]
    lanes = up_ref.shape[-1]
    hidden_width = SHARE * lanes
    piece = rows // 4
    quarter_rows = D // 4
    y, x, c = bits()
    z = lax.axis_index("tensor")
    matched = c == z // 2
    unmatched = jnp.logical_not(matched)
    own_block = block_of(y, x, c)
    send = sender(send_sems, recv_sems)
    core, near_z, diagonal, swapped = peer_of(1, 0), peer_of(0, 1), peer_of(1, 1), peer_of(1, 2)
    across_x, across_y, across_xy = peer_of(2, 0), peer_of(4, 0), peer_of(6, 0)

    def part_of(k):
        return slice(k * piece, (k + 1) * piece)

    def swap_copy(k):
        return send(tokens_ref.at[part_of(k), :], gathered_ref.at[0, part_of(k), :], k, swapped)

    def far_copy(k, source):
        return send(source.at[part_of(k), :], gathered_ref.at[2, part_of(k), :], 4 + k, near_z)

    def near_copy(k, source):
        return send(source.at[part_of(k), :], gathered_ref.at[1, part_of(k), :], 8 + k, core)

    def diagonal_copy(k):
        return send(gathered_ref.at[2, part_of(k), :], gathered_ref.at[3, part_of(k), :], 12 + k, core)

    column = 2 * y + x

    def quarter(k):
        return pl.ds(pl.multiple_of(k * quarter_rows, quarter_rows), quarter_rows)

    def heads_swap():
        return send(
            weights_ref.at[quarter(column), : 3 * width], heads_ref.at[quarter(column), :], 16, swapped
        )

    def heads_share(k, peer):
        return send(heads_ref.at[quarter(column), :], heads_ref.at[quarter(column), :], 17 + k, peer)

    heads_peers = (across_x, across_y, across_xy)
    heads_local = pltpu.make_async_copy(weights_ref.at[:, : 3 * width], heads_ref, local_sems.at[0])

    def out_copy(e):
        return send(out_here, out_far.at[e - 1], 19 + e, peer_of(0, e))

    out_local = pltpu.make_async_copy(
        weights_ref.at[row_block(own_block), 3 * width : 4 * width], out_here, local_sems.at[1]
    )
    outs = [
        Gather(
            send, lambda k, side=side: out_ref.at[row_block(k), side * 2 * width : (side + 1) * 2 * width],
            23 + side * GATHER_SEMS, side == 0,
        )
        for side in range(2)
    ]
    base = 23 + 2 * GATHER_SEMS
    targets = (up_ref, down_ref)

    def feed_source(kind):
        at = 4 * width + kind * hidden_width + own_block * lanes
        return weights_ref.at[:, pl.ds(pl.multiple_of(at, 128), lanes)]

    def feed_copy(kind, e):
        return send(feed_source(kind), targets[kind].at[e - 1, 0, 0], base + 3 * kind + e - 1, peer_of(0, e))

    half = slice(0, D // 2), slice(D // 2, D)

    def feed_one(kind, e, side):
        source = targets[kind].at[e - 1, 0, 0, half[side], :]
        target = targets[kind].at[e - 1, side, 1 - side, half[side], :]
        return send(
            source, target, base + 6 + 6 * kind + 2 * (e - 1) + side, (across_x, across_y)[side]
        )

    def feed_two(e, side):
        if side == 0:
            source, target = (up_ref.at[e - 1, dy, 0:2, half[0], :] for dy in range(2))
        else:
            source, target = (up_ref.at[e - 1, 0:2, dx, half[1], :] for dx in range(2))
        return send(source, target, base + 18 + 2 * (e - 1) + side, (across_y, across_x)[side])

    def first_hop(kind, e):
        feed_copy(kind, e).wait()
        for side in range(2):
            feed_one(kind, e, side).start()

    def second_hop(e):
        for side in range(2):
            feed_one(0, e, side).wait()
        for side in range(2):
            feed_two(e, side).start()

    def length_copy():
        return send(length_buf.at[0], length_buf.at[1], base + 24, core)

    def part_copy(j):
        return send(
            context_ref.at[j], parts_ref.at[j], base + 24 + j, (None, core, near_z, diagonal)[j]
        )

    def send_weights():
        for e in (3, 2, 1):
            feed_copy(0, e).start()
        for e in (3, 2, 1):
            feed_copy(1, e).start()

    out_local.start()
    length_buf[0] = jnp.full(length_buf.shape[1:], lengths[0], jnp.int32)
    greet(
        [core, near_z, diagonal, swapped, across_x, across_y, across_xy, peer_of(0, 2), peer_of(0, 3)]
    )

    @pl.when(matched)
    def _():
        for k in range(4):
            far_copy(k, tokens_ref).start()
            near_copy(k, tokens_ref).start()
        heads_local.start()
        gathered_ref[0] = tokens_ref[...]

    @pl.when(unmatched)
    def _():
        for k in range(4):
            swap_copy(k).start()
        heads_swap().start()

    length_copy().start()

    @pl.when(unmatched)
    def _():
        for k in range(4):
            swap_copy(k).wait()
            far_copy(k, gathered_ref.at[0]).start()
            near_copy(k, gathered_ref.at[0]).start()
        heads_swap().wait()
        for k, peer in enumerate(heads_peers):
            heads_share(k, peer).start()

    for k in range(4):
        far_copy(k, tokens_ref).wait()
        diagonal_copy(k).start()
    out_local.wait()
    for e in (1, 2, 3):
        out_copy(e).start()
    send_weights()
    out_ref[row_block(own_block), :width] = out_here[...]

    @pl.when(matched)
    def _():
        heads_local.wait()

    @pl.when(unmatched)
    def _():
        for k, peer in enumerate(heads_peers):
            heads_share(k, peer).wait()

    length_copy().wait()
    length_ref[...] = jnp.where(matched, length_buf[0], length_buf[1])
    length = length_ref[:1, :]
    own_quarter = jnp.where(matched, z, z + 2 - 4 * (z // 2))
    wide = 256

    def project(j):
        def columns(n, carry):
            at = pl.ds(pl.multiple_of(n * wide, wide), wide)
            mixed_ref[j, :, at] = jnp.dot(
                gathered_ref[j], heads_ref[:, at], preferred_element_type=f32
            ).astype(bf16)
            return carry

        lax.fori_loop(0, 3 * width // wide, columns, 0)

    def arrange(j):
        at_quarter = own_quarter
        if j in (1, 3):
            at_quarter = at_quarter + 2 - 4 * (at_quarter // 2)
        if j in (2, 3):
            at_quarter = at_quarter + 1 - 2 * (at_quarter % 2)
        for h in range(width // HEAD_DIM):
            at = width + (h // 2) * 128
            keys[h, j * rows : (j + 1) * rows, :] = head_keys(
                mixed_ref[j, :, at : at + 128], h % 2, at_quarter * rows, length
            )
        values[j * rows : (j + 1) * rows, :] = mixed_ref[j, :, 2 * width :]

    for j in (0, 2, 1, 3):
        if j == 1:
            for k in range(4):
                near_copy(k, tokens_ref).wait()
        if j == 3:
            for k in range(4):
                diagonal_copy(k).wait()
        project(j)
        arrange(j)

    lane = lax.broadcasted_iota(jnp.int32, (rows, 128), 1)

    def attend(step, carry):
        chunk = chunks - 1 - step
        logs = jnp.zeros((rows, 128), f32)
        for pair in range(width // 128):
            queries = mixed_ref[chunk, :, pair * 128 : pair * 128 + 128]
            both = []
            for side in range(2):
                h = pair * 2 + side
                scores = contract(head_queries(queries, side), keys[h], 1, 1)
                top = jnp.max(scores, axis=1, keepdims=True)
                weight = jnp.exp(scores - top)
                total = jnp.sum(weight, axis=1, keepdims=True)
                out = contract(weight.astype(bf16), values[:, pair * 128 : pair * 128 + 128], 1, 0)
                both.append(out / total)
                logs = jnp.where(lane == h, top + jnp.log(total), logs)
            context_ref[chunk, :, pair * 128 : pair * 128 + 128] = jnp.where(
                lane < HEAD_DIM, both[0], both[1]
            ).astype(bf16)
        lse_ref[chunk] = jnp.transpose(logs)[:8, :]

        @pl.when(step == 0)
        def _():
            part_copy(3).start()
            for e in (1, 2, 3):
                out_copy(e).wait()
                out_ref[row_block(own_block), e * width : (e + 1) * width] = out_far[e - 1]
            for gather in outs:
                gather.start()
            first_hop(0, 3)

        @pl.when(step == 1)
        def _():
            part_copy(2).start()
            for gather in outs:
                gather.relay()
            first_hop(0, 2)
            second_hop(3)

        @pl.when(step == 2)
        def _():
            part_copy(1).start()
            for gather in outs:
                gather.last()
            first_hop(0, 1)
            second_hop(2)

        return carry

    lax.fori_loop(0, chunks, attend, 0)
    parts_ref[0] = context_ref[0]
    for gather in outs:
        gather.finish()
    second_hop(1)
    for e in (3, 2, 1):
        first_hop(1, e)
    for j in (3, 2, 1):
        part_copy(j).wait()
    for e in (3, 2, 1):
        for side in range(2):
            feed_two(e, side).wait()
            feed_one(1, e, side).wait()


def start_block(lengths, tokens, weights):
    rows = tokens.shape[0]
    chunks = 4
    tile = D // 4
    seq = chunks * rows
    lanes = FF // 4 // SHARE
    heads = tile // HEAD_DIM
    sems = 23 + 2 * GATHER_SEMS + 28
    share_rows = D // SHARE
    vmem, anywhere = pl.BlockSpec(memory_space=pltpu.VMEM), pl.BlockSpec(memory_space=pl.ANY)
    return pl.pallas_call(
        start_body,
        name="start_block",
        in_specs=[pl.BlockSpec(memory_space=pltpu.SMEM), vmem, anywhere],
        out_specs=[vmem] * 8 + [anywhere] * 2,
        out_shape=[
            jax.ShapeDtypeStruct((chunks, rows, D), bf16),
            jax.ShapeDtypeStruct((chunks, rows, 3 * tile), bf16),
            jax.ShapeDtypeStruct((chunks, rows, tile), bf16),
            jax.ShapeDtypeStruct((chunks, rows, tile), bf16),
            jax.ShapeDtypeStruct((chunks, 8, rows), f32),
            jax.ShapeDtypeStruct((D, 3 * tile), bf16),
            jax.ShapeDtypeStruct((D, D), bf16),
            jax.ShapeDtypeStruct((8, 128), jnp.int32),
            jax.ShapeDtypeStruct((3, 2, 2, D, lanes), bf16),
            jax.ShapeDtypeStruct((3, 2, 2, D, lanes), bf16),
        ],
        scratch_shapes=[
            pltpu.VMEM((heads, seq, 128), bf16),
            pltpu.VMEM((seq, tile), bf16),
            pltpu.VMEM((2, 8, 128), jnp.int32),
            pltpu.VMEM((share_rows, tile), bf16),
            pltpu.VMEM((3, share_rows, tile), bf16),
            pltpu.SemaphoreType.DMA((2,)),
            pltpu.SemaphoreType.DMA((sems,)),
            pltpu.SemaphoreType.DMA((sems,)),
        ],
        compiler_params=pltpu.CompilerParams(
            vmem_limit_bytes=60 << 20, collective_id=0, has_side_effects=True
        ),
        cost_estimate=pl.CostEstimate(
            flops=24 * heads * seq * seq * HEAD_DIM, bytes_accessed=20 << 20, transcendentals=0
        ),
    )(lengths, tokens, weights)


def back_body(
    info, mixed_ref, context_ref, upstream_ref, lse_ref, weight_ref, branch_ref, norm_ref, outputs_ref, gathered,
    up_grads, down_sums, out_grads,
    input_ref, outputs_out, norm_out, attention_out, feed_out,
    keys, turned, key_sum, value_sum, query_t, grad, rows_held, heads_sum, kept, got_one, got_two, got_three,
    leaving, landed, share, heads, heads_one, heads_two, heads_mine, heads_far, out_held, out_core, out_one, out_two, out_z,
    norm_here, norm_there, local_sems, send_sems, recv_sems,
):
    chunks, rows, _ = mixed_ref.shape
    width = context_ref.shape[-1]
    scale = HEAD_DIM ** (-0.5)
    part = 256
    core, near_z = peer_of(1, 0), peer_of(0, 1)
    across = (peer_of(2, 0), peer_of(4, 0))
    send = sender(send_sems, recv_sems)
    y, x, c = bits()
    z = lax.axis_index("tensor")
    matched = c == z // 2
    own_block = block_of(y, x, c)

    def stage_one(b):
        source = up_grads.at[b, 1] if b >= 2 else up_grads.at[b, :, 1]
        return send(source, got_one.at[b], b, across[0 if b >= 2 else 1])

    def stage_two(b, kind):
        return send(
            kept.at[b, kind, 1], got_two.at[b, kind], 8 + 2 * b + kind, across[(b >= 2) != (kind == 1)]
        )

    def stage_three(b):
        return send(kept.at[b, :, 0], got_three.at[b - 1], 15 + b, peer_of(0, b))

    def load(b, kind):
        if kind:
            source = down_sums.at[b]
        else:
            source = up_grads.at[b, 0] if b >= 2 else up_grads.at[b, :, 0]
        return pltpu.make_async_copy(source, kept.at[b, kind], local_sems.at[2 * b + kind])

    def start_two(b):
        for kind in range(2):
            load(b, kind).wait()
        stage_two(b, 1).start()
        stage_one(b).wait()
        for k in (1, 0):
            kept[b, 0, k] = (kept[b, 0, k].astype(f32) + got_one[b, k].astype(f32)).astype(bf16)
        stage_two(b, 0).start()

    def start_three(b):
        for kind in range(2):
            stage_two(b, kind).wait()
            kept[b, kind, 0] = (
                kept[b, kind, 0].astype(f32) + got_two[b, kind].astype(f32)
            ).astype(bf16)
        if b:
            stage_three(b).start()

    def load_rows(j):
        return pltpu.make_async_copy(gathered.at[j], rows_held.at[j], local_sems.at[8 + j])

    def out_load():
        return pltpu.make_async_copy(out_grads, out_held, local_sems.at[12])

    def out_core_copy(k):
        at = row_block(block_of(k // 2, k % 2, 1 - c))
        return send(out_grads.at[at, :], out_core.at[k], 22 + k, core)

    out_sums = RowSums(
        send, out_held, lambda yy, xx: block_of(yy, xx, c) * 128, 128, out_one, out_two, 26
    )

    def out_z_copy(e):
        at = (row_block(own_block), slice(e * width, (e + 1) * width))
        return send(out_held.at[at], out_z.at[e - 1], 31 + e, peer_of(0, e))

    def out_start():
        out_load().wait()
        for k in range(4):
            out_core_copy(k).wait()
        for k in range(4):
            at = row_block(block_of(k // 2, k % 2, c))
            out_held[at, :] = (out_held[at, :].astype(f32) + out_core[k].astype(f32)).astype(bf16)
        out_sums.start()

    def out_last():
        out_sums.finish()
        for e in (1, 2, 3):
            out_z_copy(e).start()

    norm_turns = ((1, 0), (2, 0), (4, 0), (0, 1), (0, 2))

    def norm_copy(k):
        return send(norm_here.at[k], norm_there.at[k], 35 + k, peer_of(*norm_turns[k]))

    def norm_step(k):
        norm_copy(k).wait()
        total = norm_here[k] + norm_there[k]
        if k + 1 < len(norm_turns):
            norm_here[k + 1] = total
            norm_copy(k + 1).start()
        else:
            norm_out[...] = total

    for b in (3, 2, 1, 0):
        for kind in range(2):
            load(b, kind).start()
    for j in range(chunks):
        load_rows(j).start()
    out_load().start()
    norm_here[0] = norm_ref[...]
    greet([core, near_z, across[0], across[1], peer_of(0, 2), peer_of(0, 3), peer_of(1, 2)])
    for k in range(4):
        out_core_copy(k).start()
    norm_copy(0).start()
    for b in (3, 1, 2, 0):
        stage_one(b).start()

    def return_copy(source, target, k):
        return send(source, target, 49 + 4 * GATHER_SEMS + k, peer_of(1, 2))

    outputs_local = pltpu.make_async_copy(outputs_ref, outputs_out, local_sems.at[15])

    @pl.when(matched)
    def _():
        outputs_local.start()

    @pl.when(jnp.logical_not(matched))
    def _():
        return_copy(outputs_ref, outputs_out, 0).start()

    key_sum[...] = jnp.zeros_like(key_sum)
    value_sum[...] = jnp.zeros_like(value_sum)
    for j in range(chunks):
        for h in range(width // HEAD_DIM):
            at = width + (h // 2) * 128
            keys[h, j * rows : (j + 1) * rows, :] = head_keys(
                mixed_ref[j, :, at : at + 128], h % 2, info[1 + j], info[0]
            )
        turned[:, j * rows : (j + 1) * rows] = jnp.transpose(
            mixed_ref[j, :, width : 2 * width].astype(f32)
        ).astype(bf16)
    feature = lax.broadcasted_iota(jnp.int32, (8, width), 1) // HEAD_DIM
    picks = (feature == lax.broadcasted_iota(jnp.int32, (8, width), 0)).astype(f32)
    per_chunk = rows // part

    def attend(step, carry):
        chunk = step // per_chunk
        at = pl.ds(pl.multiple_of((step % per_chunk) * part, part), part)
        upstream = upstream_ref[chunk, at, :]
        product = upstream.astype(f32) * context_ref[chunk, at, :].astype(f32)
        delta = lax.dot_general(
            picks, product, (((1,), (1,)), ((), ())), precision=lax.Precision.HIGHEST,
            preferred_element_type=f32,
        )
        lse = lse_ref[chunk, :, at]
        for pair in range(width // 128):
            lanes = slice(pair * 128, pair * 128 + 128)
            queries = mixed_ref[chunk, at, lanes]
            value_rows = mixed_ref[:, :, 2 * width + pair * 128 : 2 * width + pair * 128 + 128]
            value_rows = value_rows.reshape(chunks * rows, 128)
            for half in range(2):
                h = pair * 2 + half
                scores = contract(keys[h], head_queries(queries, half), 1, 1)
                weight = jnp.exp(scores - lse[h : h + 1, :])
                up_half = head_half(upstream[:, lanes], half)
                back = contract(value_rows, up_half, 1, 1)
                score_grad = (weight * (back - delta[h : h + 1, :])).astype(bf16)
                value_sum[pair] += contract(weight.astype(bf16), up_half, 1, 0)
                key_sum[pair] += contract(score_grad, head_half(queries, half), 1, 0)
                query_t[h * HEAD_DIM : (h + 1) * HEAD_DIM, :] = (
                    contract(turned[h * HEAD_DIM : (h + 1) * HEAD_DIM, :], score_grad, 1, 0) * scale
                )
        grad[chunk, at, :width] = jnp.transpose(query_t[...]).astype(bf16)

        @pl.when(step == 0)
        def _():
            norm_step(0)
            out_start()

        @pl.when(step == 1)
        def _():
            norm_step(1)
            start_two(3)
            start_two(1)

        @pl.when(step == 2)
        def _():
            norm_step(2)
            out_sums.relay()

        @pl.when(step == 3)
        def _():
            norm_step(3)
            start_two(2)
            start_two(0)
            start_three(3)
            start_three(1)

        @pl.when(step == 4)
        def _():
            norm_step(4)
            out_last()

        @pl.when(step == 5)
        def _():
            start_three(2)

        return carry

    lax.fori_loop(0, chunks * per_chunk, attend, 0)
    for j in range(chunks):
        at = slice(j * rows, (j + 1) * rows)
        for pair in range(width // 128):
            left = width + pair * 128
            grad[j, :, left : left + 128] = (key_sum[pair, at, :] * scale).astype(bf16)
            grad[j, :, left + width : left + width + 128] = value_sum[pair, at, :].astype(bf16)
    start_three(0)

    def rows_back(j):
        return contract(grad[j], weight_ref[...], 1, 1)

    core_copies = {}
    for k, j in enumerate((3, 1)):
        leaving[k] = rows_back(j).astype(bf16)
        core_copies[j] = send(leaving.at[k], landed.at[k], 19 + k, core)
        core_copies[j].start()
    far = rows_back(2)
    core_copies[3].wait()
    leaving[2] = (far + landed[0].astype(f32)).astype(bf16)
    far_copy = send(leaving.at[2], landed.at[2], 21, near_z)
    far_copy.start()
    branch_ref_value = branch_ref[...] + rows_back(0)
    core_copies[1].wait()
    own_rows = branch_ref_value + landed[1].astype(f32)

    total = kept[0, :, 0].astype(f32)
    for b in (3, 1, 2):
        stage_three(b).wait()
        total = total + got_three[b - 1].astype(f32)
    share[...] = total.astype(bf16)
    own_feed = [
        pltpu.make_async_copy(share.at[kind], feed_out.at[own_block, kind], local_sems.at[13 + kind])
        for kind in range(2)
    ]
    for copy in own_feed:
        copy.start()
    feeds = [
        Gather(send, lambda k, kind=kind: feed_out.at[k, kind], 49 + kind * GATHER_SEMS, kind == 0)
        for kind in range(2)
    ]
    heads_sum[...] = jnp.zeros_like(heads_sum)
    for copy in own_feed:
        copy.wait()
    for feed in feeds:
        feed.start()
    for j in range(chunks):
        load_rows(j).wait()

    def weigh(j, carry):
        heads_sum[...] += contract(rows_held[j], grad[j], 0, 0)
        return carry

    lax.fori_loop(0, chunks, weigh, 0)
    heads[...] = heads_sum[...].astype(bf16)
    head_sums = RowSums(
        send, heads, lambda yy, xx: block_of(yy, xx, 0) * 128, 256, heads_one, heads_two, 40
    )
    head_sums.start()
    for feed in feeds:
        feed.relay()
    head_sums.relay()
    far_copy.wait()
    input_ref[...] = (own_rows + landed[2].astype(f32)).astype(bf16)
    head_sums.finish()

    def half_rows(k):
        return row_block(block_of(y, x, k))

    @pl.when(matched)
    def _():
        send(heads.at[half_rows(1 - c), :], heads_mine, 46, core).start()

    @pl.when(jnp.logical_not(matched))
    def _():
        send(heads.at[half_rows(c), :], heads_far, 47, peer_of(0, 2)).start()
        send(heads.at[half_rows(1 - c), :], heads_far, 48, peer_of(1, 2)).start()

    sum_out = out_held[row_block(own_block), :width].astype(f32)
    for e in (1, 2, 3):
        out_z_copy(e).wait()
        sum_out = sum_out + out_z[e - 1].astype(f32)
    attention_out[row_block(own_block), 3 * width :] = sum_out.astype(bf16)

    @pl.when(matched)
    def _():
        send(heads.at[half_rows(1 - c), :], heads_mine, 46, core).wait_send()
        heads_mine[...] = heads[half_rows(c), :]

    @pl.when(jnp.logical_not(matched))
    def _():
        send(heads.at[half_rows(c), :], heads_far, 47, peer_of(0, 2)).wait_send()
        send(heads.at[half_rows(1 - c), :], heads_far, 48, peer_of(1, 2)).wait_send()
        send(heads.at[half_rows(c), :], heads_mine, 46, core).wait_recv()

    @pl.when(matched)
    def _():
        send(heads.at[half_rows(c), :], heads_far, 47, peer_of(0, 2)).wait_recv()

    @pl.when(jnp.logical_not(matched))
    def _():
        send(heads.at[half_rows(c), :], heads_far, 48, peer_of(1, 2)).wait_recv()

    attention_out[row_block(own_block), : 3 * width] = (
        heads_mine[...].astype(f32) + heads_far[...].astype(f32)
    ).astype(bf16)
    sides = [
        Gather(
            send,
            lambda k, side=side: attention_out.at[row_block(k), side * 2 * width : (side + 1) * 2 * width],
            49 + (2 + side) * GATHER_SEMS, side == 0,
        )
        for side in range(2)
    ]
    for side in sides:
        side.start()
    for side in sides:
        side.relay()
    for gather in feeds + sides:
        gather.last()
    for gather in feeds + sides:
        gather.finish()

    @pl.when(matched)
    def _():
        outputs_local.wait()

    @pl.when(jnp.logical_not(matched))
    def _():
        return_copy(outputs_ref, outputs_out, 0).wait()


def back_block(info, mixed, context, upstream, lse, weight, branch, norm_sums, outputs, gathered, up_grads,
               down_sums, out_grads):
    chunks, rows, width3 = mixed.shape
    width = width3 // 3
    seq = chunks * rows
    heads = width // HEAD_DIM
    lanes = up_grads.shape[-1]
    share_rows = D // SHARE
    sems = 51 + 4 * GATHER_SEMS
    vmem, anywhere = pl.BlockSpec(memory_space=pltpu.VMEM), pl.BlockSpec(memory_space=pl.ANY)
    return pl.pallas_call(
        back_body,
        name="back_block",
        in_specs=[pl.BlockSpec(memory_space=pltpu.SMEM)] + [vmem] * 7 + [anywhere] * 5,
        out_specs=[vmem, vmem, vmem, vmem, anywhere],
        out_shape=[
            jax.ShapeDtypeStruct((rows, D), bf16),
            jax.ShapeDtypeStruct((rows, D), bf16),
            jax.ShapeDtypeStruct((4, D), f32),
            jax.ShapeDtypeStruct((D, 4 * width), bf16),
            jax.ShapeDtypeStruct((SHARE, 2, D, lanes), bf16),
        ],
        scratch_shapes=[
            pltpu.VMEM((heads, seq, 128), bf16),
            pltpu.VMEM((width, seq), bf16),
            pltpu.VMEM((width // 128, seq, 128), f32),
            pltpu.VMEM((width // 128, seq, 128), f32),
            pltpu.VMEM((width, 256), f32),
            pltpu.VMEM((chunks, rows, width3), bf16),
            pltpu.VMEM((chunks, rows, D), bf16),
            pltpu.VMEM((D, width3), f32),
            pltpu.VMEM((4, 2, 2, D, lanes), bf16),
            pltpu.VMEM((4, 2, D, lanes), bf16),
            pltpu.VMEM((4, 2, D, lanes), bf16),
            pltpu.VMEM((3, 2, D, lanes), bf16),
            pltpu.VMEM((3, rows, D), bf16),
            pltpu.VMEM((3, rows, D), bf16),
            pltpu.VMEM((2, D, lanes), bf16),
            pltpu.VMEM((D, width3), bf16),
            pltpu.VMEM((2, 2, 2 * share_rows, width3 // 2), bf16),
            pltpu.VMEM((2, 2 * share_rows, width3 // 2), bf16),
            pltpu.VMEM((share_rows, width3), bf16),
            pltpu.VMEM((share_rows, width3), bf16),
            pltpu.VMEM((D, 4 * width), bf16),
            pltpu.VMEM((4, share_rows, 4 * width), bf16),
            pltpu.VMEM((2, 2, share_rows, 2 * width), bf16),
            pltpu.VMEM((2, share_rows, 2 * width), bf16),
            pltpu.VMEM((3, share_rows, width), bf16),
            pltpu.VMEM((5, 4, D), f32),
            pltpu.VMEM((5, 4, D), f32),
            pltpu.SemaphoreType.DMA((16,)),
            pltpu.SemaphoreType.DMA((sems,)),
            pltpu.SemaphoreType.DMA((sems,)),
        ],
        compiler_params=pltpu.CompilerParams(
            vmem_limit_bytes=67043328, collective_id=2, has_side_effects=True
        ),
        cost_estimate=pl.CostEstimate(
            flops=40 * heads * seq * seq * HEAD_DIM, bytes_accessed=40 << 20, transcendentals=0
        ),
    )(
        info, mixed, context, upstream, lse, weight, branch, norm_sums, outputs, gathered, up_grads, down_sums,
        out_grads,
    )


def adam_body(owned, attention_ref, feed_ref, master_ref, one_ref, two_ref,
              grad_out, master_out, one_out, two_out, tiles_out, up_out, down_out):
    tile = grad_out.shape[-1] // 4
    for s in range(4):
        at = slice(s * tile, (s + 1) * tile)
        grad = jnp.zeros((grad_out.shape[0], tile), f32)
        for i in range(4):
            value = attention_ref[:, i * tile : (i + 1) * tile].astype(f32)
            grad = jnp.where(owned[s, i] > 0, value, grad)
        for kind in range(2):
            value = jnp.concatenate([feed_ref[2 * s + k, kind] for k in range(2)], axis=-1)
            grad = jnp.where(owned[s, 4 + 4 * kind + s] > 0, value.astype(f32), grad)
        occupied = (owned[s, 12] > 0).astype(f32)
        param, first, second = adam_update(
            grad, master_ref[:, at], one_ref[:, at], two_ref[:, at], occupied, weight_decay
        )
        grad_out[:, at] = grad
        master_out[:, at] = param
        one_out[:, at] = first
        two_out[:, at] = second
        low = param.astype(bf16)
        none = jnp.zeros_like(low)
        for i in range(4):
            mine = jnp.where(owned[s, i] > 0, low, none)
            there = slice(i * tile, (i + 1) * tile)
            tiles_out[:, there] = mine if s == 0 else tiles_out[:, there] + mine
        for kind, target in ((0, up_out), (1, down_out)):
            mine = jnp.where(owned[s, 4 + 4 * kind + s] > 0, low, none)
            for k in range(2):
                target[2 * s + k] = mine[:, k * tile // 2 : (k + 1) * tile // 2]


def adam_block(owned, attention_grad, feed_grad, master, one, two):
    part = 128
    wide = pl.BlockSpec((part, D), lambda i: (i, 0))
    lanes = feed_grad.shape[-1]
    split = pl.BlockSpec((SHARE, part, lanes), lambda i: (0, i, 0))
    return pl.pallas_call(
        adam_body,
        grid=(D // part,),
        name="adam_block",
        in_specs=[
            pl.BlockSpec(memory_space=pltpu.SMEM), wide,
            pl.BlockSpec((SHARE, 2, part, lanes), lambda i: (0, 0, i, 0)), wide, wide, wide,
        ],
        out_specs=[wide] * 5 + [split] * 2,
        out_shape=[jax.ShapeDtypeStruct((D, D), f32)] * 4
        + [jax.ShapeDtypeStruct((D, D), bf16)]
        + [jax.ShapeDtypeStruct((SHARE, D, lanes), bf16)] * 2,
        compiler_params=pltpu.CompilerParams(vmem_limit_bytes=62 << 20),
        cost_estimate=pl.CostEstimate(flops=40 * D * D, bytes_accessed=40 << 20, transcendentals=0),
    )(owned, attention_grad, feed_grad, master, one, two)


def tiles_body(tiles_ref, up_ref, down_ref, input_ref, tiles_out, up_out, down_out, input_out, *scratch):
    core_got = scratch[:3]
    one_got, two_got = scratch[3:5], scratch[5:7]
    work = scratch[7:10]
    row_one, row_two, local_sems, send_sems, recv_sems = scratch[10:]
    matched = lax.axis_index("dp") % 2 == lax.axis_index("tensor") // 2
    send = sender(send_sems, recv_sems)
    y, x, c = bits()
    core = peer_of(1, 0)
    own_block = block_of(y, x, c)
    greet([core, peer_of(2, 0), peer_of(4, 0), peer_of(1, 2)])
    input_local = pltpu.make_async_copy(input_ref, input_out, local_sems.at[0])
    input_swap = send(input_ref, input_out, 24 + 4 * GATHER_SEMS, peer_of(1, 2))

    @pl.when(matched)
    def _():
        input_local.start()

    @pl.when(jnp.logical_not(matched))
    def _():
        input_swap.start()

    arrays = ((up_ref, up_out), (down_ref, down_out), (tiles_ref, tiles_out))

    def place(n, ref, block):
        return ref.at[row_block(block), :] if n == 2 else ref.at[block]

    def core_copy(n, k):
        return send(
            place(n, arrays[n][0], block_of(k // 2, k % 2, 1 - c)), core_got[n].at[k], 4 * n + k, core
        )

    def core_add(n):
        source, target = arrays[n][0], work[n]
        for k in range(4):
            core_copy(n, k).wait()
        for k in range(4):
            block = block_of(k // 2, k % 2, c)
            if n == 2:
                at = row_block(block)
                target[at, :] = source[at, :] + core_got[n][k]
            else:
                target[k] = source[block] + core_got[n][k]

    def first(n, k):
        y_, x_ = ((k, 1 - x), (1 - y, k))[n]
        return send(
            work[n].at[2 * y_ + x_], one_got[n].at[k], 12 + 2 * n + k,
            peer_of((2, 4)[n], 0),
        )

    def second(n):
        y_, x_ = ((1 - y, x), (y, 1 - x))[n]
        return send(
            work[n].at[2 * y_ + x_], two_got[n], 16 + n, peer_of((4, 2)[n], 0)
        )

    def relay(n):
        target = work[n]
        for k in range(2):
            first(n, k).wait()
        for k in range(2):
            y_, x_ = ((k, x), (y, k))[n]
            block = 2 * y_ + x_
            target[block] = target[block] + one_got[n][k]
        second(n).start()

    def settle(n):
        second(n).wait()
        arrays[n][1][own_block] = work[n][2 * y + x] + two_got[n][...]

    for n in range(3):
        for k in range(4):
            core_copy(n, k).start()
    for n in range(2):
        core_add(n)
        for k in range(2):
            first(n, k).start()
    core_add(2)
    rows = RowSums(
        send, work[2], lambda yy, xx: block_of(yy, xx, c) * 128, 128, row_one, row_two, 18
    )
    rows.start()
    for n in range(2):
        relay(n)
    rows.relay()
    gathers = []
    for n in range(2):
        settle(n)
        gathers.append(
            Gather(send, lambda k, n=n: arrays[n][1].at[k], 24 + n * GATHER_SEMS, n == 0)
        )
        gathers[-1].start()
    rows.finish()
    tiles_out[row_block(own_block), :] = work[2][row_block(own_block), :]
    half = tiles_out.shape[-1] // 2
    for side in range(2):
        gathers.append(
            Gather(
                send,
                lambda k, side=side: tiles_out.at[row_block(k), side * half : (side + 1) * half],
                24 + (2 + side) * GATHER_SEMS, side == 0,
            )
        )
        gathers[-1].start()
    for gather in gathers:
        gather.relay()
    for gather in gathers:
        gather.last()
    for gather in gathers:
        gather.finish()

    @pl.when(matched)
    def _():
        input_local.wait()

    @pl.when(jnp.logical_not(matched))
    def _():
        input_swap.wait()


def spread_tiles(tiles, up, down, rows):
    share_rows = D // SHARE
    lanes = up.shape[-1]
    sems = 25 + 4 * GATHER_SEMS
    piece = (D, lanes)
    vmem = pl.BlockSpec(memory_space=pltpu.VMEM)
    return pl.pallas_call(
        tiles_body,
        name="spread_tiles",
        in_specs=[vmem] * 3 + [pl.BlockSpec(memory_space=pl.ANY)],
        out_specs=[vmem] * 4,
        out_shape=[jax.ShapeDtypeStruct(v.shape, bf16) for v in (tiles, up, down, rows)],
        scratch_shapes=[
            pltpu.VMEM((4,) + piece, bf16),
            pltpu.VMEM((4,) + piece, bf16),
            pltpu.VMEM((4, share_rows, D), bf16),
            pltpu.VMEM((2,) + piece, bf16),
            pltpu.VMEM((2,) + piece, bf16),
            pltpu.VMEM(piece, bf16),
            pltpu.VMEM(piece, bf16),
            pltpu.VMEM((4,) + piece, bf16),
            pltpu.VMEM((4,) + piece, bf16),
            pltpu.VMEM((D, D), bf16),
            pltpu.VMEM((2, 2, share_rows, D // 2), bf16),
            pltpu.VMEM((2, share_rows, D // 2), bf16),
            pltpu.SemaphoreType.DMA((1,)),
            pltpu.SemaphoreType.DMA((sems,)),
            pltpu.SemaphoreType.DMA((sems,)),
        ],
        compiler_params=pltpu.CompilerParams(
            vmem_limit_bytes=48 << 20, collective_id=3, has_side_effects=True
        ),
        cost_estimate=pl.CostEstimate(flops=D * D, bytes_accessed=12 << 20, transcendentals=0),
    )(tiles, up, down, rows)


def joined(held, i, kind):
    return jnp.concatenate(
        [held[kind, 2 * (i // 2) + m, i % 2, k] for k in range(2) for m in range(2)], axis=-1
    )


def gelu_parts(value):
    bell = jnp.exp(-0.5 * value * value)
    t = 1.0 / (1.0 + (0.3275911 * 0.5**0.5) * jnp.abs(value))
    tail = 0.5 * 1.061405429
    for c in (-1.453152027, 1.421413741, -0.284496736, 0.254829592):
        tail = tail * t + 0.5 * c
    tail = tail * t * bell
    area = jnp.where(value > 0, 1.0 - tail, tail)
    return value * area, area + value * bell * (0.5 / jnp.pi) ** 0.5


def feed_body(
    info, first_ref, cotangent_ref, norms_ref, weights_ref, up_ref, down_ref,
    out_ref, low_ref, both_ref, pre_ref, grad_ref, sums_ref, down_sums,
    held, hidden_ref, slope, total, leaving, landed, seed_held, low_t, grads, got, local_sems, send_sems, recv_sems,
):
    rows = first_ref.shape[0]
    steps = hidden_ref.shape[0]
    lanes = held.shape[-1]
    y, x, c = bits()
    peer = peer_of(1, 0)
    send = sender(send_sems, recv_sems)
    half = slice(0, D // 2), slice(D // 2, D)
    loads = []
    for kind in range(2):
        for dy in range(2):
            for dx in range(2):
                block = block_of(1 - y if dy else y, 1 - x if dx else x, c)
                at = D + kind * SHARE * lanes + block * lanes
                loads.append(
                    (weights_ref.at[:, pl.ds(pl.multiple_of(at, 128), lanes)], held.at[kind, 0, dy, dx])
                )
    loads.append((up_ref, held.at[0, 1:4]))
    loads.append((down_ref.at[:, 0, 0:2, half[0], :], held.at[1, 1:4, 0, 0:2, half[0], :]))
    loads.append((down_ref.at[:, 0:2, 0, half[1], :], held.at[1, 1:4, 0:2, 0, half[1], :]))
    loads = [pltpu.make_async_copy(a, b, local_sems.at[k]) for k, (a, b) in enumerate(loads)]
    for load in loads:
        load.start()
    greet([peer, peer_of(2, 0), peer_of(4, 0), peer_of(1, 2)])
    matched = c == lax.axis_index("tensor") // 2
    seed_local = pltpu.make_async_copy(cotangent_ref, seed_held, local_sems.at[len(loads)])
    seed_swap = send(cotangent_ref, seed_held, 6, peer_of(1, 2))
    hops = [
        send(
            down_ref.at[:, 0, 0:2, half[0], :], held.at[1, 1:4, 1, 0:2, half[0], :], 4, peer_of(4, 0)
        ),
        send(
            down_ref.at[:, 0:2, 0, half[1], :], held.at[1, 1:4, 0:2, 1, half[1], :], 5, peer_of(2, 0)
        ),
    ]
    for hop in hops:
        hop.start()

    @pl.when(matched)
    def _():
        seed_local.start()

    @pl.when(jnp.logical_not(matched))
    def _():
        seed_swap.start()

    def across(source, target, k):
        return send(source, target, k, peer)

    middle_row = rows // 2
    both_ref[0] = first_ref[...].astype(bf16)
    first_copy = across(both_ref.at[0], both_ref.at[1], 0)
    first_copy.start()

    def up(i, slot):
        weight = joined(held, i, 0)
        for r in range(0, rows, middle_row):
            at = slice(r, r + middle_row)
            value = jnp.dot(both_ref[slot, at, :], weight, preferred_element_type=f32)
            hidden, steep = gelu_parts(value)
            hidden_ref[i, slot, at, :] = hidden.astype(bf16)
            slope[i, slot, at, :] = steep.astype(bf16)

    def down(i, slot):
        total[slot] += contract(hidden_ref[i, slot], joined(held, i, 1), 1, 1)

    def back(i, slot):
        weight = joined(held, i, 1)
        for r in range(0, rows, middle_row):
            at = slice(r, r + middle_row)
            value = jnp.dot(low_ref[slot, at, :], weight, preferred_element_type=f32)
            pre_ref[i, slot, at, :] = (value * slope[i, slot, at, :].astype(f32)).astype(bf16)

    def back_up(i, slot):
        total[slot] += contract(pre_ref[i, slot], joined(held, i, 0), 1, 1)

    def loop(*works):
        def body(i, carry):
            for work in works:
                work(i)
            return carry

        lax.fori_loop(0, steps, body, 0)

    total[...] = jnp.zeros_like(total)
    for load in loads:
        load.wait()
    loop(lambda i: up(i, 0))
    first_copy.wait()
    loop(lambda i: up(i, 1))
    for hop in hops:
        hop.wait()
    loop(lambda i: down(i, 1))
    leaving[...] = total[1].astype(bf16)
    feed_copy = across(leaving, landed.at[0], 1)
    feed_copy.start()
    loop(lambda i: down(i, 0))
    feed_copy.wait()

    @pl.when(matched)
    def _():
        seed_local.wait()

    @pl.when(jnp.logical_not(matched))
    def _():
        seed_swap.wait()

    sums_ref[...] = jnp.zeros_like(sums_ref)
    part = 128

    def middle(r, carry):
        at = pl.ds(pl.multiple_of(r * part, part), part)
        second, normed, inverse = norm_parts(
            first_ref[at, :] + (total[0, at, :] + landed[0, at, :].astype(f32)),
            norms_ref[2:3, :], norms_ref[3:4, :],
        )
        out_ref[at, :] = second.astype(bf16)
        row = lax.broadcasted_iota(jnp.int32, (part, 1), 0) + r * part + info[1]
        seed = seed_held[at, :].astype(f32) * (row < info[0]).astype(f32)
        grad = norm_back(seed, normed, inverse, norms_ref[2:3, :])
        sums_ref[0:1, :] += jnp.sum(seed * normed, axis=0, keepdims=True)
        sums_ref[1:2, :] += jnp.sum(seed, axis=0, keepdims=True)
        total[0, at, :] = grad
        low_ref[0, at, :] = grad.astype(bf16)
        return carry

    lax.fori_loop(0, rows // part, middle, 0)
    low_copy = across(low_ref.at[0], low_ref.at[1], 2)
    low_copy.start()
    total[1] = jnp.zeros_like(total[1])
    loop(lambda i: back(i, 0))
    low_copy.wait()
    for slot in range(2):
        low_t[:, slot * rows : (slot + 1) * rows] = jnp.transpose(low_ref[slot].astype(f32)).astype(bf16)

    def down_copy(b):
        source = grads.at[b, 1] if b >= 2 else grads.at[b, :, 1]
        return send(source, got.at[b], 7 + b, peer_of(4, 0) if b >= 2 else peer_of(2, 0))

    for nf in (1, 0):

        def weigh(dy, carry, nf=nf):
            hidden = hidden_ref[2 * nf + dy].reshape(2 * rows, hidden_ref.shape[-1])
            value = jnp.dot(low_t[...], hidden, preferred_element_type=f32).astype(bf16)
            for k in range(2):
                for m in range(2):
                    at = (2 * k + m) * lanes
                    grads[2 * nf + m, dy, k] = value[:, at : at + lanes]
            return carry

        lax.fori_loop(0, 2, weigh, 0)
        for b in (2 * nf + 1, 2 * nf):
            down_copy(b).start()
    loop(lambda i: back(i, 1), lambda i: back_up(i, 1))
    leaving[...] = total[1].astype(bf16)
    grad_copy = across(leaving, landed.at[1], 3)
    grad_copy.start()
    loop(lambda i: back_up(i, 0))
    grad_copy.wait()
    grad_ref[...] = total[0] + landed[1].astype(f32)
    for b in (3, 2, 1, 0):
        down_copy(b).wait()
        for k in range(2):
            own = grads[b, 0, k] if b >= 2 else grads[b, k, 0]
            down_sums[b, k] = (own.astype(f32) + got[b, k].astype(f32)).astype(bf16)


def feed_block(info, first, cotangent, norms, weights, up, down):
    rows = first.shape[0]
    lanes = up.shape[-1]
    width = 4 * lanes
    vmem, anywhere = pl.BlockSpec(memory_space=pltpu.VMEM), pl.BlockSpec(memory_space=pl.ANY)
    return pl.pallas_call(
        feed_body,
        name="feed_block",
        in_specs=[pl.BlockSpec(memory_space=pltpu.SMEM), vmem, anywhere, vmem] + [anywhere] * 3,
        out_specs=[vmem] * 7,
        out_shape=[
            jax.ShapeDtypeStruct((rows, D), bf16),
            jax.ShapeDtypeStruct((2, rows, D), bf16),
            jax.ShapeDtypeStruct((2, rows, D), bf16),
            jax.ShapeDtypeStruct((4, 2, rows, width), bf16),
            jax.ShapeDtypeStruct((rows, D), f32),
            jax.ShapeDtypeStruct((2, D), f32),
            jax.ShapeDtypeStruct((4, 2, D, lanes), bf16),
        ],
        scratch_shapes=[
            pltpu.VMEM((2, 4, 2, 2, D, lanes), bf16),
            pltpu.VMEM((4, 2, rows, width), bf16),
            pltpu.VMEM((4, 2, rows, width), bf16),
            pltpu.VMEM((2, rows, D), f32),
            pltpu.VMEM((rows, D), bf16),
            pltpu.VMEM((2, rows, D), bf16),
            pltpu.VMEM((rows, D), bf16),
            pltpu.VMEM((D, 2 * rows), bf16),
            pltpu.VMEM((4, 2, 2, D, lanes), bf16),
            pltpu.VMEM((4, 2, D, lanes), bf16),
            pltpu.SemaphoreType.DMA((12,)),
            pltpu.SemaphoreType.DMA((11,)),
            pltpu.SemaphoreType.DMA((11,)),
        ],
        compiler_params=pltpu.CompilerParams(
            vmem_limit_bytes=60 << 20, collective_id=1, has_side_effects=True
        ),
        cost_estimate=pl.CostEstimate(
            flops=64 * rows * D * width, bytes_accessed=30 << 20, transcendentals=0
        ),
    )(info, first, cotangent, norms, weights, up, down)


def feed_grads_body(first_ref, pre_ref, up_ref, first_t):
    rows = first_ref.shape[1]

    @pl.when(pl.program_id(0) == 0)
    def _():
        for slot in range(2):
            first_t[:, slot * rows : (slot + 1) * rows] = jnp.transpose(
                first_ref[slot].astype(f32)
            ).astype(bf16)

    lanes = up_ref.shape[-1]
    grad = jnp.dot(
        first_t[...], pre_ref[0].reshape(2 * rows, pre_ref.shape[-1]), preferred_element_type=f32
    ).astype(bf16)
    for k in range(2):
        for m in range(2):
            at = (2 * k + m) * lanes
            up_ref[m, k, 0] = grad[:, at : at + lanes]


def feed_grads(first, pre):
    count, _, rows, width = pre.shape
    lanes = width // 4
    return pl.pallas_call(
        feed_grads_body,
        grid=(count,),
        name="feed_grads",
        in_specs=[
            pl.BlockSpec((2, rows, D), lambda i: (0, 0, 0)),
            pl.BlockSpec((1, 2, rows, width), lambda i: (i, 0, 0, 0)),
        ],
        out_specs=pl.BlockSpec((2, 2, 1, D, lanes), lambda i: (i // 2, 0, i % 2, 0, 0)),
        out_shape=jax.ShapeDtypeStruct((count, 2, 2, D, lanes), bf16),
        scratch_shapes=[pltpu.VMEM((D, 2 * rows), bf16)],
        compiler_params=pltpu.CompilerParams(vmem_limit_bytes=48 << 20),
        cost_estimate=pl.CostEstimate(
            flops=4 * rows * D * width * count, bytes_accessed=10 << 20, transcendentals=0
        ),
    )(first, pre)


def layer(n_dp, n_tensor, tokens, weights, norms, cotangent, lengths, owners, master, moment_one,
          moment_two, norm_master, norm_one, norm_two):
    tile = D // n_tensor
    rows = tokens.shape[0]
    device = lax.axis_index("dp")
    z = lax.axis_index("tensor")
    core = device % 2
    matched = core == z // 2
    quarter = jnp.where(matched, z, z ^ 2)

    def flip(x, dd, dz):
        pairs = [
            (d * n_tensor + t, (d ^ dd) * n_tensor + (t ^ dz))
            for d in range(n_dp)
            for t in range(n_tensor)
        ]
        return lax.ppermute(x, AXES, pairs)

    gathered, mixed, context, parts, lse, w_heads, w_out_all, length, up_all, down_all = start_block(
        lengths, tokens[:, 0, :], weights
    )
    own = gathered[0]
    base = jnp.stack([quarter ^ k for k in (0, 2, 1, 3)]) * rows
    info = jnp.concatenate([length[0, :1], base]).astype(jnp.int32)

    context_all = jnp.where(
        matched,
        jnp.concatenate([parts[k] for k in (0, 2, 1, 3)], axis=1),
        jnp.concatenate([parts[k] for k in (1, 3, 0, 2)], axis=1),
    )
    branch = contract(context_all, w_out_all, 1, 1)
    first, first_normed, first_inverse = norm_parts(
        own.astype(f32) + branch, norms[0], norms[1]
    )
    outputs, _, both_first, pre_grad, first_grad, sums_two, down_sums = feed_block(
        info, first, cotangent[:, 0, :], norms, weights, up_all, down_all
    )
    branch_grad = norm_back(first_grad, first_normed, first_inverse, norms[0])
    gain_one = jnp.sum(first_grad * first_normed, axis=0)
    shift_one = jnp.sum(first_grad, axis=0)
    branch_low = branch_grad.astype(bf16)
    context_grad = jnp.dot(branch_low, w_out_all, preferred_element_type=f32).astype(bf16)
    blocks = [context_grad[:, k * tile : (k + 1) * tile] for k in range(4)]
    blocks = [
        jnp.where(matched, blocks[a], blocks[b]) for a, b in ((0, 2), (2, 0), (1, 3), (3, 1))
    ]
    upstream = jnp.stack(
        [blocks[0], flip(blocks[1], 1, 0), flip(blocks[2], 0, 1), flip(blocks[3], 1, 1)]
    )

    def add(a, b):
        return (a.astype(f32) + b.astype(f32)).astype(bf16)

    up_grads = feed_grads(both_first, pre_grad)
    out_grad = contract(branch_low, context_all, 0, 0).astype(bf16)
    norm_sums = jnp.concatenate([jnp.stack([gain_one, shift_one]), sums_two])
    input_grad, outputs, norm_grads, attention_grad, feed_grad = back_block(
        info, mixed, context, upstream, lse, w_heads, branch_grad, norm_sums, outputs, gathered, up_grads, down_sums,
        out_grad,
    )

    def over_groups(value, combine):
        bit = SHARE
        while bit < n_dp:
            value = combine(value, flip(value, bit, 0))
            bit *= 2
        return value

    def plus(a, b):
        return a + b

    norm_grads = over_groups(norm_grads, plus)
    attention_grad = over_groups(attention_grad, add)
    feed_grad = over_groups(feed_grad, add)

    tile_owner, slot_index = slot_table(owners)
    slot_ids = jnp.arange(FF // D, dtype=jnp.int32)
    owned = (
        (tile_owner[None, :] == device) & (slot_index[None, :] == slot_ids[:, None])
    ).astype(jnp.int32)
    owned = jnp.concatenate([owned, jnp.sum(owned, axis=1, keepdims=True)], axis=1)
    slot_grad, new_master, new_one, new_two, tiles, up_tiles, down_tiles = adam_block(
        owned, attention_grad, feed_grad, master[0], moment_one[0], moment_two[0]
    )
    tiles, up_tiles, down_tiles, input_grad = spread_tiles(tiles, up_tiles, down_tiles, input_grad)
    tiles, up_tiles, down_tiles = (over_groups(v, plus) for v in (tiles, up_tiles, down_tiles))
    new_weights = jnp.concatenate(
        [tiles] + [up_tiles[k] for k in range(SHARE)] + [down_tiles[k] for k in range(SHARE)], axis=1
    )
    norm_owner = (device == owners[6]).astype(f32)
    new_norm_master, new_norm_one, new_norm_two = adam_update(
        norm_grads, norm_master[0], norm_one[0], norm_two[0], norm_owner, 0.0
    )
    return (
        outputs[:, None, :],
        input_grad[:, None, :],
        slot_grad[None],
        new_master[None],
        new_one[None],
        new_two[None],
        new_weights,
        norm_grads,
        new_norm_master[None],
        new_norm_one[None],
        new_norm_two[None],
    )


def solution(mesh):
    in_specs = (
        P("tensor", "dp", None),
        P(None, "tensor"),
        P(),
        P("tensor", "dp", None),
        P("dp"),
        P(),
        P("dp", None, "tensor"),
        P("dp", None, "tensor"),
        P("dp", None, "tensor"),
        P("dp", None, None),
        P("dp", None, None),
        P("dp", None, None),
    )
    out_specs = (
        P("tensor", "dp", None),
        P("tensor", "dp", None),
        P("dp", None, "tensor"),
        P("dp", None, "tensor"),
        P("dp", None, "tensor"),
        P("dp", None, "tensor"),
        P(None, "tensor"),
        P(),
        P("dp", None, None),
        P("dp", None, None),
        P("dp", None, None),
    )
    return jax.shard_map(
        partial(layer, mesh.shape["dp"], mesh.shape["tensor"]),
        mesh=mesh,
        in_specs=in_specs,
        out_specs=out_specs,
        check_vma=False,
    )
```

```python
from functools import partial

import jax
import jax.numpy as jnp
from jax import lax
from jax.experimental import pallas as pl
from jax.experimental.pallas import tpu as pltpu
from jax.sharding import PartitionSpec as P

D = 1024
FF = 4096
ADAM_STEP = 10
HEAD_DIM = 64
SHARE = 8


f32, bf16 = jnp.float32, jnp.bfloat16
beta_one = 0.9
beta_two = 0.999
learn_rate = 0.02
weight_decay = 0.1
adam_eps = 1e-08
norm_eps = 1e-05
masked_score = -1e30
AXES = ("dp", "tensor")


def contract(a, b, ca, cb):
    return lax.dot_general(a, b, (((ca,), (cb,)), ((), ())), preferred_element_type=f32)


def norm_parts(value, gain, shift):
    average = jnp.mean(value, axis=-1, keepdims=True)
    centred = value - average
    variance = jnp.mean(centred * centred, axis=-1, keepdims=True)
    inverse = lax.rsqrt(variance + norm_eps)
    normed = centred * inverse
    return normed * gain + shift, normed, inverse


def norm_back(upstream, normed, inverse, gain):
    scaled = upstream * gain
    inner = (
        scaled
        - jnp.mean(scaled, axis=-1, keepdims=True)
        - normed * jnp.mean(scaled * normed, axis=-1, keepdims=True)
    )
    return inner * inverse


def slot_table(owners):
    repeat = FF // D
    tile_matrix = jnp.array([0, 1, 2, 3] + [4] * repeat + [5] * repeat, dtype=jnp.int32)
    choose = (tile_matrix[:, None] == jnp.arange(7, dtype=jnp.int32)[None, :]).astype(jnp.int32)
    tile_owner = jnp.sum(choose * owners[None, :], axis=1)
    position = jnp.arange(tile_matrix.shape[0], dtype=jnp.int32)
    before = (tile_owner[None, :] == tile_owner[:, None]) & (position[None, :] < position[:, None])
    slot_index = jnp.sum(before.astype(jnp.int32), axis=1)
    return (tile_owner, slot_index)


def adam_update(grad, param, first, second, occupied, decay_rate):
    first_new = occupied * (beta_one * first + (1.0 - beta_one) * grad)
    second_new = occupied * (beta_two * second + (1.0 - beta_two) * grad * grad)
    correct_one = 1.0 - beta_one**ADAM_STEP
    correct_two = 1.0 - beta_two**ADAM_STEP
    direction = first_new / correct_one / (jnp.sqrt(second_new / correct_two) + adam_eps)
    param_new = occupied * (param - learn_rate * (direction + decay_rate * param))
    return (param_new, first_new, second_new)


def head_keys(keys, half, start, length):
    lane = lax.broadcasted_iota(jnp.int32, keys.shape, 1)
    row = lax.broadcasted_iota(jnp.int32, keys.shape, 0)
    bias = jnp.where(start + row < length, 0.0, masked_score).astype(f32)
    extra = jnp.where(lane == (1 - half) * HEAD_DIM, bias, 0.0)
    return jnp.where(lane // HEAD_DIM == half, keys.astype(f32), extra).astype(bf16)


def head_half(rows, half):
    lane = lax.broadcasted_iota(jnp.int32, rows.shape, 1)
    return jnp.where(lane // HEAD_DIM == half, rows, jnp.zeros_like(rows))


def head_queries(rows, half):
    lane = lax.broadcasted_iota(jnp.int32, rows.shape, 1)
    scaled = rows.astype(f32) * HEAD_DIM ** (-0.5)
    extra = jnp.where(lane == (1 - half) * HEAD_DIM, 1.0, 0.0)
    return jnp.where(lane // HEAD_DIM == half, scaled, extra).astype(bf16)


def peer_of(bit, turn):
    device, z = lax.axis_index("dp"), lax.axis_index("tensor")
    for one in (1, 2, 4):
        if bit & one:
            device = device + one - 2 * one * ((device // one) % 2)
    if turn == 1:
        z = z + 1 - 2 * (z % 2)
    elif turn == 2:
        z = z + 2 - 4 * (z // 2)
    elif turn == 3:
        z = 3 - z
    return (device, z)


def greet(peers):
    barrier = pltpu.get_barrier_semaphore()
    for peer in peers:
        pl.semaphore_signal(barrier, inc=1, device_id=peer, device_id_type=pl.DeviceIdType.MESH)
    pl.semaphore_wait(barrier, len(peers))


def sender(send_sems, recv_sems):
    def send(source, target, k, peer):
        return pltpu.make_async_remote_copy(
            source, target, send_sems.at[k], recv_sems.at[k], device_id=peer,
            device_id_type=pl.DeviceIdType.MESH,
        )

    return send


def bits():
    device = lax.axis_index("dp")
    return (device // 4) % 2, (device // 2) % 2, device % 2


def block_of(y, x, c):
    return 4 * y + 2 * x + c


def row_block(index, count=1):
    rows = D // SHARE
    return pl.ds(pl.multiple_of(index * rows, rows), count * rows)


class Gather:
    def __init__(self, send, view, first_sem, x_first):
        self.send, self.view, self.sem = send, view, first_sem
        self.y, self.x, self.c = bits()
        self.one, self.two = (2, 4) if x_first else (4, 2)

    def block(self, turn):
        y, x, c = self.y, self.x, self.c
        y = 1 - y if turn & 4 else y
        x = 1 - x if turn & 2 else x
        c = 1 - c if turn & 1 else c
        return block_of(y, x, c)

    def copy(self, turn, over, k):
        place = self.view(self.block(turn))
        return self.send(place, place, self.sem + k, peer_of(over, 0))

    def start(self):
        self.copy(0, self.one, 0).start()
        self.copy(0, self.two, 1).start()
        self.copy(0, 1, 3).start()

    def relay(self):
        self.copy(0, self.one, 0).wait()
        self.copy(self.one, self.two, 2).start()
        self.copy(self.one, 1, 4).start()
        self.copy(0, self.two, 1).wait()
        self.copy(self.two, 1, 5).start()

    def last(self):
        self.copy(self.one, self.two, 2).wait()
        self.copy(6, 1, 6).start()

    def finish(self):
        for turn, k in ((0, 3), (self.one, 4), (self.two, 5), (6, 6)):
            self.copy(turn, 1, k).wait()


GATHER_SEMS = 7


class RowSums:
    def __init__(self, send, ref, place, height, got_one, got_two, first_sem):
        self.send, self.ref, self.place, self.height = send, ref, place, height
        self.got_one, self.got_two, self.sem = got_one, got_two, first_sem
        self.y, self.x, _ = bits()
        self.half = ref.shape[-1] // 2

    def at(self, y, x, side):
        rows = pl.ds(pl.multiple_of(self.place(y, x), 128), self.height)
        return (rows, slice(side * self.half, (side + 1) * self.half))

    def pairs(self, k, mine):
        y, x = self.y, self.x
        return [
            (y if mine else 1 - y, k, 0),
            (k, x if mine else 1 - x, 1),
        ]

    def first(self, k, side):
        y, x, _ = self.pairs(k, False)[side]
        return self.send(
            self.ref.at[self.at(y, x, side)], self.got_one.at[side, k], self.sem + 2 * side + k,
            peer_of((4, 2)[side], 0),
        )

    def second(self, side):
        y, x = ((self.y, 1 - self.x), (1 - self.y, self.x))[side]
        return self.send(
            self.ref.at[self.at(y, x, side)], self.got_two.at[side], self.sem + 4 + side,
            peer_of((2, 4)[side], 0),
        )

    def start(self):
        for side in range(2):
            for k in range(2):
                self.first(k, side).start()

    def relay(self):
        for side in range(2):
            for k in range(2):
                self.first(k, side).wait()
        for side in range(2):
            for k in range(2):
                y, x, _ = self.pairs(k, True)[side]
                at = self.at(y, x, side)
                self.ref[at] = (
                    self.ref[at].astype(f32) + self.got_one[side, k].astype(f32)
                ).astype(bf16)
        for side in range(2):
            self.second(side).start()

    def finish(self):
        for side in range(2):
            self.second(side).wait()
            at = self.at(self.y, self.x, side)
            self.ref[at] = (
                self.ref[at].astype(f32) + self.got_two[side].astype(f32)
            ).astype(bf16)


ROW_SEMS = 6


def start_body(
    lengths, tokens_ref, weights_ref,
    gathered_ref, mixed_ref, context_ref, parts_ref, lse_ref, heads_ref, out_ref, length_ref, up_ref, down_ref,
    keys, values, length_buf, out_here, out_far, local_sems, send_sems, recv_sems,
):
    chunks, rows, _ = gathered_ref.shape
    width = context_ref.shape[-1]
    lanes = up_ref.shape[-1]
    hidden_width = SHARE * lanes
    piece = rows // 4
    quarter_rows = D // 4
    y, x, c = bits()
    z = lax.axis_index("tensor")
    matched = c == z // 2
    unmatched = jnp.logical_not(matched)
    own_block = block_of(y, x, c)
    send = sender(send_sems, recv_sems)
    core, near_z, diagonal, swapped = peer_of(1, 0), peer_of(0, 1), peer_of(1, 1), peer_of(1, 2)
    across_x, across_y, across_xy = peer_of(2, 0), peer_of(4, 0), peer_of(6, 0)

    def part_of(k):
        return slice(k * piece, (k + 1) * piece)

    def swap_copy(k):
        return send(tokens_ref.at[part_of(k), :], gathered_ref.at[0, part_of(k), :], k, swapped)

    def far_copy(k, source):
        return send(source.at[part_of(k), :], gathered_ref.at[2, part_of(k), :], 4 + k, near_z)

    def near_copy(k, source):
        return send(source.at[part_of(k), :], gathered_ref.at[1, part_of(k), :], 8 + k, core)

    def diagonal_copy(k):
        return send(gathered_ref.at[2, part_of(k), :], gathered_ref.at[3, part_of(k), :], 12 + k, core)

    column = 2 * y + x

    def quarter(k):
        return pl.ds(pl.multiple_of(k * quarter_rows, quarter_rows), quarter_rows)

    def heads_swap():
        return send(
            weights_ref.at[quarter(column), : 3 * width], heads_ref.at[quarter(column), :], 16, swapped
        )

    def heads_share(k, peer):
        return send(heads_ref.at[quarter(column), :], heads_ref.at[quarter(column), :], 17 + k, peer)

    heads_peers = (across_x, across_y, across_xy)
    heads_local = pltpu.make_async_copy(weights_ref.at[:, : 3 * width], heads_ref, local_sems.at[0])

    def out_copy(e):
        return send(out_here, out_far.at[e - 1], 19 + e, peer_of(0, e))

    out_local = pltpu.make_async_copy(
        weights_ref.at[row_block(own_block), 3 * width : 4 * width], out_here, local_sems.at[1]
    )
    outs = [
        Gather(
            send, lambda k, side=side: out_ref.at[row_block(k), side * 2 * width : (side + 1) * 2 * width],
            23 + side * GATHER_SEMS, side == 0,
        )
        for side in range(2)
    ]
    base = 23 + 2 * GATHER_SEMS
    targets = (up_ref, down_ref)

    def feed_source(kind):
        at = 4 * width + kind * hidden_width + own_block * lanes
        return weights_ref.at[:, pl.ds(pl.multiple_of(at, 128), lanes)]

    def feed_copy(kind, e):
        return send(feed_source(kind), targets[kind].at[e - 1, 0, 0], base + 3 * kind + e - 1, peer_of(0, e))

    half = slice(0, D // 2), slice(D // 2, D)

    def feed_one(kind, e, side):
        source = targets[kind].at[e - 1, 0, 0, half[side], :]
        target = targets[kind].at[e - 1, side, 1 - side, half[side], :]
        return send(
            source, target, base + 6 + 6 * kind + 2 * (e - 1) + side, (across_x, across_y)[side]
        )

    def feed_two(e, side):
        if side == 0:
            source, target = (up_ref.at[e - 1, dy, 0:2, half[0], :] for dy in range(2))
        else:
            source, target = (up_ref.at[e - 1, 0:2, dx, half[1], :] for dx in range(2))
        return send(source, target, base + 18 + 2 * (e - 1) + side, (across_y, across_x)[side])

    def first_hop(kind, e):
        feed_copy(kind, e).wait()
        for side in range(2):
            feed_one(kind, e, side).start()

    def second_hop(e):
        for side in range(2):
            feed_one(0, e, side).wait()
        for side in range(2):
            feed_two(e, side).start()

    def length_copy():
        return send(length_buf.at[0], length_buf.at[1], base + 24, core)

    def part_copy(j):
        return send(
            context_ref.at[j], parts_ref.at[j], base + 24 + j, (None, core, near_z, diagonal)[j]
        )

    def send_weights():
        for e in (3, 2, 1):
            feed_copy(0, e).start()
        for e in (3, 2, 1):
            feed_copy(1, e).start()

    out_local.start()
    length_buf[0] = jnp.full(length_buf.shape[1:], lengths[0], jnp.int32)
    greet(
        [core, near_z, diagonal, swapped, across_x, across_y, across_xy, peer_of(0, 2), peer_of(0, 3)]
    )

    @pl.when(matched)
    def _():
        for k in range(4):
            far_copy(k, tokens_ref).start()
            near_copy(k, tokens_ref).start()
        heads_local.start()
        gathered_ref[0] = tokens_ref[...]

    @pl.when(unmatched)
    def _():
        for k in range(4):
            swap_copy(k).start()
        heads_swap().start()

    length_copy().start()

    @pl.when(unmatched)
    def _():
        for k in range(4):
            swap_copy(k).wait()
            far_copy(k, gathered_ref.at[0]).start()
            near_copy(k, gathered_ref.at[0]).start()
        heads_swap().wait()
        for k, peer in enumerate(heads_peers):
            heads_share(k, peer).start()

    for k in range(4):
        far_copy(k, tokens_ref).wait()
        diagonal_copy(k).start()
    out_local.wait()
    for e in (1, 2, 3):
        out_copy(e).start()
    send_weights()
    out_ref[row_block(own_block), :width] = out_here[...]

    @pl.when(matched)
    def _():
        heads_local.wait()

    @pl.when(unmatched)
    def _():
        for k, peer in enumerate(heads_peers):
            heads_share(k, peer).wait()

    length_copy().wait()
    length_ref[...] = jnp.where(matched, length_buf[0], length_buf[1])
    length = length_ref[:1, :]
    own_quarter = jnp.where(matched, z, z + 2 - 4 * (z // 2))
    wide = 256

    def project(j):
        def columns(n, carry):
            at = pl.ds(pl.multiple_of(n * wide, wide), wide)
            mixed_ref[j, :, at] = jnp.dot(
                gathered_ref[j], heads_ref[:, at], preferred_element_type=f32
            ).astype(bf16)
            return carry

        lax.fori_loop(0, 3 * width // wide, columns, 0)

    def arrange(j):
        at_quarter = own_quarter
        if j in (1, 3):
            at_quarter = at_quarter + 2 - 4 * (at_quarter // 2)
        if j in (2, 3):
            at_quarter = at_quarter + 1 - 2 * (at_quarter % 2)
        for h in range(width // HEAD_DIM):
            at = width + (h // 2) * 128
            keys[h, j * rows : (j + 1) * rows, :] = head_keys(
                mixed_ref[j, :, at : at + 128], h % 2, at_quarter * rows, length
            )
        values[j * rows : (j + 1) * rows, :] = mixed_ref[j, :, 2 * width :]

    for j in (0, 2, 1, 3):
        if j == 1:
            for k in range(4):
                near_copy(k, tokens_ref).wait()
        if j == 3:
            for k in range(4):
                diagonal_copy(k).wait()
        project(j)
        arrange(j)

    lane = lax.broadcasted_iota(jnp.int32, (rows, 128), 1)

    def attend(step, carry):
        chunk = chunks - 1 - step
        logs = jnp.zeros((rows, 128), f32)
        for pair in range(width // 128):
            queries = mixed_ref[chunk, :, pair * 128 : pair * 128 + 128]
            both = []
            for side in range(2):
                h = pair * 2 + side
                scores = contract(head_queries(queries, side), keys[h], 1, 1)
                top = jnp.max(scores, axis=1, keepdims=True)
                weight = jnp.exp(scores - top)
                total = jnp.sum(weight, axis=1, keepdims=True)
                out = contract(weight.astype(bf16), values[:, pair * 128 : pair * 128 + 128], 1, 0)
                both.append(out / total)
                logs = jnp.where(lane == h, top + jnp.log(total), logs)
            context_ref[chunk, :, pair * 128 : pair * 128 + 128] = jnp.where(
                lane < HEAD_DIM, both[0], both[1]
            ).astype(bf16)
        lse_ref[chunk] = jnp.transpose(logs)[:8, :]

        @pl.when(step == 0)
        def _():
            part_copy(3).start()
            for e in (1, 2, 3):
                out_copy(e).wait()
                out_ref[row_block(own_block), e * width : (e + 1) * width] = out_far[e - 1]
            for gather in outs:
                gather.start()
            first_hop(0, 3)

        @pl.when(step == 1)
        def _():
            part_copy(2).start()
            for gather in outs:
                gather.relay()
            first_hop(0, 2)
            second_hop(3)

        @pl.when(step == 2)
        def _():
            part_copy(1).start()
            for gather in outs:
                gather.last()
            first_hop(0, 1)
            second_hop(2)

        return carry

    lax.fori_loop(0, chunks, attend, 0)
    parts_ref[0] = context_ref[0]
    for gather in outs:
        gather.finish()
    second_hop(1)
    for e in (3, 2, 1):
        first_hop(1, e)
    for j in (3, 2, 1):
        part_copy(j).wait()
    for e in (3, 2, 1):
        for side in range(2):
            feed_two(e, side).wait()
            feed_one(1, e, side).wait()


def start_block(lengths, tokens, weights):
    rows = tokens.shape[0]
    chunks = 4
    tile = D // 4
    seq = chunks * rows
    lanes = FF // 4 // SHARE
    heads = tile // HEAD_DIM
    sems = 23 + 2 * GATHER_SEMS + 28
    share_rows = D // SHARE
    vmem, anywhere = pl.BlockSpec(memory_space=pltpu.VMEM), pl.BlockSpec(memory_space=pl.ANY)
    return pl.pallas_call(
        start_body,
        name="start_block",
        in_specs=[pl.BlockSpec(memory_space=pltpu.SMEM), vmem, anywhere],
        out_specs=[vmem] * 8 + [anywhere] * 2,
        out_shape=[
            jax.ShapeDtypeStruct((chunks, rows, D), bf16),
            jax.ShapeDtypeStruct((chunks, rows, 3 * tile), bf16),
            jax.ShapeDtypeStruct((chunks, rows, tile), bf16),
            jax.ShapeDtypeStruct((chunks, rows, tile), bf16),
            jax.ShapeDtypeStruct((chunks, 8, rows), f32),
            jax.ShapeDtypeStruct((D, 3 * tile), bf16),
            jax.ShapeDtypeStruct((D, D), bf16),
            jax.ShapeDtypeStruct((8, 128), jnp.int32),
            jax.ShapeDtypeStruct((3, 2, 2, D, lanes), bf16),
            jax.ShapeDtypeStruct((3, 2, 2, D, lanes), bf16),
        ],
        scratch_shapes=[
            pltpu.VMEM((heads, seq, 128), bf16),
            pltpu.VMEM((seq, tile), bf16),
            pltpu.VMEM((2, 8, 128), jnp.int32),
            pltpu.VMEM((share_rows, tile), bf16),
            pltpu.VMEM((3, share_rows, tile), bf16),
            pltpu.SemaphoreType.DMA((2,)),
            pltpu.SemaphoreType.DMA((sems,)),
            pltpu.SemaphoreType.DMA((sems,)),
        ],
        compiler_params=pltpu.CompilerParams(
            vmem_limit_bytes=60 << 20, collective_id=0, has_side_effects=True
        ),
        cost_estimate=pl.CostEstimate(
            flops=24 * heads * seq * seq * HEAD_DIM, bytes_accessed=20 << 20, transcendentals=0
        ),
    )(lengths, tokens, weights)


def back_body(
    info, mixed_ref, context_ref, upstream_ref, lse_ref, weight_ref, branch_ref, norm_ref, outputs_ref, gathered,
    up_grads, down_grads, out_grads,
    input_ref, outputs_out, norm_out, attention_out, feed_out,
    keys, turned, key_sum, value_sum, query_t, grad, rows_held, heads_sum, kept, got_one, got_two, got_three,
    leaving, landed, share, heads, heads_one, heads_two, heads_mine, heads_far, out_held, out_core, out_one, out_two, out_z,
    norm_here, norm_there, local_sems, send_sems, recv_sems,
):
    chunks, rows, _ = mixed_ref.shape
    width = context_ref.shape[-1]
    scale = HEAD_DIM ** (-0.5)
    part = 256
    core, near_z = peer_of(1, 0), peer_of(0, 1)
    across = (peer_of(2, 0), peer_of(4, 0))
    send = sender(send_sems, recv_sems)
    sources = (up_grads, down_grads)
    y, x, c = bits()
    z = lax.axis_index("tensor")
    matched = c == z // 2
    own_block = block_of(y, x, c)

    def stage_one(b, kind):
        return send(sources[kind].at[b, 1], got_one.at[b, kind], 2 * b + kind, across[kind])

    def stage_two(b, kind):
        return send(kept.at[b, kind, 1], got_two.at[b, kind], 8 + 2 * b + kind, across[1 - kind])

    def stage_three(b):
        return send(kept.at[b, :, 0], got_three.at[b - 1], 15 + b, peer_of(0, b))

    def load(b, kind):
        return pltpu.make_async_copy(
            sources[kind].at[b, 0], kept.at[b, kind], local_sems.at[2 * b + kind]
        )

    def start_one(b):
        for kind in range(2):
            stage_one(b, kind).start()

    def start_two(b):
        for kind in range(2):
            load(b, kind).wait()
            stage_one(b, kind).wait()
            for k in (1, 0):
                kept[b, kind, k] = (
                    kept[b, kind, k].astype(f32) + got_one[b, kind, k].astype(f32)
                ).astype(bf16)
        for kind in range(2):
            stage_two(b, kind).start()

    def start_three(b):
        for kind in range(2):
            stage_two(b, kind).wait()
            kept[b, kind, 0] = (
                kept[b, kind, 0].astype(f32) + got_two[b, kind].astype(f32)
            ).astype(bf16)
        if b:
            stage_three(b).start()

    def load_rows(j):
        return pltpu.make_async_copy(gathered.at[j], rows_held.at[j], local_sems.at[8 + j])

    def out_load():
        return pltpu.make_async_copy(out_grads, out_held, local_sems.at[12])

    def out_core_copy(k):
        at = row_block(block_of(k // 2, k % 2, 1 - c))
        return send(out_grads.at[at, :], out_core.at[k], 22 + k, core)

    out_sums = RowSums(
        send, out_held, lambda yy, xx: block_of(yy, xx, c) * 128, 128, out_one, out_two, 26
    )

    def out_z_copy(e):
        at = (row_block(own_block), slice(e * width, (e + 1) * width))
        return send(out_held.at[at], out_z.at[e - 1], 31 + e, peer_of(0, e))

    def out_start():
        out_load().wait()
        for k in range(4):
            out_core_copy(k).wait()
        for k in range(4):
            at = row_block(block_of(k // 2, k % 2, c))
            out_held[at, :] = (out_held[at, :].astype(f32) + out_core[k].astype(f32)).astype(bf16)
        out_sums.start()

    def out_last():
        out_sums.finish()
        for e in (1, 2, 3):
            out_z_copy(e).start()

    norm_turns = ((1, 0), (2, 0), (4, 0), (0, 1), (0, 2))

    def norm_copy(k):
        return send(norm_here.at[k], norm_there.at[k], 35 + k, peer_of(*norm_turns[k]))

    def norm_step(k):
        norm_copy(k).wait()
        total = norm_here[k] + norm_there[k]
        if k + 1 < len(norm_turns):
            norm_here[k + 1] = total
            norm_copy(k + 1).start()
        else:
            norm_out[...] = total

    for b in (3, 2, 1, 0):
        for kind in range(2):
            load(b, kind).start()
    for j in range(chunks):
        load_rows(j).start()
    out_load().start()
    norm_here[0] = norm_ref[...]
    greet([core, near_z, across[0], across[1], peer_of(0, 2), peer_of(0, 3), peer_of(1, 2)])
    for k in range(4):
        out_core_copy(k).start()
    norm_copy(0).start()
    start_one(3)
    start_one(2)

    def return_copy(source, target, k):
        return send(source, target, 49 + 4 * GATHER_SEMS + k, peer_of(1, 2))

    outputs_local = pltpu.make_async_copy(outputs_ref, outputs_out, local_sems.at[15])

    @pl.when(matched)
    def _():
        outputs_local.start()

    @pl.when(jnp.logical_not(matched))
    def _():
        return_copy(outputs_ref, outputs_out, 0).start()

    key_sum[...] = jnp.zeros_like(key_sum)
    value_sum[...] = jnp.zeros_like(value_sum)
    for j in range(chunks):
        for h in range(width // HEAD_DIM):
            at = width + (h // 2) * 128
            keys[h, j * rows : (j + 1) * rows, :] = head_keys(
                mixed_ref[j, :, at : at + 128], h % 2, info[1 + j], info[0]
            )
        turned[:, j * rows : (j + 1) * rows] = jnp.transpose(
            mixed_ref[j, :, width : 2 * width].astype(f32)
        ).astype(bf16)
    feature = lax.broadcasted_iota(jnp.int32, (8, width), 1) // HEAD_DIM
    picks = (feature == lax.broadcasted_iota(jnp.int32, (8, width), 0)).astype(f32)
    per_chunk = rows // part

    def attend(step, carry):
        chunk = step // per_chunk
        at = pl.ds(pl.multiple_of((step % per_chunk) * part, part), part)
        upstream = upstream_ref[chunk, at, :]
        product = upstream.astype(f32) * context_ref[chunk, at, :].astype(f32)
        delta = lax.dot_general(
            picks, product, (((1,), (1,)), ((), ())), precision=lax.Precision.HIGHEST,
            preferred_element_type=f32,
        )
        lse = lse_ref[chunk, :, at]
        for pair in range(width // 128):
            lanes = slice(pair * 128, pair * 128 + 128)
            queries = mixed_ref[chunk, at, lanes]
            value_rows = mixed_ref[:, :, 2 * width + pair * 128 : 2 * width + pair * 128 + 128]
            value_rows = value_rows.reshape(chunks * rows, 128)
            for half in range(2):
                h = pair * 2 + half
                scores = contract(keys[h], head_queries(queries, half), 1, 1)
                weight = jnp.exp(scores - lse[h : h + 1, :])
                up_half = head_half(upstream[:, lanes], half)
                back = contract(value_rows, up_half, 1, 1)
                score_grad = (weight * (back - delta[h : h + 1, :])).astype(bf16)
                value_sum[pair] += contract(weight.astype(bf16), up_half, 1, 0)
                key_sum[pair] += contract(score_grad, head_half(queries, half), 1, 0)
                query_t[h * HEAD_DIM : (h + 1) * HEAD_DIM, :] = (
                    contract(turned[h * HEAD_DIM : (h + 1) * HEAD_DIM, :], score_grad, 1, 0) * scale
                )
        grad[chunk, at, :width] = jnp.transpose(query_t[...]).astype(bf16)

        @pl.when(step == 0)
        def _():
            norm_step(0)
            out_start()

        @pl.when(step == 1)
        def _():
            norm_step(1)
            start_two(3)
            start_one(1)

        @pl.when(step == 2)
        def _():
            norm_step(2)
            out_sums.relay()

        @pl.when(step == 3)
        def _():
            norm_step(3)
            start_two(2)
            start_one(0)
            start_three(3)

        @pl.when(step == 4)
        def _():
            norm_step(4)
            out_last()

        @pl.when(step == 6)
        def _():
            start_two(1)

        return carry

    lax.fori_loop(0, chunks * per_chunk, attend, 0)
    for j in range(chunks):
        at = slice(j * rows, (j + 1) * rows)
        for pair in range(width // 128):
            left = width + pair * 128
            grad[j, :, left : left + 128] = (key_sum[pair, at, :] * scale).astype(bf16)
            grad[j, :, left + width : left + width + 128] = value_sum[pair, at, :].astype(bf16)
    start_three(2)

    def rows_back(j):
        return contract(grad[j], weight_ref[...], 1, 1)

    core_copies = {}
    for k, j in enumerate((3, 1)):
        leaving[k] = rows_back(j).astype(bf16)
        core_copies[j] = send(leaving.at[k], landed.at[k], 19 + k, core)
        core_copies[j].start()
    far = rows_back(2)
    core_copies[3].wait()
    leaving[2] = (far + landed[0].astype(f32)).astype(bf16)
    far_copy = send(leaving.at[2], landed.at[2], 21, near_z)
    branch_ref_value = branch_ref[...] + rows_back(0)
    core_copies[1].wait()
    own_rows = branch_ref_value + landed[1].astype(f32)

    heads_sum[...] = jnp.zeros_like(heads_sum)
    for j in range(chunks):
        load_rows(j).wait()

    def weigh(j, carry):
        heads_sum[...] += contract(rows_held[j], grad[j], 0, 0)
        return carry

    lax.fori_loop(0, chunks, weigh, 0)
    heads[...] = heads_sum[...].astype(bf16)
    head_sums = RowSums(
        send, heads, lambda yy, xx: block_of(yy, xx, 0) * 128, 256, heads_one, heads_two, 40
    )
    head_sums.start()
    start_three(1)
    far_copy.start()
    start_two(0)
    head_sums.relay()
    start_three(0)
    head_sums.finish()

    def half_rows(k):
        return row_block(block_of(y, x, k))

    @pl.when(matched)
    def _():
        send(heads.at[half_rows(1 - c), :], heads_mine, 46, core).start()

    @pl.when(jnp.logical_not(matched))
    def _():
        send(heads.at[half_rows(c), :], heads_far, 47, peer_of(0, 2)).start()
        send(heads.at[half_rows(1 - c), :], heads_far, 48, peer_of(1, 2)).start()

    total = kept[0, :, 0].astype(f32)
    for b in (3, 2, 1):
        stage_three(b).wait()
        total = total + got_three[b - 1].astype(f32)
    share[...] = total.astype(bf16)
    own_feed = [
        pltpu.make_async_copy(share.at[kind], feed_out.at[own_block, kind], local_sems.at[13 + kind])
        for kind in range(2)
    ]
    for copy in own_feed:
        copy.start()
    feeds = [
        Gather(send, lambda k, kind=kind: feed_out.at[k, kind], 49 + kind * GATHER_SEMS, kind == 0)
        for kind in range(2)
    ]
    for copy in own_feed:
        copy.wait()
    for feed in feeds:
        feed.start()
    sum_out = out_held[row_block(own_block), :width].astype(f32)
    for e in (1, 2, 3):
        out_z_copy(e).wait()
        sum_out = sum_out + out_z[e - 1].astype(f32)
    attention_out[row_block(own_block), 3 * width :] = sum_out.astype(bf16)

    @pl.when(matched)
    def _():
        send(heads.at[half_rows(1 - c), :], heads_mine, 46, core).wait_send()
        heads_mine[...] = heads[half_rows(c), :]

    @pl.when(jnp.logical_not(matched))
    def _():
        send(heads.at[half_rows(c), :], heads_far, 47, peer_of(0, 2)).wait_send()
        send(heads.at[half_rows(1 - c), :], heads_far, 48, peer_of(1, 2)).wait_send()
        send(heads.at[half_rows(c), :], heads_mine, 46, core).wait_recv()

    @pl.when(matched)
    def _():
        send(heads.at[half_rows(c), :], heads_far, 47, peer_of(0, 2)).wait_recv()

    @pl.when(jnp.logical_not(matched))
    def _():
        send(heads.at[half_rows(c), :], heads_far, 48, peer_of(1, 2)).wait_recv()

    attention_out[row_block(own_block), : 3 * width] = (
        heads_mine[...].astype(f32) + heads_far[...].astype(f32)
    ).astype(bf16)
    sides = [
        Gather(
            send,
            lambda k, side=side: attention_out.at[row_block(k), side * 2 * width : (side + 1) * 2 * width],
            49 + (2 + side) * GATHER_SEMS, side == 0,
        )
        for side in range(2)
    ]
    for side in sides:
        side.start()
    far_copy.wait()
    input_ref[...] = (own_rows + landed[2].astype(f32)).astype(bf16)
    for gather in feeds + sides:
        gather.relay()
    for gather in feeds + sides:
        gather.last()
    for gather in feeds + sides:
        gather.finish()
    @pl.when(matched)
    def _():
        outputs_local.wait()

    @pl.when(jnp.logical_not(matched))
    def _():
        return_copy(outputs_ref, outputs_out, 0).wait()


def back_block(info, mixed, context, upstream, lse, weight, branch, norm_sums, outputs, gathered, up_grads,
               down_grads, out_grads):
    chunks, rows, width3 = mixed.shape
    width = width3 // 3
    seq = chunks * rows
    heads = width // HEAD_DIM
    lanes = up_grads.shape[-1]
    share_rows = D // SHARE
    sems = 51 + 4 * GATHER_SEMS
    vmem, anywhere = pl.BlockSpec(memory_space=pltpu.VMEM), pl.BlockSpec(memory_space=pl.ANY)
    return pl.pallas_call(
        back_body,
        name="back_block",
        in_specs=[pl.BlockSpec(memory_space=pltpu.SMEM)] + [vmem] * 7 + [anywhere] * 5,
        out_specs=[vmem, vmem, vmem, vmem, anywhere],
        out_shape=[
            jax.ShapeDtypeStruct((rows, D), bf16),
            jax.ShapeDtypeStruct((rows, D), bf16),
            jax.ShapeDtypeStruct((4, D), f32),
            jax.ShapeDtypeStruct((D, 4 * width), bf16),
            jax.ShapeDtypeStruct((SHARE, 2, D, lanes), bf16),
        ],
        scratch_shapes=[
            pltpu.VMEM((heads, seq, 128), bf16),
            pltpu.VMEM((width, seq), bf16),
            pltpu.VMEM((width // 128, seq, 128), f32),
            pltpu.VMEM((width // 128, seq, 128), f32),
            pltpu.VMEM((width, 256), f32),
            pltpu.VMEM((chunks, rows, width3), bf16),
            pltpu.VMEM((chunks, rows, D), bf16),
            pltpu.VMEM((D, width3), f32),
            pltpu.VMEM((4, 2, 2, D, lanes), bf16),
            pltpu.VMEM((4, 2, 2, D, lanes), bf16),
            pltpu.VMEM((4, 2, D, lanes), bf16),
            pltpu.VMEM((3, 2, D, lanes), bf16),
            pltpu.VMEM((3, rows, D), bf16),
            pltpu.VMEM((3, rows, D), bf16),
            pltpu.VMEM((2, D, lanes), bf16),
            pltpu.VMEM((D, width3), bf16),
            pltpu.VMEM((2, 2, 2 * share_rows, width3 // 2), bf16),
            pltpu.VMEM((2, 2 * share_rows, width3 // 2), bf16),
            pltpu.VMEM((share_rows, width3), bf16),
            pltpu.VMEM((share_rows, width3), bf16),
            pltpu.VMEM((D, 4 * width), bf16),
            pltpu.VMEM((4, share_rows, 4 * width), bf16),
            pltpu.VMEM((2, 2, share_rows, 2 * width), bf16),
            pltpu.VMEM((2, share_rows, 2 * width), bf16),
            pltpu.VMEM((3, share_rows, width), bf16),
            pltpu.VMEM((5, 4, D), f32),
            pltpu.VMEM((5, 4, D), f32),
            pltpu.SemaphoreType.DMA((16,)),
            pltpu.SemaphoreType.DMA((sems,)),
            pltpu.SemaphoreType.DMA((sems,)),
        ],
        compiler_params=pltpu.CompilerParams(
            vmem_limit_bytes=67043328, collective_id=2, has_side_effects=True
        ),
        cost_estimate=pl.CostEstimate(
            flops=40 * heads * seq * seq * HEAD_DIM, bytes_accessed=40 << 20, transcendentals=0
        ),
    )(
        info, mixed, context, upstream, lse, weight, branch, norm_sums, outputs, gathered, up_grads, down_grads,
        out_grads,
    )


def adam_body(owned, attention_ref, feed_ref, master_ref, one_ref, two_ref,
              grad_out, master_out, one_out, two_out, tiles_out, up_out, down_out):
    tile = grad_out.shape[-1] // 4
    for s in range(4):
        at = slice(s * tile, (s + 1) * tile)
        grad = jnp.zeros((grad_out.shape[0], tile), f32)
        for i in range(4):
            value = attention_ref[:, i * tile : (i + 1) * tile].astype(f32)
            grad = jnp.where(owned[s, i] > 0, value, grad)
        for kind in range(2):
            value = jnp.concatenate([feed_ref[2 * s + k, kind] for k in range(2)], axis=-1)
            grad = jnp.where(owned[s, 4 + 4 * kind + s] > 0, value.astype(f32), grad)
        occupied = (owned[s, 12] > 0).astype(f32)
        param, first, second = adam_update(
            grad, master_ref[:, at], one_ref[:, at], two_ref[:, at], occupied, weight_decay
        )
        grad_out[:, at] = grad
        master_out[:, at] = param
        one_out[:, at] = first
        two_out[:, at] = second
        low = param.astype(bf16)
        none = jnp.zeros_like(low)
        for i in range(4):
            mine = jnp.where(owned[s, i] > 0, low, none)
            there = slice(i * tile, (i + 1) * tile)
            tiles_out[:, there] = mine if s == 0 else tiles_out[:, there] + mine
        for kind, target in ((0, up_out), (1, down_out)):
            mine = jnp.where(owned[s, 4 + 4 * kind + s] > 0, low, none)
            for k in range(2):
                target[2 * s + k] = mine[:, k * tile // 2 : (k + 1) * tile // 2]


def adam_block(owned, attention_grad, feed_grad, master, one, two):
    part = 128
    wide = pl.BlockSpec((part, D), lambda i: (i, 0))
    lanes = feed_grad.shape[-1]
    split = pl.BlockSpec((SHARE, part, lanes), lambda i: (0, i, 0))
    return pl.pallas_call(
        adam_body,
        grid=(D // part,),
        name="adam_block",
        in_specs=[
            pl.BlockSpec(memory_space=pltpu.SMEM), wide,
            pl.BlockSpec((SHARE, 2, part, lanes), lambda i: (0, 0, i, 0)), wide, wide, wide,
        ],
        out_specs=[wide] * 5 + [split] * 2,
        out_shape=[jax.ShapeDtypeStruct((D, D), f32)] * 4
        + [jax.ShapeDtypeStruct((D, D), bf16)]
        + [jax.ShapeDtypeStruct((SHARE, D, lanes), bf16)] * 2,
        compiler_params=pltpu.CompilerParams(vmem_limit_bytes=62 << 20),
        cost_estimate=pl.CostEstimate(flops=40 * D * D, bytes_accessed=40 << 20, transcendentals=0),
    )(owned, attention_grad, feed_grad, master, one, two)


def tiles_body(tiles_ref, up_ref, down_ref, input_ref, tiles_out, up_out, down_out, input_out, *scratch):
    core_got = scratch[:3]
    one_got, two_got = scratch[3:5], scratch[5:7]
    work = scratch[7:10]
    row_one, row_two, local_sems, send_sems, recv_sems = scratch[10:]
    matched = lax.axis_index("dp") % 2 == lax.axis_index("tensor") // 2
    send = sender(send_sems, recv_sems)
    y, x, c = bits()
    core = peer_of(1, 0)
    own_block = block_of(y, x, c)
    greet([core, peer_of(2, 0), peer_of(4, 0), peer_of(1, 2)])
    input_local = pltpu.make_async_copy(input_ref, input_out, local_sems.at[0])
    input_swap = send(input_ref, input_out, 24 + 4 * GATHER_SEMS, peer_of(1, 2))

    @pl.when(matched)
    def _():
        input_local.start()

    @pl.when(jnp.logical_not(matched))
    def _():
        input_swap.start()

    arrays = ((up_ref, up_out), (down_ref, down_out), (tiles_ref, tiles_out))

    def place(n, ref, block):
        return ref.at[row_block(block), :] if n == 2 else ref.at[block]

    def core_copy(n, k):
        return send(
            place(n, arrays[n][0], block_of(k // 2, k % 2, 1 - c)), core_got[n].at[k], 4 * n + k, core
        )

    def core_add(n):
        source, target = arrays[n][0], work[n]
        for k in range(4):
            core_copy(n, k).wait()
        for k in range(4):
            block = block_of(k // 2, k % 2, c)
            if n == 2:
                at = row_block(block)
                target[at, :] = source[at, :] + core_got[n][k]
            else:
                target[k] = source[block] + core_got[n][k]

    def first(n, k):
        y_, x_ = ((k, 1 - x), (1 - y, k))[n]
        return send(
            work[n].at[2 * y_ + x_], one_got[n].at[k], 12 + 2 * n + k,
            peer_of((2, 4)[n], 0),
        )

    def second(n):
        y_, x_ = ((1 - y, x), (y, 1 - x))[n]
        return send(
            work[n].at[2 * y_ + x_], two_got[n], 16 + n, peer_of((4, 2)[n], 0)
        )

    def relay(n):
        target = work[n]
        for k in range(2):
            first(n, k).wait()
        for k in range(2):
            y_, x_ = ((k, x), (y, k))[n]
            block = 2 * y_ + x_
            target[block] = target[block] + one_got[n][k]
        second(n).start()

    def settle(n):
        second(n).wait()
        arrays[n][1][own_block] = work[n][2 * y + x] + two_got[n][...]

    for n in range(3):
        for k in range(4):
            core_copy(n, k).start()
    for n in range(2):
        core_add(n)
        for k in range(2):
            first(n, k).start()
    core_add(2)
    rows = RowSums(
        send, work[2], lambda yy, xx: block_of(yy, xx, c) * 128, 128, row_one, row_two, 18
    )
    rows.start()
    for n in range(2):
        relay(n)
    rows.relay()
    gathers = []
    for n in range(2):
        settle(n)
        gathers.append(
            Gather(send, lambda k, n=n: arrays[n][1].at[k], 24 + n * GATHER_SEMS, n == 0)
        )
        gathers[-1].start()
    rows.finish()
    tiles_out[row_block(own_block), :] = work[2][row_block(own_block), :]
    half = tiles_out.shape[-1] // 2
    for side in range(2):
        gathers.append(
            Gather(
                send,
                lambda k, side=side: tiles_out.at[row_block(k), side * half : (side + 1) * half],
                24 + (2 + side) * GATHER_SEMS, side == 0,
            )
        )
        gathers[-1].start()
    for gather in gathers:
        gather.relay()
    for gather in gathers:
        gather.last()
    for gather in gathers:
        gather.finish()

    @pl.when(matched)
    def _():
        input_local.wait()

    @pl.when(jnp.logical_not(matched))
    def _():
        input_swap.wait()


def spread_tiles(tiles, up, down, rows):
    share_rows = D // SHARE
    lanes = up.shape[-1]
    sems = 25 + 4 * GATHER_SEMS
    piece = (D, lanes)
    vmem = pl.BlockSpec(memory_space=pltpu.VMEM)
    return pl.pallas_call(
        tiles_body,
        name="spread_tiles",
        in_specs=[vmem] * 3 + [pl.BlockSpec(memory_space=pl.ANY)],
        out_specs=[vmem] * 4,
        out_shape=[jax.ShapeDtypeStruct(v.shape, bf16) for v in (tiles, up, down, rows)],
        scratch_shapes=[
            pltpu.VMEM((4,) + piece, bf16),
            pltpu.VMEM((4,) + piece, bf16),
            pltpu.VMEM((4, share_rows, D), bf16),
            pltpu.VMEM((2,) + piece, bf16),
            pltpu.VMEM((2,) + piece, bf16),
            pltpu.VMEM(piece, bf16),
            pltpu.VMEM(piece, bf16),
            pltpu.VMEM((4,) + piece, bf16),
            pltpu.VMEM((4,) + piece, bf16),
            pltpu.VMEM((D, D), bf16),
            pltpu.VMEM((2, 2, share_rows, D // 2), bf16),
            pltpu.VMEM((2, share_rows, D // 2), bf16),
            pltpu.SemaphoreType.DMA((1,)),
            pltpu.SemaphoreType.DMA((sems,)),
            pltpu.SemaphoreType.DMA((sems,)),
        ],
        compiler_params=pltpu.CompilerParams(
            vmem_limit_bytes=48 << 20, collective_id=3, has_side_effects=True
        ),
        cost_estimate=pl.CostEstimate(flops=D * D, bytes_accessed=12 << 20, transcendentals=0),
    )(tiles, up, down, rows)


def joined(held, i, kind):
    return jnp.concatenate(
        [held[kind, 2 * (i // 2) + m, i % 2, k] for k in range(2) for m in range(2)], axis=-1
    )


def gelu_parts(value):
    bell = jnp.exp(-0.5 * value * value)
    t = 1.0 / (1.0 + (0.3275911 * 0.5**0.5) * jnp.abs(value))
    tail = 0.5 * 1.061405429
    for c in (-1.453152027, 1.421413741, -0.284496736, 0.254829592):
        tail = tail * t + 0.5 * c
    tail = tail * t * bell
    area = jnp.where(value > 0, 1.0 - tail, tail)
    return value * area, area + value * bell * (0.5 / jnp.pi) ** 0.5


def feed_body(
    info, first_ref, cotangent_ref, norms_ref, weights_ref, up_ref, down_ref,
    out_ref, low_ref, both_ref, hidden_ref, pre_ref, grad_ref, sums_ref,
    held, slope, total, leaving, landed, seed_held, local_sems, send_sems, recv_sems,
):
    rows = first_ref.shape[0]
    steps = hidden_ref.shape[0]
    lanes = held.shape[-1]
    y, x, c = bits()
    peer = peer_of(1, 0)
    send = sender(send_sems, recv_sems)
    half = slice(0, D // 2), slice(D // 2, D)
    loads = []
    for kind in range(2):
        for dy in range(2):
            for dx in range(2):
                block = block_of(1 - y if dy else y, 1 - x if dx else x, c)
                at = D + kind * SHARE * lanes + block * lanes
                loads.append(
                    (weights_ref.at[:, pl.ds(pl.multiple_of(at, 128), lanes)], held.at[kind, 0, dy, dx])
                )
    loads.append((up_ref, held.at[0, 1:4]))
    loads.append((down_ref.at[:, 0, 0:2, half[0], :], held.at[1, 1:4, 0, 0:2, half[0], :]))
    loads.append((down_ref.at[:, 0:2, 0, half[1], :], held.at[1, 1:4, 0:2, 0, half[1], :]))
    loads = [pltpu.make_async_copy(a, b, local_sems.at[k]) for k, (a, b) in enumerate(loads)]
    for load in loads:
        load.start()
    greet([peer, peer_of(2, 0), peer_of(4, 0), peer_of(1, 2)])
    matched = c == lax.axis_index("tensor") // 2
    seed_local = pltpu.make_async_copy(cotangent_ref, seed_held, local_sems.at[len(loads)])
    seed_swap = send(cotangent_ref, seed_held, 6, peer_of(1, 2))
    hops = [
        send(
            down_ref.at[:, 0, 0:2, half[0], :], held.at[1, 1:4, 1, 0:2, half[0], :], 4, peer_of(4, 0)
        ),
        send(
            down_ref.at[:, 0:2, 0, half[1], :], held.at[1, 1:4, 0:2, 1, half[1], :], 5, peer_of(2, 0)
        ),
    ]
    for hop in hops:
        hop.start()

    @pl.when(matched)
    def _():
        seed_local.start()

    @pl.when(jnp.logical_not(matched))
    def _():
        seed_swap.start()

    def across(source, target, k):
        return send(source, target, k, peer)

    middle_row = rows // 2
    both_ref[0] = first_ref[...].astype(bf16)
    first_copy = across(both_ref.at[0], both_ref.at[1], 0)
    first_copy.start()

    def up(i, slot):
        weight = joined(held, i, 0)
        for r in range(0, rows, middle_row):
            at = slice(r, r + middle_row)
            value = jnp.dot(both_ref[slot, at, :], weight, preferred_element_type=f32)
            hidden, steep = gelu_parts(value)
            hidden_ref[i, slot, at, :] = hidden.astype(bf16)
            slope[i, slot, at, :] = steep.astype(bf16)

    def down(i, slot):
        total[slot] += contract(hidden_ref[i, slot], joined(held, i, 1), 1, 1)

    def back(i, slot):
        weight = joined(held, i, 1)
        for r in range(0, rows, middle_row):
            at = slice(r, r + middle_row)
            value = jnp.dot(low_ref[slot, at, :], weight, preferred_element_type=f32)
            pre_ref[i, slot, at, :] = (value * slope[i, slot, at, :].astype(f32)).astype(bf16)

    def back_up(i, slot):
        total[slot] += contract(pre_ref[i, slot], joined(held, i, 0), 1, 1)

    def loop(*works):
        def body(i, carry):
            for work in works:
                work(i)
            return carry

        lax.fori_loop(0, steps, body, 0)

    total[...] = jnp.zeros_like(total)
    for load in loads:
        load.wait()
    loop(lambda i: up(i, 0))
    first_copy.wait()
    loop(lambda i: up(i, 1))
    for hop in hops:
        hop.wait()
    loop(lambda i: down(i, 1))
    leaving[...] = total[1].astype(bf16)
    feed_copy = across(leaving, landed.at[0], 1)
    feed_copy.start()
    loop(lambda i: down(i, 0))
    feed_copy.wait()

    @pl.when(matched)
    def _():
        seed_local.wait()

    @pl.when(jnp.logical_not(matched))
    def _():
        seed_swap.wait()

    sums_ref[...] = jnp.zeros_like(sums_ref)
    part = 128

    def middle(r, carry):
        at = pl.ds(pl.multiple_of(r * part, part), part)
        second, normed, inverse = norm_parts(
            first_ref[at, :] + (total[0, at, :] + landed[0, at, :].astype(f32)),
            norms_ref[2:3, :], norms_ref[3:4, :],
        )
        out_ref[at, :] = second.astype(bf16)
        row = lax.broadcasted_iota(jnp.int32, (part, 1), 0) + r * part + info[1]
        seed = seed_held[at, :].astype(f32) * (row < info[0]).astype(f32)
        grad = norm_back(seed, normed, inverse, norms_ref[2:3, :])
        sums_ref[0:1, :] += jnp.sum(seed * normed, axis=0, keepdims=True)
        sums_ref[1:2, :] += jnp.sum(seed, axis=0, keepdims=True)
        total[0, at, :] = grad
        low_ref[0, at, :] = grad.astype(bf16)
        return carry

    lax.fori_loop(0, rows // part, middle, 0)
    low_copy = across(low_ref.at[0], low_ref.at[1], 2)
    low_copy.start()
    total[1] = jnp.zeros_like(total[1])
    loop(lambda i: back(i, 0))
    low_copy.wait()
    loop(lambda i: back(i, 1), lambda i: back_up(i, 1))
    leaving[...] = total[1].astype(bf16)
    grad_copy = across(leaving, landed.at[1], 3)
    grad_copy.start()
    loop(lambda i: back_up(i, 0))
    grad_copy.wait()
    grad_ref[...] = total[0] + landed[1].astype(f32)


def feed_block(info, first, cotangent, norms, weights, up, down):
    rows = first.shape[0]
    lanes = up.shape[-1]
    width = 4 * lanes
    vmem, anywhere = pl.BlockSpec(memory_space=pltpu.VMEM), pl.BlockSpec(memory_space=pl.ANY)
    return pl.pallas_call(
        feed_body,
        name="feed_block",
        in_specs=[pl.BlockSpec(memory_space=pltpu.SMEM), vmem, anywhere, vmem] + [anywhere] * 3,
        out_specs=[vmem] * 7,
        out_shape=[
            jax.ShapeDtypeStruct((rows, D), bf16),
            jax.ShapeDtypeStruct((2, rows, D), bf16),
            jax.ShapeDtypeStruct((2, rows, D), bf16),
            jax.ShapeDtypeStruct((4, 2, rows, width), bf16),
            jax.ShapeDtypeStruct((4, 2, rows, width), bf16),
            jax.ShapeDtypeStruct((rows, D), f32),
            jax.ShapeDtypeStruct((2, D), f32),
        ],
        scratch_shapes=[
            pltpu.VMEM((2, 4, 2, 2, D, lanes), bf16),
            pltpu.VMEM((4, 2, rows, width), bf16),
            pltpu.VMEM((2, rows, D), f32),
            pltpu.VMEM((rows, D), bf16),
            pltpu.VMEM((2, rows, D), bf16),
            pltpu.VMEM((rows, D), bf16),
            pltpu.SemaphoreType.DMA((12,)),
            pltpu.SemaphoreType.DMA((7,)),
            pltpu.SemaphoreType.DMA((7,)),
        ],
        compiler_params=pltpu.CompilerParams(
            vmem_limit_bytes=60 << 20, collective_id=1, has_side_effects=True
        ),
        cost_estimate=pl.CostEstimate(
            flops=64 * rows * D * width, bytes_accessed=30 << 20, transcendentals=0
        ),
    )(info, first, cotangent, norms, weights, up, down)


def feed_grads_body(first_ref, low_ref, hidden_ref, pre_ref, up_ref, down_ref, first_t, low_t):
    rows = first_ref.shape[1]

    @pl.when(pl.program_id(0) == 0)
    def _():
        for slot in range(2):
            at = slice(slot * rows, (slot + 1) * rows)
            first_t[:, at] = jnp.transpose(first_ref[slot].astype(f32)).astype(bf16)
            low_t[:, at] = jnp.transpose(low_ref[slot].astype(f32)).astype(bf16)

    lanes = up_ref.shape[-1]
    width = pre_ref.shape[-1]
    for target, source, turned in ((up_ref, pre_ref, first_t), (down_ref, hidden_ref, low_t)):
        grad = jnp.dot(
            turned[...], source[0].reshape(2 * rows, width), preferred_element_type=f32
        ).astype(bf16)
        for k in range(2):
            for m in range(2):
                at = (2 * k + m) * lanes
                if target is up_ref:
                    target[m, k, 0] = grad[:, at : at + lanes]
                else:
                    target[m, 0, k] = grad[:, at : at + lanes]


def feed_grads(first, low, hidden, pre):
    count, _, rows, width = hidden.shape
    full = pl.BlockSpec((2, rows, D), lambda i: (0, 0, 0))
    piece = pl.BlockSpec((1, 2, rows, width), lambda i: (i, 0, 0, 0))
    lanes = width // 4
    return pl.pallas_call(
        feed_grads_body,
        grid=(count,),
        name="feed_grads",
        in_specs=[full, full, piece, piece],
        out_specs=[
            pl.BlockSpec((2, 2, 1, D, lanes), lambda i: (i // 2, 0, i % 2, 0, 0)),
            pl.BlockSpec((2, 1, 2, D, lanes), lambda i: (i // 2, i % 2, 0, 0, 0)),
        ],
        out_shape=[jax.ShapeDtypeStruct((count, 2, 2, D, lanes), bf16)] * 2,
        scratch_shapes=[pltpu.VMEM((D, 2 * rows), bf16), pltpu.VMEM((D, 2 * rows), bf16)],
        compiler_params=pltpu.CompilerParams(vmem_limit_bytes=48 << 20),
        cost_estimate=pl.CostEstimate(
            flops=8 * rows * D * width * count, bytes_accessed=20 << 20, transcendentals=0
        ),
    )(first, low, hidden, pre)


def layer(n_dp, n_tensor, tokens, weights, norms, cotangent, lengths, owners, master, moment_one,
          moment_two, norm_master, norm_one, norm_two):
    tile = D // n_tensor
    rows = tokens.shape[0]
    device = lax.axis_index("dp")
    z = lax.axis_index("tensor")
    core = device % 2
    matched = core == z // 2
    quarter = jnp.where(matched, z, z ^ 2)

    def flip(x, dd, dz):
        pairs = [
            (d * n_tensor + t, (d ^ dd) * n_tensor + (t ^ dz))
            for d in range(n_dp)
            for t in range(n_tensor)
        ]
        return lax.ppermute(x, AXES, pairs)

    gathered, mixed, context, parts, lse, w_heads, w_out_all, length, up_all, down_all = start_block(
        lengths, tokens[:, 0, :], weights
    )
    own = gathered[0]
    base = jnp.stack([quarter ^ k for k in (0, 2, 1, 3)]) * rows
    info = jnp.concatenate([length[0, :1], base]).astype(jnp.int32)

    context_all = jnp.where(
        matched,
        jnp.concatenate([parts[k] for k in (0, 2, 1, 3)], axis=1),
        jnp.concatenate([parts[k] for k in (1, 3, 0, 2)], axis=1),
    )
    branch = contract(context_all, w_out_all, 1, 1)
    first, first_normed, first_inverse = norm_parts(
        own.astype(f32) + branch, norms[0], norms[1]
    )
    outputs, both_low, both_first, hidden, pre_grad, first_grad, sums_two = feed_block(
        info, first, cotangent[:, 0, :], norms, weights, up_all, down_all
    )
    branch_grad = norm_back(first_grad, first_normed, first_inverse, norms[0])
    gain_one = jnp.sum(first_grad * first_normed, axis=0)
    shift_one = jnp.sum(first_grad, axis=0)
    branch_low = branch_grad.astype(bf16)
    context_grad = jnp.dot(branch_low, w_out_all, preferred_element_type=f32).astype(bf16)
    blocks = [context_grad[:, k * tile : (k + 1) * tile] for k in range(4)]
    blocks = [
        jnp.where(matched, blocks[a], blocks[b]) for a, b in ((0, 2), (2, 0), (1, 3), (3, 1))
    ]
    upstream = jnp.stack(
        [blocks[0], flip(blocks[1], 1, 0), flip(blocks[2], 0, 1), flip(blocks[3], 1, 1)]
    )

    def add(a, b):
        return (a.astype(f32) + b.astype(f32)).astype(bf16)

    up_grads, down_grads = feed_grads(both_first, both_low, hidden, pre_grad)
    out_grad = contract(branch_low, context_all, 0, 0).astype(bf16)
    norm_sums = jnp.concatenate([jnp.stack([gain_one, shift_one]), sums_two])
    input_grad, outputs, norm_grads, attention_grad, feed_grad = back_block(
        info, mixed, context, upstream, lse, w_heads, branch_grad, norm_sums, outputs, gathered, up_grads, down_grads,
        out_grad,
    )

    def over_groups(value, combine):
        bit = SHARE
        while bit < n_dp:
            value = combine(value, flip(value, bit, 0))
            bit *= 2
        return value

    def plus(a, b):
        return a + b

    norm_grads = over_groups(norm_grads, plus)
    attention_grad = over_groups(attention_grad, add)
    feed_grad = over_groups(feed_grad, add)

    tile_owner, slot_index = slot_table(owners)
    slot_ids = jnp.arange(FF // D, dtype=jnp.int32)
    owned = (
        (tile_owner[None, :] == device) & (slot_index[None, :] == slot_ids[:, None])
    ).astype(jnp.int32)
    owned = jnp.concatenate([owned, jnp.sum(owned, axis=1, keepdims=True)], axis=1)
    slot_grad, new_master, new_one, new_two, tiles, up_tiles, down_tiles = adam_block(
        owned, attention_grad, feed_grad, master[0], moment_one[0], moment_two[0]
    )
    tiles, up_tiles, down_tiles, input_grad = spread_tiles(tiles, up_tiles, down_tiles, input_grad)
    tiles, up_tiles, down_tiles = (over_groups(v, plus) for v in (tiles, up_tiles, down_tiles))
    new_weights = jnp.concatenate(
        [tiles] + [up_tiles[k] for k in range(SHARE)] + [down_tiles[k] for k in range(SHARE)], axis=1
    )
    norm_owner = (device == owners[6]).astype(f32)
    new_norm_master, new_norm_one, new_norm_two = adam_update(
        norm_grads, norm_master[0], norm_one[0], norm_two[0], norm_owner, 0.0
    )
    return (
        outputs[:, None, :],
        input_grad[:, None, :],
        slot_grad[None],
        new_master[None],
        new_one[None],
        new_two[None],
        new_weights,
        norm_grads,
        new_norm_master[None],
        new_norm_one[None],
        new_norm_two[None],
    )


def solution(mesh):
    in_specs = (
        P("tensor", "dp", None),
        P(None, "tensor"),
        P(),
        P("tensor", "dp", None),
        P("dp"),
        P(),
        P("dp", None, "tensor"),
        P("dp", None, "tensor"),
        P("dp", None, "tensor"),
        P("dp", None, None),
        P("dp", None, None),
        P("dp", None, None),
    )
    out_specs = (
        P("tensor", "dp", None),
        P("tensor", "dp", None),
        P("dp", None, "tensor"),
        P("dp", None, "tensor"),
        P("dp", None, "tensor"),
        P("dp", None, "tensor"),
        P(None, "tensor"),
        P(),
        P("dp", None, None),
        P("dp", None, None),
        P("dp", None, None),
    )
    return jax.shard_map(
        partial(layer, mesh.shape["dp"], mesh.shape["tensor"]),
        mesh=mesh,
        in_specs=in_specs,
        out_specs=out_specs,
        check_vma=False,
    )
```

```python
from functools import partial

import jax
import jax.numpy as jnp
from jax import lax
from jax.experimental import pallas as pl
from jax.experimental.pallas import tpu as pltpu
from jax.sharding import PartitionSpec as P

D = 1024
FF = 4096
ADAM_STEP = 10
HEAD_DIM = 64
SHARE = 8


f32, bf16 = jnp.float32, jnp.bfloat16
beta_one = 0.9
beta_two = 0.999
learn_rate = 0.02
weight_decay = 0.1
adam_eps = 1e-08
norm_eps = 1e-05
masked_score = -1e30
AXES = ("dp", "tensor")


def contract(a, b, ca, cb):
    return lax.dot_general(a, b, (((ca,), (cb,)), ((), ())), preferred_element_type=f32)


def norm_parts(value, gain, shift):
    average = jnp.mean(value, axis=-1, keepdims=True)
    centred = value - average
    variance = jnp.mean(centred * centred, axis=-1, keepdims=True)
    inverse = lax.rsqrt(variance + norm_eps)
    normed = centred * inverse
    return normed * gain + shift, normed, inverse


def norm_back(upstream, normed, inverse, gain):
    scaled = upstream * gain
    inner = (
        scaled
        - jnp.mean(scaled, axis=-1, keepdims=True)
        - normed * jnp.mean(scaled * normed, axis=-1, keepdims=True)
    )
    return inner * inverse


def slot_table(owners):
    repeat = FF // D
    tile_matrix = jnp.array([0, 1, 2, 3] + [4] * repeat + [5] * repeat, dtype=jnp.int32)
    choose = (tile_matrix[:, None] == jnp.arange(7, dtype=jnp.int32)[None, :]).astype(jnp.int32)
    tile_owner = jnp.sum(choose * owners[None, :], axis=1)
    position = jnp.arange(tile_matrix.shape[0], dtype=jnp.int32)
    before = (tile_owner[None, :] == tile_owner[:, None]) & (position[None, :] < position[:, None])
    slot_index = jnp.sum(before.astype(jnp.int32), axis=1)
    return (tile_owner, slot_index)


def adam_update(grad, param, first, second, occupied, decay_rate):
    first_new = occupied * (beta_one * first + (1.0 - beta_one) * grad)
    second_new = occupied * (beta_two * second + (1.0 - beta_two) * grad * grad)
    correct_one = 1.0 - beta_one**ADAM_STEP
    correct_two = 1.0 - beta_two**ADAM_STEP
    direction = first_new / correct_one / (jnp.sqrt(second_new / correct_two) + adam_eps)
    param_new = occupied * (param - learn_rate * (direction + decay_rate * param))
    return (param_new, first_new, second_new)


def head_keys(keys, half, start, length):
    lane = lax.broadcasted_iota(jnp.int32, keys.shape, 1)
    row = lax.broadcasted_iota(jnp.int32, keys.shape, 0)
    bias = jnp.where(start + row < length, 0.0, masked_score).astype(f32)
    extra = jnp.where(lane == (1 - half) * HEAD_DIM, bias, 0.0)
    return jnp.where(lane // HEAD_DIM == half, keys.astype(f32), extra).astype(bf16)


def head_half(rows, half):
    lane = lax.broadcasted_iota(jnp.int32, rows.shape, 1)
    return jnp.where(lane // HEAD_DIM == half, rows, jnp.zeros_like(rows))


def head_queries(rows, half):
    lane = lax.broadcasted_iota(jnp.int32, rows.shape, 1)
    scaled = rows.astype(f32) * HEAD_DIM ** (-0.5)
    extra = jnp.where(lane == (1 - half) * HEAD_DIM, 1.0, 0.0)
    return jnp.where(lane // HEAD_DIM == half, scaled, extra).astype(bf16)


def peer_of(bit, turn):
    device, z = lax.axis_index("dp"), lax.axis_index("tensor")
    for one in (1, 2, 4):
        if bit & one:
            device = device + one - 2 * one * ((device // one) % 2)
    if turn == 1:
        z = z + 1 - 2 * (z % 2)
    elif turn == 2:
        z = z + 2 - 4 * (z // 2)
    elif turn == 3:
        z = 3 - z
    return (device, z)


def greet(peers):
    barrier = pltpu.get_barrier_semaphore()
    for peer in peers:
        pl.semaphore_signal(barrier, inc=1, device_id=peer, device_id_type=pl.DeviceIdType.MESH)
    pl.semaphore_wait(barrier, len(peers))


def sender(send_sems, recv_sems):
    def send(source, target, k, peer):
        return pltpu.make_async_remote_copy(
            source, target, send_sems.at[k], recv_sems.at[k], device_id=peer,
            device_id_type=pl.DeviceIdType.MESH,
        )

    return send


def bits():
    device = lax.axis_index("dp")
    return (device // 4) % 2, (device // 2) % 2, device % 2


def block_of(y, x, c):
    return 4 * y + 2 * x + c


def row_block(index, count=1):
    rows = D // SHARE
    return pl.ds(pl.multiple_of(index * rows, rows), count * rows)


class Gather:
    def __init__(self, send, view, first_sem, x_first):
        self.send, self.view, self.sem = send, view, first_sem
        self.y, self.x, self.c = bits()
        self.one, self.two = (2, 4) if x_first else (4, 2)

    def block(self, turn):
        y, x, c = self.y, self.x, self.c
        y = 1 - y if turn & 4 else y
        x = 1 - x if turn & 2 else x
        c = 1 - c if turn & 1 else c
        return block_of(y, x, c)

    def copy(self, turn, over, k):
        place = self.view(self.block(turn))
        return self.send(place, place, self.sem + k, peer_of(over, 0))

    def start(self):
        self.copy(0, self.one, 0).start()
        self.copy(0, self.two, 1).start()
        self.copy(0, 1, 3).start()

    def relay(self):
        self.copy(0, self.one, 0).wait()
        self.copy(self.one, self.two, 2).start()
        self.copy(self.one, 1, 4).start()
        self.copy(0, self.two, 1).wait()
        self.copy(self.two, 1, 5).start()

    def last(self):
        self.copy(self.one, self.two, 2).wait()
        self.copy(6, 1, 6).start()

    def finish(self):
        for turn, k in ((0, 3), (self.one, 4), (self.two, 5), (6, 6)):
            self.copy(turn, 1, k).wait()


GATHER_SEMS = 7


class RowSums:
    def __init__(self, send, ref, place, height, got_one, got_two, first_sem):
        self.send, self.ref, self.place, self.height = send, ref, place, height
        self.got_one, self.got_two, self.sem = got_one, got_two, first_sem
        self.y, self.x, _ = bits()
        self.half = ref.shape[-1] // 2

    def at(self, y, x, side):
        rows = pl.ds(pl.multiple_of(self.place(y, x), 128), self.height)
        return (rows, slice(side * self.half, (side + 1) * self.half))

    def pairs(self, k, mine):
        y, x = self.y, self.x
        return [
            (y if mine else 1 - y, k, 0),
            (k, x if mine else 1 - x, 1),
        ]

    def first(self, k, side):
        y, x, _ = self.pairs(k, False)[side]
        return self.send(
            self.ref.at[self.at(y, x, side)], self.got_one.at[side, k], self.sem + 2 * side + k,
            peer_of((4, 2)[side], 0),
        )

    def second(self, side):
        y, x = ((self.y, 1 - self.x), (1 - self.y, self.x))[side]
        return self.send(
            self.ref.at[self.at(y, x, side)], self.got_two.at[side], self.sem + 4 + side,
            peer_of((2, 4)[side], 0),
        )

    def start(self):
        for side in range(2):
            for k in range(2):
                self.first(k, side).start()

    def relay(self):
        for side in range(2):
            for k in range(2):
                self.first(k, side).wait()
        for side in range(2):
            for k in range(2):
                y, x, _ = self.pairs(k, True)[side]
                at = self.at(y, x, side)
                self.ref[at] = (
                    self.ref[at].astype(f32) + self.got_one[side, k].astype(f32)
                ).astype(bf16)
        for side in range(2):
            self.second(side).start()

    def finish(self):
        for side in range(2):
            self.second(side).wait()
            at = self.at(self.y, self.x, side)
            self.ref[at] = (
                self.ref[at].astype(f32) + self.got_two[side].astype(f32)
            ).astype(bf16)


ROW_SEMS = 6


def start_body(
    lengths, tokens_ref, weights_ref,
    gathered_ref, mixed_ref, context_ref, parts_ref, lse_ref, heads_ref, out_ref, length_ref, up_ref, down_ref,
    keys, values, length_buf, out_here, out_far, local_sems, send_sems, recv_sems,
):
    chunks, rows, _ = gathered_ref.shape
    width = context_ref.shape[-1]
    lanes = up_ref.shape[-1]
    hidden_width = SHARE * lanes
    piece = rows // 4
    quarter_rows = D // 4
    y, x, c = bits()
    z = lax.axis_index("tensor")
    matched = c == z // 2
    unmatched = jnp.logical_not(matched)
    own_block = block_of(y, x, c)
    send = sender(send_sems, recv_sems)
    core, near_z, diagonal, swapped = peer_of(1, 0), peer_of(0, 1), peer_of(1, 1), peer_of(1, 2)
    across_x, across_y, across_xy = peer_of(2, 0), peer_of(4, 0), peer_of(6, 0)

    def part_of(k):
        return slice(k * piece, (k + 1) * piece)

    def swap_copy(k):
        return send(tokens_ref.at[part_of(k), :], gathered_ref.at[0, part_of(k), :], k, swapped)

    def far_copy(k, source):
        return send(source.at[part_of(k), :], gathered_ref.at[2, part_of(k), :], 4 + k, near_z)

    def near_copy(k, source):
        return send(source.at[part_of(k), :], gathered_ref.at[1, part_of(k), :], 8 + k, core)

    def diagonal_copy(k):
        return send(gathered_ref.at[2, part_of(k), :], gathered_ref.at[3, part_of(k), :], 12 + k, core)

    column = 2 * y + x

    def quarter(k):
        return pl.ds(pl.multiple_of(k * quarter_rows, quarter_rows), quarter_rows)

    def heads_swap():
        return send(
            weights_ref.at[quarter(column), : 3 * width], heads_ref.at[quarter(column), :], 16, swapped
        )

    def heads_share(k, peer):
        return send(heads_ref.at[quarter(column), :], heads_ref.at[quarter(column), :], 17 + k, peer)

    heads_peers = (across_x, across_y, across_xy)
    heads_local = pltpu.make_async_copy(weights_ref.at[:, : 3 * width], heads_ref, local_sems.at[0])

    def out_copy(e):
        return send(out_here, out_far.at[e - 1], 19 + e, peer_of(0, e))

    out_local = pltpu.make_async_copy(
        weights_ref.at[row_block(own_block), 3 * width : 4 * width], out_here, local_sems.at[1]
    )
    outs = [
        Gather(
            send, lambda k, side=side: out_ref.at[row_block(k), side * 2 * width : (side + 1) * 2 * width],
            23 + side * GATHER_SEMS, side == 0,
        )
        for side in range(2)
    ]
    base = 23 + 2 * GATHER_SEMS
    targets = (up_ref, down_ref)

    def feed_source(kind):
        at = 4 * width + kind * hidden_width + own_block * lanes
        return weights_ref.at[:, pl.ds(pl.multiple_of(at, 128), lanes)]

    def feed_copy(kind, e):
        return send(feed_source(kind), targets[kind].at[e - 1, 0, 0], base + 3 * kind + e - 1, peer_of(0, e))

    half = slice(0, D // 2), slice(D // 2, D)

    def feed_one(kind, e, side):
        source = targets[kind].at[e - 1, 0, 0, half[side], :]
        target = targets[kind].at[e - 1, side, 1 - side, half[side], :]
        return send(
            source, target, base + 6 + 6 * kind + 2 * (e - 1) + side, (across_x, across_y)[side]
        )

    def feed_two(e, side):
        if side == 0:
            source, target = (up_ref.at[e - 1, dy, 0:2, half[0], :] for dy in range(2))
        else:
            source, target = (up_ref.at[e - 1, 0:2, dx, half[1], :] for dx in range(2))
        return send(source, target, base + 18 + 2 * (e - 1) + side, (across_y, across_x)[side])

    def first_hop(kind, e):
        feed_copy(kind, e).wait()
        for side in range(2):
            feed_one(kind, e, side).start()

    def second_hop(e):
        for side in range(2):
            feed_one(0, e, side).wait()
        for side in range(2):
            feed_two(e, side).start()

    def length_copy():
        return send(length_buf.at[0], length_buf.at[1], base + 24, core)

    def part_copy(j):
        return send(
            context_ref.at[j], parts_ref.at[j], base + 24 + j, (None, core, near_z, diagonal)[j]
        )

    def send_weights():
        for e in (3, 2, 1):
            feed_copy(0, e).start()
        for e in (3, 2, 1):
            feed_copy(1, e).start()

    out_local.start()
    length_buf[0] = jnp.full(length_buf.shape[1:], lengths[0], jnp.int32)
    greet(
        [core, near_z, diagonal, swapped, across_x, across_y, across_xy, peer_of(0, 2), peer_of(0, 3)]
    )

    @pl.when(matched)
    def _():
        for k in range(4):
            far_copy(k, tokens_ref).start()
            near_copy(k, tokens_ref).start()
        heads_local.start()
        gathered_ref[0] = tokens_ref[...]

    @pl.when(unmatched)
    def _():
        for k in range(4):
            swap_copy(k).start()
        heads_swap().start()

    length_copy().start()

    @pl.when(unmatched)
    def _():
        for k in range(4):
            swap_copy(k).wait()
            far_copy(k, gathered_ref.at[0]).start()
            near_copy(k, gathered_ref.at[0]).start()
        heads_swap().wait()
        for k, peer in enumerate(heads_peers):
            heads_share(k, peer).start()

    for k in range(4):
        far_copy(k, tokens_ref).wait()
        diagonal_copy(k).start()
    out_local.wait()
    for e in (1, 2, 3):
        out_copy(e).start()
    send_weights()
    out_ref[row_block(own_block), :width] = out_here[...]

    @pl.when(matched)
    def _():
        heads_local.wait()

    @pl.when(unmatched)
    def _():
        for k, peer in enumerate(heads_peers):
            heads_share(k, peer).wait()

    length_copy().wait()
    length_ref[...] = jnp.where(matched, length_buf[0], length_buf[1])
    length = length_ref[:1, :]
    own_quarter = jnp.where(matched, z, z + 2 - 4 * (z // 2))
    wide = 256

    def project(j):
        def columns(n, carry):
            at = pl.ds(pl.multiple_of(n * wide, wide), wide)
            mixed_ref[j, :, at] = jnp.dot(
                gathered_ref[j], heads_ref[:, at], preferred_element_type=f32
            ).astype(bf16)
            return carry

        lax.fori_loop(0, 3 * width // wide, columns, 0)

    def arrange(j):
        at_quarter = own_quarter
        if j in (1, 3):
            at_quarter = at_quarter + 2 - 4 * (at_quarter // 2)
        if j in (2, 3):
            at_quarter = at_quarter + 1 - 2 * (at_quarter % 2)
        for h in range(width // HEAD_DIM):
            at = width + (h // 2) * 128
            keys[h, j * rows : (j + 1) * rows, :] = head_keys(
                mixed_ref[j, :, at : at + 128], h % 2, at_quarter * rows, length
            )
        values[j * rows : (j + 1) * rows, :] = mixed_ref[j, :, 2 * width :]

    for j in (0, 2, 1, 3):
        if j == 1:
            for k in range(4):
                near_copy(k, tokens_ref).wait()
        if j == 3:
            for k in range(4):
                diagonal_copy(k).wait()
        project(j)
        arrange(j)

    lane = lax.broadcasted_iota(jnp.int32, (rows, 128), 1)

    def attend(step, carry):
        chunk = chunks - 1 - step
        logs = jnp.zeros((rows, 128), f32)
        for pair in range(width // 128):
            queries = mixed_ref[chunk, :, pair * 128 : pair * 128 + 128]
            both = []
            for side in range(2):
                h = pair * 2 + side
                scores = contract(head_queries(queries, side), keys[h], 1, 1)
                top = jnp.max(scores, axis=1, keepdims=True)
                weight = jnp.exp(scores - top)
                total = jnp.sum(weight, axis=1, keepdims=True)
                out = contract(weight.astype(bf16), values[:, pair * 128 : pair * 128 + 128], 1, 0)
                both.append(out / total)
                logs = jnp.where(lane == h, top + jnp.log(total), logs)
            context_ref[chunk, :, pair * 128 : pair * 128 + 128] = jnp.where(
                lane < HEAD_DIM, both[0], both[1]
            ).astype(bf16)
        lse_ref[chunk] = jnp.transpose(logs)[:8, :]

        @pl.when(step == 0)
        def _():
            part_copy(3).start()
            for e in (1, 2, 3):
                out_copy(e).wait()
                out_ref[row_block(own_block), e * width : (e + 1) * width] = out_far[e - 1]
            for gather in outs:
                gather.start()
            first_hop(0, 3)

        @pl.when(step == 1)
        def _():
            part_copy(2).start()
            for gather in outs:
                gather.relay()
            first_hop(0, 2)
            second_hop(3)

        @pl.when(step == 2)
        def _():
            part_copy(1).start()
            for gather in outs:
                gather.last()
            first_hop(0, 1)
            second_hop(2)

        return carry

    lax.fori_loop(0, chunks, attend, 0)
    parts_ref[0] = context_ref[0]
    for gather in outs:
        gather.finish()
    second_hop(1)
    for e in (3, 2, 1):
        first_hop(1, e)
    for j in (3, 2, 1):
        part_copy(j).wait()
    for e in (3, 2, 1):
        for side in range(2):
            feed_two(e, side).wait()
            feed_one(1, e, side).wait()


def start_block(lengths, tokens, weights):
    rows = tokens.shape[0]
    chunks = 4
    tile = D // 4
    seq = chunks * rows
    lanes = FF // 4 // SHARE
    heads = tile // HEAD_DIM
    sems = 23 + 2 * GATHER_SEMS + 28
    share_rows = D // SHARE
    vmem, anywhere = pl.BlockSpec(memory_space=pltpu.VMEM), pl.BlockSpec(memory_space=pl.ANY)
    return pl.pallas_call(
        start_body,
        name="start_block",
        in_specs=[pl.BlockSpec(memory_space=pltpu.SMEM), vmem, anywhere],
        out_specs=[vmem] * 8 + [anywhere] * 2,
        out_shape=[
            jax.ShapeDtypeStruct((chunks, rows, D), bf16),
            jax.ShapeDtypeStruct((chunks, rows, 3 * tile), bf16),
            jax.ShapeDtypeStruct((chunks, rows, tile), bf16),
            jax.ShapeDtypeStruct((chunks, rows, tile), bf16),
            jax.ShapeDtypeStruct((chunks, 8, rows), f32),
            jax.ShapeDtypeStruct((D, 3 * tile), bf16),
            jax.ShapeDtypeStruct((D, D), bf16),
            jax.ShapeDtypeStruct((8, 128), jnp.int32),
            jax.ShapeDtypeStruct((3, 2, 2, D, lanes), bf16),
            jax.ShapeDtypeStruct((3, 2, 2, D, lanes), bf16),
        ],
        scratch_shapes=[
            pltpu.VMEM((heads, seq, 128), bf16),
            pltpu.VMEM((seq, tile), bf16),
            pltpu.VMEM((2, 8, 128), jnp.int32),
            pltpu.VMEM((share_rows, tile), bf16),
            pltpu.VMEM((3, share_rows, tile), bf16),
            pltpu.SemaphoreType.DMA((2,)),
            pltpu.SemaphoreType.DMA((sems,)),
            pltpu.SemaphoreType.DMA((sems,)),
        ],
        compiler_params=pltpu.CompilerParams(
            vmem_limit_bytes=60 << 20, collective_id=0, has_side_effects=True
        ),
        cost_estimate=pl.CostEstimate(
            flops=24 * heads * seq * seq * HEAD_DIM, bytes_accessed=20 << 20, transcendentals=0
        ),
    )(lengths, tokens, weights)


def back_body(
    info, mixed_ref, context_ref, upstream_ref, lse_ref, weight_ref, branch_ref, norm_ref, outputs_ref, gathered,
    up_grads, down_grads, out_grads,
    input_ref, outputs_out, norm_out, attention_out, feed_out,
    keys, turned, key_sum, value_sum, query_t, grad, rows_held, heads_sum, kept, got_one, got_two, got_three,
    leaving, landed, share, heads, heads_one, heads_two, heads_mine, heads_far, out_held, out_core, out_one, out_two, out_z,
    norm_here, norm_there, local_sems, send_sems, recv_sems,
):
    chunks, rows, _ = mixed_ref.shape
    width = context_ref.shape[-1]
    scale = HEAD_DIM ** (-0.5)
    part = 256
    core, near_z = peer_of(1, 0), peer_of(0, 1)
    across = (peer_of(2, 0), peer_of(4, 0))
    send = sender(send_sems, recv_sems)
    sources = (up_grads, down_grads)
    y, x, c = bits()
    z = lax.axis_index("tensor")
    matched = c == z // 2
    own_block = block_of(y, x, c)

    def stage_one(b, kind):
        return send(sources[kind].at[b, 1], got_one.at[b, kind], 2 * b + kind, across[kind])

    def stage_two(b, kind):
        return send(kept.at[b, kind, 1], got_two.at[b, kind], 8 + 2 * b + kind, across[1 - kind])

    def stage_three(b):
        return send(kept.at[b, :, 0], got_three.at[b - 1], 15 + b, peer_of(0, b))

    def load(b, kind):
        return pltpu.make_async_copy(
            sources[kind].at[b, 0], kept.at[b, kind], local_sems.at[2 * b + kind]
        )

    def start_one(b):
        for kind in range(2):
            stage_one(b, kind).start()

    def start_two(b):
        for kind in range(2):
            load(b, kind).wait()
            stage_one(b, kind).wait()
            for k in (1, 0):
                kept[b, kind, k] = (
                    kept[b, kind, k].astype(f32) + got_one[b, kind, k].astype(f32)
                ).astype(bf16)
        for kind in range(2):
            stage_two(b, kind).start()

    def start_three(b):
        for kind in range(2):
            stage_two(b, kind).wait()
            kept[b, kind, 0] = (
                kept[b, kind, 0].astype(f32) + got_two[b, kind].astype(f32)
            ).astype(bf16)
        if b:
            stage_three(b).start()

    def load_rows(j):
        return pltpu.make_async_copy(gathered.at[j], rows_held.at[j], local_sems.at[8 + j])

    def out_load():
        return pltpu.make_async_copy(out_grads, out_held, local_sems.at[12])

    def out_core_copy(k):
        at = row_block(block_of(k // 2, k % 2, 1 - c))
        return send(out_grads.at[at, :], out_core.at[k], 22 + k, core)

    out_sums = RowSums(
        send, out_held, lambda yy, xx: block_of(yy, xx, c) * 128, 128, out_one, out_two, 26
    )

    def out_z_copy(e):
        at = (row_block(own_block), slice(e * width, (e + 1) * width))
        return send(out_held.at[at], out_z.at[e - 1], 31 + e, peer_of(0, e))

    def out_start():
        out_load().wait()
        for k in range(4):
            out_core_copy(k).wait()
        for k in range(4):
            at = row_block(block_of(k // 2, k % 2, c))
            out_held[at, :] = (out_held[at, :].astype(f32) + out_core[k].astype(f32)).astype(bf16)
        out_sums.start()

    def out_last():
        out_sums.finish()
        for e in (1, 2, 3):
            out_z_copy(e).start()

    norm_turns = ((1, 0), (2, 0), (4, 0), (0, 1), (0, 2))

    def norm_copy(k):
        return send(norm_here.at[k], norm_there.at[k], 35 + k, peer_of(*norm_turns[k]))

    def norm_step(k):
        norm_copy(k).wait()
        total = norm_here[k] + norm_there[k]
        if k + 1 < len(norm_turns):
            norm_here[k + 1] = total
            norm_copy(k + 1).start()
        else:
            norm_out[...] = total

    for b in (3, 2, 1, 0):
        for kind in range(2):
            load(b, kind).start()
    for j in range(chunks):
        load_rows(j).start()
    out_load().start()
    norm_here[0] = norm_ref[...]
    greet([core, near_z, across[0], across[1], peer_of(0, 2), peer_of(0, 3), peer_of(1, 2)])
    for k in range(4):
        out_core_copy(k).start()
    norm_copy(0).start()
    start_one(3)
    start_one(2)

    def return_copy(source, target, k):
        return send(source, target, 49 + 4 * GATHER_SEMS + k, peer_of(1, 2))

    outputs_local = pltpu.make_async_copy(outputs_ref, outputs_out, local_sems.at[15])

    @pl.when(matched)
    def _():
        outputs_local.start()

    @pl.when(jnp.logical_not(matched))
    def _():
        return_copy(outputs_ref, outputs_out, 0).start()

    key_sum[...] = jnp.zeros_like(key_sum)
    value_sum[...] = jnp.zeros_like(value_sum)
    for j in range(chunks):
        for h in range(width // HEAD_DIM):
            at = width + (h // 2) * 128
            keys[h, j * rows : (j + 1) * rows, :] = head_keys(
                mixed_ref[j, :, at : at + 128], h % 2, info[1 + j], info[0]
            )
        turned[:, j * rows : (j + 1) * rows] = jnp.transpose(
            mixed_ref[j, :, width : 2 * width].astype(f32)
        ).astype(bf16)
    feature = lax.broadcasted_iota(jnp.int32, (8, width), 1) // HEAD_DIM
    picks = (feature == lax.broadcasted_iota(jnp.int32, (8, width), 0)).astype(f32)
    per_chunk = rows // part

    def attend(step, carry):
        chunk = step // per_chunk
        at = pl.ds(pl.multiple_of((step % per_chunk) * part, part), part)
        upstream = upstream_ref[chunk, at, :]
        product = upstream.astype(f32) * context_ref[chunk, at, :].astype(f32)
        delta = lax.dot_general(
            picks, product, (((1,), (1,)), ((), ())), precision=lax.Precision.HIGHEST,
            preferred_element_type=f32,
        )
        lse = lse_ref[chunk, :, at]
        for pair in range(width // 128):
            lanes = slice(pair * 128, pair * 128 + 128)
            queries = mixed_ref[chunk, at, lanes]
            value_rows = mixed_ref[:, :, 2 * width + pair * 128 : 2 * width + pair * 128 + 128]
            value_rows = value_rows.reshape(chunks * rows, 128)
            for half in range(2):
                h = pair * 2 + half
                scores = contract(keys[h], head_queries(queries, half), 1, 1)
                weight = jnp.exp(scores - lse[h : h + 1, :])
                up_half = head_half(upstream[:, lanes], half)
                back = contract(value_rows, up_half, 1, 1)
                score_grad = (weight * (back - delta[h : h + 1, :])).astype(bf16)
                value_sum[pair] += contract(weight.astype(bf16), up_half, 1, 0)
                key_sum[pair] += contract(score_grad, head_half(queries, half), 1, 0)
                query_t[h * HEAD_DIM : (h + 1) * HEAD_DIM, :] = (
                    contract(turned[h * HEAD_DIM : (h + 1) * HEAD_DIM, :], score_grad, 1, 0) * scale
                )
        grad[chunk, at, :width] = jnp.transpose(query_t[...]).astype(bf16)

        @pl.when(step == 0)
        def _():
            norm_step(0)
            out_start()

        @pl.when(step == 1)
        def _():
            norm_step(1)
            start_two(3)
            start_one(1)

        @pl.when(step == 2)
        def _():
            norm_step(2)
            out_sums.relay()

        @pl.when(step == 3)
        def _():
            norm_step(3)
            start_two(2)
            start_one(0)
            start_three(3)

        @pl.when(step == 4)
        def _():
            norm_step(4)
            out_last()

        @pl.when(step == 6)
        def _():
            start_two(1)

        return carry

    lax.fori_loop(0, chunks * per_chunk, attend, 0)
    for j in range(chunks):
        at = slice(j * rows, (j + 1) * rows)
        for pair in range(width // 128):
            left = width + pair * 128
            grad[j, :, left : left + 128] = (key_sum[pair, at, :] * scale).astype(bf16)
            grad[j, :, left + width : left + width + 128] = value_sum[pair, at, :].astype(bf16)
    start_three(2)

    def rows_back(j):
        return contract(grad[j], weight_ref[...], 1, 1)

    core_copies = {}
    for k, j in enumerate((3, 1)):
        leaving[k] = rows_back(j).astype(bf16)
        core_copies[j] = send(leaving.at[k], landed.at[k], 19 + k, core)
        core_copies[j].start()
    far = rows_back(2)
    core_copies[3].wait()
    leaving[2] = (far + landed[0].astype(f32)).astype(bf16)
    far_copy = send(leaving.at[2], landed.at[2], 21, near_z)
    branch_ref_value = branch_ref[...] + rows_back(0)
    core_copies[1].wait()
    own_rows = branch_ref_value + landed[1].astype(f32)

    heads_sum[...] = jnp.zeros_like(heads_sum)
    for j in range(chunks):
        load_rows(j).wait()

    def weigh(j, carry):
        heads_sum[...] += contract(rows_held[j], grad[j], 0, 0)
        return carry

    lax.fori_loop(0, chunks, weigh, 0)
    heads[...] = heads_sum[...].astype(bf16)
    head_sums = RowSums(
        send, heads, lambda yy, xx: block_of(yy, xx, 0) * 128, 256, heads_one, heads_two, 40
    )
    head_sums.start()
    start_three(1)
    far_copy.start()
    start_two(0)
    head_sums.relay()
    start_three(0)
    head_sums.finish()

    def half_rows(k):
        return row_block(block_of(y, x, k))

    @pl.when(matched)
    def _():
        send(heads.at[half_rows(1 - c), :], heads_mine, 46, core).start()

    @pl.when(jnp.logical_not(matched))
    def _():
        send(heads.at[half_rows(c), :], heads_far, 47, peer_of(0, 2)).start()
        send(heads.at[half_rows(1 - c), :], heads_far, 48, peer_of(1, 2)).start()

    total = kept[0, :, 0].astype(f32)
    for b in (3, 2, 1):
        stage_three(b).wait()
        total = total + got_three[b - 1].astype(f32)
    share[...] = total.astype(bf16)
    own_feed = [
        pltpu.make_async_copy(share.at[kind], feed_out.at[own_block, kind], local_sems.at[13 + kind])
        for kind in range(2)
    ]
    for copy in own_feed:
        copy.start()
    feeds = [
        Gather(send, lambda k, kind=kind: feed_out.at[k, kind], 49 + kind * GATHER_SEMS, kind == 0)
        for kind in range(2)
    ]
    for copy in own_feed:
        copy.wait()
    for feed in feeds:
        feed.start()
    sum_out = out_held[row_block(own_block), :width].astype(f32)
    for e in (1, 2, 3):
        out_z_copy(e).wait()
        sum_out = sum_out + out_z[e - 1].astype(f32)
    attention_out[row_block(own_block), 3 * width :] = sum_out.astype(bf16)

    @pl.when(matched)
    def _():
        send(heads.at[half_rows(1 - c), :], heads_mine, 46, core).wait_send()
        heads_mine[...] = heads[half_rows(c), :]

    @pl.when(jnp.logical_not(matched))
    def _():
        send(heads.at[half_rows(c), :], heads_far, 47, peer_of(0, 2)).wait_send()
        send(heads.at[half_rows(1 - c), :], heads_far, 48, peer_of(1, 2)).wait_send()
        send(heads.at[half_rows(c), :], heads_mine, 46, core).wait_recv()

    @pl.when(matched)
    def _():
        send(heads.at[half_rows(c), :], heads_far, 47, peer_of(0, 2)).wait_recv()

    @pl.when(jnp.logical_not(matched))
    def _():
        send(heads.at[half_rows(c), :], heads_far, 48, peer_of(1, 2)).wait_recv()

    attention_out[row_block(own_block), : 3 * width] = (
        heads_mine[...].astype(f32) + heads_far[...].astype(f32)
    ).astype(bf16)
    sides = [
        Gather(
            send,
            lambda k, side=side: attention_out.at[row_block(k), side * 2 * width : (side + 1) * 2 * width],
            49 + (2 + side) * GATHER_SEMS, side == 0,
        )
        for side in range(2)
    ]
    for side in sides:
        side.start()
    far_copy.wait()
    input_ref[...] = (own_rows + landed[2].astype(f32)).astype(bf16)
    for gather in feeds + sides:
        gather.relay()
    for gather in feeds + sides:
        gather.last()
    for gather in feeds + sides:
        gather.finish()
    @pl.when(matched)
    def _():
        outputs_local.wait()

    @pl.when(jnp.logical_not(matched))
    def _():
        return_copy(outputs_ref, outputs_out, 0).wait()


def back_block(info, mixed, context, upstream, lse, weight, branch, norm_sums, outputs, gathered, up_grads,
               down_grads, out_grads):
    chunks, rows, width3 = mixed.shape
    width = width3 // 3
    seq = chunks * rows
    heads = width // HEAD_DIM
    lanes = up_grads.shape[-1]
    share_rows = D // SHARE
    sems = 51 + 4 * GATHER_SEMS
    vmem, anywhere = pl.BlockSpec(memory_space=pltpu.VMEM), pl.BlockSpec(memory_space=pl.ANY)
    return pl.pallas_call(
        back_body,
        name="back_block",
        in_specs=[pl.BlockSpec(memory_space=pltpu.SMEM)] + [vmem] * 7 + [anywhere] * 5,
        out_specs=[vmem, vmem, vmem, vmem, anywhere],
        out_shape=[
            jax.ShapeDtypeStruct((rows, D), bf16),
            jax.ShapeDtypeStruct((rows, D), bf16),
            jax.ShapeDtypeStruct((4, D), f32),
            jax.ShapeDtypeStruct((D, 4 * width), bf16),
            jax.ShapeDtypeStruct((SHARE, 2, D, lanes), bf16),
        ],
        scratch_shapes=[
            pltpu.VMEM((heads, seq, 128), bf16),
            pltpu.VMEM((width, seq), bf16),
            pltpu.VMEM((width // 128, seq, 128), f32),
            pltpu.VMEM((width // 128, seq, 128), f32),
            pltpu.VMEM((width, 256), f32),
            pltpu.VMEM((chunks, rows, width3), bf16),
            pltpu.VMEM((chunks, rows, D), bf16),
            pltpu.VMEM((D, width3), f32),
            pltpu.VMEM((4, 2, 2, D, lanes), bf16),
            pltpu.VMEM((4, 2, 2, D, lanes), bf16),
            pltpu.VMEM((4, 2, D, lanes), bf16),
            pltpu.VMEM((3, 2, D, lanes), bf16),
            pltpu.VMEM((3, rows, D), bf16),
            pltpu.VMEM((3, rows, D), bf16),
            pltpu.VMEM((2, D, lanes), bf16),
            pltpu.VMEM((D, width3), bf16),
            pltpu.VMEM((2, 2, 2 * share_rows, width3 // 2), bf16),
            pltpu.VMEM((2, 2 * share_rows, width3 // 2), bf16),
            pltpu.VMEM((share_rows, width3), bf16),
            pltpu.VMEM((share_rows, width3), bf16),
            pltpu.VMEM((D, 4 * width), bf16),
            pltpu.VMEM((4, share_rows, 4 * width), bf16),
            pltpu.VMEM((2, 2, share_rows, 2 * width), bf16),
            pltpu.VMEM((2, share_rows, 2 * width), bf16),
            pltpu.VMEM((3, share_rows, width), bf16),
            pltpu.VMEM((5, 4, D), f32),
            pltpu.VMEM((5, 4, D), f32),
            pltpu.SemaphoreType.DMA((16,)),
            pltpu.SemaphoreType.DMA((sems,)),
            pltpu.SemaphoreType.DMA((sems,)),
        ],
        compiler_params=pltpu.CompilerParams(
            vmem_limit_bytes=67043328, collective_id=2, has_side_effects=True
        ),
        cost_estimate=pl.CostEstimate(
            flops=40 * heads * seq * seq * HEAD_DIM, bytes_accessed=40 << 20, transcendentals=0
        ),
    )(
        info, mixed, context, upstream, lse, weight, branch, norm_sums, outputs, gathered, up_grads, down_grads,
        out_grads,
    )


def adam_body(owned, attention_ref, feed_ref, master_ref, one_ref, two_ref,
              grad_out, master_out, one_out, two_out, tiles_out, up_out, down_out):
    tile = grad_out.shape[-1] // 4
    for s in range(4):
        at = slice(s * tile, (s + 1) * tile)
        grad = jnp.zeros((grad_out.shape[0], tile), f32)
        for i in range(4):
            value = attention_ref[:, i * tile : (i + 1) * tile].astype(f32)
            grad = jnp.where(owned[s, i] > 0, value, grad)
        for kind in range(2):
            value = jnp.concatenate([feed_ref[2 * s + k, kind] for k in range(2)], axis=-1)
            grad = jnp.where(owned[s, 4 + 4 * kind + s] > 0, value.astype(f32), grad)
        occupied = (owned[s, 12] > 0).astype(f32)
        param, first, second = adam_update(
            grad, master_ref[:, at], one_ref[:, at], two_ref[:, at], occupied, weight_decay
        )
        grad_out[:, at] = grad
        master_out[:, at] = param
        one_out[:, at] = first
        two_out[:, at] = second
        low = param.astype(bf16)
        none = jnp.zeros_like(low)
        for i in range(4):
            mine = jnp.where(owned[s, i] > 0, low, none)
            there = slice(i * tile, (i + 1) * tile)
            tiles_out[:, there] = mine if s == 0 else tiles_out[:, there] + mine
        for kind, target in ((0, up_out), (1, down_out)):
            mine = jnp.where(owned[s, 4 + 4 * kind + s] > 0, low, none)
            for k in range(2):
                target[2 * s + k] = mine[:, k * tile // 2 : (k + 1) * tile // 2]


def adam_block(owned, attention_grad, feed_grad, master, one, two):
    part = 64
    wide = pl.BlockSpec((part, D), lambda i: (i, 0))
    lanes = feed_grad.shape[-1]
    split = pl.BlockSpec((SHARE, part, lanes), lambda i: (0, i, 0))
    return pl.pallas_call(
        adam_body,
        grid=(D // part,),
        name="adam_block",
        in_specs=[
            pl.BlockSpec(memory_space=pltpu.SMEM), wide,
            pl.BlockSpec((SHARE, 2, part, lanes), lambda i: (0, 0, i, 0)), wide, wide, wide,
        ],
        out_specs=[wide] * 5 + [split] * 2,
        out_shape=[jax.ShapeDtypeStruct((D, D), f32)] * 4
        + [jax.ShapeDtypeStruct((D, D), bf16)]
        + [jax.ShapeDtypeStruct((SHARE, D, lanes), bf16)] * 2,
        compiler_params=pltpu.CompilerParams(vmem_limit_bytes=62 << 20),
        cost_estimate=pl.CostEstimate(flops=40 * D * D, bytes_accessed=40 << 20, transcendentals=0),
    )(owned, attention_grad, feed_grad, master, one, two)


def tiles_body(tiles_ref, up_ref, down_ref, input_ref, tiles_out, up_out, down_out, input_out, *scratch):
    core_got = scratch[:3]
    one_got, two_got = scratch[3:5], scratch[5:7]
    work = scratch[7:10]
    row_one, row_two, local_sems, send_sems, recv_sems = scratch[10:]
    matched = lax.axis_index("dp") % 2 == lax.axis_index("tensor") // 2
    send = sender(send_sems, recv_sems)
    y, x, c = bits()
    core = peer_of(1, 0)
    own_block = block_of(y, x, c)
    greet([core, peer_of(2, 0), peer_of(4, 0), peer_of(1, 2)])
    input_local = pltpu.make_async_copy(input_ref, input_out, local_sems.at[0])
    input_swap = send(input_ref, input_out, 24 + 4 * GATHER_SEMS, peer_of(1, 2))

    @pl.when(matched)
    def _():
        input_local.start()

    @pl.when(jnp.logical_not(matched))
    def _():
        input_swap.start()

    arrays = ((up_ref, up_out), (down_ref, down_out), (tiles_ref, tiles_out))

    def place(n, ref, block):
        return ref.at[row_block(block), :] if n == 2 else ref.at[block]

    def core_copy(n, k):
        return send(
            place(n, arrays[n][0], block_of(k // 2, k % 2, 1 - c)), core_got[n].at[k], 4 * n + k, core
        )

    def core_add(n):
        source, target = arrays[n][0], work[n]
        for k in range(4):
            core_copy(n, k).wait()
        for k in range(4):
            block = block_of(k // 2, k % 2, c)
            if n == 2:
                at = row_block(block)
                target[at, :] = source[at, :] + core_got[n][k]
            else:
                target[k] = source[block] + core_got[n][k]

    def first(n, k):
        y_, x_ = ((k, 1 - x), (1 - y, k))[n]
        return send(
            work[n].at[2 * y_ + x_], one_got[n].at[k], 12 + 2 * n + k,
            peer_of((2, 4)[n], 0),
        )

    def second(n):
        y_, x_ = ((1 - y, x), (y, 1 - x))[n]
        return send(
            work[n].at[2 * y_ + x_], two_got[n], 16 + n, peer_of((4, 2)[n], 0)
        )

    def relay(n):
        target = work[n]
        for k in range(2):
            first(n, k).wait()
        for k in range(2):
            y_, x_ = ((k, x), (y, k))[n]
            block = 2 * y_ + x_
            target[block] = target[block] + one_got[n][k]
        second(n).start()

    def settle(n):
        second(n).wait()
        arrays[n][1][own_block] = work[n][2 * y + x] + two_got[n][...]

    for n in range(3):
        for k in range(4):
            core_copy(n, k).start()
    for n in range(2):
        core_add(n)
        for k in range(2):
            first(n, k).start()
    core_add(2)
    rows = RowSums(
        send, work[2], lambda yy, xx: block_of(yy, xx, c) * 128, 128, row_one, row_two, 18
    )
    rows.start()
    for n in range(2):
        relay(n)
    rows.relay()
    gathers = []
    for n in range(2):
        settle(n)
        gathers.append(
            Gather(send, lambda k, n=n: arrays[n][1].at[k], 24 + n * GATHER_SEMS, n == 0)
        )
        gathers[-1].start()
    rows.finish()
    tiles_out[row_block(own_block), :] = work[2][row_block(own_block), :]
    half = tiles_out.shape[-1] // 2
    for side in range(2):
        gathers.append(
            Gather(
                send,
                lambda k, side=side: tiles_out.at[row_block(k), side * half : (side + 1) * half],
                24 + (2 + side) * GATHER_SEMS, side == 0,
            )
        )
        gathers[-1].start()
    for gather in gathers:
        gather.relay()
    for gather in gathers:
        gather.last()
    for gather in gathers:
        gather.finish()

    @pl.when(matched)
    def _():
        input_local.wait()

    @pl.when(jnp.logical_not(matched))
    def _():
        input_swap.wait()


def spread_tiles(tiles, up, down, rows):
    share_rows = D // SHARE
    lanes = up.shape[-1]
    sems = 25 + 4 * GATHER_SEMS
    piece = (D, lanes)
    vmem = pl.BlockSpec(memory_space=pltpu.VMEM)
    return pl.pallas_call(
        tiles_body,
        name="spread_tiles",
        in_specs=[vmem] * 3 + [pl.BlockSpec(memory_space=pl.ANY)],
        out_specs=[vmem] * 4,
        out_shape=[jax.ShapeDtypeStruct(v.shape, bf16) for v in (tiles, up, down, rows)],
        scratch_shapes=[
            pltpu.VMEM((4,) + piece, bf16),
            pltpu.VMEM((4,) + piece, bf16),
            pltpu.VMEM((4, share_rows, D), bf16),
            pltpu.VMEM((2,) + piece, bf16),
            pltpu.VMEM((2,) + piece, bf16),
            pltpu.VMEM(piece, bf16),
            pltpu.VMEM(piece, bf16),
            pltpu.VMEM((4,) + piece, bf16),
            pltpu.VMEM((4,) + piece, bf16),
            pltpu.VMEM((D, D), bf16),
            pltpu.VMEM((2, 2, share_rows, D // 2), bf16),
            pltpu.VMEM((2, share_rows, D // 2), bf16),
            pltpu.SemaphoreType.DMA((1,)),
            pltpu.SemaphoreType.DMA((sems,)),
            pltpu.SemaphoreType.DMA((sems,)),
        ],
        compiler_params=pltpu.CompilerParams(
            vmem_limit_bytes=48 << 20, collective_id=3, has_side_effects=True
        ),
        cost_estimate=pl.CostEstimate(flops=D * D, bytes_accessed=12 << 20, transcendentals=0),
    )(tiles, up, down, rows)


def joined(held, i, kind):
    return jnp.concatenate(
        [held[kind, 2 * (i // 2) + m, i % 2, k] for k in range(2) for m in range(2)], axis=-1
    )


def gelu_parts(value):
    bell = jnp.exp(-0.5 * value * value)
    t = 1.0 / (1.0 + (0.3275911 * 0.5**0.5) * jnp.abs(value))
    tail = 0.5 * 1.061405429
    for c in (-1.453152027, 1.421413741, -0.284496736, 0.254829592):
        tail = tail * t + 0.5 * c
    tail = tail * t * bell
    area = jnp.where(value > 0, 1.0 - tail, tail)
    return value * area, area + value * bell * (0.5 / jnp.pi) ** 0.5


def feed_body(
    info, first_ref, cotangent_ref, norms_ref, weights_ref, up_ref, down_ref,
    out_ref, low_ref, both_ref, hidden_ref, pre_ref, grad_ref, sums_ref,
    held, slope, total, leaving, landed, seed_held, local_sems, send_sems, recv_sems,
):
    rows = first_ref.shape[0]
    steps = hidden_ref.shape[0]
    lanes = held.shape[-1]
    y, x, c = bits()
    peer = peer_of(1, 0)
    send = sender(send_sems, recv_sems)
    half = slice(0, D // 2), slice(D // 2, D)
    loads = []
    for kind in range(2):
        for dy in range(2):
            for dx in range(2):
                block = block_of(1 - y if dy else y, 1 - x if dx else x, c)
                at = D + kind * SHARE * lanes + block * lanes
                loads.append(
                    (weights_ref.at[:, pl.ds(pl.multiple_of(at, 128), lanes)], held.at[kind, 0, dy, dx])
                )
    loads.append((up_ref, held.at[0, 1:4]))
    loads.append((down_ref.at[:, 0, 0:2, half[0], :], held.at[1, 1:4, 0, 0:2, half[0], :]))
    loads.append((down_ref.at[:, 0:2, 0, half[1], :], held.at[1, 1:4, 0:2, 0, half[1], :]))
    loads = [pltpu.make_async_copy(a, b, local_sems.at[k]) for k, (a, b) in enumerate(loads)]
    for load in loads:
        load.start()
    greet([peer, peer_of(2, 0), peer_of(4, 0), peer_of(1, 2)])
    matched = c == lax.axis_index("tensor") // 2
    seed_local = pltpu.make_async_copy(cotangent_ref, seed_held, local_sems.at[len(loads)])
    seed_swap = send(cotangent_ref, seed_held, 6, peer_of(1, 2))
    hops = [
        send(
            down_ref.at[:, 0, 0:2, half[0], :], held.at[1, 1:4, 1, 0:2, half[0], :], 4, peer_of(4, 0)
        ),
        send(
            down_ref.at[:, 0:2, 0, half[1], :], held.at[1, 1:4, 0:2, 1, half[1], :], 5, peer_of(2, 0)
        ),
    ]
    for hop in hops:
        hop.start()

    @pl.when(matched)
    def _():
        seed_local.start()

    @pl.when(jnp.logical_not(matched))
    def _():
        seed_swap.start()

    def across(source, target, k):
        return send(source, target, k, peer)

    middle_row = rows // 2
    both_ref[0] = first_ref[...].astype(bf16)
    first_copy = across(both_ref.at[0], both_ref.at[1], 0)
    first_copy.start()

    def up(i, slot):
        weight = joined(held, i, 0)
        for r in range(0, rows, middle_row):
            at = slice(r, r + middle_row)
            value = jnp.dot(both_ref[slot, at, :], weight, preferred_element_type=f32)
            hidden, steep = gelu_parts(value)
            hidden_ref[i, slot, at, :] = hidden.astype(bf16)
            slope[i, slot, at, :] = steep.astype(bf16)

    def down(i, slot):
        total[slot] += contract(hidden_ref[i, slot], joined(held, i, 1), 1, 1)

    def back(i, slot):
        weight = joined(held, i, 1)
        for r in range(0, rows, middle_row):
            at = slice(r, r + middle_row)
            value = jnp.dot(low_ref[slot, at, :], weight, preferred_element_type=f32)
            pre_ref[i, slot, at, :] = (value * slope[i, slot, at, :].astype(f32)).astype(bf16)

    def back_up(i, slot):
        total[slot] += contract(pre_ref[i, slot], joined(held, i, 0), 1, 1)

    def loop(*works):
        def body(i, carry):
            for work in works:
                work(i)
            return carry

        lax.fori_loop(0, steps, body, 0)

    total[...] = jnp.zeros_like(total)
    for load in loads:
        load.wait()
    loop(lambda i: up(i, 0))
    first_copy.wait()
    loop(lambda i: up(i, 1))
    for hop in hops:
        hop.wait()
    loop(lambda i: down(i, 1))
    leaving[...] = total[1].astype(bf16)
    feed_copy = across(leaving, landed.at[0], 1)
    feed_copy.start()
    loop(lambda i: down(i, 0))
    feed_copy.wait()

    @pl.when(matched)
    def _():
        seed_local.wait()

    @pl.when(jnp.logical_not(matched))
    def _():
        seed_swap.wait()

    sums_ref[...] = jnp.zeros_like(sums_ref)
    part = 128

    def middle(r, carry):
        at = pl.ds(pl.multiple_of(r * part, part), part)
        second, normed, inverse = norm_parts(
            first_ref[at, :] + (total[0, at, :] + landed[0, at, :].astype(f32)),
            norms_ref[2:3, :], norms_ref[3:4, :],
        )
        out_ref[at, :] = second.astype(bf16)
        row = lax.broadcasted_iota(jnp.int32, (part, 1), 0) + r * part + info[1]
        seed = seed_held[at, :].astype(f32) * (row < info[0]).astype(f32)
        grad = norm_back(seed, normed, inverse, norms_ref[2:3, :])
        sums_ref[0:1, :] += jnp.sum(seed * normed, axis=0, keepdims=True)
        sums_ref[1:2, :] += jnp.sum(seed, axis=0, keepdims=True)
        total[0, at, :] = grad
        low_ref[0, at, :] = grad.astype(bf16)
        return carry

    lax.fori_loop(0, rows // part, middle, 0)
    low_copy = across(low_ref.at[0], low_ref.at[1], 2)
    low_copy.start()
    total[1] = jnp.zeros_like(total[1])
    loop(lambda i: back(i, 0))
    low_copy.wait()
    loop(lambda i: back(i, 1), lambda i: back_up(i, 1))
    leaving[...] = total[1].astype(bf16)
    grad_copy = across(leaving, landed.at[1], 3)
    grad_copy.start()
    loop(lambda i: back_up(i, 0))
    grad_copy.wait()
    grad_ref[...] = total[0] + landed[1].astype(f32)


def feed_block(info, first, cotangent, norms, weights, up, down):
    rows = first.shape[0]
    lanes = up.shape[-1]
    width = 4 * lanes
    vmem, anywhere = pl.BlockSpec(memory_space=pltpu.VMEM), pl.BlockSpec(memory_space=pl.ANY)
    return pl.pallas_call(
        feed_body,
        name="feed_block",
        in_specs=[pl.BlockSpec(memory_space=pltpu.SMEM), vmem, anywhere, vmem] + [anywhere] * 3,
        out_specs=[vmem] * 7,
        out_shape=[
            jax.ShapeDtypeStruct((rows, D), bf16),
            jax.ShapeDtypeStruct((2, rows, D), bf16),
            jax.ShapeDtypeStruct((2, rows, D), bf16),
            jax.ShapeDtypeStruct((4, 2, rows, width), bf16),
            jax.ShapeDtypeStruct((4, 2, rows, width), bf16),
            jax.ShapeDtypeStruct((rows, D), f32),
            jax.ShapeDtypeStruct((2, D), f32),
        ],
        scratch_shapes=[
            pltpu.VMEM((2, 4, 2, 2, D, lanes), bf16),
            pltpu.VMEM((4, 2, rows, width), bf16),
            pltpu.VMEM((2, rows, D), f32),
            pltpu.VMEM((rows, D), bf16),
            pltpu.VMEM((2, rows, D), bf16),
            pltpu.VMEM((rows, D), bf16),
            pltpu.SemaphoreType.DMA((12,)),
            pltpu.SemaphoreType.DMA((7,)),
            pltpu.SemaphoreType.DMA((7,)),
        ],
        compiler_params=pltpu.CompilerParams(
            vmem_limit_bytes=60 << 20, collective_id=1, has_side_effects=True
        ),
        cost_estimate=pl.CostEstimate(
            flops=64 * rows * D * width, bytes_accessed=30 << 20, transcendentals=0
        ),
    )(info, first, cotangent, norms, weights, up, down)


def feed_grads_body(first_ref, low_ref, hidden_ref, pre_ref, up_ref, down_ref, first_t, low_t):
    rows = first_ref.shape[1]

    @pl.when(pl.program_id(0) == 0)
    def _():
        for slot in range(2):
            at = slice(slot * rows, (slot + 1) * rows)
            first_t[:, at] = jnp.transpose(first_ref[slot].astype(f32)).astype(bf16)
            low_t[:, at] = jnp.transpose(low_ref[slot].astype(f32)).astype(bf16)

    lanes = up_ref.shape[-1]
    width = pre_ref.shape[-1]
    for target, source, turned in ((up_ref, pre_ref, first_t), (down_ref, hidden_ref, low_t)):
        grad = jnp.dot(
            turned[...], source[0].reshape(2 * rows, width), preferred_element_type=f32
        ).astype(bf16)
        for k in range(2):
            for m in range(2):
                at = (2 * k + m) * lanes
                if target is up_ref:
                    target[m, k, 0] = grad[:, at : at + lanes]
                else:
                    target[m, 0, k] = grad[:, at : at + lanes]


def feed_grads(first, low, hidden, pre):
    count, _, rows, width = hidden.shape
    full = pl.BlockSpec((2, rows, D), lambda i: (0, 0, 0))
    piece = pl.BlockSpec((1, 2, rows, width), lambda i: (i, 0, 0, 0))
    lanes = width // 4
    return pl.pallas_call(
        feed_grads_body,
        grid=(count,),
        name="feed_grads",
        in_specs=[full, full, piece, piece],
        out_specs=[
            pl.BlockSpec((2, 2, 1, D, lanes), lambda i: (i // 2, 0, i % 2, 0, 0)),
            pl.BlockSpec((2, 1, 2, D, lanes), lambda i: (i // 2, i % 2, 0, 0, 0)),
        ],
        out_shape=[jax.ShapeDtypeStruct((count, 2, 2, D, lanes), bf16)] * 2,
        scratch_shapes=[pltpu.VMEM((D, 2 * rows), bf16), pltpu.VMEM((D, 2 * rows), bf16)],
        compiler_params=pltpu.CompilerParams(vmem_limit_bytes=48 << 20),
        cost_estimate=pl.CostEstimate(
            flops=8 * rows * D * width * count, bytes_accessed=20 << 20, transcendentals=0
        ),
    )(first, low, hidden, pre)


def layer(n_dp, n_tensor, tokens, weights, norms, cotangent, lengths, owners, master, moment_one,
          moment_two, norm_master, norm_one, norm_two):
    tile = D // n_tensor
    rows = tokens.shape[0]
    device = lax.axis_index("dp")
    z = lax.axis_index("tensor")
    core = device % 2
    matched = core == z // 2
    quarter = jnp.where(matched, z, z ^ 2)

    def flip(x, dd, dz):
        pairs = [
            (d * n_tensor + t, (d ^ dd) * n_tensor + (t ^ dz))
            for d in range(n_dp)
            for t in range(n_tensor)
        ]
        return lax.ppermute(x, AXES, pairs)

    gathered, mixed, context, parts, lse, w_heads, w_out_all, length, up_all, down_all = start_block(
        lengths, tokens[:, 0, :], weights
    )
    own = gathered[0]
    base = jnp.stack([quarter ^ k for k in (0, 2, 1, 3)]) * rows
    info = jnp.concatenate([length[0, :1], base]).astype(jnp.int32)

    context_all = jnp.where(
        matched,
        jnp.concatenate([parts[k] for k in (0, 2, 1, 3)], axis=1),
        jnp.concatenate([parts[k] for k in (1, 3, 0, 2)], axis=1),
    )
    branch = contract(context_all, w_out_all, 1, 1)
    first, first_normed, first_inverse = norm_parts(
        own.astype(f32) + branch, norms[0], norms[1]
    )
    outputs, both_low, both_first, hidden, pre_grad, first_grad, sums_two = feed_block(
        info, first, cotangent[:, 0, :], norms, weights, up_all, down_all
    )
    branch_grad = norm_back(first_grad, first_normed, first_inverse, norms[0])
    gain_one = jnp.sum(first_grad * first_normed, axis=0)
    shift_one = jnp.sum(first_grad, axis=0)
    branch_low = branch_grad.astype(bf16)
    context_grad = jnp.dot(branch_low, w_out_all, preferred_element_type=f32).astype(bf16)
    blocks = [context_grad[:, k * tile : (k + 1) * tile] for k in range(4)]
    blocks = [
        jnp.where(matched, blocks[a], blocks[b]) for a, b in ((0, 2), (2, 0), (1, 3), (3, 1))
    ]
    upstream = jnp.stack(
        [blocks[0], flip(blocks[1], 1, 0), flip(blocks[2], 0, 1), flip(blocks[3], 1, 1)]
    )

    def add(a, b):
        return (a.astype(f32) + b.astype(f32)).astype(bf16)

    up_grads, down_grads = feed_grads(both_first, both_low, hidden, pre_grad)
    out_grad = contract(branch_low, context_all, 0, 0).astype(bf16)
    norm_sums = jnp.concatenate([jnp.stack([gain_one, shift_one]), sums_two])
    input_grad, outputs, norm_grads, attention_grad, feed_grad = back_block(
        info, mixed, context, upstream, lse, w_heads, branch_grad, norm_sums, outputs, gathered, up_grads, down_grads,
        out_grad,
    )

    def over_groups(value, combine):
        bit = SHARE
        while bit < n_dp:
            value = combine(value, flip(value, bit, 0))
            bit *= 2
        return value

    def plus(a, b):
        return a + b

    norm_grads = over_groups(norm_grads, plus)
    attention_grad = over_groups(attention_grad, add)
    feed_grad = over_groups(feed_grad, add)

    tile_owner, slot_index = slot_table(owners)
    slot_ids = jnp.arange(FF // D, dtype=jnp.int32)
    owned = (
        (tile_owner[None, :] == device) & (slot_index[None, :] == slot_ids[:, None])
    ).astype(jnp.int32)
    owned = jnp.concatenate([owned, jnp.sum(owned, axis=1, keepdims=True)], axis=1)
    slot_grad, new_master, new_one, new_two, tiles, up_tiles, down_tiles = adam_block(
        owned, attention_grad, feed_grad, master[0], moment_one[0], moment_two[0]
    )
    tiles, up_tiles, down_tiles, input_grad = spread_tiles(tiles, up_tiles, down_tiles, input_grad)
    tiles, up_tiles, down_tiles = (over_groups(v, plus) for v in (tiles, up_tiles, down_tiles))
    new_weights = jnp.concatenate(
        [tiles] + [up_tiles[k] for k in range(SHARE)] + [down_tiles[k] for k in range(SHARE)], axis=1
    )
    norm_owner = (device == owners[6]).astype(f32)
    new_norm_master, new_norm_one, new_norm_two = adam_update(
        norm_grads, norm_master[0], norm_one[0], norm_two[0], norm_owner, 0.0
    )
    return (
        outputs[:, None, :],
        input_grad[:, None, :],
        slot_grad[None],
        new_master[None],
        new_one[None],
        new_two[None],
        new_weights,
        norm_grads,
        new_norm_master[None],
        new_norm_one[None],
        new_norm_two[None],
    )


def solution(mesh):
    in_specs = (
        P("tensor", "dp", None),
        P(None, "tensor"),
        P(),
        P("tensor", "dp", None),
        P("dp"),
        P(),
        P("dp", None, "tensor"),
        P("dp", None, "tensor"),
        P("dp", None, "tensor"),
        P("dp", None, None),
        P("dp", None, None),
        P("dp", None, None),
    )
    out_specs = (
        P("tensor", "dp", None),
        P("tensor", "dp", None),
        P("dp", None, "tensor"),
        P("dp", None, "tensor"),
        P("dp", None, "tensor"),
        P("dp", None, "tensor"),
        P(None, "tensor"),
        P(),
        P("dp", None, None),
        P("dp", None, None),
        P("dp", None, None),
    )
    return jax.shard_map(
        partial(layer, mesh.shape["dp"], mesh.shape["tensor"]),
        mesh=mesh,
        in_specs=in_specs,
        out_specs=out_specs,
        check_vma=False,
    )
```
